256 devices in a mesh: tm: 32 (over z_lo, y, core), space: 8 (over x, z_hi).
Axes of the slice: x: 4, y: 4, z: 8 (z_hi: 2, z_lo: 4; z = z_hi * 4 + z_lo), core: 2. Of those that a mesh axis runs over, the one named last changes fastest.
Arguments:
- iterate: float32 [32, 4, 128, 64, 128], P('tm', None, 'space'), may hold values from -6 to 6
- right_side: float32 [32, 4, 128, 64, 128], P('tm', None, 'space'), may hold values from -6 to 6
- diffusivity: float32 [128, 64, 128], P('space'), may hold values from 0.5 to 2
- velocity: float32 [3], replicated, may hold values from -2 to 2
Outputs:
- next_iterate: float32 [32, 4, 128, 64, 128], P('tm', None, 'space')
The draws below stay inside these ranges and needn't reach their ends.
All inputs are finite; a program needn't handle non-finite values.
Results may differ from the reference program's by a relative error of at most 0.0003.
Values sent between devices are 32-bit elements; how exact they have to be, the bound alone decides.
A program may use at most 128 MiB of HBM per device.

```python
import math
import jax
import jax.numpy as jnp
from jax import lax

NX = 128
NY = 128
NZ = 64
NODES = 4
STEPS = 32


def draw_right_side(key, part):
    rough_key = jax.random.fold_in(jax.random.fold_in(key, 17), 0)
    rough = jax.random.truncated_normal(rough_key, -6.0, 6.0, (STEPS, NODES, NX, NZ, NY), jnp.float32)
    return rough


def block_levels(key, extent, pieces, least, largest):
    def one(axis_at, shards_of):
        steps = jax.random.uniform(jax.random.fold_in(jax.random.fold_in(key, 6), axis_at), (shards_of,), jnp.float32, least / len(pieces), largest / len(pieces))
        return jnp.repeat(jnp.exp(steps), extent[axis_at] // shards_of).reshape((-1,) + (1,) * (len(extent) - axis_at - 1))

    factor_of = one(*pieces[0])
    for cut in pieces[1:]:
        factor_of = factor_of * one(*cut)
    return factor_of


def centred(own_key, shape, spread, limit, pieces=(), kind=jnp.bfloat16):
    level = block_levels(own_key, shape, pieces, -0.22, 0.18) if pieces else 1.0
    values = jax.random.normal(own_key, shape, jnp.float32) * spread * level
    return jnp.minimum(jnp.maximum(values, -limit), limit).astype(kind)


def setup_inputs(seed: int = 0) -> dict:
    streams_of = jax.random.split(jax.random.key(seed), 5)
    return {
        "iterate": centred(streams_of[0], (STEPS, NODES, NX, NZ, NY), 1.0, 6.0, ((0, 32), (2, 8)), jnp.float32),
        "right_side": draw_right_side(jax.random.fold_in(streams_of[4], 71), 0),
        "diffusivity": jnp.clip(jnp.exp(math.log(2.0) - 1.3862944 * jax.random.uniform(streams_of[2], (NX, NZ, NY), jnp.float32) ** block_levels(streams_of[2], (NX, NZ, NY), ((0, 8),), -0.2, 0.2)), 0.5, 2.0),
        "velocity": jnp.clip(jax.random.uniform(streams_of[3], (3,), jnp.float32, -2.0, 2.0), -2.0, 2.0),
    }


diffusion_number = 16.0
circulant_alpha = 0.1


def collocation_matrix():
    radau_nodes = [0.088587959512703947, 0.40946686444073471, 0.78765946176084706, 1.0]
    matrix = [[0.0] * 4 for row_index in range(4)]
    for column_index in range(4):
        coefficients = [1.0]
        for other_index in range(4):
            if other_index != column_index:
                scale_value = 1.0 / (radau_nodes[column_index] - radau_nodes[other_index])
                shifted = [0.0] + [value * scale_value for value in coefficients]
                lowered = [-radau_nodes[other_index] * scale_value * value for value in coefficients] + [0.0]
                coefficients = [left_value + right_value for left_value, right_value in zip(shifted, lowered)]
        for row_index in range(4):
            total = 0.0
            for power_index in range(len(coefficients)):
                total = total + coefficients[power_index] * radau_nodes[row_index] ** (power_index + 1) / (power_index + 1)
            matrix[row_index][column_index] = total
    return matrix


def solve_system(matrix, target):
    count = len(target)
    rows_list = [list(matrix[row_index]) + [target[row_index]] for row_index in range(count)]
    for column in range(count):
        best_row = column
        for candidate in range(column + 1, count):
            if abs(rows_list[candidate][column]) > abs(rows_list[best_row][column]):
                best_row = candidate
        saved_row = rows_list[column]
        rows_list[column] = rows_list[best_row]
        rows_list[best_row] = saved_row
        leader = rows_list[column][column]
        for other_row in range(count):
            if other_row != column:
                factor = rows_list[other_row][column] / leader
                rows_list[other_row] = [left_value - factor * right_value for left_value, right_value in zip(rows_list[other_row], rows_list[column])]
    return [rows_list[row_index][count] / rows_list[row_index][row_index] for row_index in range(count)]


def node_basis():
    matrix = collocation_matrix()
    helper = [[0.0] * 4 for row_index in range(4)]
    coefficients = [0.0, 0.0, 0.0, 0.0, 1.0]
    for order in range(1, 5):
        product = [[sum(matrix[row_index][inner] * helper[inner][column] for inner in range(4)) for column in range(4)] for row_index in range(4)]
        for row_index in range(4):
            product[row_index][row_index] = product[row_index][row_index] + coefficients[5 - order]
        helper = product
        trace_value = sum(sum(matrix[row_index][inner] * helper[inner][row_index] for inner in range(4)) for row_index in range(4))
        coefficients[4 - order] = -trace_value / order
    roots_list = [(0.4 + 0.9j) ** power_index for power_index in range(4)]
    for sweep in range(400):
        for root_index in range(4):
            current = roots_list[root_index]
            numer = 0.0
            for power_index in range(4, -1, -1):
                numer = numer * current + coefficients[power_index]
            denom = 1.0
            for other_index in range(4):
                if other_index != root_index:
                    denom = denom * (current - roots_list[other_index])
            roots_list[root_index] = current - numer / denom
    vectors = [[0.0] * 4 for row_index in range(4)]
    for root_index in range(4):
        shifted = [[matrix[row_index][column] - (roots_list[root_index] if row_index == column else 0.0) for column in range(3)] for row_index in range(3)]
        target = [-matrix[row_index][3] for row_index in range(3)]
        parts = solve_system(shifted, target) + [1.0 + 0.0j]
        for row_index in range(4):
            vectors[row_index][root_index] = parts[row_index]
    inverse = [[0.0] * 4 for row_index in range(4)]
    for column in range(4):
        unit = [1.0 if row_index == column else 0.0 for row_index in range(4)]
        parts = solve_system(vectors, unit)
        for row_index in range(4):
            inverse[row_index][column] = parts[row_index]
    weights = [sum(inverse[row_index][column] for column in range(4)) for row_index in range(4)]
    return roots_list, vectors, inverse, weights


def complex_vector(numbers):
    real_values = jnp.asarray([complex(value).real for value in numbers], jnp.float32)
    imag_values = jnp.asarray([complex(value).imag for value in numbers], jnp.float32)
    return real_values + 1j * imag_values


def complex_matrix(numbers):
    real_values = jnp.asarray([[complex(value).real for value in row] for row in numbers], jnp.float32)
    imag_values = jnp.asarray([[complex(value).imag for value in row] for row in numbers], jnp.float32)
    return real_values + 1j * imag_values


def spatial_operator(field_values, diffusivity, velocity):
    upper_x = jnp.roll(field_values, -1, axis=2)
    lower_x = jnp.roll(field_values, 1, axis=2)
    upper_z = jnp.roll(field_values, -1, axis=3)
    lower_z = jnp.roll(field_values, 1, axis=3)
    upper_y = jnp.roll(field_values, -1, axis=4)
    lower_y = jnp.roll(field_values, 1, axis=4)
    laplace = (upper_x + lower_x) + (upper_z + lower_z) + (upper_y + lower_y) - 6.0 * field_values
    transport = velocity[0] * (upper_x - lower_x) + velocity[1] * (upper_y - lower_y) + velocity[2] * (upper_z - lower_z)
    return diffusion_number * diffusivity * laplace - 0.5 * transport


def reference(iterate, right_side, diffusivity, velocity):
    collocation = jnp.asarray(collocation_matrix(), jnp.float32)
    applied = spatial_operator(iterate, diffusivity, velocity)
    coupled = jnp.einsum("mn,snxzy->smxzy", collocation, applied, precision=lax.Precision.HIGHEST)
    previous = jnp.concatenate([jnp.zeros_like(iterate[:1, 3]), iterate[:-1, 3]], axis=0)
    residual = right_side - iterate + coupled + previous[:, None]
    gamma_base = circulant_alpha ** (1.0 / STEPS)
    step_power = jnp.arange(STEPS, dtype=jnp.int32).astype(jnp.float32)
    step_scale = jnp.power(jnp.float32(gamma_base), step_power)
    spectrum = jnp.fft.rfftn(residual * step_scale[:, None, None, None, None], axes=(0, 2, 3, 4))
    theta_x = jnp.arange(NX, dtype=jnp.int32).astype(jnp.float32) * (2.0 * math.pi / NX)
    theta_z = jnp.arange(NZ, dtype=jnp.int32).astype(jnp.float32) * (2.0 * math.pi / NZ)
    theta_y = jnp.arange(NY // 2 + 1, dtype=jnp.int32).astype(jnp.float32) * (2.0 * math.pi / NY)
    symbol_real = diffusion_number * ((2.0 * jnp.cos(theta_x)[:, None, None] - 2.0) + (2.0 * jnp.cos(theta_z)[None, :, None] - 2.0) + (2.0 * jnp.cos(theta_y)[None, None, :] - 2.0))
    symbol_imag = -(velocity[0] * jnp.sin(theta_x)[:, None, None] + velocity[1] * jnp.sin(theta_y)[None, None, :] + velocity[2] * jnp.sin(theta_z)[None, :, None])
    symbol = symbol_real + 1j * symbol_imag
    values, vectors, inverse, weights = node_basis()
    eigen = complex_vector(values)
    basis = complex_matrix(vectors)
    basis_inverse = complex_matrix(inverse)
    ones_weights = complex_vector(weights)
    damping = 1.0 / (1.0 - eigen[:, None, None, None] * symbol[None])
    ones_image = jnp.einsum("pm,mxzy->pxzy", basis, ones_weights[:, None, None, None] * damping, precision=lax.Precision.HIGHEST)
    phases = jnp.arange(STEPS, dtype=jnp.int32).astype(jnp.float32) * (2.0 * math.pi / STEPS)
    shift_factors = gamma_base * (jnp.cos(phases) - 1j * jnp.sin(phases))

    def solve_one(operands):
        block, shift_factor = operands
        inner = jnp.einsum("mn,nxzy->mxzy", basis_inverse, block, precision=lax.Precision.HIGHEST) * damping
        image = jnp.einsum("pm,mxzy->pxzy", basis, inner, precision=lax.Precision.HIGHEST)
        factor = shift_factor * image[3] / (1.0 - shift_factor * ones_image[3])
        return image + ones_image * factor[None]

    solved = lax.map(solve_one, (spectrum, shift_factors))
    correction = jnp.fft.irfftn(solved, s=(STEPS, NX, NZ, NY), axes=(0, 2, 3, 4))
    unscale = jnp.power(jnp.float32(gamma_base), -step_power)
    return iterate + correction * unscale[:, None, None, None, None]
```

```python
import functools
import math

import jax
import jax.numpy as jnp
import numpy as np
from jax import lax
from jax.experimental import pallas as pl
from jax.experimental.pallas import tpu as pltpu
from jax.sharding import PartitionSpec as P

NX, NY, NZ, STEPS = 128, 128, 64, 32
SLABS, WIDE = 8, 16
OWNERS = 64
ROWS = 24
MESH = pl.DeviceIdType.MESH
f32, bf16 = jnp.float32, jnp.bfloat16

diffusion_number = 16.0
circulant_alpha = 0.1


def collocation_matrix():
    radau_nodes = [0.08858795951270394, 0.4094668644407347, 0.7876594617608471, 1.0]
    matrix = [[0.0] * 4 for row_index in range(4)]
    for column_index in range(4):
        coefficients = [1.0]
        for other_index in range(4):
            if other_index != column_index:
                scale_value = 1.0 / (radau_nodes[column_index] - radau_nodes[other_index])
                shifted = [0.0] + [value * scale_value for value in coefficients]
                lowered = [
                    -radau_nodes[other_index] * scale_value * value for value in coefficients
                ] + [0.0]
                coefficients = [
                    left_value + right_value for left_value, right_value in zip(shifted, lowered)
                ]
        for row_index in range(4):
            total = 0.0
            for power_index in range(len(coefficients)):
                total = total + coefficients[power_index] * radau_nodes[row_index] ** (
                    power_index + 1
                ) / (power_index + 1)
            matrix[row_index][column_index] = total
    return matrix


def solve_system(matrix, target):
    count = len(target)
    rows_list = [list(matrix[row_index]) + [target[row_index]] for row_index in range(count)]
    for column in range(count):
        best_row = column
        for candidate in range(column + 1, count):
            if abs(rows_list[candidate][column]) > abs(rows_list[best_row][column]):
                best_row = candidate
        saved_row = rows_list[column]
        rows_list[column] = rows_list[best_row]
        rows_list[best_row] = saved_row
        leader = rows_list[column][column]
        for other_row in range(count):
            if other_row != column:
                factor = rows_list[other_row][column] / leader
                rows_list[other_row] = [
                    left_value - factor * right_value
                    for left_value, right_value in zip(rows_list[other_row], rows_list[column])
                ]
    return [
        rows_list[row_index][count] / rows_list[row_index][row_index] for row_index in range(count)
    ]


def node_basis():
    matrix = collocation_matrix()
    helper = [[0.0] * 4 for row_index in range(4)]
    coefficients = [0.0, 0.0, 0.0, 0.0, 1.0]
    for order in range(1, 5):
        product = [
            [
                sum((matrix[row_index][inner] * helper[inner][column] for inner in range(4)))
                for column in range(4)
            ]
            for row_index in range(4)
        ]
        for row_index in range(4):
            product[row_index][row_index] = product[row_index][row_index] + coefficients[5 - order]
        helper = product
        trace_value = sum(
            (
                sum((matrix[row_index][inner] * helper[inner][row_index] for inner in range(4)))
                for row_index in range(4)
            )
        )
        coefficients[4 - order] = -trace_value / order
    roots_list = [(0.4 + 0.9j) ** power_index for power_index in range(4)]
    for sweep in range(400):
        for root_index in range(4):
            current = roots_list[root_index]
            numer = 0.0
            for power_index in range(4, -1, -1):
                numer = numer * current + coefficients[power_index]
            denom = 1.0
            for other_index in range(4):
                if other_index != root_index:
                    denom = denom * (current - roots_list[other_index])
            roots_list[root_index] = current - numer / denom
    vectors = [[0.0] * 4 for row_index in range(4)]
    for root_index in range(4):
        shifted = [
            [
                matrix[row_index][column] - (roots_list[root_index] if row_index == column else 0.0)
                for column in range(3)
            ]
            for row_index in range(3)
        ]
        target = [-matrix[row_index][3] for row_index in range(3)]
        parts = solve_system(shifted, target) + [1.0 + 0j]
        for row_index in range(4):
            vectors[row_index][root_index] = parts[row_index]
    inverse = [[0.0] * 4 for row_index in range(4)]
    for column in range(4):
        unit = [1.0 if row_index == column else 0.0 for row_index in range(4)]
        parts = solve_system(vectors, unit)
        for row_index in range(4):
            inverse[row_index][column] = parts[row_index]
    weights = [sum((inverse[row_index][column] for column in range(4))) for row_index in range(4)]
    return (roots_list, vectors, inverse, weights)


VALUES, VECTORS, INVERSE, WEIGHTS = node_basis()
PAIRS = [m for m in range(4) if complex(VALUES[m]).imag > 0]
MU = [complex(VALUES[m]) for m in PAIRS]
COLUMN = [[complex(VECTORS[n][m]) for n in range(4)] for m in PAIRS]
ROW = [[complex(INVERSE[m][n]) for n in range(4)] for m in PAIRS]
EPS = [complex(WEIGHTS[m]) for m in PAIRS]


def wave_order(n):
    index = np.arange(n)
    return np.where(index <= n // 2, index, n + n // 2 - index)


def split(values):
    values = np.asarray(values, np.float64)
    high = values.astype(np.float32).astype(bf16)
    low = (values - high.astype(np.float64)).astype(np.float32).astype(bf16)
    return high, low


def side_table(values):
    high, low = split(values)
    return np.concatenate([high, high, low], axis=1)


def halves(x):
    high = x.astype(bf16)
    return high, (x - high.astype(f32)).astype(bf16)


def left_dot(table, x):
    high, low = halves(x)
    return jnp.dot(table, jnp.concatenate([high, low, high], axis=0), preferred_element_type=f32)


def right_dot(high, low, table_high, table_low):
    return (
        jnp.dot(high, table_high, preferred_element_type=f32)
        + jnp.dot(low, table_high, preferred_element_type=f32)
        + jnp.dot(high, table_low, preferred_element_type=f32)
    )


def complex_block(matrix):
    return np.block([[matrix.real, -matrix.imag], [matrix.imag, matrix.real]])


def make_tables():
    ky, kz = wave_order(NY), wave_order(NZ)
    kx, x = np.arange(NX), np.arange(NX)
    to_y = np.exp(-2j * np.pi * np.outer(ky, np.arange(NY)) / NY)
    to_z = np.exp(-2j * np.pi * np.outer(kz, np.arange(NZ)) / NZ)
    tables = {}
    tables["ty"] = np.stack(split(complex_block(to_y).T))
    tables["tz"] = side_table(complex_block(to_z))
    tables["uy"] = np.stack(split(complex_block(np.conj(to_y.T) / NY).T))
    tables["uz"] = side_table(complex_block(np.conj(to_z.T) / NZ))
    cells = (np.arange(SLABS)[:, None] * WIDE + np.arange(8)[None, :]).reshape(-1)
    theta = 2 * np.pi * kx / NX
    at = np.exp(-1j * np.outer(theta, cells))
    shifted = np.exp(-8j * theta)[:, None]
    from_own = at * (1 - 1j * shifted) / 2
    from_partner = at * (1 + 1j * shifted) / 2
    own = complex_block(from_own)
    partner = complex_block(from_partner) * np.concatenate([np.ones(64), -np.ones(64)])[None, :]
    tables["tg"] = side_table(np.concatenate([own, partner], axis=1))
    firsts = np.arange(SLABS) * WIDE
    start = np.exp(-1j * np.outer(theta, firsts))
    before = np.exp(-1j * np.outer(theta, firsts - 1))
    tables["td"] = side_table(np.concatenate([complex_block(start), complex_block(before)], axis=1))
    back = np.exp(1j * np.outer(cells, theta)) * (1 + 1j * np.exp(8j * theta))[None, :] / NX
    tables["tw"] = side_table(complex_block(back))
    ends = [complex_block(np.exp(1j * np.outer(firsts + k, theta)) / NX) for k in (0, 1, 15)]
    tables["tb"] = side_table(np.concatenate(ends, axis=0))
    trig_y = 2 * np.pi * ky / NY
    trig_z = 2 * np.pi * kz / NZ
    tables["lane"] = np.stack([np.cos(trig_y), np.sin(trig_y)]).astype(np.float32)
    tables["row"] = np.stack(
        [np.broadcast_to(v[:, None], (NZ, NY)) for v in (np.cos(trig_z), np.sin(trig_z))]
    ).astype(np.float32)
    tables["wave_x"] = np.stack(
        [np.broadcast_to(v[:, None], (NX, 128)) for v in (np.cos(theta), np.sin(theta))]
    ).astype(np.float32)
    lane = np.arange(128)
    second = (lane % 64) >= 32
    own_lane, own_row = [], []
    for owner in range(OWNERS):
        half, pair = owner // 32, owner % 32
        own_lane.append(trig_y[lane - 32 * second + 32 * half])
        own_row.append(trig_z[pair + 32 * second])
    own_lane, own_row = np.stack(own_lane), np.stack(own_row)
    tables["own"] = np.stack(
        [np.cos(own_lane), np.sin(own_lane), np.cos(own_row), np.sin(own_row)], axis=1
    ).astype(np.float32)
    return tables


TABLES = make_tables()


def times(a, b):
    return (a[0] * b[0] - a[1] * b[1], a[0] * b[1] + a[1] * b[0])


def plus(a, b):
    return (a[0] + b[0], a[1] + b[1])


def minus(a, b):
    return (a[0] - b[0], a[1] - b[1])


def scaled(number, a):
    return (number.real * a[0] - number.imag * a[1], number.real * a[1] + number.imag * a[0])


def inverse_of(a):
    size = 1.0 / (a[0] * a[0] + a[1] * a[1])
    return (a[0] * size, -a[1] * size)


def root_of(a):
    size = jnp.sqrt(a[0] * a[0] + a[1] * a[1])
    main = jnp.sqrt(0.5 * (size + jnp.abs(a[0])))
    other = a[1] / (2.0 * main)
    positive = a[0] >= 0.0
    return (
        jnp.where(positive, main, jnp.abs(other)),
        jnp.where(positive, other, jnp.where(a[1] >= 0.0, main, -main)),
    )


def cross_symbol(cos_y, sin_y, cos_z, sin_z, v1, v2):
    return (
        diffusion_number * ((2.0 * cos_y - 2.0) + (2.0 * cos_z - 2.0)),
        -(v1 * sin_y + v2 * sin_z),
    )


def factors(mu, cross, v0):
    c_up = -mu.real * (diffusion_number - 0.5 * v0), -mu.imag * (diffusion_number - 0.5 * v0)
    c_down = -mu.real * (diffusion_number + 0.5 * v0), -mu.imag * (diffusion_number + 0.5 * v0)
    moved = scaled(mu, cross)
    c_mid = (1.0 + 2.0 * diffusion_number * mu.real - moved[0], 2.0 * diffusion_number * mu.imag - moved[1])
    product = times(c_up, c_down)
    square = times(c_mid, c_mid)
    root = root_of((square[0] - 4.0 * product[0], square[1] - 4.0 * product[1]))
    same = c_mid[0] * root[0] + c_mid[1] * root[1] >= 0.0
    kappa = (
        0.5 * (c_mid[0] + jnp.where(same, root[0], -root[0])),
        0.5 * (c_mid[1] + jnp.where(same, root[1], -root[1])),
    )
    inv = inverse_of(kappa)
    p = times(inv, c_down)
    q = times(inv, c_up)
    return (-p[0], -p[1]), (-q[0], -q[1]), kappa, inv


def plane_partner(low, high, lane, first_row):
    ends = (lane == 0) | (lane == 64)

    def turned(v):
        return jnp.where(ends, v, pltpu.roll(v, 64, 1))

    low_turned, high_turned = [turned(v) for v in low], [turned(v) for v in high]
    to_low = [jnp.where(first_row, a, b) for a, b in zip(low_turned, high_turned)]
    to_high = [jnp.where(first_row, b, a) for a, b in zip(low_turned, high_turned)]
    return (to_low[0], -to_low[1]), (to_high[0], -to_high[1])


def chunk_factors(t, lane_ref, row_ref, velocity_ref, mu):
    cos_y, sin_y = lane_ref[0:1, :], lane_ref[1:2, :]
    found = []
    for base in (0, 32):
        rows = pl.ds(pl.multiple_of(base + 8 * t, 8), 8)
        cross = cross_symbol(
            cos_y, sin_y, row_ref[0, rows, :], row_ref[1, rows, :], velocity_ref[1], velocity_ref[2]
        )
        found.append([factors(number, cross, velocity_ref[0]) for number in mu])
    return found


def forward_kernel(
    velocity_ref, step_ref, iterate_ref, right_ref, kappa_ref, below_ref, above_ref,
    ty_ref, tz_ref, lane_ref, row_ref,
    u_ref, send_ref,
    high_ref, low_ref, spec_ref,
):
    v0, v1, v2 = velocity_ref[0], velocity_ref[1], velocity_ref[2]

    def put(at, real, imag):
        rows = pl.ds(pl.multiple_of(at * 64, 64), 64)
        for k, part in enumerate((real, imag)):
            high, low = halves(part)
            high_ref[rows, k * 128 : (k + 1) * 128] = high
            low_ref[rows, k * 128 : (k + 1) * 128] = low

    def combine(plain, applied, plane):
        for m in range(2):
            real = imag = None
            for n in range(4):
                c = ROW[m][n]
                d = MU[m] * c
                terms = [(d, applied[n])]
                if plain is not None:
                    terms.append((c, plain[n]))
                for factor, value in terms:
                    a, b = factor.real * value, factor.imag * value
                    real = a if real is None else real + a
                    imag = b if imag is None else imag + b
            put(m * 18 + plane, real, imag)

    def inner(x, below, above):
        plain, applied = [], []
        kappa = kappa_ref[x]
        for n in range(4):
            f = iterate_ref[n, x]
            up_z, down_z = pltpu.roll(f, NZ - 1, 0), pltpu.roll(f, 1, 0)
            up_y, down_y = pltpu.roll(f, NY - 1, 1), pltpu.roll(f, 1, 1)
            total = (up_z + down_z) + (up_y + down_y) - 6.0 * f
            moved = v1 * (up_y - down_y) + v2 * (up_z - down_z)
            if above:
                up_x = iterate_ref[n, x + 1]
                total, moved = total + up_x, moved + v0 * up_x
            if below:
                down_x = iterate_ref[n, x - 1]
                total, moved = total + down_x, moved - v0 * down_x
            applied.append((diffusion_number * kappa) * total - 0.5 * moved)
            plain.append(right_ref[n, x] - f)
        combine(plain, applied, x + 1)

    outer = diffusion_number * below_ref[...] - 0.5 * v0
    combine(None, [outer * iterate_ref[n, 0] for n in range(4)], 0)
    outer = diffusion_number * above_ref[...] + 0.5 * v0
    combine(None, [outer * iterate_ref[n, WIDE - 1] for n in range(4)], 17)
    inner(0, False, True)
    inner(WIDE - 1, True, False)

    @pl.loop(1, WIDE - 1)
    def _(x):
        inner(x, True, True)

    keep = jnp.where(step_ref[0] < STEPS - 1, 1.0, 0.0).astype(f32)

    @pl.loop(0, 8)
    def _(x):
        put(36 + x, keep * iterate_ref[3, x], keep * iterate_ref[3, x + 8])

    @pl.loop(0, 11)
    def _(block):
        rows = pl.ds(pl.multiple_of(block * 256, 256), 256)
        mid = right_dot(high_ref[rows, :], low_ref[rows, :], ty_ref[0], ty_ref[1])
        stacked = jnp.concatenate(
            [
                jnp.concatenate([mid[64 * k : 64 * k + 64, :128], mid[64 * k : 64 * k + 64, 128:]], axis=0)
                for k in range(4)
            ],
            axis=1,
        )
        out = left_dot(tz_ref[...], stacked)
        for k in range(4):
            spec_ref[block * 4 + k] = out[:, 128 * k : 128 * k + 128]

    lane = lax.broadcasted_iota(jnp.int32, (8, 128), 1)
    sub = lax.broadcasted_iota(jnp.int32, (8, 128), 0)
    narrow = (lane % 64) < 32

    @pl.loop(0, 4)
    def _(t):
        first_row = (sub + t) == 0
        found = chunk_factors(t, lane_ref, row_ref, velocity_ref, MU)
        bases = [pl.multiple_of(base + 8 * t, 8) for base in (0, 32)]

        def plane(at, base):
            return spec_ref[at, pl.ds(base, 8), :], spec_ref[at, pl.ds(base + 64, 8), :]

        def send(value, low, high):
            start = 8 * t * ROWS + value
            send_ref[pl.ds(start, 8, stride=ROWS), :] = jnp.where(narrow, low, pltpu.roll(high, 32, 1))
            send_ref[pl.ds(start + 32 * ROWS, 8, stride=ROWS), :] = jnp.where(
                narrow, pltpu.roll(low, 96, 1), high
            )

        sums = [[None, None] for x in range(WIDE)]
        for m in range(2):
            carries = []
            for half in range(2):
                base = bases[half]
                p, q, kappa, inv = found[half][m]
                under, over = plane(m * 18, base), plane(m * 18 + 17, base)
                u = plus(plane(m * 18 + 1, base), times(p, under))
                us = [u]
                for x in range(1, WIDE):
                    u = plus(plane(m * 18 + 1 + x, base), times(p, u))
                    us.append(u)
                for x in range(WIDE):
                    u_ref[m * 16 + x, pl.ds(base, 8), :] = us[x][0]
                    u_ref[m * 16 + x, pl.ds(base + 64, 8), :] = us[x][1]
                outflow = plus(times(p, us[-1]), over)
                y = us[-1]
                for x in range(WIDE - 1, -1, -1):
                    if x < WIDE - 1:
                        y = plus(us[x], times(q, y))
                    z = times(inv, y)
                    sums[x][half] = z if m == 0 else plus(sums[x][half], z)
                carries.append((outflow, plus(times(q, y), under)))
            for k in range(2):
                for part in range(2):
                    send(16 + m * 4 + k * 2 + part, carries[0][k][part], carries[1][k][part])
        for x in range(8):
            own, other = [], []
            for half in range(2):
                first, second = sums[x][half], sums[x + 8][half]
                own.append((first[0] - second[1], first[1] + second[0]))
                other.append((first[0] + second[1], first[1] - second[0]))
            partners = plane_partner(other[0], other[1], lane, first_row)
            packed = [
                plus(plus(own[half], partners[half]), plane(36 + x, bases[half])) for half in range(2)
            ]
            for part in range(2):
                send(part * 8 + x, packed[0][part], packed[1][part])


def backward_kernel(
    velocity_ref, iterate_ref, u_ref, got_ref, uy_ref, uz_ref, lane_ref, row_ref,
    out_ref,
    spec_ref,
):
    lane = lax.broadcasted_iota(jnp.int32, (8, 128), 1)
    sub = lax.broadcasted_iota(jnp.int32, (8, 128), 0)
    narrow = (lane % 64) < 32

    @pl.loop(0, 4)
    def _(t):
        first_row = (sub + t) == 0
        found = chunk_factors(t, lane_ref, row_ref, velocity_ref, MU)
        bases = [pl.multiple_of(base + 8 * t, 8) for base in (0, 32)]

        def take(value):
            start = 8 * t * ROWS + value
            a = got_ref[pl.ds(start, 8, stride=ROWS), :]
            b = got_ref[pl.ds(start + 32 * ROWS, 8, stride=ROWS), :]
            return jnp.where(narrow, a, pltpu.roll(b, 32, 1)), jnp.where(narrow, pltpu.roll(a, 96, 1), b)

        last = [[None, None] for x in range(WIDE)]
        for x in range(8):
            real, imag = take(x), take(8 + x)
            packed = [(real[half], imag[half]) for half in range(2)]
            partners = plane_partner(packed[0], packed[1], lane, first_row)
            for half in range(2):
                both, apart = plus(packed[half], partners[half]), minus(packed[half], partners[half])
                last[x][half] = (0.5 * both[0], 0.5 * both[1])
                last[x + 8][half] = (0.5 * apart[1], -0.5 * apart[0])
        for m in range(2):
            carried = [take(16 + m * 4 + k) for k in range(4)]
            for half in range(2):
                base = bases[half]
                p, q, kappa, inv = found[half][m]

                def old(x):
                    return (
                        u_ref[m * 16 + x, pl.ds(base, 8), :],
                        u_ref[m * 16 + x, pl.ds(base + 64, 8), :],
                    )

                u = (carried[0][half], carried[1][half])
                totals = [plus(u, old(0))]
                for x in range(1, WIDE - 1):
                    u = plus(scaled(EPS[m], last[x][half]), times(p, u))
                    totals.append(plus(u, old(x)))
                y = plus(times(inv, old(WIDE - 1)), (carried[2][half], carried[3][half]))
                for x in range(WIDE - 1, -1, -1):
                    if x < WIDE - 1:
                        y = plus(times(inv, totals[x]), times(q, y))
                    spec_ref[m * 16 + x, pl.ds(base, 8), :] = y[0]
                    spec_ref[m * 16 + x, pl.ds(base + 64, 8), :] = y[1]

    @pl.loop(0, 8)
    def _(block):
        planes = [2 * block, 2 * block + 1, 16 + 2 * block, 17 + 2 * block]
        stacked = jnp.concatenate([spec_ref[at] for at in planes], axis=1)
        mid = left_dot(uz_ref[...], stacked)
        rows = jnp.concatenate(
            [
                jnp.concatenate([mid[:64, 128 * k : 128 * k + 128], mid[64:, 128 * k : 128 * k + 128]], axis=1)
                for k in range(4)
            ],
            axis=0,
        )
        high, low = halves(rows)
        out = right_dot(high, low, uy_ref[0], uy_ref[1])
        for k in range(2):
            x = 2 * block + k
            parts = []
            for m in range(2):
                piece = out[(2 * m + k) * 64 : (2 * m + k) * 64 + 64]
                parts.append((piece[:, :128], piece[:, 128:]))
            for n in range(4):
                total = iterate_ref[n, x]
                for m in range(2):
                    c = COLUMN[m][n]
                    total = total + (2.0 * c.real) * parts[m][0] - (2.0 * c.imag) * parts[m][1]
                out_ref[n, x] = total


def mode_kernel(
    velocity_ref, place_ref, got_ref, own_ref, wave_ref, tg_ref, td_ref, tw_ref, tb_ref,
    back_ref,
    damp_ref, ratio_ref, last_ref, drive_ref, kept_ref,
):
    v0, v1, v2 = velocity_ref[0], velocity_ref[1], velocity_ref[2]
    half, pair = place_ref[0], place_ref[1]
    own = [jnp.broadcast_to(own_ref[k : k + 1, :], (8, 128)) for k in range(4)]
    cross = cross_symbol(own[0], own[1], own[2], own[3], v1, v2)
    mu = [MU[0], MU[0].conjugate(), MU[1], MU[1].conjugate()]
    eps = [EPS[0], EPS[0].conjugate(), EPS[1], EPS[1].conjugate()]
    found = [factors(number, cross, v0) for number in mu]

    @pl.loop(0, 16)
    def _(at):
        rows = pl.ds(pl.multiple_of(at * 8, 8), 8)
        lower = pl.ds(pl.multiple_of(at * 8 + 128, 8), 8)
        symbol = (
            diffusion_number * (2.0 * wave_ref[0, rows, :] - 2.0) + cross[0],
            cross[1] - v0 * wave_ref[1, rows, :],
        )
        total = None
        for m in range(4):
            moved = scaled(mu[m], symbol)
            damp = inverse_of((1.0 - moved[0], -moved[1]))
            damp_ref[m, rows, :] = damp[0]
            damp_ref[m, lower, :] = damp[1]
            term = scaled(eps[m], damp)
            total = term if total is None else plus(total, term)
        ratio_ref[rows, :] = total[0]
        ratio_ref[lower, :] = total[1]
        last_ref[rows, :] = jnp.zeros((8, 128), f32)
        last_ref[lower, :] = jnp.zeros((8, 128), f32)

    lane = lax.broadcasted_iota(jnp.int32, (8, 128), 1)
    narrow = (lane % 64) < 32
    special = ((lane % 32) == 0) & (half == 0)
    plain_pair = pair > 0
    take_own = special & jnp.logical_not(plain_pair)
    take_64 = jnp.logical_not(plain_pair)
    take_32 = narrow ^ special

    def partner(v):
        swapped = jnp.where(take_32, pltpu.roll(v, 32, 1), pltpu.roll(v, 96, 1))
        return jnp.where(take_own, v, jnp.where(take_64, pltpu.roll(v, 64, 1), swapped))

    @pl.loop(0, STEPS)
    def _(s):
        top = pl.multiple_of(s * (SLABS * ROWS), 8)
        pieces = [got_ref[pl.ds(pl.multiple_of(top + x * ROWS, 8), 8), :] for x in range(SLABS)]
        pieces += [got_ref[pl.ds(pl.multiple_of(top + x * ROWS + 8, 8), 8), :] for x in range(SLABS)]
        stacked = jnp.concatenate(pieces + [partner(v) for v in pieces], axis=0)
        drive = left_dot(tg_ref[...], stacked)
        fields = []
        for m in range(2):
            plain = [got_ref[pl.ds(top + 16 + m * 4 + k, SLABS, stride=ROWS), :] for k in range(4)]
            turned = [partner(v) for v in plain]
            fields.append(plain)
            fields.append([turned[0], -turned[1], turned[2], -turned[3]])
        sources = []
        for m in range(4):
            a, b = (fields[m][0], fields[m][1]), (fields[m][2], fields[m][3])
            a = tuple(pltpu.roll(v, 1, 0) for v in a)
            first = minus(a, times(found[m][0], b))
            sources.append(jnp.concatenate([first[0], first[1], b[0], b[1]], axis=0))
        point = left_dot(td_ref[...], jnp.concatenate(sources, axis=1))
        total = (drive[:128], drive[128:])
        for m in range(4):
            d = (point[:128, 128 * m : 128 * m + 128], point[128:, 128 * m : 128 * m + 128])
            y = times((damp_ref[m, :128, :], damp_ref[m, 128:, :]), d)
            if m % 2 == 0:
                kept_ref[s, m // 2, :128, :] = y[0]
                kept_ref[s, m // 2, 128:, :] = y[1]
            total = plus(total, y)
        drive_ref[s, :128, :] = total[0]
        drive_ref[s, 128:, :] = total[1]
        ratio = (ratio_ref[:128, :], ratio_ref[128:, :])
        summed = plus(total, times(ratio, (last_ref[:128, :], last_ref[128:, :])))
        last_ref[:128, :] = summed[0]
        last_ref[128:, :] = summed[1]

    @pl.loop(0, 16)
    def _(at):
        rows = pl.ds(pl.multiple_of(at * 8, 8), 8)
        lower = pl.ds(pl.multiple_of(at * 8 + 128, 8), 8)
        power = (ratio_ref[rows, :], ratio_ref[lower, :])
        for k in range(5):
            power = times(power, power)
        closing = inverse_of((1.0 - circulant_alpha * power[0], -circulant_alpha * power[1]))
        first = times(closing, (last_ref[rows, :], last_ref[lower, :]))
        last_ref[rows, :] = circulant_alpha * first[0]
        last_ref[lower, :] = circulant_alpha * first[1]
        for m in (0, 2):
            weighted = scaled(eps[m], (damp_ref[m, rows, :], damp_ref[m, lower, :]))
            damp_ref[m, rows, :] = weighted[0]
            damp_ref[m, lower, :] = weighted[1]

    @pl.loop(0, STEPS)
    def _(s):
        top = pl.multiple_of(s * (SLABS * ROWS), 8)
        last = (last_ref[:128, :], last_ref[128:, :])
        packed = left_dot(tw_ref[...], last_ref[...])
        for x in range(SLABS):
            back_ref[pl.ds(pl.multiple_of(top + x * ROWS, 8), 8), :] = packed[8 * x : 8 * x + 8]
            back_ref[pl.ds(pl.multiple_of(top + x * ROWS + 8, 8), 8), :] = packed[64 + 8 * x : 72 + 8 * x]
        lines = []
        for m in range(2):
            y = times((damp_ref[2 * m, :128, :], damp_ref[2 * m, 128:, :]), last)
            y = plus(y, (kept_ref[s, m, :128, :], kept_ref[s, m, 128:, :]))
            lines.append(jnp.concatenate([y[0], y[1]], axis=0))
        ends = left_dot(tb_ref[...], jnp.concatenate(lines, axis=1))
        for m in range(2):
            part = [ends[8 * k : 8 * k + 8, 128 * m : 128 * m + 128] for k in range(6)]
            p, q, kappa, inv = found[2 * m]
            u = times(kappa, minus((part[0], part[1]), times(q, (part[2], part[3]))))
            for k, value in enumerate((u[0], u[1], part[4], part[5])):
                back_ref[pl.ds(top + 16 + m * 4 + k, SLABS, stride=ROWS), :] = value
        ratio = (ratio_ref[:128, :], ratio_ref[128:, :])
        following = plus((drive_ref[s, :128, :], drive_ref[s, 128:, :]), times(ratio, last))
        last_ref[:128, :] = following[0]
        last_ref[128:, :] = following[1]


def owner_place(owner):
    x, y, z_pair = owner // 16, (owner // 4) % 4, owner % 4
    z = 2 * z_pair + (x + y) % 2
    return ((z % 4) * 4 + y) * 2 + 1, x * 2 + z // 4


def owner_of(tm, space):
    y, z, x = (tm // 2) % 4, (tm // 8) + 4 * (space % 2), space // 2
    owner = x * 16 + y * 4 + z // 2
    return owner, ((tm % 2) == 1) & ((x + y + z) % 2 == 0)


def gather_kernel(send_ref, got_ref, send_sem, recv_sem, own_sem):
    tm, space = lax.axis_index("tm"), lax.axis_index("space")
    owner, is_owner = owner_of(tm, space)
    here = (tm * SLABS + space) * ROWS

    def copy(target):
        to_tm, to_space = owner_place(target)
        return pltpu.make_async_remote_copy(
            src_ref=send_ref.at[pl.ds(pl.multiple_of(target * ROWS, 8), ROWS), :],
            dst_ref=got_ref.at[pl.ds(pl.multiple_of(here, 8), ROWS), :],
            send_sem=send_sem,
            recv_sem=recv_sem,
            device_id=(to_tm, to_space),
            device_id_type=MESH,
        )

    def kept():
        return pltpu.make_async_copy(
            send_ref.at[pl.ds(pl.multiple_of(owner * ROWS, 8), ROWS), :],
            got_ref.at[pl.ds(pl.multiple_of(here, 8), ROWS), :],
            own_sem,
        )

    @pl.when(is_owner)
    def _():
        kept().start()

    @pl.loop(0, OWNERS)
    def _(k):
        target = (owner + k) % OWNERS

        @pl.when(jnp.logical_not(is_owner) | (k > 0))
        def _():
            copy(target).start()

    def waiter(rows_sent, rows_got):
        return pltpu.make_async_remote_copy(
            src_ref=send_ref.at[pl.ds(0, rows_sent), :],
            dst_ref=got_ref.at[pl.ds(0, rows_got), :],
            send_sem=send_sem,
            recv_sem=recv_sem,
            device_id=(tm, space),
            device_id_type=MESH,
        )

    @pl.when(is_owner)
    def _():
        kept().wait()
        both = waiter((OWNERS - 1) * ROWS, (STEPS * SLABS - 1) * ROWS)
        both.wait_send()
        both.wait_recv()

    @pl.when(jnp.logical_not(is_owner))
    def _():
        waiter(OWNERS * ROWS, OWNERS * ROWS).wait_send()


def scatter_kernel(back_ref, got_ref, send_sem, recv_sem, own_sem):
    tm, space = lax.axis_index("tm"), lax.axis_index("space")
    owner, is_owner = owner_of(tm, space)
    me = tm * SLABS + space
    count = STEPS * SLABS

    def copy(target):
        return pltpu.make_async_remote_copy(
            src_ref=back_ref.at[pl.ds(pl.multiple_of(target * ROWS, 8), ROWS), :],
            dst_ref=got_ref.at[pl.ds(pl.multiple_of(owner * ROWS, 8), ROWS), :],
            send_sem=send_sem,
            recv_sem=recv_sem,
            device_id=(target // SLABS, target % SLABS),
            device_id_type=MESH,
        )

    def kept():
        return pltpu.make_async_copy(
            back_ref.at[pl.ds(pl.multiple_of(me * ROWS, 8), ROWS), :],
            got_ref.at[pl.ds(pl.multiple_of(owner * ROWS, 8), ROWS), :],
            own_sem,
        )

    def waiter(rows_sent, rows_got):
        return pltpu.make_async_remote_copy(
            src_ref=back_ref.at[pl.ds(0, rows_sent), :],
            dst_ref=got_ref.at[pl.ds(0, rows_got), :],
            send_sem=send_sem,
            recv_sem=recv_sem,
            device_id=(tm, space),
            device_id_type=MESH,
        )

    @pl.when(is_owner)
    def _():
        kept().start()

        @pl.loop(1, count)
        def _(k):
            copy((me + k) % count).start()

        kept().wait()
        both = waiter((count - 1) * ROWS, (OWNERS - 1) * ROWS)
        both.wait_send()
        both.wait_recv()

    @pl.when(jnp.logical_not(is_owner))
    def _():
        waiter(OWNERS * ROWS, OWNERS * ROWS).wait_recv()


VMEM, SMEM, ANY = pltpu.VMEM, pltpu.SMEM, pl.ANY


def spec(space):
    return pl.BlockSpec(memory_space=space)


def shape(*dims):
    return jax.ShapeDtypeStruct(dims, f32)


PARAMS = pltpu.CompilerParams(vmem_limit_bytes=60 * 1024 * 1024)


def forward(velocity, step, iterate, right_side, kappa, below, above, interpret=False):
    return pl.pallas_call(
        forward_kernel,
        out_shape=(shape(32, 128, 128), shape(OWNERS * ROWS, 128)),
        in_specs=[spec(SMEM)] * 2 + [spec(VMEM)] * 9,
        out_specs=(spec(VMEM), spec(VMEM)),
        scratch_shapes=[VMEM((2816, 256), bf16), VMEM((2816, 256), bf16), VMEM((44, 128, 128), f32)],
        compiler_params=PARAMS,
        interpret=interpret,
        name="forward",
    )(
        velocity, step, iterate, right_side, kappa, below, above,
        TABLES["ty"], TABLES["tz"], TABLES["lane"], TABLES["row"],
    )


def modes(velocity, place, got, own, interpret=False):
    return pl.pallas_call(
        mode_kernel,
        out_shape=shape(STEPS * SLABS * ROWS, 128),
        in_specs=[spec(SMEM)] * 2 + [spec(VMEM)] * 7,
        out_specs=spec(VMEM),
        scratch_shapes=[
            VMEM((4, 256, 128), f32), VMEM((256, 128), f32), VMEM((256, 128), f32),
            VMEM((STEPS, 256, 128), f32), VMEM((STEPS, 2, 256, 128), f32),
        ],
        compiler_params=PARAMS,
        interpret=interpret,
        name="modes",
    )(
        velocity, place, got, own,
        TABLES["wave_x"], TABLES["tg"], TABLES["td"], TABLES["tw"], TABLES["tb"],
    )


def backward(velocity, iterate, u, got, interpret=False):
    return pl.pallas_call(
        backward_kernel,
        out_shape=shape(4, WIDE, NZ, NY),
        in_specs=[spec(SMEM)] + [spec(VMEM)] * 7,
        out_specs=spec(VMEM),
        scratch_shapes=[VMEM((32, 128, 128), f32)],
        compiler_params=PARAMS,
        interpret=interpret,
        name="backward",
    )(velocity, iterate, u, got, TABLES["uy"], TABLES["uz"], TABLES["lane"], TABLES["row"])


def exchange(kernel, value, rows, name):
    return pl.pallas_call(
        kernel,
        out_shape=shape(rows, 128),
        in_specs=[spec(ANY)],
        out_specs=spec(ANY),
        scratch_shapes=[pltpu.SemaphoreType.DMA] * 3,
        compiler_params=pltpu.CompilerParams(has_side_effects=True),
        name=name,
    )(value)


def shards(iterate, right_side, diffusivity, velocity):
    iterate, right_side = iterate[0], right_side[0]
    tm, space = lax.axis_index("tm"), lax.axis_index("space")
    up = [(i, (i + 1) % SLABS) for i in range(SLABS)]
    down = [(i, (i - 1) % SLABS) for i in range(SLABS)]
    below = lax.ppermute(diffusivity[WIDE - 1], "space", up)
    above = lax.ppermute(diffusivity[0], "space", down)
    step = tm.astype(jnp.int32)[None]
    u, sent = forward(velocity, step, iterate, right_side, diffusivity, below, above)
    got = exchange(gather_kernel, sent, STEPS * SLABS * ROWS, "gather")
    owner, _ = owner_of(tm, space)
    place = jnp.stack([owner // 32, owner % 32]).astype(jnp.int32)
    own = lax.dynamic_index_in_dim(jnp.asarray(TABLES["own"]), owner, 0, keepdims=False)
    back = modes(velocity, place, got, own)
    returned = exchange(scatter_kernel, back, OWNERS * ROWS, "scatter")
    return backward(velocity, iterate, u, returned)[None]


def solution(mesh):
    placed = (
        P("tm", None, "space", None, None),
        P("tm", None, "space", None, None),
        P("space", None, None),
        P(),
    )
    return jax.shard_map(
        shards,
        mesh=mesh,
        in_specs=placed,
        out_specs=P("tm", None, "space", None, None),
        check_vma=False,
    )
```

```python
import functools
import math

import jax
import jax.numpy as jnp
import numpy as np
from jax import lax
from jax.experimental import pallas as pl
from jax.experimental.pallas import tpu as pltpu
from jax.sharding import PartitionSpec as P

NX, NY, NZ, STEPS = 128, 128, 64, 32
SLABS, WIDE = 8, 16
OWNERS = 128
ROWS = 12
MESH = pl.DeviceIdType.MESH
f32, bf16 = jnp.float32, jnp.bfloat16

diffusion_number = 16.0
circulant_alpha = 0.1


def collocation_matrix():
    radau_nodes = [0.08858795951270394, 0.4094668644407347, 0.7876594617608471, 1.0]
    matrix = [[0.0] * 4 for row_index in range(4)]
    for column_index in range(4):
        coefficients = [1.0]
        for other_index in range(4):
            if other_index != column_index:
                scale_value = 1.0 / (radau_nodes[column_index] - radau_nodes[other_index])
                shifted = [0.0] + [value * scale_value for value in coefficients]
                lowered = [
                    -radau_nodes[other_index] * scale_value * value for value in coefficients
                ] + [0.0]
                coefficients = [
                    left_value + right_value for left_value, right_value in zip(shifted, lowered)
                ]
        for row_index in range(4):
            total = 0.0
            for power_index in range(len(coefficients)):
                total = total + coefficients[power_index] * radau_nodes[row_index] ** (
                    power_index + 1
                ) / (power_index + 1)
            matrix[row_index][column_index] = total
    return matrix


def solve_system(matrix, target):
    count = len(target)
    rows_list = [list(matrix[row_index]) + [target[row_index]] for row_index in range(count)]
    for column in range(count):
        best_row = column
        for candidate in range(column + 1, count):
            if abs(rows_list[candidate][column]) > abs(rows_list[best_row][column]):
                best_row = candidate
        saved_row = rows_list[column]
        rows_list[column] = rows_list[best_row]
        rows_list[best_row] = saved_row
        leader = rows_list[column][column]
        for other_row in range(count):
            if other_row != column:
                factor = rows_list[other_row][column] / leader
                rows_list[other_row] = [
                    left_value - factor * right_value
                    for left_value, right_value in zip(rows_list[other_row], rows_list[column])
                ]
    return [
        rows_list[row_index][count] / rows_list[row_index][row_index] for row_index in range(count)
    ]


def node_basis():
    matrix = collocation_matrix()
    helper = [[0.0] * 4 for row_index in range(4)]
    coefficients = [0.0, 0.0, 0.0, 0.0, 1.0]
    for order in range(1, 5):
        product = [
            [
                sum((matrix[row_index][inner] * helper[inner][column] for inner in range(4)))
                for column in range(4)
            ]
            for row_index in range(4)
        ]
        for row_index in range(4):
            product[row_index][row_index] = product[row_index][row_index] + coefficients[5 - order]
        helper = product
        trace_value = sum(
            (
                sum((matrix[row_index][inner] * helper[inner][row_index] for inner in range(4)))
                for row_index in range(4)
            )
        )
        coefficients[4 - order] = -trace_value / order
    roots_list = [(0.4 + 0.9j) ** power_index for power_index in range(4)]
    for sweep in range(400):
        for root_index in range(4):
            current = roots_list[root_index]
            numer = 0.0
            for power_index in range(4, -1, -1):
                numer = numer * current + coefficients[power_index]
            denom = 1.0
            for other_index in range(4):
                if other_index != root_index:
                    denom = denom * (current - roots_list[other_index])
            roots_list[root_index] = current - numer / denom
    vectors = [[0.0] * 4 for row_index in range(4)]
    for root_index in range(4):
        shifted = [
            [
                matrix[row_index][column] - (roots_list[root_index] if row_index == column else 0.0)
                for column in range(3)
            ]
            for row_index in range(3)
        ]
        target = [-matrix[row_index][3] for row_index in range(3)]
        parts = solve_system(shifted, target) + [1.0 + 0j]
        for row_index in range(4):
            vectors[row_index][root_index] = parts[row_index]
    inverse = [[0.0] * 4 for row_index in range(4)]
    for column in range(4):
        unit = [1.0 if row_index == column else 0.0 for row_index in range(4)]
        parts = solve_system(vectors, unit)
        for row_index in range(4):
            inverse[row_index][column] = parts[row_index]
    weights = [sum((inverse[row_index][column] for column in range(4))) for row_index in range(4)]
    return (roots_list, vectors, inverse, weights)


VALUES, VECTORS, INVERSE, WEIGHTS = node_basis()
PAIRS = [m for m in range(4) if complex(VALUES[m]).imag > 0]
MU = [complex(VALUES[m]) for m in PAIRS]
COLUMN = [[complex(VECTORS[n][m]) for n in range(4)] for m in PAIRS]
ROW = [[complex(INVERSE[m][n]) for n in range(4)] for m in PAIRS]
EPS = [complex(WEIGHTS[m]) for m in PAIRS]


def wave_order_z():
    index = np.arange(NZ)
    return np.where(index <= NZ // 2, index, NZ + NZ // 2 - index)


def wave_order_y():
    lane = np.arange(NY)
    index = 16 * (lane // 32) + lane % 16
    return np.where(lane % 32 < 16, index, np.where(index == 0, NY // 2, NY - index))


def split(values):
    values = np.asarray(values, np.float64)
    high = values.astype(np.float32).astype(bf16)
    low = (values - high.astype(np.float64)).astype(np.float32).astype(bf16)
    return high, low


def side_table(values):
    high, low = split(values)
    return np.concatenate([high, high, low], axis=1)


def halves(x):
    high = x.astype(bf16)
    return high, (x - high.astype(f32)).astype(bf16)


def left_dot(table, x):
    high, low = halves(x)
    return jnp.dot(table, jnp.concatenate([high, low, high], axis=0), preferred_element_type=f32)


def right_dot(high, low, table_high, table_low):
    return (
        jnp.dot(high, table_high, preferred_element_type=f32)
        + jnp.dot(low, table_high, preferred_element_type=f32)
        + jnp.dot(high, table_low, preferred_element_type=f32)
    )


def complex_block(matrix):
    return np.block([[matrix.real, -matrix.imag], [matrix.imag, matrix.real]])


def make_tables():
    ky, kz = wave_order_y(), wave_order_z()
    kx, x = np.arange(NX), np.arange(NX)
    to_y = np.exp(-2j * np.pi * np.outer(ky, np.arange(NY)) / NY)
    to_z = np.exp(-2j * np.pi * np.outer(kz, np.arange(NZ)) / NZ)
    tables = {}
    tables["ty"] = np.stack(split(complex_block(to_y).T))
    tables["tz"] = side_table(complex_block(to_z))
    tables["uy"] = np.stack(split(complex_block(np.conj(to_y.T) / NY).T))
    tables["uz"] = side_table(complex_block(np.conj(to_z.T) / NZ))
    cells = (np.arange(SLABS)[:, None] * WIDE + np.arange(8)[None, :]).reshape(-1)
    theta = 2 * np.pi * kx / NX
    at = np.exp(-1j * np.outer(theta, cells))
    shifted = np.exp(-8j * theta)[:, None]
    from_own = at * (1 - 1j * shifted) / 2
    from_partner = at * (1 + 1j * shifted) / 2
    firsts = np.arange(SLABS) * WIDE

    def lane_block(matrix):
        return np.concatenate([matrix.real, -matrix.imag], axis=1)

    def drive_table(from_x):
        table = np.zeros((NX, SLABS, ROWS), complex)
        table[:, :, :8] = from_x.reshape(NX, SLABS, 8)
        return table

    def point_tables():
        out = []
        for m in range(2):
            table = np.zeros((NX, SLABS, ROWS), complex)
            table[:, :, 8 + 2 * m] = np.exp(-1j * np.outer(theta, firsts + WIDE))
            table[:, :, 9 + 2 * m] = np.exp(-1j * np.outer(theta, firsts - 1))
            out.append(table)
        for m in range(2):
            table = np.zeros((8, SLABS, ROWS), complex)
            table[:, :, 9 + 2 * m] = np.exp(-1j * np.outer(theta[:8], firsts))
            out.append(table)
        return out

    def flat(pieces):
        return lane_block(np.concatenate(pieces, axis=0).reshape(-1, SLABS * ROWS))

    tables["tg"] = np.stack(
        [side_table(flat([drive_table(k)] + point_tables())) for k in (from_own, from_partner)]
    )
    back = np.exp(1j * np.outer(cells, theta)) * (1 + 1j * np.exp(8j * theta))[None, :] / NX
    tables["tw"] = side_table(lane_block(back))
    ends = [np.exp(1j * np.outer(firsts + k, theta)) / NX for k in (0, 1, 15)]
    tables["tb"] = side_table(lane_block(np.concatenate(ends, axis=0)))
    trig_y = 2 * np.pi * ky / NY
    trig_z = 2 * np.pi * kz / NZ
    tables["lane"] = np.stack([np.cos(trig_y), np.sin(trig_y)]).astype(np.float32)
    tables["row"] = np.stack(
        [np.broadcast_to(v[:, None], (NZ, NY)) for v in (np.cos(trig_z), np.sin(trig_z))]
    ).astype(np.float32)
    tables["wave_x"] = np.stack(
        [np.broadcast_to(v[:, None], (NX, 128)) for v in (np.cos(theta), np.sin(theta))]
    ).astype(np.float32)
    lane = np.arange(128)
    own = np.zeros((OWNERS, 8, 128))
    for owner in range(OWNERS):
        part, pair = owner // 32, owner % 32
        piece = (lane // 32 - part) % 4
        at_y, row = (lane - 32 * piece) % 128, piece % 2
        other_y = np.where((at_y == 0) | (at_y == 16), at_y, at_y ^ 16)
        other_row = row if pair == 0 else 1 - row
        other = (other_y + 32 * (2 * (piece // 2) + other_row)) % 128
        y, z = trig_y[at_y], trig_z[pair + 32 * row]
        own[owner] = np.stack(
            [
                np.cos(y), np.sin(y), np.cos(z), np.sin(z),
                other, np.roll(other, -64), np.where(piece < 2, 1.0, -1.0), (lane + 64) % 128,
            ]
        )
    tables["own"] = own.astype(np.float32)
    return tables


TABLES = make_tables()


def times(a, b):
    return (a[0] * b[0] - a[1] * b[1], a[0] * b[1] + a[1] * b[0])


def plus(a, b):
    return (a[0] + b[0], a[1] + b[1])


def minus(a, b):
    return (a[0] - b[0], a[1] - b[1])


def scaled(number, a):
    return (number.real * a[0] - number.imag * a[1], number.real * a[1] + number.imag * a[0])


def inverse_of(a):
    size = 1.0 / (a[0] * a[0] + a[1] * a[1])
    return (a[0] * size, -a[1] * size)


def root_of(a):
    size = jnp.sqrt(a[0] * a[0] + a[1] * a[1])
    main = jnp.sqrt(0.5 * (size + jnp.abs(a[0])))
    other = a[1] / (2.0 * main)
    positive = a[0] >= 0.0
    return (
        jnp.where(positive, main, jnp.abs(other)),
        jnp.where(positive, other, jnp.where(a[1] >= 0.0, main, -main)),
    )


def cross_symbol(cos_y, sin_y, cos_z, sin_z, v1, v2):
    return (
        diffusion_number * ((2.0 * cos_y - 2.0) + (2.0 * cos_z - 2.0)),
        -(v1 * sin_y + v2 * sin_z),
    )


def factors(mu, cross, v0):
    c_up = -mu.real * (diffusion_number - 0.5 * v0), -mu.imag * (diffusion_number - 0.5 * v0)
    c_down = -mu.real * (diffusion_number + 0.5 * v0), -mu.imag * (diffusion_number + 0.5 * v0)
    moved = scaled(mu, cross)
    c_mid = (1.0 + 2.0 * diffusion_number * mu.real - moved[0], 2.0 * diffusion_number * mu.imag - moved[1])
    product = times(c_up, c_down)
    square = times(c_mid, c_mid)
    root = root_of((square[0] - 4.0 * product[0], square[1] - 4.0 * product[1]))
    same = c_mid[0] * root[0] + c_mid[1] * root[1] >= 0.0
    kappa = (
        0.5 * (c_mid[0] + jnp.where(same, root[0], -root[0])),
        0.5 * (c_mid[1] + jnp.where(same, root[1], -root[1])),
    )
    inv = inverse_of(kappa)
    p = times(inv, c_down)
    q = times(inv, c_up)
    return (-p[0], -p[1]), (-q[0], -q[1]), kappa, inv


def plane_partner(low, high, lane, first_row):
    ends = (lane == 0) | (lane == 16)
    first = (lane % 32) < 16

    def turned(v):
        return jnp.where(ends, v, jnp.where(first, pltpu.roll(v, 112, 1), pltpu.roll(v, 16, 1)))

    low_turned, high_turned = [turned(v) for v in low], [turned(v) for v in high]
    to_low = [jnp.where(first_row, a, b) for a, b in zip(low_turned, high_turned)]
    to_high = [jnp.where(first_row, b, a) for a, b in zip(low_turned, high_turned)]
    return (to_low[0], -to_low[1]), (to_high[0], -to_high[1])


def packed_for(low, high, block):
    pieces = [low[0], high[0], low[1], high[1]]
    pieces = [pieces[0]] + [pltpu.roll(pieces[c], 32 * c, 1) for c in (1, 2, 3)]
    out = []
    for h in range(4):
        value = pieces[3]
        for c in (2, 1, 0):
            value = jnp.where(block == (h + c) % 4, pieces[c], value)
        out.append(value)
    return out


def unpacked_from(values, block):
    out = []
    for c in range(4):
        piece = values[(3 - c) % 4]
        for d in (2, 1, 0):
            piece = jnp.where(block == d, values[(d - c) % 4], piece)
        out.append(piece if c == 0 else pltpu.roll(piece, 128 - 32 * c, 1))
    return (out[0], out[2]), (out[1], out[3])


def chunk_factors(t, lane_ref, row_ref, velocity_ref, mu):
    cos_y, sin_y = lane_ref[0:1, :], lane_ref[1:2, :]
    found = []
    for base in (0, 32):
        rows = pl.ds(pl.multiple_of(base + 8 * t, 8), 8)
        cross = cross_symbol(
            cos_y, sin_y, row_ref[0, rows, :], row_ref[1, rows, :], velocity_ref[1], velocity_ref[2]
        )
        found.append([factors(number, cross, velocity_ref[0]) for number in mu])
    return found


def dft_block(high, low, ty_ref, tz_ref):
    mid = right_dot(high, low, ty_ref[0], ty_ref[1])
    stacked = jnp.concatenate(
        [
            jnp.concatenate([mid[64 * k : 64 * k + 64, :128], mid[64 * k : 64 * k + 64, 128:]], axis=0)
            for k in range(4)
        ],
        axis=1,
    )
    return left_dot(tz_ref[...], stacked)


def source_kernel(
    velocity_ref, step_ref, iterate_ref, right_ref, kappa_ref, ty_ref, tz_ref,
    spec_ref, mixed_ref,
    high_ref, low_ref,
):
    v0, v1, v2 = velocity_ref[0], velocity_ref[1], velocity_ref[2]

    def put(at, real, imag):
        rows = pl.ds(pl.multiple_of(at * 64, 64), 64)
        for k, part in enumerate((real, imag)):
            high, low = halves(part)
            high_ref[rows, k * 128 : (k + 1) * 128] = high
            low_ref[rows, k * 128 : (k + 1) * 128] = low

    def mixture(m, groups):
        real = imag = None
        for scale, values in groups:
            for n in range(4):
                factor = scale * ROW[m][n]
                a, b = factor.real * values[n], factor.imag * values[n]
                real = a if real is None else real + a
                imag = b if imag is None else imag + b
        return real, imag

    def inner(x, below, above):
        plain, applied = [], []
        kappa = kappa_ref[x]
        for n in range(4):
            f = iterate_ref[n, x]
            up_z, down_z = pltpu.roll(f, NZ - 1, 0), pltpu.roll(f, 1, 0)
            up_y, down_y = pltpu.roll(f, NY - 1, 1), pltpu.roll(f, 1, 1)
            total = (up_z + down_z) + (up_y + down_y) - 6.0 * f
            moved = v1 * (up_y - down_y) + v2 * (up_z - down_z)
            if above:
                up_x = iterate_ref[n, x + 1]
                total, moved = total + up_x, moved + v0 * up_x
            if below:
                down_x = iterate_ref[n, x - 1]
                total, moved = total + down_x, moved - v0 * down_x
            applied.append((diffusion_number * kappa) * total - 0.5 * moved)
            plain.append(right_ref[n, x] - f)
        for m in range(2):
            real, imag = mixture(m, [(1.0, plain), (MU[m], applied)])
            put(m * 16 + x, real, imag)

    for side, x in enumerate((0, WIDE - 1)):
        for m in range(2):
            real, imag = mixture(m, [(MU[m], [iterate_ref[n, x] for n in range(4)])])
            mixed_ref[side * 4 + m * 2] = real
            mixed_ref[side * 4 + m * 2 + 1] = imag
    inner(0, False, True)
    inner(WIDE - 1, True, False)

    @pl.loop(1, WIDE - 1)
    def _(x):
        inner(x, True, True)

    keep = jnp.where(step_ref[0] < STEPS - 1, 1.0, 0.0).astype(f32)

    @pl.loop(0, 8)
    def _(x):
        put(32 + x, keep * iterate_ref[3, x], keep * iterate_ref[3, x + 8])

    @pl.loop(0, 10)
    def _(block):
        rows = pl.ds(pl.multiple_of(block * 256, 256), 256)
        out = dft_block(high_ref[rows, :], low_ref[rows, :], ty_ref, tz_ref)
        for k in range(4):
            spec_ref[block * 4 + k] = out[:, 128 * k : 128 * k + 128]


def slab_kernel(
    velocity_ref, spec_ref, mixed_ref, below_ref, above_ref, ty_ref, tz_ref, lane_ref, row_ref,
    u_ref, send_ref,
    edge_ref,
):
    v0 = velocity_ref[0]
    outer = [diffusion_number * below_ref[...] - 0.5 * v0, diffusion_number * above_ref[...] + 0.5 * v0]
    edges = [
        jnp.concatenate([outer[side] * mixed_ref[side * 4 + m * 2 + part] for part in range(2)], axis=1)
        for m in range(2)
        for side in range(2)
    ]
    high, low = halves(jnp.concatenate(edges, axis=0))
    out = dft_block(high, low, ty_ref, tz_ref)
    for k in range(4):
        edge_ref[k] = out[:, 128 * k : 128 * k + 128]

    lane = lax.broadcasted_iota(jnp.int32, (8, 128), 1)
    sub = lax.broadcasted_iota(jnp.int32, (8, 128), 0)
    block = lane // 32

    @pl.loop(0, 4)
    def _(t):
        first_row = (sub + t) == 0
        found = chunk_factors(t, lane_ref, row_ref, velocity_ref, MU)
        bases = [pl.multiple_of(base + 8 * t, 8) for base in (0, 32)]

        def plane(at, base, ref=spec_ref):
            return ref[at, pl.ds(base, 8), :], ref[at, pl.ds(base + 64, 8), :]

        def send(value, low, high):
            for h, packed in enumerate(packed_for(low, high, block)):
                send_ref[pl.ds((32 * h + 8 * t) * ROWS + value, 8, stride=ROWS), :] = packed

        sums = [[None, None] for x in range(WIDE)]
        for m in range(2):
            carries = []
            for half in range(2):
                base = bases[half]
                p, q, kappa, inv = found[half][m]
                under, over = plane(m * 2, base, edge_ref), plane(m * 2 + 1, base, edge_ref)
                u = plus(plane(m * 16, base), times(p, under))
                us = [u]
                for x in range(1, WIDE):
                    u = plus(plane(m * 16 + x, base), times(p, u))
                    us.append(u)
                for x in range(WIDE):
                    u_ref[m * 16 + x, pl.ds(base, 8), :] = us[x][0]
                    u_ref[m * 16 + x, pl.ds(base + 64, 8), :] = us[x][1]
                outflow = plus(times(p, us[-1]), over)
                y = us[-1]
                for x in range(WIDE - 1, -1, -1):
                    if x < WIDE - 1:
                        y = plus(us[x], times(q, y))
                    z = times(inv, y)
                    sums[x][half] = z if m == 0 else plus(sums[x][half], z)
                carries.append((outflow, plus(times(q, y), under)))
            for k in range(2):
                send(8 + m * 2 + k, carries[0][k], carries[1][k])
        for x in range(8):
            own, other = [], []
            for half in range(2):
                first, second = sums[x][half], sums[x + 8][half]
                own.append((first[0] - second[1], first[1] + second[0]))
                other.append((first[0] + second[1], first[1] - second[0]))
            partners = plane_partner(other[0], other[1], lane, first_row)
            packed = [
                plus(plus(own[half], partners[half]), plane(32 + x, bases[half])) for half in range(2)
            ]
            send(x, packed[0], packed[1])


def backward_kernel(
    velocity_ref, iterate_ref, u_ref, got_ref, uy_ref, uz_ref, lane_ref, row_ref,
    out_ref,
    spec_ref,
):
    lane = lax.broadcasted_iota(jnp.int32, (8, 128), 1)
    sub = lax.broadcasted_iota(jnp.int32, (8, 128), 0)
    block = lane // 32

    @pl.loop(0, 4)
    def _(t):
        first_row = (sub + t) == 0
        found = chunk_factors(t, lane_ref, row_ref, velocity_ref, MU)
        bases = [pl.multiple_of(base + 8 * t, 8) for base in (0, 32)]

        def take(value):
            values = [
                got_ref[pl.ds((32 * h + 8 * t) * ROWS + value, 8, stride=ROWS), :] for h in range(4)
            ]
            return unpacked_from(values, block)

        last = [[None, None] for x in range(WIDE)]
        for x in range(8):
            packed = take(x)
            partners = plane_partner(packed[0], packed[1], lane, first_row)
            for half in range(2):
                both, apart = plus(packed[half], partners[half]), minus(packed[half], partners[half])
                last[x][half] = (0.5 * both[0], 0.5 * both[1])
                last[x + 8][half] = (0.5 * apart[1], -0.5 * apart[0])
        for m in range(2):
            start, end = take(8 + m * 2), take(9 + m * 2)
            for half in range(2):
                base = bases[half]
                p, q, kappa, inv = found[half][m]

                def old(x):
                    return (
                        u_ref[m * 16 + x, pl.ds(base, 8), :],
                        u_ref[m * 16 + x, pl.ds(base + 64, 8), :],
                    )

                u = start[half]
                totals = [plus(u, old(0))]
                for x in range(1, WIDE - 1):
                    u = plus(scaled(EPS[m], last[x][half]), times(p, u))
                    totals.append(plus(u, old(x)))
                y = plus(times(inv, old(WIDE - 1)), end[half])
                for x in range(WIDE - 1, -1, -1):
                    if x < WIDE - 1:
                        y = plus(times(inv, totals[x]), times(q, y))
                    spec_ref[m * 16 + x, pl.ds(base, 8), :] = y[0]
                    spec_ref[m * 16 + x, pl.ds(base + 64, 8), :] = y[1]

    @pl.loop(0, 8)
    def _(block):
        planes = [2 * block, 2 * block + 1, 16 + 2 * block, 17 + 2 * block]
        stacked = jnp.concatenate([spec_ref[at] for at in planes], axis=1)
        mid = left_dot(uz_ref[...], stacked)
        rows = jnp.concatenate(
            [
                jnp.concatenate([mid[:64, 128 * k : 128 * k + 128], mid[64:, 128 * k : 128 * k + 128]], axis=1)
                for k in range(4)
            ],
            axis=0,
        )
        high, low = halves(rows)
        out = right_dot(high, low, uy_ref[0], uy_ref[1])
        for k in range(2):
            x = 2 * block + k
            parts = []
            for m in range(2):
                piece = out[(2 * m + k) * 64 : (2 * m + k) * 64 + 64]
                parts.append((piece[:, :128], piece[:, 128:]))
            for n in range(4):
                total = iterate_ref[n, x]
                for m in range(2):
                    c = COLUMN[m][n]
                    total = total + (2.0 * c.real) * parts[m][0] - (2.0 * c.imag) * parts[m][1]
                out_ref[n, x] = total


def mode_kernel(
    remote, velocity_ref, own_ref, wave_ref, tg_ref, tw_ref, tb_ref, sent_ref,
    returned_ref,
    got_ref, back_ref, damp_ref, ratio_ref, last_ref, drive_ref, kept_ref, turn_ref,
    gather_sem, arrive_sem, scatter_sem, return_sem, own_sem,
):
    count = STEPS * SLABS
    tm, space = remote.place()
    is_owner = tm % 2 == 1
    owner = (tm // 2) * SLABS + space
    me = tm * SLABS + space

    def rows_of(index, number=1):
        return pl.ds(pl.multiple_of(index * ROWS, 4), number * ROWS)

    @pl.loop(0, OWNERS)
    def _(k):
        pair = (tm // 2 + STEPS // 2 - k // SLABS) % (STEPS // 2)
        to_space = ((space // 2 + (k % SLABS) // 2) % (SLABS // 2)) * 2 + (space + k) % 2
        target = pair * SLABS + to_space

        @pl.when(jnp.logical_not(is_owner) | (k > 0))
        def _():
            remote.start(
                sent_ref.at[rows_of(target), :], got_ref.at[rows_of(me), :],
                gather_sem, arrive_sem.at[tm], (2 * pair + 1, to_space),
            )

    @pl.when(is_owner)
    def _():
        got_ref[rows_of(me), :] = sent_ref[rows_of(owner), :]
        solve_modes(
            remote, owner, tm, me, rows_of,
            velocity_ref, own_ref, wave_ref, tg_ref, tw_ref, tb_ref,
            sent_ref, returned_ref,
            got_ref, back_ref, damp_ref, ratio_ref, last_ref, drive_ref, kept_ref, turn_ref,
            arrive_sem, scatter_sem, return_sem, own_sem,
        )
        remote.wait_sent(sent_ref.at[rows_of(0, OWNERS - 1), :], gather_sem)
        remote.wait_sent(back_ref.at[rows_of(0, count - 1), :], scatter_sem)
        remote.local(back_ref.at[rows_of(me), :], returned_ref.at[rows_of(owner), :], own_sem).wait()
        remote.wait_got(returned_ref.at[rows_of(0, OWNERS - 1), :], return_sem)

    @pl.when(jnp.logical_not(is_owner))
    def _():
        remote.wait_sent(sent_ref.at[rows_of(0, OWNERS), :], gather_sem)
        remote.wait_got(returned_ref.at[rows_of(0, OWNERS), :], return_sem)


def solve_modes(
    remote, owner, tm, me, rows_of,
    velocity_ref, own_ref, wave_ref, tg_ref, tw_ref, tb_ref,
    sent_ref, returned_ref,
    got_ref, back_ref, damp_ref, ratio_ref, last_ref, drive_ref, kept_ref, turn_ref,
    arrive_sem, scatter_sem, return_sem, own_sem,
):
    v0, v1, v2 = velocity_ref[0], velocity_ref[1], velocity_ref[2]
    own = own_ref[owner]
    line = [own[k : k + 1, :] for k in range(8)]
    wide = [jnp.broadcast_to(v, (8, 128)) for v in line]
    sign = wide[6]
    cross = cross_symbol(wide[0], wide[1], wide[2], wide[3], v1, v2)
    mu = [MU[0], MU[1], MU[0].conjugate(), MU[1].conjugate()]
    eps = [EPS[0], EPS[1], EPS[0].conjugate(), EPS[1].conjugate()]
    found = [factors(number, cross, v0) for number in mu]

    def crossed(a):
        return (a[0], -(sign * a[1]))

    def times_lanes(v, table):
        return v * table[0] + pltpu.roll(v, 64, 1) * table[1]

    row = lax.broadcasted_iota(jnp.int32, (128, 128), 0).astype(f32)
    turn_ref[:, 0:128] = jnp.where(row == line[7], line[6], 0.0).astype(bf16)
    turn_ref[:, 128:256] = jnp.where(row == line[4], line[6], 0.0).astype(bf16)
    turn_ref[:, 256:384] = jnp.where(row == line[5], -1.0, 0.0).astype(bf16)

    @pl.loop(0, 16)
    def _(at):
        rows = pl.ds(pl.multiple_of(at * 8, 8), 8)
        symbol = (
            diffusion_number * (2.0 * wave_ref[0, rows, :] - 2.0) + cross[0],
            cross[1] - v0 * wave_ref[1, rows, :],
        )
        total = None
        for m in range(4):
            moved = scaled(mu[m], symbol)
            damp = inverse_of((1.0 - moved[0], -moved[1]))
            for k, value in enumerate(crossed(damp)):
                damp_ref[m, k, rows, :] = value
            term = scaled(eps[m], damp)
            if m < 2:
                for k, value in enumerate(crossed(term)):
                    damp_ref[4 + m, k, rows, :] = value
            total = term if total is None else plus(total, term)
        for k, value in enumerate(crossed(total)):
            ratio_ref[k, rows, :] = value
        power = total
        for k in range(5):
            power = times(power, power)
        closing = inverse_of((1.0 - circulant_alpha * power[0], -circulant_alpha * power[1]))
        for k, value in enumerate(crossed(closing)):
            ratio_ref[2 + k, rows, :] = value
        last_ref[rows, :] = jnp.zeros((8, 128), f32)

    first_step = tm - tm % 2
    roots = [crossed(found[m][0]) for m in range(4)]

    @pl.loop(0, STEPS)
    def _(i):
        s = (first_step + i) % STEPS
        block = pl.ds(pl.multiple_of(s * (SLABS * ROWS), 8), SLABS * ROWS)

        @pl.when(s == tm)
        def _():
            remote.wait_got(got_ref.at[rows_of(0, SLABS - 1), :], arrive_sem.at[s])

        @pl.when(s != tm)
        def _():
            remote.wait_got(got_ref.at[rows_of(0, SLABS), :], arrive_sem.at[s])

        high, low = halves(got_ref[block, :])
        both = jnp.concatenate([high, low], axis=0)
        turned = jnp.dot(both, turn_ref[...], preferred_element_type=f32).astype(bf16)
        cut = SLABS * ROWS
        pieces = [high, turned[:cut, :128], low, turned[cut:, :128], high, turned[:cut, :128]]
        mine = jnp.dot(tg_ref[0], jnp.concatenate(pieces, axis=0), preferred_element_type=f32)
        pieces = [
            turned[:cut, 128:256], turned[:cut, 256:], turned[cut:, 128:256], turned[cut:, 256:],
            turned[:cut, 128:256], turned[:cut, 256:],
        ]
        theirs = jnp.dot(tg_ref[1], jnp.concatenate(pieces, axis=0), preferred_element_type=f32)
        total = mine[:128] + theirs[:128]
        for m in range(4):
            out = mine if m < 2 else theirs
            k = m % 2
            point = times_lanes(out[384 + 8 * k : 392 + 8 * k], roots[m])
            d = out[128 + 128 * k : 256 + 128 * k] - jnp.concatenate([point] * 16, axis=0)
            y = times_lanes(d, (damp_ref[m, 0], damp_ref[m, 1]))
            if m < 2:
                kept_ref[s, m] = y
            total = total + y
        drive_ref[s] = total
        wrap = jnp.where(s == 0, circulant_alpha, 1.0).astype(f32)
        last_ref[...] = total + times_lanes(wrap * last_ref[...], (ratio_ref[0], ratio_ref[1]))

    last_ref[...] = times_lanes(last_ref[...], (ratio_ref[2], ratio_ref[3]))
    kappas = [crossed(found[m][2]) for m in range(2)]
    ups = [crossed(found[m][1]) for m in range(2)]
    flip = jnp.concatenate([sign] * 16, axis=0)

    def both_parts(v):
        return jnp.concatenate([v, flip * pltpu.roll(v, 64, 1)], axis=0)

    def send(s):
        for x in range(SLABS):
            target = s * SLABS + x

            @pl.when(target != me)
            def _():
                remote.start(
                    back_ref.at[rows_of(target), :], returned_ref.at[rows_of(owner), :],
                    scatter_sem, return_sem, (s, x),
                )

            @pl.when(target == me)
            def _():
                remote.local(
                    back_ref.at[rows_of(me), :], returned_ref.at[rows_of(owner), :], own_sem
                ).start()

    @pl.loop(0, STEPS)
    def _(i):
        s = (first_step + i) % STEPS
        top = pl.multiple_of(s * (SLABS * ROWS), 8)
        wrap = jnp.where(s == 0, circulant_alpha, 1.0).astype(f32)
        last = wrap * last_ref[...]
        packed = left_dot(tw_ref[...], both_parts(last))
        for x in range(SLABS):
            back_ref[pl.ds(top + x * ROWS, 8), :] = packed[8 * x : 8 * x + 8]
        lines = []
        for m in range(2):
            y = times_lanes(last, (damp_ref[4 + m, 0], damp_ref[4 + m, 1])) + kept_ref[s, m]
            lines.append(both_parts(y))
        ends = left_dot(tb_ref[...], jnp.concatenate(lines, axis=1))
        for m in range(2):
            part = [ends[8 * k : 8 * k + 8, 128 * m : 128 * m + 128] for k in range(3)]
            u = times_lanes(part[0] - times_lanes(part[1], ups[m]), kappas[m])
            back_ref[pl.ds(top + 8 + m * 2, SLABS, stride=ROWS), :] = u
            back_ref[pl.ds(top + 9 + m * 2, SLABS, stride=ROWS), :] = part[2]
        last_ref[...] = drive_ref[s] + times_lanes(last, (ratio_ref[0], ratio_ref[1]))

        @pl.when(i > 0)
        def _():
            send((s + STEPS - 1) % STEPS)

    send((first_step + STEPS - 1) % STEPS)


class Remote:
    def place(self):
        return lax.axis_index("tm"), lax.axis_index("space")

    def start(self, source, target, send_sem, recv_sem, device):
        pltpu.make_async_remote_copy(
            src_ref=source, dst_ref=target, send_sem=send_sem, recv_sem=recv_sem,
            device_id=device, device_id_type=MESH,
        ).start()

    def local(self, source, target, sem):
        return pltpu.make_async_copy(source, target, sem)

    def bytes_of(self, ref, sem):
        return pltpu.make_async_remote_copy(
            src_ref=ref, dst_ref=ref, send_sem=sem, recv_sem=sem,
            device_id=self.place(), device_id_type=MESH,
        )

    def wait_sent(self, ref, sem):
        self.bytes_of(ref, sem).wait_send()

    def wait_got(self, ref, sem):
        self.bytes_of(ref, sem).wait_recv()


VMEM, SMEM, ANY = pltpu.VMEM, pltpu.SMEM, pl.ANY


def spec(space):
    return pl.BlockSpec(memory_space=space)


def shape(*dims):
    return jax.ShapeDtypeStruct(dims, f32)


PARAMS = pltpu.CompilerParams(vmem_limit_bytes=60 * 1024 * 1024)


def sources(velocity, step, iterate, right_side, kappa, interpret=False):
    return pl.pallas_call(
        source_kernel,
        out_shape=(shape(40, 128, 128), shape(8, 64, 128)),
        in_specs=[spec(SMEM)] * 2 + [spec(VMEM)] * 5,
        out_specs=(spec(VMEM), spec(VMEM)),
        scratch_shapes=[VMEM((2560, 256), bf16), VMEM((2560, 256), bf16)],
        compiler_params=PARAMS,
        cost_estimate=pl.CostEstimate(flops=4_000_000_000, bytes_accessed=8_000_000, transcendentals=0),
        interpret=interpret,
        name="sources",
    )(velocity, step, iterate, right_side, kappa, TABLES["ty"], TABLES["tz"])


def slab(velocity, spectra, mixed, below, above, interpret=False):
    return pl.pallas_call(
        slab_kernel,
        out_shape=(shape(32, 128, 128), shape(OWNERS * ROWS, 128)),
        in_specs=[spec(SMEM)] + [spec(VMEM)] * 8,
        out_specs=(spec(VMEM), spec(VMEM)),
        scratch_shapes=[VMEM((4, 128, 128), f32)],
        compiler_params=PARAMS,
        interpret=interpret,
        name="slab",
    )(
        velocity, spectra, mixed, below, above,
        TABLES["ty"], TABLES["tz"], TABLES["lane"], TABLES["row"],
    )


def modes(velocity, sent, remote=Remote(), interpret=False):
    return pl.pallas_call(
        functools.partial(mode_kernel, remote),
        out_shape=shape(OWNERS * ROWS, 128),
        in_specs=[spec(SMEM)] + [spec(VMEM)] * 6,
        out_specs=spec(ANY),
        scratch_shapes=[
            VMEM((STEPS * SLABS * ROWS, 128), f32), VMEM((STEPS * SLABS * ROWS, 128), f32),
            VMEM((6, 2, 128, 128), f32), VMEM((4, 128, 128), f32), VMEM((128, 128), f32),
            VMEM((STEPS, 128, 128), f32), VMEM((STEPS, 2, 128, 128), f32), VMEM((128, 384), bf16),
            pltpu.SemaphoreType.DMA, pltpu.SemaphoreType.DMA((STEPS,)),
            pltpu.SemaphoreType.DMA, pltpu.SemaphoreType.DMA, pltpu.SemaphoreType.DMA,
        ],
        compiler_params=pltpu.CompilerParams(
            vmem_limit_bytes=60 * 1024 * 1024, has_side_effects=True
        ),
        interpret=interpret,
        name="modes",
    )(velocity, TABLES["own"], TABLES["wave_x"], TABLES["tg"], TABLES["tw"], TABLES["tb"], sent)


def backward(velocity, iterate, u, got, interpret=False):
    return pl.pallas_call(
        backward_kernel,
        out_shape=shape(4, WIDE, NZ, NY),
        in_specs=[spec(SMEM)] + [spec(VMEM)] * 7,
        out_specs=spec(VMEM),
        scratch_shapes=[VMEM((32, 128, 128), f32)],
        compiler_params=PARAMS,
        interpret=interpret,
        name="backward",
    )(velocity, iterate, u, got, TABLES["uy"], TABLES["uz"], TABLES["lane"], TABLES["row"])


def shards(iterate, right_side, diffusivity, velocity):
    iterate, right_side = iterate[0], right_side[0]
    tm = lax.axis_index("tm")
    up = [(i, (i + 1) % SLABS) for i in range(SLABS)]
    down = [(i, (i - 1) % SLABS) for i in range(SLABS)]
    below = lax.ppermute(diffusivity[WIDE - 1], "space", up)
    above = lax.ppermute(diffusivity[0], "space", down)
    step = tm.astype(jnp.int32)[None]
    spectra, mixed = sources(velocity, step, iterate, right_side, diffusivity)
    u, sent = slab(velocity, spectra, mixed, below, above)
    returned = modes(velocity, sent)
    return backward(velocity, iterate, u, returned)[None]


def solution(mesh):
    placed = (
        P("tm", None, "space", None, None),
        P("tm", None, "space", None, None),
        P("space", None, None),
        P(),
    )
    return jax.shard_map(
        shards,
        mesh=mesh,
        in_specs=placed,
        out_specs=P("tm", None, "space", None, None),
        check_vma=False,
    )
```

```python
import functools
import math

import jax
import jax.numpy as jnp
import numpy as np
from jax import lax
from jax.experimental import pallas as pl
from jax.experimental.pallas import tpu as pltpu
from jax.sharding import PartitionSpec as P

NX, NY, NZ, STEPS = 128, 128, 64, 32
SLABS, WIDE = 8, 16
OWNERS = 128
ROWS = 12
MESH = pl.DeviceIdType.MESH
f32, bf16 = jnp.float32, jnp.bfloat16

diffusion_number = 16.0
circulant_alpha = 0.1


def collocation_matrix():
    radau_nodes = [0.08858795951270394, 0.4094668644407347, 0.7876594617608471, 1.0]
    matrix = [[0.0] * 4 for row_index in range(4)]
    for column_index in range(4):
        coefficients = [1.0]
        for other_index in range(4):
            if other_index != column_index:
                scale_value = 1.0 / (radau_nodes[column_index] - radau_nodes[other_index])
                shifted = [0.0] + [value * scale_value for value in coefficients]
                lowered = [
                    -radau_nodes[other_index] * scale_value * value for value in coefficients
                ] + [0.0]
                coefficients = [
                    left_value + right_value for left_value, right_value in zip(shifted, lowered)
                ]
        for row_index in range(4):
            total = 0.0
            for power_index in range(len(coefficients)):
                total = total + coefficients[power_index] * radau_nodes[row_index] ** (
                    power_index + 1
                ) / (power_index + 1)
            matrix[row_index][column_index] = total
    return matrix


def solve_system(matrix, target):
    count = len(target)
    rows_list = [list(matrix[row_index]) + [target[row_index]] for row_index in range(count)]
    for column in range(count):
        best_row = column
        for candidate in range(column + 1, count):
            if abs(rows_list[candidate][column]) > abs(rows_list[best_row][column]):
                best_row = candidate
        saved_row = rows_list[column]
        rows_list[column] = rows_list[best_row]
        rows_list[best_row] = saved_row
        leader = rows_list[column][column]
        for other_row in range(count):
            if other_row != column:
                factor = rows_list[other_row][column] / leader
                rows_list[other_row] = [
                    left_value - factor * right_value
                    for left_value, right_value in zip(rows_list[other_row], rows_list[column])
                ]
    return [
        rows_list[row_index][count] / rows_list[row_index][row_index] for row_index in range(count)
    ]


def node_basis():
    matrix = collocation_matrix()
    helper = [[0.0] * 4 for row_index in range(4)]
    coefficients = [0.0, 0.0, 0.0, 0.0, 1.0]
    for order in range(1, 5):
        product = [
            [
                sum((matrix[row_index][inner] * helper[inner][column] for inner in range(4)))
                for column in range(4)
            ]
            for row_index in range(4)
        ]
        for row_index in range(4):
            product[row_index][row_index] = product[row_index][row_index] + coefficients[5 - order]
        helper = product
        trace_value = sum(
            (
                sum((matrix[row_index][inner] * helper[inner][row_index] for inner in range(4)))
                for row_index in range(4)
            )
        )
        coefficients[4 - order] = -trace_value / order
    roots_list = [(0.4 + 0.9j) ** power_index for power_index in range(4)]
    for sweep in range(400):
        for root_index in range(4):
            current = roots_list[root_index]
            numer = 0.0
            for power_index in range(4, -1, -1):
                numer = numer * current + coefficients[power_index]
            denom = 1.0
            for other_index in range(4):
                if other_index != root_index:
                    denom = denom * (current - roots_list[other_index])
            roots_list[root_index] = current - numer / denom
    vectors = [[0.0] * 4 for row_index in range(4)]
    for root_index in range(4):
        shifted = [
            [
                matrix[row_index][column] - (roots_list[root_index] if row_index == column else 0.0)
                for column in range(3)
            ]
            for row_index in range(3)
        ]
        target = [-matrix[row_index][3] for row_index in range(3)]
        parts = solve_system(shifted, target) + [1.0 + 0j]
        for row_index in range(4):
            vectors[row_index][root_index] = parts[row_index]
    inverse = [[0.0] * 4 for row_index in range(4)]
    for column in range(4):
        unit = [1.0 if row_index == column else 0.0 for row_index in range(4)]
        parts = solve_system(vectors, unit)
        for row_index in range(4):
            inverse[row_index][column] = parts[row_index]
    weights = [sum((inverse[row_index][column] for column in range(4))) for row_index in range(4)]
    return (roots_list, vectors, inverse, weights)


VALUES, VECTORS, INVERSE, WEIGHTS = node_basis()
PAIRS = [m for m in range(4) if complex(VALUES[m]).imag > 0]
MU = [complex(VALUES[m]) for m in PAIRS]
COLUMN = [[complex(VECTORS[n][m]) for n in range(4)] for m in PAIRS]
ROW = [[complex(INVERSE[m][n]) for n in range(4)] for m in PAIRS]
EPS = [complex(WEIGHTS[m]) for m in PAIRS]


def wave_order_z():
    index = np.arange(NZ)
    return np.where(index <= NZ // 2, index, NZ + NZ // 2 - index)


def wave_order_y():
    lane = np.arange(NY)
    index = 16 * (lane // 32) + lane % 16
    return np.where(lane % 32 < 16, index, np.where(index == 0, NY // 2, NY - index))


def split(values):
    values = np.asarray(values, np.float64)
    high = values.astype(np.float32).astype(bf16)
    low = (values - high.astype(np.float64)).astype(np.float32).astype(bf16)
    return high, low


def side_table(values):
    high, low = split(values)
    return np.concatenate([high, high, low], axis=1)


def halves(x):
    high = x.astype(bf16)
    return high, (x - high.astype(f32)).astype(bf16)


def left_dot(table, x):
    high, low = halves(x)
    return jnp.dot(table, jnp.concatenate([high, low, high], axis=0), preferred_element_type=f32)


def right_dot(high, low, table_high, table_low):
    return (
        jnp.dot(high, table_high, preferred_element_type=f32)
        + jnp.dot(low, table_high, preferred_element_type=f32)
        + jnp.dot(high, table_low, preferred_element_type=f32)
    )


def complex_block(matrix):
    return np.block([[matrix.real, -matrix.imag], [matrix.imag, matrix.real]])


def make_tables():
    ky, kz = wave_order_y(), wave_order_z()
    kx, x = np.arange(NX), np.arange(NX)
    to_y = np.exp(-2j * np.pi * np.outer(ky, np.arange(NY)) / NY)
    to_z = np.exp(-2j * np.pi * np.outer(kz, np.arange(NZ)) / NZ)
    tables = {}
    tables["ty"] = np.stack(split(complex_block(to_y).T))
    tables["tz"] = side_table(complex_block(to_z))
    tables["uy"] = np.stack(split(complex_block(np.conj(to_y.T) / NY).T))
    tables["uz"] = side_table(complex_block(np.conj(to_z.T) / NZ))
    cells = (np.arange(SLABS)[:, None] * WIDE + np.arange(8)[None, :]).reshape(-1)
    theta = 2 * np.pi * kx / NX
    at = np.exp(-1j * np.outer(theta, cells))
    shifted = np.exp(-8j * theta)[:, None]
    from_own = at * (1 - 1j * shifted) / 2
    from_partner = at * (1 + 1j * shifted) / 2
    firsts = np.arange(SLABS) * WIDE

    def lane_block(matrix):
        return np.concatenate([matrix.real, -matrix.imag], axis=1)

    tables["tg"] = side_table(np.concatenate([lane_block(from_own), lane_block(from_partner)], axis=1))

    def point_rows(waves, shifts):
        out = []
        for m in range(2):
            table = np.zeros((len(waves), 4, SLABS), complex)
            for field, shift in shifts:
                table[:, 2 * m + field] = np.exp(-1j * np.outer(waves, firsts + shift))
            out.append(table.reshape(len(waves), 4 * SLABS))
        return out

    tables["td"] = side_table(
        lane_block(
            np.concatenate(
                point_rows(theta, ((0, WIDE), (1, -1))) + point_rows(theta[:8], ((1, 0),)), axis=0
            )
        )
    )
    back = np.exp(1j * np.outer(cells, theta)) * (1 + 1j * np.exp(8j * theta))[None, :] / NX
    tables["tw"] = side_table(lane_block(back))
    ends = [np.exp(1j * np.outer(firsts + k, theta)) / NX for k in (0, 1, 15)]
    tables["tb"] = side_table(lane_block(np.concatenate(ends, axis=0)))
    trig_y = 2 * np.pi * ky / NY
    trig_z = 2 * np.pi * kz / NZ
    tables["lane"] = np.stack([np.cos(trig_y), np.sin(trig_y)]).astype(np.float32)
    tables["row"] = np.stack(
        [np.broadcast_to(v[:, None], (NZ, NY)) for v in (np.cos(trig_z), np.sin(trig_z))]
    ).astype(np.float32)
    tables["wave_x"] = np.stack(
        [np.broadcast_to(v[:, None], (NX, 128)) for v in (np.cos(theta), np.sin(theta))]
    ).astype(np.float32)
    lane = np.arange(128)
    own = np.zeros((OWNERS, 8, 128))
    for owner in range(OWNERS):
        part, pair = owner // 32, owner % 32
        piece = (lane // 32 - part) % 4
        at_y, row = (lane - 32 * piece) % 128, piece % 2
        other_y = np.where((at_y == 0) | (at_y == 16), at_y, at_y ^ 16)
        other_row = row if pair == 0 else 1 - row
        other = (other_y + 32 * (2 * (piece // 2) + other_row)) % 128
        y, z = trig_y[at_y], trig_z[pair + 32 * row]
        own[owner] = np.stack(
            [
                np.cos(y), np.sin(y), np.cos(z), np.sin(z),
                other, np.roll(other, -64), np.where(piece < 2, 1.0, -1.0), (lane + 64) % 128,
            ]
        )
    tables["own"] = own.astype(np.float32)
    return tables


TABLES = make_tables()


def times(a, b):
    return (a[0] * b[0] - a[1] * b[1], a[0] * b[1] + a[1] * b[0])


def plus(a, b):
    return (a[0] + b[0], a[1] + b[1])


def minus(a, b):
    return (a[0] - b[0], a[1] - b[1])


def scaled(number, a):
    return (number.real * a[0] - number.imag * a[1], number.real * a[1] + number.imag * a[0])


def inverse_of(a):
    size = 1.0 / (a[0] * a[0] + a[1] * a[1])
    return (a[0] * size, -a[1] * size)


def root_of(a):
    size = jnp.sqrt(a[0] * a[0] + a[1] * a[1])
    main = jnp.sqrt(0.5 * (size + jnp.abs(a[0])))
    other = a[1] / (2.0 * main)
    positive = a[0] >= 0.0
    return (
        jnp.where(positive, main, jnp.abs(other)),
        jnp.where(positive, other, jnp.where(a[1] >= 0.0, main, -main)),
    )


def cross_symbol(cos_y, sin_y, cos_z, sin_z, v1, v2):
    return (
        diffusion_number * ((2.0 * cos_y - 2.0) + (2.0 * cos_z - 2.0)),
        -(v1 * sin_y + v2 * sin_z),
    )


def factors(mu, cross, v0):
    c_up = -mu.real * (diffusion_number - 0.5 * v0), -mu.imag * (diffusion_number - 0.5 * v0)
    c_down = -mu.real * (diffusion_number + 0.5 * v0), -mu.imag * (diffusion_number + 0.5 * v0)
    moved = scaled(mu, cross)
    c_mid = (1.0 + 2.0 * diffusion_number * mu.real - moved[0], 2.0 * diffusion_number * mu.imag - moved[1])
    product = times(c_up, c_down)
    square = times(c_mid, c_mid)
    root = root_of((square[0] - 4.0 * product[0], square[1] - 4.0 * product[1]))
    same = c_mid[0] * root[0] + c_mid[1] * root[1] >= 0.0
    kappa = (
        0.5 * (c_mid[0] + jnp.where(same, root[0], -root[0])),
        0.5 * (c_mid[1] + jnp.where(same, root[1], -root[1])),
    )
    inv = inverse_of(kappa)
    p = times(inv, c_down)
    q = times(inv, c_up)
    return (-p[0], -p[1]), (-q[0], -q[1]), kappa, inv


def plane_partner(low, high, lane, first_row):
    ends = (lane == 0) | (lane == 16)
    first = (lane % 32) < 16

    def turned(v):
        return jnp.where(ends, v, jnp.where(first, pltpu.roll(v, 112, 1), pltpu.roll(v, 16, 1)))

    low_turned, high_turned = [turned(v) for v in low], [turned(v) for v in high]
    to_low = [jnp.where(first_row, a, b) for a, b in zip(low_turned, high_turned)]
    to_high = [jnp.where(first_row, b, a) for a, b in zip(low_turned, high_turned)]
    return (to_low[0], -to_low[1]), (to_high[0], -to_high[1])


def packed_for(low, high, block):
    pieces = [low[0], high[0], low[1], high[1]]
    pieces = [pieces[0]] + [pltpu.roll(pieces[c], 32 * c, 1) for c in (1, 2, 3)]
    out = []
    for h in range(4):
        value = pieces[3]
        for c in (2, 1, 0):
            value = jnp.where(block == (h + c) % 4, pieces[c], value)
        out.append(value)
    return out


def unpacked_from(values, block):
    out = []
    for c in range(4):
        piece = values[(3 - c) % 4]
        for d in (2, 1, 0):
            piece = jnp.where(block == d, values[(d - c) % 4], piece)
        out.append(piece if c == 0 else pltpu.roll(piece, 128 - 32 * c, 1))
    return (out[0], out[2]), (out[1], out[3])


def chunk_factors(t, lane_ref, row_ref, velocity_ref, mu):
    cos_y, sin_y = lane_ref[0:1, :], lane_ref[1:2, :]
    found = []
    for base in (0, 32):
        rows = pl.ds(pl.multiple_of(base + 8 * t, 8), 8)
        cross = cross_symbol(
            cos_y, sin_y, row_ref[0, rows, :], row_ref[1, rows, :], velocity_ref[1], velocity_ref[2]
        )
        found.append([factors(number, cross, velocity_ref[0]) for number in mu])
    return found


def dft_block(high, low, ty_ref, tz_ref):
    mid = right_dot(high, low, ty_ref[0], ty_ref[1])
    stacked = jnp.concatenate(
        [
            jnp.concatenate([mid[64 * k : 64 * k + 64, :128], mid[64 * k : 64 * k + 64, 128:]], axis=0)
            for k in range(4)
        ],
        axis=1,
    )
    return left_dot(tz_ref[...], stacked)


def source_kernel(
    velocity_ref, step_ref, iterate_ref, right_ref, kappa_ref, ty_ref, tz_ref,
    spec_ref, mixed_ref,
    high_ref, low_ref,
):
    v0, v1, v2 = velocity_ref[0], velocity_ref[1], velocity_ref[2]

    def put(at, real, imag):
        rows = pl.ds(pl.multiple_of(at * 64, 64), 64)
        for k, part in enumerate((real, imag)):
            high, low = halves(part)
            high_ref[rows, k * 128 : (k + 1) * 128] = high
            low_ref[rows, k * 128 : (k + 1) * 128] = low

    def mixture(m, groups):
        real = imag = None
        for scale, values in groups:
            for n in range(4):
                factor = scale * ROW[m][n]
                a, b = factor.real * values[n], factor.imag * values[n]
                real = a if real is None else real + a
                imag = b if imag is None else imag + b
        return real, imag

    def inner(x, below, above):
        plain, applied = [], []
        kappa = kappa_ref[x]
        for n in range(4):
            f = iterate_ref[n, x]
            up_z, down_z = pltpu.roll(f, NZ - 1, 0), pltpu.roll(f, 1, 0)
            up_y, down_y = pltpu.roll(f, NY - 1, 1), pltpu.roll(f, 1, 1)
            total = (up_z + down_z) + (up_y + down_y) - 6.0 * f
            moved = v1 * (up_y - down_y) + v2 * (up_z - down_z)
            if above:
                up_x = iterate_ref[n, x + 1]
                total, moved = total + up_x, moved + v0 * up_x
            if below:
                down_x = iterate_ref[n, x - 1]
                total, moved = total + down_x, moved - v0 * down_x
            applied.append((diffusion_number * kappa) * total - 0.5 * moved)
            plain.append(right_ref[n, x] - f)
        for m in range(2):
            real, imag = mixture(m, [(1.0, plain), (MU[m], applied)])
            put(m * 16 + x, real, imag)

    for side, x in enumerate((0, WIDE - 1)):
        for m in range(2):
            real, imag = mixture(m, [(MU[m], [iterate_ref[n, x] for n in range(4)])])
            mixed_ref[side * 4 + m * 2] = real
            mixed_ref[side * 4 + m * 2 + 1] = imag
    inner(0, False, True)
    inner(WIDE - 1, True, False)

    @pl.loop(1, WIDE - 1)
    def _(x):
        inner(x, True, True)

    keep = jnp.where(step_ref[0] < STEPS - 1, 1.0, 0.0).astype(f32)

    @pl.loop(0, 8)
    def _(x):
        put(32 + x, keep * iterate_ref[3, x], keep * iterate_ref[3, x + 8])

    @pl.loop(0, 10)
    def _(block):
        rows = pl.ds(pl.multiple_of(block * 256, 256), 256)
        out = dft_block(high_ref[rows, :], low_ref[rows, :], ty_ref, tz_ref)
        for k in range(4):
            spec_ref[block * 4 + k] = out[:, 128 * k : 128 * k + 128]


def slab_kernel(
    velocity_ref, spec_ref, mixed_ref, below_ref, above_ref, ty_ref, tz_ref, lane_ref, row_ref,
    u_ref, send_ref,
    edge_ref,
):
    v0 = velocity_ref[0]
    outer = [diffusion_number * below_ref[...] - 0.5 * v0, diffusion_number * above_ref[...] + 0.5 * v0]
    edges = [
        jnp.concatenate([outer[side] * mixed_ref[side * 4 + m * 2 + part] for part in range(2)], axis=1)
        for m in range(2)
        for side in range(2)
    ]
    high, low = halves(jnp.concatenate(edges, axis=0))
    out = dft_block(high, low, ty_ref, tz_ref)
    for k in range(4):
        edge_ref[k] = out[:, 128 * k : 128 * k + 128]

    lane = lax.broadcasted_iota(jnp.int32, (8, 128), 1)
    sub = lax.broadcasted_iota(jnp.int32, (8, 128), 0)
    block = lane // 32

    @pl.loop(0, 4)
    def _(t):
        first_row = (sub + t) == 0
        found = chunk_factors(t, lane_ref, row_ref, velocity_ref, MU)
        bases = [pl.multiple_of(base + 8 * t, 8) for base in (0, 32)]

        def plane(at, base, ref=spec_ref):
            return ref[at, pl.ds(base, 8), :], ref[at, pl.ds(base + 64, 8), :]

        def send(value, low, high):
            for h, packed in enumerate(packed_for(low, high, block)):
                send_ref[pl.ds((32 * h + 8 * t) * ROWS + value, 8, stride=ROWS), :] = packed

        sums = [[None, None] for x in range(WIDE)]
        for m in range(2):
            carries = []
            for half in range(2):
                base = bases[half]
                p, q, kappa, inv = found[half][m]
                under, over = plane(m * 2, base, edge_ref), plane(m * 2 + 1, base, edge_ref)
                u = plus(plane(m * 16, base), times(p, under))
                us = [u]
                for x in range(1, WIDE):
                    u = plus(plane(m * 16 + x, base), times(p, u))
                    us.append(u)
                for x in range(WIDE):
                    u_ref[m * 16 + x, pl.ds(base, 8), :] = us[x][0]
                    u_ref[m * 16 + x, pl.ds(base + 64, 8), :] = us[x][1]
                outflow = plus(times(p, us[-1]), over)
                y = us[-1]
                for x in range(WIDE - 1, -1, -1):
                    if x < WIDE - 1:
                        y = plus(us[x], times(q, y))
                    z = times(inv, y)
                    sums[x][half] = z if m == 0 else plus(sums[x][half], z)
                carries.append((outflow, plus(times(q, y), under)))
            for k in range(2):
                send(8 + m * 2 + k, carries[0][k], carries[1][k])
        for x in range(8):
            own, other = [], []
            for half in range(2):
                first, second = sums[x][half], sums[x + 8][half]
                own.append((first[0] - second[1], first[1] + second[0]))
                other.append((first[0] + second[1], first[1] - second[0]))
            partners = plane_partner(other[0], other[1], lane, first_row)
            packed = [
                plus(plus(own[half], partners[half]), plane(32 + x, bases[half])) for half in range(2)
            ]
            send(x, packed[0], packed[1])


def backward_kernel(
    velocity_ref, iterate_ref, u_ref, got_ref, uy_ref, uz_ref, lane_ref, row_ref,
    out_ref,
    spec_ref,
):
    lane = lax.broadcasted_iota(jnp.int32, (8, 128), 1)
    sub = lax.broadcasted_iota(jnp.int32, (8, 128), 0)
    block = lane // 32

    @pl.loop(0, 4)
    def _(t):
        first_row = (sub + t) == 0
        found = chunk_factors(t, lane_ref, row_ref, velocity_ref, MU)
        bases = [pl.multiple_of(base + 8 * t, 8) for base in (0, 32)]

        def take(value):
            values = [
                got_ref[pl.ds((32 * h + 8 * t) * ROWS + value, 8, stride=ROWS), :] for h in range(4)
            ]
            return unpacked_from(values, block)

        last = [[None, None] for x in range(WIDE)]
        for x in range(8):
            packed = take(x)
            partners = plane_partner(packed[0], packed[1], lane, first_row)
            for half in range(2):
                both, apart = plus(packed[half], partners[half]), minus(packed[half], partners[half])
                last[x][half] = (0.5 * both[0], 0.5 * both[1])
                last[x + 8][half] = (0.5 * apart[1], -0.5 * apart[0])
        for m in range(2):
            start, end = take(8 + m * 2), take(9 + m * 2)
            for half in range(2):
                base = bases[half]
                p, q, kappa, inv = found[half][m]

                def old(x):
                    return (
                        u_ref[m * 16 + x, pl.ds(base, 8), :],
                        u_ref[m * 16 + x, pl.ds(base + 64, 8), :],
                    )

                u = start[half]
                totals = [plus(u, old(0))]
                for x in range(1, WIDE - 1):
                    u = plus(scaled(EPS[m], last[x][half]), times(p, u))
                    totals.append(plus(u, old(x)))
                y = plus(times(inv, old(WIDE - 1)), end[half])
                for x in range(WIDE - 1, -1, -1):
                    if x < WIDE - 1:
                        y = plus(times(inv, totals[x]), times(q, y))
                    spec_ref[m * 16 + x, pl.ds(base, 8), :] = y[0]
                    spec_ref[m * 16 + x, pl.ds(base + 64, 8), :] = y[1]

    @pl.loop(0, 8)
    def _(block):
        planes = [2 * block, 2 * block + 1, 16 + 2 * block, 17 + 2 * block]
        stacked = jnp.concatenate([spec_ref[at] for at in planes], axis=1)
        mid = left_dot(uz_ref[...], stacked)
        rows = jnp.concatenate(
            [
                jnp.concatenate([mid[:64, 128 * k : 128 * k + 128], mid[64:, 128 * k : 128 * k + 128]], axis=1)
                for k in range(4)
            ],
            axis=0,
        )
        high, low = halves(rows)
        out = right_dot(high, low, uy_ref[0], uy_ref[1])
        for k in range(2):
            x = 2 * block + k
            parts = []
            for m in range(2):
                piece = out[(2 * m + k) * 64 : (2 * m + k) * 64 + 64]
                parts.append((piece[:, :128], piece[:, 128:]))
            for n in range(4):
                total = iterate_ref[n, x]
                for m in range(2):
                    c = COLUMN[m][n]
                    total = total + (2.0 * c.real) * parts[m][0] - (2.0 * c.imag) * parts[m][1]
                out_ref[n, x] = total


def mode_kernel(
    remote, velocity_ref, own_ref, wave_ref, tg_ref, td_ref, tw_ref, tb_ref, sent_ref,
    returned_ref,
    got_ref, back_ref, damp_ref, ratio_ref, last_ref, drive_ref, kept_ref, turn_ref,
    gather_sem, arrive_sem, swap_out_sem, swap_in_sem, scatter_sem, return_sem, own_sem,
):
    tm, space = remote.place()
    core = tm % 2
    owner = (tm // 2) * SLABS + space

    def rows_of(index, number=1):
        return pl.ds(pl.multiple_of(index * ROWS, 4), number * ROWS)

    @pl.loop(1, OWNERS)
    def _(k):
        pair = (tm // 2 + STEPS // 2 - k // SLABS) % (STEPS // 2)
        to_space = ((space // 2 + (k % SLABS) // 2) % (SLABS // 2)) * 2 + (space + k) % 2
        remote.start(
            sent_ref.at[rows_of(pair * SLABS + to_space), :],
            got_ref.at[rows_of((tm // 2) * SLABS + space), :],
            gather_sem, arrive_sem.at[tm // 2], (2 * pair + core, to_space),
        )

    got_ref[rows_of(owner), :] = sent_ref[rows_of(owner), :]
    solve_modes(
        remote, 2, owner, tm, space, rows_of,
        velocity_ref, own_ref, wave_ref, tg_ref, td_ref, tw_ref, tb_ref, returned_ref,
        got_ref, back_ref, damp_ref, ratio_ref, last_ref, drive_ref, kept_ref, turn_ref,
        arrive_sem, swap_out_sem, swap_in_sem, scatter_sem, return_sem, own_sem,
    )
    remote.wait_sent(sent_ref.at[rows_of(0, OWNERS - 1), :], gather_sem)
    remote.wait_sent(back_ref.at[rows_of(0, OWNERS - 1), :], scatter_sem)
    remote.local(back_ref.at[rows_of(owner), :], returned_ref.at[rows_of(owner), :], own_sem).wait()
    remote.wait_got(returned_ref.at[rows_of(0, OWNERS - 1), :], return_sem)


GROUP = 4


def solve_modes(
    remote, share, owner, tm, space, rows_of,
    velocity_ref, own_ref, wave_ref, tg_ref, td_ref, tw_ref, tb_ref, returned_ref,
    got_ref, back_ref, damp_ref, ratio_ref, last_ref, drive_ref, kept_ref, turn_ref,
    arrive_sem, swap_out_sem, swap_in_sem, scatter_sem, return_sem, own_sem,
):
    rounds = STEPS // share // GROUP
    core = tm % share
    v0, v1, v2 = velocity_ref[0], velocity_ref[1], velocity_ref[2]
    own = own_ref[owner]
    line = [own[k : k + 1, :] for k in range(8)]
    wide = [jnp.broadcast_to(v, (8, 128)) for v in line]
    sign = wide[6]
    cross = cross_symbol(wide[0], wide[1], wide[2], wide[3], v1, v2)
    mu = [MU[0], MU[1], MU[0].conjugate(), MU[1].conjugate()]
    eps = [EPS[0], EPS[1], EPS[0].conjugate(), EPS[1].conjugate()]
    found = [factors(number, cross, v0) for number in mu]

    def crossed(a):
        return (a[0], -(sign * a[1]))

    def times_lanes(v, table):
        return v * table[0] + pltpu.roll(v, 64, 1) * table[1]

    def repeated(v, count):
        return jnp.concatenate([v] * count, axis=0)

    row = lax.broadcasted_iota(jnp.int32, (128, 128), 0).astype(f32)
    turn_ref[:, 0:128] = jnp.where(row == line[4], line[6], 0.0).astype(bf16)
    turn_ref[:, 128:256] = jnp.where(row == line[5], -1.0, 0.0).astype(bf16)

    @pl.loop(0, 16)
    def _(at):
        rows = pl.ds(pl.multiple_of(at * 8, 8), 8)
        symbol = (
            diffusion_number * (2.0 * wave_ref[0, rows, :] - 2.0) + cross[0],
            cross[1] - v0 * wave_ref[1, rows, :],
        )
        total = None
        for m in range(4):
            moved = scaled(mu[m], symbol)
            damp = inverse_of((1.0 - moved[0], -moved[1]))
            for k, value in enumerate(crossed(damp)):
                damp_ref[m, k, rows, :] = value
            term = scaled(eps[m], damp)
            if m < 2:
                for k, value in enumerate(crossed(term)):
                    damp_ref[4 + m, k, rows, :] = value
            total = term if total is None else plus(total, term)
        for k, value in enumerate(crossed(total)):
            ratio_ref[k, rows, :] = value
        power = total
        for k in range(5):
            power = times(power, power)
        closing = inverse_of((1.0 - circulant_alpha * power[0], -circulant_alpha * power[1]))
        for k, value in enumerate(crossed(closing)):
            ratio_ref[2 + k, rows, :] = value

    first_step = tm - tm % 2
    roots = [crossed(found[m][0]) for m in range(4)]
    flip = repeated(sign, 12)

    def step_of(i):
        return (first_step + share * i + core) % STEPS

    def swap(i):
        remote.start(
            drive_ref.at[step_of(i)], drive_ref.at[step_of(i)],
            swap_out_sem, swap_in_sem, (tm + 1 - 2 * core, space),
        )

    @pl.loop(0, rounds)
    def _(round_at):
        values, crossings = [], []
        for k in range(GROUP):
            s = step_of(round_at * GROUP + k)
            slot = s // share
            top = slot * (SLABS * ROWS)

            @pl.when(s == tm)
            def _():
                remote.wait_got(got_ref.at[rows_of(0, SLABS - 1), :], arrive_sem.at[slot])

            @pl.when(s != tm)
            def _():
                remote.wait_got(got_ref.at[rows_of(0, SLABS), :], arrive_sem.at[slot])

            pieces = [got_ref[pl.ds(top + x * ROWS, 8), :] for x in range(SLABS)]
            pieces += [got_ref[pl.ds(top + 8 + f, SLABS, stride=ROWS), :] for f in range(4)]
            v = jnp.concatenate(pieces, axis=0)
            values.append(halves(v))
            crossings.append(halves(flip * pltpu.roll(v, 64, 1)))
        stacked = jnp.concatenate([half for pair in values for half in pair], axis=0)
        turned = jnp.dot(stacked, turn_ref[...], preferred_element_type=f32).astype(bf16)
        columns, own_points, other_points = [], [], []
        for k in range(GROUP):
            parts = []
            for half in range(2):
                rows = slice(96 * (2 * k + half), 96 * (2 * k + half) + 96)
                parts.append((values[k][half], crossings[k][half], turned[rows, :128], turned[rows, 128:]))
            order = (parts[0], parts[1], parts[0])
            columns.append(jnp.concatenate([piece[:64] for part in order for piece in part], axis=0))
            own_points.append(jnp.concatenate([piece[64:] for part in order for piece in part[:2]], axis=0))
            other_points.append(jnp.concatenate([piece[64:] for part in order for piece in part[2:]], axis=0))
        drive = jnp.dot(tg_ref[...], jnp.concatenate(columns, axis=1), preferred_element_type=f32)
        points = jnp.dot(
            td_ref[...], jnp.concatenate(own_points + other_points, axis=1), preferred_element_type=f32
        )
        for k in range(GROUP):
            s = step_of(round_at * GROUP + k)
            total = drive[:, 128 * k : 128 * k + 128]
            for m in range(4):
                at = 128 * (k + GROUP * (m // 2))
                j = m % 2
                point = times_lanes(points[256 + 8 * j : 264 + 8 * j, at : at + 128], roots[m])
                d = points[128 * j : 128 * j + 128, at : at + 128] - repeated(point, 16)
                y = times_lanes(d, (damp_ref[m, 0], damp_ref[m, 1]))
                if m < 2:
                    kept_ref[s // share, m] = y
                total = total + y
            drive_ref[s] = total
        if share > 1:
            @pl.when(round_at > 0)
            def _():
                for k in range(GROUP):
                    swap((round_at - 1) * GROUP + k)

    if share > 1:
        for k in range(GROUP):
            swap((rounds - 1) * GROUP + k)
        remote.wait_got(drive_ref.at[pl.ds(0, STEPS // 2)], swap_in_sem)

    def wrapped(s, v):
        return jnp.where(s == 0, circulant_alpha, 1.0).astype(f32) * v

    def following(s, v):
        return drive_ref[s] + times_lanes(v, (ratio_ref[0], ratio_ref[1]))

    last_ref[...] = jnp.zeros((128, 128), f32)

    @pl.loop(0, STEPS)
    def _(i):
        s = (first_step + i) % STEPS
        last_ref[...] = following(s, wrapped(s, last_ref[...]))

    last_ref[...] = times_lanes(last_ref[...], (ratio_ref[2], ratio_ref[3]))
    kappas = [crossed(found[m][2]) for m in range(2)]
    ups = [crossed(found[m][1]) for m in range(2)]
    flip_all = repeated(sign, 16)

    def both_parts(v):
        return jnp.concatenate([v, flip_all * pltpu.roll(v, 64, 1)], axis=0)

    def send(i):
        s = step_of(i)
        for x in range(SLABS):
            index = (s // share) * SLABS + x

            @pl.when((s != tm) | (space != x))
            def _():
                remote.start(
                    back_ref.at[rows_of(index), :], returned_ref.at[rows_of(owner), :],
                    scatter_sem, return_sem, (s, x),
                )

            @pl.when((s == tm) & (space == x))
            def _():
                remote.local(
                    back_ref.at[rows_of(owner), :], returned_ref.at[rows_of(owner), :], own_sem
                ).start()

    @pl.loop(0, rounds)
    def _(round_at):
        inputs = []
        last = last_ref[...]
        for k in range(GROUP):
            mine = None
            for c in range(share):
                s = (first_step + share * (round_at * GROUP + k) + c) % STEPS
                last = wrapped(s, last)
                mine = last if mine is None else jnp.where(core == c, last, mine)
                last = following(s, last)
            inputs.append(mine)
        last_ref[...] = last
        packed = left_dot(tw_ref[...], jnp.concatenate([both_parts(v) for v in inputs], axis=1))
        lines = []
        for k in range(GROUP):
            slot = step_of(round_at * GROUP + k) // share
            for m in range(2):
                y = times_lanes(inputs[k], (damp_ref[4 + m, 0], damp_ref[4 + m, 1])) + kept_ref[slot, m]
                lines.append(both_parts(y))
        ends = left_dot(tb_ref[...], jnp.concatenate(lines, axis=1))
        for k in range(GROUP):
            top = (step_of(round_at * GROUP + k) // share) * (SLABS * ROWS)
            for x in range(SLABS):
                back_ref[pl.ds(top + x * ROWS, 8), :] = packed[8 * x : 8 * x + 8, 128 * k : 128 * k + 128]
            for m in range(2):
                at = 128 * (2 * k + m)
                part = [ends[8 * j : 8 * j + 8, at : at + 128] for j in range(3)]
                u = times_lanes(part[0] - times_lanes(part[1], ups[m]), kappas[m])
                back_ref[pl.ds(top + 8 + m * 2, SLABS, stride=ROWS), :] = u
                back_ref[pl.ds(top + 9 + m * 2, SLABS, stride=ROWS), :] = part[2]

        @pl.when(round_at > 0)
        def _():
            @pl.loop(0, GROUP)
            def _(k):
                send((round_at - 1) * GROUP + k)

    @pl.loop(0, GROUP)
    def _(k):
        send((rounds - 1) * GROUP + k)

    if share > 1:
        remote.wait_sent(drive_ref.at[pl.ds(0, STEPS // 2)], swap_out_sem)


class Remote:
    def place(self):
        return lax.axis_index("tm"), lax.axis_index("space")

    def start(self, source, target, send_sem, recv_sem, device):
        pltpu.make_async_remote_copy(
            src_ref=source, dst_ref=target, send_sem=send_sem, recv_sem=recv_sem,
            device_id=device, device_id_type=MESH,
        ).start()

    def local(self, source, target, sem):
        return pltpu.make_async_copy(source, target, sem)

    def bytes_of(self, ref, sem):
        return pltpu.make_async_remote_copy(
            src_ref=ref, dst_ref=ref, send_sem=sem, recv_sem=sem,
            device_id=self.place(), device_id_type=MESH,
        )

    def wait_sent(self, ref, sem):
        self.bytes_of(ref, sem).wait_send()

    def wait_got(self, ref, sem):
        self.bytes_of(ref, sem).wait_recv()


VMEM, SMEM, ANY = pltpu.VMEM, pltpu.SMEM, pl.ANY


def spec(space):
    return pl.BlockSpec(memory_space=space)


def shape(*dims):
    return jax.ShapeDtypeStruct(dims, f32)


PARAMS = pltpu.CompilerParams(vmem_limit_bytes=60 * 1024 * 1024)


def sources(velocity, step, iterate, right_side, kappa, interpret=False):
    return pl.pallas_call(
        source_kernel,
        out_shape=(shape(40, 128, 128), shape(8, 64, 128)),
        in_specs=[spec(SMEM)] * 2 + [spec(VMEM)] * 5,
        out_specs=(spec(VMEM), spec(VMEM)),
        scratch_shapes=[VMEM((2560, 256), bf16), VMEM((2560, 256), bf16)],
        compiler_params=PARAMS,
        cost_estimate=pl.CostEstimate(flops=4_000_000_000, bytes_accessed=8_000_000, transcendentals=0),
        interpret=interpret,
        name="sources",
    )(velocity, step, iterate, right_side, kappa, TABLES["ty"], TABLES["tz"])


def slab(velocity, spectra, mixed, below, above, interpret=False):
    return pl.pallas_call(
        slab_kernel,
        out_shape=(shape(32, 128, 128), shape(OWNERS * ROWS, 128)),
        in_specs=[spec(SMEM)] + [spec(VMEM)] * 8,
        out_specs=(spec(VMEM), spec(VMEM)),
        scratch_shapes=[VMEM((4, 128, 128), f32)],
        compiler_params=PARAMS,
        interpret=interpret,
        name="slab",
    )(
        velocity, spectra, mixed, below, above,
        TABLES["ty"], TABLES["tz"], TABLES["lane"], TABLES["row"],
    )


def modes(velocity, sent, remote=Remote(), interpret=False):
    return pl.pallas_call(
        functools.partial(mode_kernel, remote),
        out_shape=shape(OWNERS * ROWS, 128),
        in_specs=[spec(SMEM)] + [spec(VMEM)] * 7,
        out_specs=spec(ANY),
        scratch_shapes=[
            VMEM((OWNERS * ROWS, 128), f32), VMEM((OWNERS * ROWS, 128), f32),
            VMEM((6, 2, 128, 128), f32), VMEM((4, 128, 128), f32), VMEM((128, 128), f32),
            VMEM((STEPS, 128, 128), f32), VMEM((STEPS // 2, 2, 128, 128), f32), VMEM((128, 256), bf16),
            pltpu.SemaphoreType.DMA, pltpu.SemaphoreType.DMA((STEPS // 2,)),
        ] + [pltpu.SemaphoreType.DMA] * 5,
        compiler_params=pltpu.CompilerParams(
            vmem_limit_bytes=60 * 1024 * 1024, has_side_effects=True
        ),
        interpret=interpret,
        name="modes",
    )(velocity, TABLES["own"], TABLES["wave_x"], TABLES["tg"], TABLES["td"], TABLES["tw"], TABLES["tb"], sent)


def backward(velocity, iterate, u, got, interpret=False):
    return pl.pallas_call(
        backward_kernel,
        out_shape=shape(4, WIDE, NZ, NY),
        in_specs=[spec(SMEM)] + [spec(VMEM)] * 7,
        out_specs=spec(VMEM),
        scratch_shapes=[VMEM((32, 128, 128), f32)],
        compiler_params=PARAMS,
        interpret=interpret,
        name="backward",
    )(velocity, iterate, u, got, TABLES["uy"], TABLES["uz"], TABLES["lane"], TABLES["row"])


def shards(iterate, right_side, diffusivity, velocity):
    iterate, right_side = iterate[0], right_side[0]
    tm = lax.axis_index("tm")
    up = [(i, (i + 1) % SLABS) for i in range(SLABS)]
    down = [(i, (i - 1) % SLABS) for i in range(SLABS)]
    below = lax.ppermute(diffusivity[WIDE - 1], "space", up)
    above = lax.ppermute(diffusivity[0], "space", down)
    step = tm.astype(jnp.int32)[None]
    spectra, mixed = sources(velocity, step, iterate, right_side, diffusivity)
    u, sent = slab(velocity, spectra, mixed, below, above)
    returned = modes(velocity, sent)
    return backward(velocity, iterate, u, returned)[None]


def solution(mesh):
    placed = (
        P("tm", None, "space", None, None),
        P("tm", None, "space", None, None),
        P("space", None, None),
        P(),
    )
    return jax.shard_map(
        shards,
        mesh=mesh,
        in_specs=placed,
        out_specs=P("tm", None, "space", None, None),
        check_vma=False,
    )
```

```python
import functools
import math

import jax
import jax.numpy as jnp
import numpy as np
from jax import lax
from jax.experimental import pallas as pl
from jax.experimental.pallas import tpu as pltpu
from jax.sharding import PartitionSpec as P

NX, NY, NZ, STEPS = 128, 128, 64, 32
SLABS, WIDE = 8, 16
OWNERS = 128
ROWS = 12
MESH = pl.DeviceIdType.MESH
f32, bf16 = jnp.float32, jnp.bfloat16

diffusion_number = 16.0
circulant_alpha = 0.1


def collocation_matrix():
    radau_nodes = [0.08858795951270394, 0.4094668644407347, 0.7876594617608471, 1.0]
    matrix = [[0.0] * 4 for row_index in range(4)]
    for column_index in range(4):
        coefficients = [1.0]
        for other_index in range(4):
            if other_index != column_index:
                scale_value = 1.0 / (radau_nodes[column_index] - radau_nodes[other_index])
                shifted = [0.0] + [value * scale_value for value in coefficients]
                lowered = [
                    -radau_nodes[other_index] * scale_value * value for value in coefficients
                ] + [0.0]
                coefficients = [
                    left_value + right_value for left_value, right_value in zip(shifted, lowered)
                ]
        for row_index in range(4):
            total = 0.0
            for power_index in range(len(coefficients)):
                total = total + coefficients[power_index] * radau_nodes[row_index] ** (
                    power_index + 1
                ) / (power_index + 1)
            matrix[row_index][column_index] = total
    return matrix


def solve_system(matrix, target):
    count = len(target)
    rows_list = [list(matrix[row_index]) + [target[row_index]] for row_index in range(count)]
    for column in range(count):
        best_row = column
        for candidate in range(column + 1, count):
            if abs(rows_list[candidate][column]) > abs(rows_list[best_row][column]):
                best_row = candidate
        saved_row = rows_list[column]
        rows_list[column] = rows_list[best_row]
        rows_list[best_row] = saved_row
        leader = rows_list[column][column]
        for other_row in range(count):
            if other_row != column:
                factor = rows_list[other_row][column] / leader
                rows_list[other_row] = [
                    left_value - factor * right_value
                    for left_value, right_value in zip(rows_list[other_row], rows_list[column])
                ]
    return [
        rows_list[row_index][count] / rows_list[row_index][row_index] for row_index in range(count)
    ]


def node_basis():
    matrix = collocation_matrix()
    helper = [[0.0] * 4 for row_index in range(4)]
    coefficients = [0.0, 0.0, 0.0, 0.0, 1.0]
    for order in range(1, 5):
        product = [
            [
                sum((matrix[row_index][inner] * helper[inner][column] for inner in range(4)))
                for column in range(4)
            ]
            for row_index in range(4)
        ]
        for row_index in range(4):
            product[row_index][row_index] = product[row_index][row_index] + coefficients[5 - order]
        helper = product
        trace_value = sum(
            (
                sum((matrix[row_index][inner] * helper[inner][row_index] for inner in range(4)))
                for row_index in range(4)
            )
        )
        coefficients[4 - order] = -trace_value / order
    roots_list = [(0.4 + 0.9j) ** power_index for power_index in range(4)]
    for sweep in range(400):
        for root_index in range(4):
            current = roots_list[root_index]
            numer = 0.0
            for power_index in range(4, -1, -1):
                numer = numer * current + coefficients[power_index]
            denom = 1.0
            for other_index in range(4):
                if other_index != root_index:
                    denom = denom * (current - roots_list[other_index])
            roots_list[root_index] = current - numer / denom
    vectors = [[0.0] * 4 for row_index in range(4)]
    for root_index in range(4):
        shifted = [
            [
                matrix[row_index][column] - (roots_list[root_index] if row_index == column else 0.0)
                for column in range(3)
            ]
            for row_index in range(3)
        ]
        target = [-matrix[row_index][3] for row_index in range(3)]
        parts = solve_system(shifted, target) + [1.0 + 0j]
        for row_index in range(4):
            vectors[row_index][root_index] = parts[row_index]
    inverse = [[0.0] * 4 for row_index in range(4)]
    for column in range(4):
        unit = [1.0 if row_index == column else 0.0 for row_index in range(4)]
        parts = solve_system(vectors, unit)
        for row_index in range(4):
            inverse[row_index][column] = parts[row_index]
    weights = [sum((inverse[row_index][column] for column in range(4))) for row_index in range(4)]
    return (roots_list, vectors, inverse, weights)


VALUES, VECTORS, INVERSE, WEIGHTS = node_basis()
PAIRS = [m for m in range(4) if complex(VALUES[m]).imag > 0]
MU = [complex(VALUES[m]) for m in PAIRS]
COLUMN = [[complex(VECTORS[n][m]) for n in range(4)] for m in PAIRS]
ROW = [[complex(INVERSE[m][n]) for n in range(4)] for m in PAIRS]
EPS = [complex(WEIGHTS[m]) for m in PAIRS]


def wave_order_z():
    index = np.arange(NZ)
    return np.where(index <= NZ // 2, index, NZ + NZ // 2 - index)


def wave_order_y():
    lane = np.arange(NY)
    index = 16 * (lane // 32) + lane % 16
    return np.where(lane % 32 < 16, index, np.where(index == 0, NY // 2, NY - index))


def split(values):
    values = np.asarray(values, np.float64)
    high = values.astype(np.float32).astype(bf16)
    low = (values - high.astype(np.float64)).astype(np.float32).astype(bf16)
    return high, low


def side_table(values):
    high, low = split(values)
    return np.concatenate([high, high, low], axis=1)


def halves(x):
    high = x.astype(bf16)
    return high, (x - high.astype(f32)).astype(bf16)


def left_dot(table, x):
    high, low = halves(x)
    return jnp.dot(table, jnp.concatenate([high, low, high], axis=0), preferred_element_type=f32)


def right_dot(high, low, table_high, table_low):
    return (
        jnp.dot(high, table_high, preferred_element_type=f32)
        + jnp.dot(low, table_high, preferred_element_type=f32)
        + jnp.dot(high, table_low, preferred_element_type=f32)
    )


def complex_block(matrix):
    return np.block([[matrix.real, -matrix.imag], [matrix.imag, matrix.real]])


def make_tables():
    ky, kz = wave_order_y(), wave_order_z()
    kx, x = np.arange(NX), np.arange(NX)
    to_y = np.exp(-2j * np.pi * np.outer(ky, np.arange(NY)) / NY)
    to_z = np.exp(-2j * np.pi * np.outer(kz, np.arange(NZ)) / NZ)
    tables = {}
    tables["ty"] = np.stack(split(complex_block(to_y).T))
    tables["tz"] = side_table(complex_block(to_z))
    tables["uy"] = np.stack(split(complex_block(np.conj(to_y.T) / NY).T))
    tables["uz"] = side_table(complex_block(np.conj(to_z.T) / NZ))
    cells = (np.arange(SLABS)[:, None] * WIDE + np.arange(8)[None, :]).reshape(-1)
    theta = 2 * np.pi * kx / NX
    at = np.exp(-1j * np.outer(theta, cells))
    shifted = np.exp(-8j * theta)[:, None]
    from_own = at * (1 - 1j * shifted) / 2
    from_partner = at * (1 + 1j * shifted) / 2
    firsts = np.arange(SLABS) * WIDE

    def lane_block(matrix):
        return np.concatenate([matrix.real, -matrix.imag], axis=1)

    tables["tg"] = side_table(np.concatenate([lane_block(from_own), lane_block(from_partner)], axis=1))

    def point_rows(waves, shifts):
        out = []
        for m in range(2):
            table = np.zeros((len(waves), 4, SLABS), complex)
            for field, shift in shifts:
                table[:, 2 * m + field] = np.exp(-1j * np.outer(waves, firsts + shift))
            out.append(table.reshape(len(waves), 4 * SLABS))
        return out

    tables["td"] = side_table(
        lane_block(
            np.concatenate(
                point_rows(theta, ((0, WIDE), (1, -1))) + point_rows(theta[:8], ((1, 0),)), axis=0
            )
        )
    )
    back = np.exp(1j * np.outer(cells, theta)) * (1 + 1j * np.exp(8j * theta))[None, :] / NX
    tables["tw"] = side_table(lane_block(back))
    ends = [np.exp(1j * np.outer(firsts + k, theta)) / NX for k in (0, 1, 15)]
    tables["tb"] = side_table(lane_block(np.concatenate(ends, axis=0)))
    trig_y = 2 * np.pi * ky / NY
    trig_z = 2 * np.pi * kz / NZ
    tables["lane"] = np.stack([np.cos(trig_y), np.sin(trig_y)]).astype(np.float32)
    tables["row"] = np.stack(
        [np.broadcast_to(v[:, None], (NZ, NY)) for v in (np.cos(trig_z), np.sin(trig_z))]
    ).astype(np.float32)
    tables["wave_x"] = np.stack(
        [np.broadcast_to(v[:, None], (NX, 128)) for v in (np.cos(theta), np.sin(theta))]
    ).astype(np.float32)
    lane = np.arange(128)
    own = np.zeros((OWNERS, 8, 128))
    for owner in range(OWNERS):
        part, pair = owner // 32, owner % 32
        piece = (lane // 32 - part) % 4
        at_y, row = (lane - 32 * piece) % 128, piece % 2
        other_y = np.where((at_y == 0) | (at_y == 16), at_y, at_y ^ 16)
        other_row = row if pair == 0 else 1 - row
        other = (other_y + 32 * (2 * (piece // 2) + other_row)) % 128
        y, z = trig_y[at_y], trig_z[pair + 32 * row]
        own[owner] = np.stack(
            [
                np.cos(y), np.sin(y), np.cos(z), np.sin(z),
                other, np.roll(other, -64), np.where(piece < 2, 1.0, -1.0), (lane + 64) % 128,
            ]
        )
    tables["own"] = own.astype(np.float32)
    return tables


TABLES = make_tables()


def times(a, b):
    return (a[0] * b[0] - a[1] * b[1], a[0] * b[1] + a[1] * b[0])


def plus(a, b):
    return (a[0] + b[0], a[1] + b[1])


def minus(a, b):
    return (a[0] - b[0], a[1] - b[1])


def scaled(number, a):
    return (number.real * a[0] - number.imag * a[1], number.real * a[1] + number.imag * a[0])


def inverse_of(a):
    size = 1.0 / (a[0] * a[0] + a[1] * a[1])
    return (a[0] * size, -a[1] * size)


def root_of(a):
    size = jnp.sqrt(a[0] * a[0] + a[1] * a[1])
    main = jnp.sqrt(0.5 * (size + jnp.abs(a[0])))
    other = a[1] / (2.0 * main)
    positive = a[0] >= 0.0
    return (
        jnp.where(positive, main, jnp.abs(other)),
        jnp.where(positive, other, jnp.where(a[1] >= 0.0, main, -main)),
    )


def cross_symbol(cos_y, sin_y, cos_z, sin_z, v1, v2):
    return (
        diffusion_number * ((2.0 * cos_y - 2.0) + (2.0 * cos_z - 2.0)),
        -(v1 * sin_y + v2 * sin_z),
    )


def factors(mu, cross, v0):
    c_up = -mu.real * (diffusion_number - 0.5 * v0), -mu.imag * (diffusion_number - 0.5 * v0)
    c_down = -mu.real * (diffusion_number + 0.5 * v0), -mu.imag * (diffusion_number + 0.5 * v0)
    moved = scaled(mu, cross)
    c_mid = (1.0 + 2.0 * diffusion_number * mu.real - moved[0], 2.0 * diffusion_number * mu.imag - moved[1])
    product = times(c_up, c_down)
    square = times(c_mid, c_mid)
    root = root_of((square[0] - 4.0 * product[0], square[1] - 4.0 * product[1]))
    same = c_mid[0] * root[0] + c_mid[1] * root[1] >= 0.0
    kappa = (
        0.5 * (c_mid[0] + jnp.where(same, root[0], -root[0])),
        0.5 * (c_mid[1] + jnp.where(same, root[1], -root[1])),
    )
    inv = inverse_of(kappa)
    p = times(inv, c_down)
    q = times(inv, c_up)
    return (-p[0], -p[1]), (-q[0], -q[1]), kappa, inv


def plane_partner(low, high, lane, first_row):
    ends = (lane == 0) | (lane == 16)
    first = (lane % 32) < 16

    def turned(v):
        return jnp.where(ends, v, jnp.where(first, pltpu.roll(v, 112, 1), pltpu.roll(v, 16, 1)))

    low_turned, high_turned = [turned(v) for v in low], [turned(v) for v in high]
    to_low = [jnp.where(first_row, a, b) for a, b in zip(low_turned, high_turned)]
    to_high = [jnp.where(first_row, b, a) for a, b in zip(low_turned, high_turned)]
    return (to_low[0], -to_low[1]), (to_high[0], -to_high[1])


def packed_for(low, high, block):
    pieces = [low[0], high[0], low[1], high[1]]
    pieces = [pieces[0]] + [pltpu.roll(pieces[c], 32 * c, 1) for c in (1, 2, 3)]
    out = []
    for h in range(4):
        value = pieces[3]
        for c in (2, 1, 0):
            value = jnp.where(block == (h + c) % 4, pieces[c], value)
        out.append(value)
    return out


def unpacked_from(values, block):
    out = []
    for c in range(4):
        piece = values[(3 - c) % 4]
        for d in (2, 1, 0):
            piece = jnp.where(block == d, values[(d - c) % 4], piece)
        out.append(piece if c == 0 else pltpu.roll(piece, 128 - 32 * c, 1))
    return (out[0], out[2]), (out[1], out[3])


def chunk_factors(t, lane_ref, row_ref, velocity_ref, mu):
    cos_y, sin_y = lane_ref[0:1, :], lane_ref[1:2, :]
    found = []
    for base in (0, 32):
        rows = pl.ds(pl.multiple_of(base + 8 * t, 8), 8)
        cross = cross_symbol(
            cos_y, sin_y, row_ref[0, rows, :], row_ref[1, rows, :], velocity_ref[1], velocity_ref[2]
        )
        found.append([factors(number, cross, velocity_ref[0]) for number in mu])
    return found


def dft_block(high, low, ty_ref, tz_ref):
    mid = right_dot(high, low, ty_ref[0], ty_ref[1])
    stacked = jnp.concatenate(
        [
            jnp.concatenate([mid[64 * k : 64 * k + 64, :128], mid[64 * k : 64 * k + 64, 128:]], axis=0)
            for k in range(4)
        ],
        axis=1,
    )
    return left_dot(tz_ref[...], stacked)


def put_rows(slot, at, real, imag):
    for k, part in enumerate((real, imag)):
        for ref, value in zip(slot, halves(part)):
            ref[64 * at : 64 * at + 64, k * 128 : (k + 1) * 128] = value


def mixture(m, groups):
    real = imag = None
    for scale, values in groups:
        for n in range(4):
            factor = scale * ROW[m][n]
            a, b = factor.real * values[n], factor.imag * values[n]
            real = a if real is None else real + a
            imag = b if imag is None else imag + b
    return real, imag


def source_stage(
    keep, middle, velocity_ref, iterate_ref, right_ref, kappa_ref, ty_ref, tz_ref, spec_ref, mixed_ref, slots,
):
    v0, v1, v2 = velocity_ref[0], velocity_ref[1], velocity_ref[2]

    def stencil(x, slot, at, below, above):
        plain, applied = [], []
        kappa = diffusion_number * kappa_ref[x]
        for n in range(4):
            f = iterate_ref[n, x]
            up_z, down_z = pltpu.roll(f, NZ - 1, 0), pltpu.roll(f, 1, 0)
            up_y, down_y = pltpu.roll(f, NY - 1, 1), pltpu.roll(f, 1, 1)
            total = (up_z + down_z) + (up_y + down_y) - 6.0 * f
            moved = v1 * (up_y - down_y) + v2 * (up_z - down_z)
            if above:
                up_x = iterate_ref[n, x + 1]
                total, moved = total + up_x, moved + v0 * up_x
            if below:
                down_x = iterate_ref[n, x - 1]
                total, moved = total + down_x, moved - v0 * down_x
            applied.append(kappa * total - 0.5 * moved)
            plain.append(right_ref[n, x] - f)
        for m in range(2):
            put_rows(slot, 2 * m + at, *mixture(m, [(1.0, plain), (MU[m], applied)]))

    def produce(block, slot, first=False, final=False):
        stencil(2 * block, slot, 0, not first, True)
        stencil(2 * block + 1, slot, 1, True, not final)

    def last_node(block, slot):
        for k in range(4):
            x = 4 * block + k
            put_rows(slot, k, keep * iterate_ref[3, x], keep * iterate_ref[3, x + 8])

    def transformed(block, slot):
        out = dft_block(slot[0][...], slot[1][...], ty_ref, tz_ref)
        for k in range(4):
            spec_ref[block * 4 + k] = out[:, 128 * k : 128 * k + 128]

    for side, x in enumerate((0, WIDE - 1)):
        for m in range(2):
            real, imag = mixture(m, [(MU[m], [iterate_ref[n, x] for n in range(4)])])
            mixed_ref[side * 4 + m * 2] = real
            mixed_ref[side * 4 + m * 2 + 1] = imag
    first, second = slots
    produce(0, first, first=True)

    @pl.loop(0, 3)
    def _(i):
        transformed(2 * i, first)
        produce(2 * i + 1, second)
        transformed(2 * i + 1, second)
        produce(2 * i + 2, first)

    middle()
    transformed(6, first)
    produce(7, second, final=True)
    transformed(7, second)
    last_node(0, first)
    transformed(8, first)
    last_node(1, second)
    transformed(9, second)


def slab_stage(
    velocity_ref, spec_ref, mixed_ref, below_ref, above_ref, ty_ref, tz_ref, lane_ref, row_ref,
    u_ref, send_ref,
):
    v0 = velocity_ref[0]
    outer = [diffusion_number * below_ref[...] - 0.5 * v0, diffusion_number * above_ref[...] + 0.5 * v0]
    edges = [
        jnp.concatenate([outer[side] * mixed_ref[side * 4 + m * 2 + part] for part in range(2)], axis=1)
        for m in range(2)
        for side in range(2)
    ]
    high, low = halves(jnp.concatenate(edges, axis=0))
    out = dft_block(high, low, ty_ref, tz_ref)
    for k in range(4):
        spec_ref[40 + k] = out[:, 128 * k : 128 * k + 128]

    lane = lax.broadcasted_iota(jnp.int32, (8, 128), 1)
    sub = lax.broadcasted_iota(jnp.int32, (8, 128), 0)
    block = lane // 32

    @pl.loop(0, 4)
    def _(t):
        first_row = (sub + t) == 0
        found = chunk_factors(t, lane_ref, row_ref, velocity_ref, MU)
        bases = [pl.multiple_of(base + 8 * t, 8) for base in (0, 32)]

        def plane(at, base):
            return spec_ref[at, pl.ds(base, 8), :], spec_ref[at, pl.ds(base + 64, 8), :]

        def field(m, x, base):
            return plane(4 * (x // 2) + 2 * m + x % 2, base)

        def send(value, low, high):
            for h, packed in enumerate(packed_for(low, high, block)):
                send_ref[pl.ds((32 * h + 8 * t) * ROWS + value, 8, stride=ROWS), :] = packed

        sums = [[None, None] for x in range(WIDE)]
        for m in range(2):
            carries = []
            for half in range(2):
                base = bases[half]
                p, q, kappa, inv = found[half][m]
                under, over = plane(40 + 2 * m, base), plane(41 + 2 * m, base)
                u = plus(field(m, 0, base), times(p, under))
                us = [u]
                for x in range(1, WIDE):
                    u = plus(field(m, x, base), times(p, u))
                    us.append(u)
                for x in range(WIDE):
                    u_ref[m * 16 + x, pl.ds(base, 8), :] = us[x][0]
                    u_ref[m * 16 + x, pl.ds(base + 64, 8), :] = us[x][1]
                outflow = plus(times(p, us[-1]), over)
                y = us[-1]
                for x in range(WIDE - 1, -1, -1):
                    if x < WIDE - 1:
                        y = plus(us[x], times(q, y))
                    z = times(inv, y)
                    sums[x][half] = z if m == 0 else plus(sums[x][half], z)
                carries.append((outflow, plus(times(q, y), under)))
            for k in range(2):
                send(8 + m * 2 + k, carries[0][k], carries[1][k])
        for x in range(8):
            own, other = [], []
            for half in range(2):
                first, second = sums[x][half], sums[x + 8][half]
                own.append((first[0] - second[1], first[1] + second[0]))
                other.append((first[0] + second[1], first[1] - second[0]))
            partners = plane_partner(other[0], other[1], lane, first_row)
            packed = [
                plus(plus(own[half], partners[half]), plane(32 + x, bases[half])) for half in range(2)
            ]
            send(x, packed[0], packed[1])


def backward_kernel(
    velocity_ref, iterate_ref, u_ref, got_ref, uy_ref, uz_ref, lane_ref, row_ref,
    out_ref,
    spec_ref,
):
    lane = lax.broadcasted_iota(jnp.int32, (8, 128), 1)
    sub = lax.broadcasted_iota(jnp.int32, (8, 128), 0)
    block = lane // 32

    @pl.loop(0, 4)
    def _(t):
        first_row = (sub + t) == 0
        found = chunk_factors(t, lane_ref, row_ref, velocity_ref, MU)
        bases = [pl.multiple_of(base + 8 * t, 8) for base in (0, 32)]

        def take(value):
            values = [
                got_ref[pl.ds((32 * h + 8 * t) * ROWS + value, 8, stride=ROWS), :] for h in range(4)
            ]
            return unpacked_from(values, block)

        last = [[None, None] for x in range(WIDE)]
        for x in range(8):
            packed = take(x)
            partners = plane_partner(packed[0], packed[1], lane, first_row)
            for half in range(2):
                both, apart = plus(packed[half], partners[half]), minus(packed[half], partners[half])
                last[x][half] = (0.5 * both[0], 0.5 * both[1])
                last[x + 8][half] = (0.5 * apart[1], -0.5 * apart[0])
        for m in range(2):
            start, end = take(8 + m * 2), take(9 + m * 2)
            for half in range(2):
                base = bases[half]
                p, q, kappa, inv = found[half][m]

                def old(x):
                    return (
                        u_ref[m * 16 + x, pl.ds(base, 8), :],
                        u_ref[m * 16 + x, pl.ds(base + 64, 8), :],
                    )

                u = start[half]
                totals = [plus(u, old(0))]
                for x in range(1, WIDE - 1):
                    u = plus(scaled(EPS[m], last[x][half]), times(p, u))
                    totals.append(plus(u, old(x)))
                y = plus(times(inv, old(WIDE - 1)), end[half])
                for x in range(WIDE - 1, -1, -1):
                    if x < WIDE - 1:
                        y = plus(times(inv, totals[x]), times(q, y))
                    spec_ref[m * 16 + x, pl.ds(base, 8), :] = y[0]
                    spec_ref[m * 16 + x, pl.ds(base + 64, 8), :] = y[1]

    @pl.loop(0, 8)
    def _(block):
        planes = [2 * block, 2 * block + 1, 16 + 2 * block, 17 + 2 * block]
        stacked = jnp.concatenate([spec_ref[at] for at in planes], axis=1)
        mid = left_dot(uz_ref[...], stacked)
        rows = jnp.concatenate(
            [
                jnp.concatenate([mid[:64, 128 * k : 128 * k + 128], mid[64:, 128 * k : 128 * k + 128]], axis=1)
                for k in range(4)
            ],
            axis=0,
        )
        high, low = halves(rows)
        out = right_dot(high, low, uy_ref[0], uy_ref[1])
        for k in range(2):
            x = 2 * block + k
            parts = []
            for m in range(2):
                piece = out[(2 * m + k) * 64 : (2 * m + k) * 64 + 64]
                parts.append((piece[:, :128], piece[:, 128:]))
            for n in range(4):
                total = iterate_ref[n, x]
                for m in range(2):
                    c = COLUMN[m][n]
                    total = total + (2.0 * c.real) * parts[m][0] - (2.0 * c.imag) * parts[m][1]
                out_ref[n, x] = total


def whole_kernel(
    remote, velocity_ref, iterate_ref, right_ref, kappa_ref,
    ty_ref, tz_ref, lane_ref, row_ref, own_ref, wave_ref, tg_ref, td_ref, tw_ref, tb_ref,
    u_ref, returned_ref,
    high_a, low_a, high_b, low_b, spec_ref, mixed_ref, below_ref, above_ref, sent_ref,
    got_ref, back_ref, damp_ref, ratio_ref, last_ref, drive_ref, kept_ref, turn_ref,
    edge_out_sem, below_sem, above_sem,
    gather_sem, arrive_sem, swap_out_sem, swap_in_sem, scatter_sem, return_sem, own_sem,
):
    tm, space = remote.place()
    core = tm % 2
    owner = (tm // 2) * SLABS + space

    def rows_of(index, number=1):
        return pl.ds(pl.multiple_of(index * ROWS, 4), number * ROWS)

    def other(k):
        pair = (tm // 2 + STEPS // 2 - k // SLABS) % (STEPS // 2)
        to_space = ((space // 2 + (k % SLABS) // 2) % (SLABS // 2)) * 2 + (space + k) % 2
        return pair, to_space

    remote.greet((tm + 1 - 2 * core, space))

    @pl.loop(1, OWNERS)
    def _(k):
        pair, to_space = other(k)
        remote.greet((2 * pair + core, to_space))

    def middle():
        remote.all_here(OWNERS)
        remote.start(kappa_ref.at[WIDE - 1], below_ref, edge_out_sem, below_sem, (tm, (space + 1) % SLABS))
        remote.start(kappa_ref.at[0], above_ref, edge_out_sem, above_sem, (tm, (space + SLABS - 1) % SLABS))

    keep = jnp.where(tm < STEPS - 1, 1.0, 0.0).astype(f32)
    source_stage(
        keep, middle, velocity_ref, iterate_ref, right_ref, kappa_ref, ty_ref, tz_ref, spec_ref, mixed_ref,
        ((high_a, low_a), (high_b, low_b)),
    )
    remote.wait_got(below_ref, below_sem)
    remote.wait_got(above_ref, above_sem)
    slab_stage(
        velocity_ref, spec_ref, mixed_ref, below_ref, above_ref, ty_ref, tz_ref, lane_ref, row_ref,
        u_ref, sent_ref,
    )

    @pl.loop(1, OWNERS)
    def _(k):
        pair, to_space = other(k)
        remote.start(
            sent_ref.at[rows_of(pair * SLABS + to_space), :],
            got_ref.at[rows_of((tm // 2) * SLABS + space), :],
            gather_sem, arrive_sem.at[tm // 2], (2 * pair + core, to_space),
        )

    got_ref[rows_of(owner), :] = sent_ref[rows_of(owner), :]
    solve_modes(
        remote, 2, owner, tm, space, rows_of,
        velocity_ref, own_ref, wave_ref, tg_ref, td_ref, tw_ref, tb_ref, returned_ref,
        got_ref, back_ref, damp_ref, ratio_ref, last_ref, drive_ref, kept_ref, turn_ref,
        arrive_sem, swap_out_sem, swap_in_sem, scatter_sem, return_sem, own_sem,
    )
    remote.wait_sent(kappa_ref.at[pl.ds(0, 2)], edge_out_sem)
    remote.wait_sent(sent_ref.at[rows_of(0, OWNERS - 1), :], gather_sem)
    remote.wait_sent(back_ref.at[rows_of(0, OWNERS - 1), :], scatter_sem)
    remote.local(back_ref.at[rows_of(owner), :], returned_ref.at[rows_of(owner), :], own_sem).wait()
    remote.wait_got(returned_ref.at[rows_of(0, OWNERS - 1), :], return_sem)


GROUP = 4


def solve_modes(
    remote, share, owner, tm, space, rows_of,
    velocity_ref, own_ref, wave_ref, tg_ref, td_ref, tw_ref, tb_ref, returned_ref,
    got_ref, back_ref, damp_ref, ratio_ref, last_ref, drive_ref, kept_ref, turn_ref,
    arrive_sem, swap_out_sem, swap_in_sem, scatter_sem, return_sem, own_sem,
):
    rounds = STEPS // share // GROUP
    core = tm % share
    v0, v1, v2 = velocity_ref[0], velocity_ref[1], velocity_ref[2]
    own = own_ref[owner]
    line = [own[k : k + 1, :] for k in range(8)]
    wide = [jnp.broadcast_to(v, (8, 128)) for v in line]
    sign = wide[6]
    cross = cross_symbol(wide[0], wide[1], wide[2], wide[3], v1, v2)
    mu = [MU[0], MU[1], MU[0].conjugate(), MU[1].conjugate()]
    eps = [EPS[0], EPS[1], EPS[0].conjugate(), EPS[1].conjugate()]
    found = [factors(number, cross, v0) for number in mu]

    def crossed(a):
        return (a[0], -(sign * a[1]))

    def times_lanes(v, table):
        return v * table[0] + pltpu.roll(v, 64, 1) * table[1]

    def repeated(v, count):
        return jnp.concatenate([v] * count, axis=0)

    row = lax.broadcasted_iota(jnp.int32, (128, 128), 0).astype(f32)
    turn_ref[:, 0:128] = jnp.where(row == line[4], line[6], 0.0).astype(bf16)
    turn_ref[:, 128:256] = jnp.where(row == line[5], -1.0, 0.0).astype(bf16)

    @pl.loop(0, 16)
    def _(at):
        rows = pl.ds(pl.multiple_of(at * 8, 8), 8)
        symbol = (
            diffusion_number * (2.0 * wave_ref[0, rows, :] - 2.0) + cross[0],
            cross[1] - v0 * wave_ref[1, rows, :],
        )
        total = None
        for m in range(4):
            moved = scaled(mu[m], symbol)
            damp = inverse_of((1.0 - moved[0], -moved[1]))
            for k, value in enumerate(crossed(damp)):
                damp_ref[m, k, rows, :] = value
            term = scaled(eps[m], damp)
            if m < 2:
                for k, value in enumerate(crossed(term)):
                    damp_ref[4 + m, k, rows, :] = value
            total = term if total is None else plus(total, term)
        for k, value in enumerate(crossed(total)):
            ratio_ref[k, rows, :] = value
        power = total
        for k in range(5):
            power = times(power, power)
        closing = inverse_of((1.0 - circulant_alpha * power[0], -circulant_alpha * power[1]))
        for k, value in enumerate(crossed(closing)):
            ratio_ref[2 + k, rows, :] = value

    first_step = tm - tm % 2
    roots = [crossed(found[m][0]) for m in range(4)]
    flip = repeated(sign, 12)

    def step_of(i):
        return (first_step + share * i + core) % STEPS

    def swap(i):
        remote.start(
            drive_ref.at[step_of(i)], drive_ref.at[step_of(i)],
            swap_out_sem, swap_in_sem, (tm + 1 - 2 * core, space),
        )

    @pl.loop(0, rounds)
    def _(round_at):
        values, crossings = [], []
        for k in range(GROUP):
            s = step_of(round_at * GROUP + k)
            slot = s // share
            top = slot * (SLABS * ROWS)

            @pl.when(s == tm)
            def _():
                remote.wait_got(got_ref.at[rows_of(0, SLABS - 1), :], arrive_sem.at[slot])

            @pl.when(s != tm)
            def _():
                remote.wait_got(got_ref.at[rows_of(0, SLABS), :], arrive_sem.at[slot])

            pieces = [got_ref[pl.ds(top + x * ROWS, 8), :] for x in range(SLABS)]
            pieces += [got_ref[pl.ds(top + 8 + f, SLABS, stride=ROWS), :] for f in range(4)]
            v = jnp.concatenate(pieces, axis=0)
            values.append(halves(v))
            crossings.append(halves(flip * pltpu.roll(v, 64, 1)))
        stacked = jnp.concatenate([half for pair in values for half in pair], axis=0)
        turned = jnp.dot(stacked, turn_ref[...], preferred_element_type=f32).astype(bf16)
        columns, own_points, other_points = [], [], []
        for k in range(GROUP):
            parts = []
            for half in range(2):
                rows = slice(96 * (2 * k + half), 96 * (2 * k + half) + 96)
                parts.append((values[k][half], crossings[k][half], turned[rows, :128], turned[rows, 128:]))
            order = (parts[0], parts[1], parts[0])
            columns.append(jnp.concatenate([piece[:64] for part in order for piece in part], axis=0))
            own_points.append(jnp.concatenate([piece[64:] for part in order for piece in part[:2]], axis=0))
            other_points.append(jnp.concatenate([piece[64:] for part in order for piece in part[2:]], axis=0))
        drive = jnp.dot(tg_ref[...], jnp.concatenate(columns, axis=1), preferred_element_type=f32)
        points = jnp.dot(
            td_ref[...], jnp.concatenate(own_points + other_points, axis=1), preferred_element_type=f32
        )
        for k in range(GROUP):
            s = step_of(round_at * GROUP + k)
            total = drive[:, 128 * k : 128 * k + 128]
            for m in range(4):
                at = 128 * (k + GROUP * (m // 2))
                j = m % 2
                point = times_lanes(points[256 + 8 * j : 264 + 8 * j, at : at + 128], roots[m])
                d = points[128 * j : 128 * j + 128, at : at + 128] - repeated(point, 16)
                y = times_lanes(d, (damp_ref[m, 0], damp_ref[m, 1]))
                if m < 2:
                    kept_ref[s // share, m] = y
                total = total + y
            drive_ref[s] = total
        if share > 1:
            @pl.when(round_at > 0)
            def _():
                for k in range(GROUP):
                    swap((round_at - 1) * GROUP + k)

    if share > 1:
        for k in range(GROUP):
            swap((rounds - 1) * GROUP + k)
        remote.wait_got(drive_ref.at[pl.ds(0, STEPS // 2)], swap_in_sem)

    def wrapped(s, v):
        return jnp.where(s == 0, circulant_alpha, 1.0).astype(f32) * v

    def following(s, v):
        return drive_ref[s] + times_lanes(v, (ratio_ref[0], ratio_ref[1]))

    last_ref[...] = jnp.zeros((128, 128), f32)

    @pl.loop(0, STEPS)
    def _(i):
        s = (first_step + i) % STEPS
        last_ref[...] = following(s, wrapped(s, last_ref[...]))

    last_ref[...] = times_lanes(last_ref[...], (ratio_ref[2], ratio_ref[3]))
    kappas = [crossed(found[m][2]) for m in range(2)]
    ups = [crossed(found[m][1]) for m in range(2)]
    flip_all = repeated(sign, 16)

    def both_parts(v):
        return jnp.concatenate([v, flip_all * pltpu.roll(v, 64, 1)], axis=0)

    def send(i):
        s = step_of(i)
        for x in range(SLABS):
            index = (s // share) * SLABS + x

            @pl.when((s != tm) | (space != x))
            def _():
                remote.start(
                    back_ref.at[rows_of(index), :], returned_ref.at[rows_of(owner), :],
                    scatter_sem, return_sem, (s, x),
                )

            @pl.when((s == tm) & (space == x))
            def _():
                remote.local(
                    back_ref.at[rows_of(owner), :], returned_ref.at[rows_of(owner), :], own_sem
                ).start()

    @pl.loop(0, rounds)
    def _(round_at):
        inputs = []
        last = last_ref[...]
        for k in range(GROUP):
            mine = None
            for c in range(share):
                s = (first_step + share * (round_at * GROUP + k) + c) % STEPS
                last = wrapped(s, last)
                mine = last if mine is None else jnp.where(core == c, last, mine)
                last = following(s, last)
            inputs.append(mine)
        last_ref[...] = last
        packed = left_dot(tw_ref[...], jnp.concatenate([both_parts(v) for v in inputs], axis=1))
        lines = []
        for k in range(GROUP):
            slot = step_of(round_at * GROUP + k) // share
            for m in range(2):
                y = times_lanes(inputs[k], (damp_ref[4 + m, 0], damp_ref[4 + m, 1])) + kept_ref[slot, m]
                lines.append(both_parts(y))
        ends = left_dot(tb_ref[...], jnp.concatenate(lines, axis=1))
        for k in range(GROUP):
            top = (step_of(round_at * GROUP + k) // share) * (SLABS * ROWS)
            for x in range(SLABS):
                back_ref[pl.ds(top + x * ROWS, 8), :] = packed[8 * x : 8 * x + 8, 128 * k : 128 * k + 128]
            for m in range(2):
                at = 128 * (2 * k + m)
                part = [ends[8 * j : 8 * j + 8, at : at + 128] for j in range(3)]
                u = times_lanes(part[0] - times_lanes(part[1], ups[m]), kappas[m])
                back_ref[pl.ds(top + 8 + m * 2, SLABS, stride=ROWS), :] = u
                back_ref[pl.ds(top + 9 + m * 2, SLABS, stride=ROWS), :] = part[2]

        @pl.when(round_at > 0)
        def _():
            @pl.loop(0, GROUP)
            def _(k):
                send((round_at - 1) * GROUP + k)

    @pl.loop(0, GROUP)
    def _(k):
        send((rounds - 1) * GROUP + k)

    if share > 1:
        remote.wait_sent(drive_ref.at[pl.ds(0, STEPS // 2)], swap_out_sem)


class Remote:
    def place(self):
        return lax.axis_index("tm"), lax.axis_index("space")

    def greet(self, device):
        pl.semaphore_signal(
            pltpu.get_barrier_semaphore(), inc=1, device_id=device, device_id_type=MESH
        )

    def all_here(self, count):
        pl.semaphore_wait(pltpu.get_barrier_semaphore(), count)

    def start(self, source, target, send_sem, recv_sem, device):
        pltpu.make_async_remote_copy(
            src_ref=source, dst_ref=target, send_sem=send_sem, recv_sem=recv_sem,
            device_id=device, device_id_type=MESH,
        ).start()

    def local(self, source, target, sem):
        return pltpu.make_async_copy(source, target, sem)

    def bytes_of(self, ref, sem):
        return pltpu.make_async_remote_copy(
            src_ref=ref, dst_ref=ref, send_sem=sem, recv_sem=sem,
            device_id=self.place(), device_id_type=MESH,
        )

    def wait_sent(self, ref, sem):
        self.bytes_of(ref, sem).wait_send()

    def wait_got(self, ref, sem):
        self.bytes_of(ref, sem).wait_recv()


VMEM, SMEM, ANY = pltpu.VMEM, pltpu.SMEM, pl.ANY


def spec(space):
    return pl.BlockSpec(memory_space=space)


def shape(*dims):
    return jax.ShapeDtypeStruct(dims, f32)


PARAMS = pltpu.CompilerParams(vmem_limit_bytes=60 * 1024 * 1024)


def whole(velocity, iterate, right_side, kappa, remote=Remote(), interpret=False):
    dma = pltpu.SemaphoreType.DMA
    return pl.pallas_call(
        functools.partial(whole_kernel, remote),
        out_shape=(shape(32, 128, 128), shape(OWNERS * ROWS, 128)),
        in_specs=[spec(SMEM)] + [spec(VMEM)] * 13,
        out_specs=(spec(VMEM), spec(ANY)),
        scratch_shapes=[VMEM((256, 256), bf16)] * 4
        + [
            VMEM((44, 128, 128), f32), VMEM((8, NZ, NY), f32), VMEM((NZ, NY), f32), VMEM((NZ, NY), f32),
            VMEM((OWNERS * ROWS, 128), f32),
            VMEM((OWNERS * ROWS, 128), f32), VMEM((OWNERS * ROWS, 128), f32),
            VMEM((6, 2, 128, 128), f32), VMEM((4, 128, 128), f32), VMEM((128, 128), f32),
            VMEM((STEPS, 128, 128), f32), VMEM((STEPS // 2, 2, 128, 128), f32), VMEM((128, 256), bf16),
            dma, dma, dma, dma, dma((STEPS // 2,)), dma, dma, dma, dma, dma,
        ],
        compiler_params=pltpu.CompilerParams(
            vmem_limit_bytes=60 * 1024 * 1024, has_side_effects=True, collective_id=0
        ),
        interpret=interpret,
        name="whole",
    )(
        velocity, iterate, right_side, kappa,
        TABLES["ty"], TABLES["tz"], TABLES["lane"], TABLES["row"], TABLES["own"], TABLES["wave_x"],
        TABLES["tg"], TABLES["td"], TABLES["tw"], TABLES["tb"],
    )


def backward(velocity, iterate, u, got, interpret=False):
    return pl.pallas_call(
        backward_kernel,
        out_shape=shape(4, WIDE, NZ, NY),
        in_specs=[spec(SMEM)] + [spec(VMEM)] * 7,
        out_specs=spec(VMEM),
        scratch_shapes=[VMEM((32, 128, 128), f32)],
        compiler_params=PARAMS,
        interpret=interpret,
        name="backward",
    )(velocity, iterate, u, got, TABLES["uy"], TABLES["uz"], TABLES["lane"], TABLES["row"])


def shards(iterate, right_side, diffusivity, velocity):
    iterate, right_side = iterate[0], right_side[0]
    u, returned = whole(velocity, iterate, right_side, diffusivity)
    return backward(velocity, iterate, u, returned)[None]


def solution(mesh):
    placed = (
        P("tm", None, "space", None, None),
        P("tm", None, "space", None, None),
        P("space", None, None),
        P(),
    )
    return jax.shard_map(
        shards,
        mesh=mesh,
        in_specs=placed,
        out_specs=P("tm", None, "space", None, None),
        check_vma=False,
    )
```

```python
import functools
import math

import jax
import jax.numpy as jnp
import numpy as np
from jax import lax
from jax.experimental import pallas as pl
from jax.experimental.pallas import tpu as pltpu
from jax.sharding import PartitionSpec as P

NX, NY, NZ, STEPS = 128, 128, 64, 32
SLABS, WIDE = 8, 16
OWNERS = 128
ROWS = 12
MESH = pl.DeviceIdType.MESH
f32, bf16 = jnp.float32, jnp.bfloat16

diffusion_number = 16.0
circulant_alpha = 0.1


def collocation_matrix():
    radau_nodes = [0.08858795951270394, 0.4094668644407347, 0.7876594617608471, 1.0]
    matrix = [[0.0] * 4 for row_index in range(4)]
    for column_index in range(4):
        coefficients = [1.0]
        for other_index in range(4):
            if other_index != column_index:
                scale_value = 1.0 / (radau_nodes[column_index] - radau_nodes[other_index])
                shifted = [0.0] + [value * scale_value for value in coefficients]
                lowered = [
                    -radau_nodes[other_index] * scale_value * value for value in coefficients
                ] + [0.0]
                coefficients = [
                    left_value + right_value for left_value, right_value in zip(shifted, lowered)
                ]
        for row_index in range(4):
            total = 0.0
            for power_index in range(len(coefficients)):
                total = total + coefficients[power_index] * radau_nodes[row_index] ** (
                    power_index + 1
                ) / (power_index + 1)
            matrix[row_index][column_index] = total
    return matrix


def solve_system(matrix, target):
    count = len(target)
    rows_list = [list(matrix[row_index]) + [target[row_index]] for row_index in range(count)]
    for column in range(count):
        best_row = column
        for candidate in range(column + 1, count):
            if abs(rows_list[candidate][column]) > abs(rows_list[best_row][column]):
                best_row = candidate
        saved_row = rows_list[column]
        rows_list[column] = rows_list[best_row]
        rows_list[best_row] = saved_row
        leader = rows_list[column][column]
        for other_row in range(count):
            if other_row != column:
                factor = rows_list[other_row][column] / leader
                rows_list[other_row] = [
                    left_value - factor * right_value
                    for left_value, right_value in zip(rows_list[other_row], rows_list[column])
                ]
    return [
        rows_list[row_index][count] / rows_list[row_index][row_index] for row_index in range(count)
    ]


def node_basis():
    matrix = collocation_matrix()
    helper = [[0.0] * 4 for row_index in range(4)]
    coefficients = [0.0, 0.0, 0.0, 0.0, 1.0]
    for order in range(1, 5):
        product = [
            [
                sum((matrix[row_index][inner] * helper[inner][column] for inner in range(4)))
                for column in range(4)
            ]
            for row_index in range(4)
        ]
        for row_index in range(4):
            product[row_index][row_index] = product[row_index][row_index] + coefficients[5 - order]
        helper = product
        trace_value = sum(
            (
                sum((matrix[row_index][inner] * helper[inner][row_index] for inner in range(4)))
                for row_index in range(4)
            )
        )
        coefficients[4 - order] = -trace_value / order
    roots_list = [(0.4 + 0.9j) ** power_index for power_index in range(4)]
    for sweep in range(400):
        for root_index in range(4):
            current = roots_list[root_index]
            numer = 0.0
            for power_index in range(4, -1, -1):
                numer = numer * current + coefficients[power_index]
            denom = 1.0
            for other_index in range(4):
                if other_index != root_index:
                    denom = denom * (current - roots_list[other_index])
            roots_list[root_index] = current - numer / denom
    vectors = [[0.0] * 4 for row_index in range(4)]
    for root_index in range(4):
        shifted = [
            [
                matrix[row_index][column] - (roots_list[root_index] if row_index == column else 0.0)
                for column in range(3)
            ]
            for row_index in range(3)
        ]
        target = [-matrix[row_index][3] for row_index in range(3)]
        parts = solve_system(shifted, target) + [1.0 + 0j]
        for row_index in range(4):
            vectors[row_index][root_index] = parts[row_index]
    inverse = [[0.0] * 4 for row_index in range(4)]
    for column in range(4):
        unit = [1.0 if row_index == column else 0.0 for row_index in range(4)]
        parts = solve_system(vectors, unit)
        for row_index in range(4):
            inverse[row_index][column] = parts[row_index]
    weights = [sum((inverse[row_index][column] for column in range(4))) for row_index in range(4)]
    return (roots_list, vectors, inverse, weights)


VALUES, VECTORS, INVERSE, WEIGHTS = node_basis()
PAIRS = [m for m in range(4) if complex(VALUES[m]).imag > 0]
MU = [complex(VALUES[m]) for m in PAIRS]
COLUMN = [[complex(VECTORS[n][m]) for n in range(4)] for m in PAIRS]
ROW = [[complex(INVERSE[m][n]) for n in range(4)] for m in PAIRS]
EPS = [complex(WEIGHTS[m]) for m in PAIRS]


def wave_order_z():
    index = np.arange(NZ)
    return np.where(index <= NZ // 2, index, NZ + NZ // 2 - index)


def wave_order_y():
    lane = np.arange(NY)
    index = 16 * (lane // 32) + lane % 16
    return np.where(lane % 32 < 16, index, np.where(index == 0, NY // 2, NY - index))


def split(values):
    values = np.asarray(values, np.float64)
    high = values.astype(np.float32).astype(bf16)
    low = (values - high.astype(np.float64)).astype(np.float32).astype(bf16)
    return high, low


def side_table(values):
    high, low = split(values)
    return np.concatenate([high, high, low], axis=1)


def halves(x):
    high = x.astype(bf16)
    return high, (x - high.astype(f32)).astype(bf16)


def left_dot(table, x):
    high, low = halves(x)
    return jnp.dot(table, jnp.concatenate([high, low, high], axis=0), preferred_element_type=f32)


def right_dot(high, low, table_high, table_low):
    return (
        jnp.dot(high, table_high, preferred_element_type=f32)
        + jnp.dot(low, table_high, preferred_element_type=f32)
        + jnp.dot(high, table_low, preferred_element_type=f32)
    )


def complex_block(matrix):
    return np.block([[matrix.real, -matrix.imag], [matrix.imag, matrix.real]])


def make_tables():
    ky, kz = wave_order_y(), wave_order_z()
    kx, x = np.arange(NX), np.arange(NX)
    to_y = np.exp(-2j * np.pi * np.outer(ky, np.arange(NY)) / NY)
    to_z = np.exp(-2j * np.pi * np.outer(kz, np.arange(NZ)) / NZ)
    tables = {}
    tables["ty"] = np.stack(split(complex_block(to_y).T))
    tables["tz"] = side_table(complex_block(to_z))
    tables["uy"] = np.stack(split(complex_block(np.conj(to_y.T) / NY).T))
    tables["uz"] = side_table(complex_block(np.conj(to_z.T) / NZ))
    cells = (np.arange(SLABS)[:, None] * WIDE + np.arange(8)[None, :]).reshape(-1)
    theta = 2 * np.pi * kx / NX
    at = np.exp(-1j * np.outer(theta, cells))
    shifted = np.exp(-8j * theta)[:, None]
    from_own = at * (1 - 1j * shifted) / 2
    from_partner = at * (1 + 1j * shifted) / 2
    firsts = np.arange(SLABS) * WIDE

    def lane_block(matrix):
        return np.concatenate([matrix.real, -matrix.imag], axis=1)

    tables["tg"] = side_table(np.concatenate([lane_block(from_own), lane_block(from_partner)], axis=1))

    def point_rows(waves, shifts):
        out = []
        for m in range(2):
            table = np.zeros((len(waves), 4, SLABS), complex)
            for field, shift in shifts:
                table[:, 2 * m + field] = np.exp(-1j * np.outer(waves, firsts + shift))
            out.append(table.reshape(len(waves), 4 * SLABS))
        return out

    tables["td"] = side_table(
        lane_block(
            np.concatenate(
                point_rows(theta, ((0, WIDE), (1, -1))) + point_rows(theta[:8], ((1, 0),)), axis=0
            )
        )
    )
    back = np.exp(1j * np.outer(cells, theta)) * (1 + 1j * np.exp(8j * theta))[None, :] / NX
    tables["tw"] = side_table(lane_block(back))
    ends = [np.exp(1j * np.outer(firsts + k, theta)) / NX for k in (0, 1, 15)]
    tables["tb"] = side_table(lane_block(np.concatenate(ends, axis=0)))
    trig_y = 2 * np.pi * ky / NY
    trig_z = 2 * np.pi * kz / NZ
    tables["lane"] = np.stack([np.cos(trig_y), np.sin(trig_y)]).astype(np.float32)
    tables["row"] = np.stack(
        [np.broadcast_to(v[:, None], (NZ, NY)) for v in (np.cos(trig_z), np.sin(trig_z))]
    ).astype(np.float32)
    tables["wave_x"] = np.stack(
        [np.broadcast_to(v[:, None], (NX, 128)) for v in (np.cos(theta), np.sin(theta))]
    ).astype(np.float32)
    lane = np.arange(128)
    own = np.zeros((OWNERS, 8, 128))
    for owner in range(OWNERS):
        part, pair = owner // 32, owner % 32
        piece = (lane // 32 - part) % 4
        at_y, row = (lane - 32 * piece) % 128, piece % 2
        other_y = np.where((at_y == 0) | (at_y == 16), at_y, at_y ^ 16)
        other_row = row if pair == 0 else 1 - row
        other = (other_y + 32 * (2 * (piece // 2) + other_row)) % 128
        y, z = trig_y[at_y], trig_z[pair + 32 * row]
        own[owner] = np.stack(
            [
                np.cos(y), np.sin(y), np.cos(z), np.sin(z),
                other, np.roll(other, -64), np.where(piece < 2, 1.0, -1.0), (lane + 64) % 128,
            ]
        )
    tables["own"] = own.astype(np.float32)
    return tables


TABLES = make_tables()


def times(a, b):
    return (a[0] * b[0] - a[1] * b[1], a[0] * b[1] + a[1] * b[0])


def plus(a, b):
    return (a[0] + b[0], a[1] + b[1])


def minus(a, b):
    return (a[0] - b[0], a[1] - b[1])


def scaled(number, a):
    return (number.real * a[0] - number.imag * a[1], number.real * a[1] + number.imag * a[0])


def inverse_of(a):
    size = 1.0 / (a[0] * a[0] + a[1] * a[1])
    return (a[0] * size, -a[1] * size)


def root_of(a):
    size = jnp.sqrt(a[0] * a[0] + a[1] * a[1])
    main = jnp.sqrt(0.5 * (size + jnp.abs(a[0])))
    other = a[1] / (2.0 * main)
    positive = a[0] >= 0.0
    return (
        jnp.where(positive, main, jnp.abs(other)),
        jnp.where(positive, other, jnp.where(a[1] >= 0.0, main, -main)),
    )


def cross_symbol(cos_y, sin_y, cos_z, sin_z, v1, v2):
    return (
        diffusion_number * ((2.0 * cos_y - 2.0) + (2.0 * cos_z - 2.0)),
        -(v1 * sin_y + v2 * sin_z),
    )


def factors(mu, cross, v0):
    c_up = -mu.real * (diffusion_number - 0.5 * v0), -mu.imag * (diffusion_number - 0.5 * v0)
    c_down = -mu.real * (diffusion_number + 0.5 * v0), -mu.imag * (diffusion_number + 0.5 * v0)
    moved = scaled(mu, cross)
    c_mid = (1.0 + 2.0 * diffusion_number * mu.real - moved[0], 2.0 * diffusion_number * mu.imag - moved[1])
    product = times(c_up, c_down)
    square = times(c_mid, c_mid)
    root = root_of((square[0] - 4.0 * product[0], square[1] - 4.0 * product[1]))
    same = c_mid[0] * root[0] + c_mid[1] * root[1] >= 0.0
    kappa = (
        0.5 * (c_mid[0] + jnp.where(same, root[0], -root[0])),
        0.5 * (c_mid[1] + jnp.where(same, root[1], -root[1])),
    )
    inv = inverse_of(kappa)
    p = times(inv, c_down)
    q = times(inv, c_up)
    return (-p[0], -p[1]), (-q[0], -q[1]), kappa, inv


def plane_partner(low, high, lane, first_row):
    ends = (lane == 0) | (lane == 16)
    first = (lane % 32) < 16

    def turned(v):
        return jnp.where(ends, v, jnp.where(first, pltpu.roll(v, 112, 1), pltpu.roll(v, 16, 1)))

    low_turned, high_turned = [turned(v) for v in low], [turned(v) for v in high]
    to_low = [jnp.where(first_row, a, b) for a, b in zip(low_turned, high_turned)]
    to_high = [jnp.where(first_row, b, a) for a, b in zip(low_turned, high_turned)]
    return (to_low[0], -to_low[1]), (to_high[0], -to_high[1])


def packed_for(low, high, block):
    pieces = [low[0], high[0], low[1], high[1]]
    pieces = [pieces[0]] + [pltpu.roll(pieces[c], 32 * c, 1) for c in (1, 2, 3)]
    out = []
    for h in range(4):
        value = pieces[3]
        for c in (2, 1, 0):
            value = jnp.where(block == (h + c) % 4, pieces[c], value)
        out.append(value)
    return out


def unpacked_from(values, block):
    out = []
    for c in range(4):
        piece = values[(3 - c) % 4]
        for d in (2, 1, 0):
            piece = jnp.where(block == d, values[(d - c) % 4], piece)
        out.append(piece if c == 0 else pltpu.roll(piece, 128 - 32 * c, 1))
    return (out[0], out[2]), (out[1], out[3])


def chunk_factors(t, lane_ref, row_ref, velocity_ref, mu):
    cos_y, sin_y = lane_ref[0:1, :], lane_ref[1:2, :]
    found = []
    for base in (0, 32):
        rows = pl.ds(pl.multiple_of(base + 8 * t, 8), 8)
        cross = cross_symbol(
            cos_y, sin_y, row_ref[0, rows, :], row_ref[1, rows, :], velocity_ref[1], velocity_ref[2]
        )
        found.append([factors(number, cross, velocity_ref[0]) for number in mu])
    return found


def dft_block(high, low, ty_ref, tz_ref):
    mid = right_dot(high, low, ty_ref[0], ty_ref[1])
    stacked = jnp.concatenate(
        [
            jnp.concatenate([mid[64 * k : 64 * k + 64, :128], mid[64 * k : 64 * k + 64, 128:]], axis=0)
            for k in range(4)
        ],
        axis=1,
    )
    return left_dot(tz_ref[...], stacked)


def put_rows(slot, at, real, imag):
    for k, part in enumerate((real, imag)):
        for ref, value in zip(slot, halves(part)):
            ref[64 * at : 64 * at + 64, k * 128 : (k + 1) * 128] = value


def mixture(m, groups):
    real = imag = None
    for scale, values in groups:
        for n in range(4):
            factor = scale * ROW[m][n]
            a, b = factor.real * values[n], factor.imag * values[n]
            real = a if real is None else real + a
            imag = b if imag is None else imag + b
    return real, imag


def source_stage(
    keep, ready, middle, velocity_ref, iterate_ref, right_ref, kappa_ref, ty_ref, tz_ref, spec_ref, mixed_ref, slots,
):
    v0, v1, v2 = velocity_ref[0], velocity_ref[1], velocity_ref[2]

    def stencil(x, slot, at, below, above):
        plain, applied = [], []
        kappa = diffusion_number * kappa_ref[x]
        for n in range(4):
            f = iterate_ref[n, x]
            up_z, down_z = pltpu.roll(f, NZ - 1, 0), pltpu.roll(f, 1, 0)
            up_y, down_y = pltpu.roll(f, NY - 1, 1), pltpu.roll(f, 1, 1)
            total = (up_z + down_z) + (up_y + down_y) - 6.0 * f
            moved = v1 * (up_y - down_y) + v2 * (up_z - down_z)
            if above:
                up_x = iterate_ref[n, x + 1]
                total, moved = total + up_x, moved + v0 * up_x
            if below:
                down_x = iterate_ref[n, x - 1]
                total, moved = total + down_x, moved - v0 * down_x
            applied.append(kappa * total - 0.5 * moved)
            plain.append(right_ref[n, x] - f)
        for m in range(2):
            put_rows(slot, 2 * m + at, *mixture(m, [(1.0, plain), (MU[m], applied)]))

    def produce(block, slot, first=False, final=False):
        stencil(2 * block, slot, 0, not first, True)
        stencil(2 * block + 1, slot, 1, True, not final)

    def last_node(block, slot):
        for k in range(4):
            x = 4 * block + k
            put_rows(slot, k, keep * iterate_ref[3, x], keep * iterate_ref[3, x + 8])

    def transformed(block, slot):
        out = dft_block(slot[0][...], slot[1][...], ty_ref, tz_ref)
        for k in range(4):
            spec_ref[block * 4 + k] = out[:, 128 * k : 128 * k + 128]

    first, second = slots
    ready(0)
    ready(1)
    produce(0, first, first=True)

    @pl.loop(0, 3)
    def _(i):
        ready(2 * i + 2)
        transformed(2 * i, first)
        produce(2 * i + 1, second)
        ready(2 * i + 3)
        transformed(2 * i + 1, second)
        produce(2 * i + 2, first)

    middle()
    for side, x in enumerate((0, WIDE - 1)):
        for m in range(2):
            real, imag = mixture(m, [(MU[m], [iterate_ref[n, x] for n in range(4)])])
            mixed_ref[side * 4 + m * 2] = real
            mixed_ref[side * 4 + m * 2 + 1] = imag
    transformed(6, first)
    produce(7, second, final=True)
    transformed(7, second)
    last_node(0, first)
    transformed(8, first)
    last_node(1, second)
    transformed(9, second)


def slab_stage(
    velocity_ref, spec_ref, mixed_ref, below_ref, above_ref, ty_ref, tz_ref, lane_ref, row_ref,
    u_ref, send_ref,
):
    v0 = velocity_ref[0]
    outer = [diffusion_number * below_ref[...] - 0.5 * v0, diffusion_number * above_ref[...] + 0.5 * v0]
    edges = [
        jnp.concatenate([outer[side] * mixed_ref[side * 4 + m * 2 + part] for part in range(2)], axis=1)
        for m in range(2)
        for side in range(2)
    ]
    high, low = halves(jnp.concatenate(edges, axis=0))
    out = dft_block(high, low, ty_ref, tz_ref)
    for k in range(4):
        spec_ref[40 + k] = out[:, 128 * k : 128 * k + 128]

    lane = lax.broadcasted_iota(jnp.int32, (8, 128), 1)
    sub = lax.broadcasted_iota(jnp.int32, (8, 128), 0)
    block = lane // 32

    @pl.loop(0, 4)
    def _(t):
        first_row = (sub + t) == 0
        found = chunk_factors(t, lane_ref, row_ref, velocity_ref, MU)
        bases = [pl.multiple_of(base + 8 * t, 8) for base in (0, 32)]

        def plane(at, base):
            return spec_ref[at, pl.ds(base, 8), :], spec_ref[at, pl.ds(base + 64, 8), :]

        def field(m, x, base):
            return plane(4 * (x // 2) + 2 * m + x % 2, base)

        def send(value, low, high):
            for h, packed in enumerate(packed_for(low, high, block)):
                send_ref[pl.ds((32 * h + 8 * t) * ROWS + value, 8, stride=ROWS), :] = packed

        sums = [[None, None] for x in range(WIDE)]
        for m in range(2):
            carries = []
            for half in range(2):
                base = bases[half]
                p, q, kappa, inv = found[half][m]
                under, over = plane(40 + 2 * m, base), plane(41 + 2 * m, base)
                u = plus(field(m, 0, base), times(p, under))
                us = [u]
                for x in range(1, WIDE):
                    u = plus(field(m, x, base), times(p, u))
                    us.append(u)
                for x in range(WIDE):
                    u_ref[m * 16 + x, pl.ds(base, 8), :] = us[x][0]
                    u_ref[m * 16 + x, pl.ds(base + 64, 8), :] = us[x][1]
                outflow = plus(times(p, us[-1]), over)
                y = us[-1]
                for x in range(WIDE - 1, -1, -1):
                    if x < WIDE - 1:
                        y = plus(us[x], times(q, y))
                    z = times(inv, y)
                    sums[x][half] = z if m == 0 else plus(sums[x][half], z)
                carries.append((outflow, plus(times(q, y), under)))
            for k in range(2):
                send(8 + m * 2 + k, carries[0][k], carries[1][k])
        for x in range(8):
            own, other = [], []
            for half in range(2):
                first, second = sums[x][half], sums[x + 8][half]
                own.append((first[0] - second[1], first[1] + second[0]))
                other.append((first[0] + second[1], first[1] - second[0]))
            partners = plane_partner(other[0], other[1], lane, first_row)
            packed = [
                plus(plus(own[half], partners[half]), plane(32 + x, bases[half])) for half in range(2)
            ]
            send(x, packed[0], packed[1])


def backward_kernel(
    velocity_ref, iterate_hbm, u_ref, got_ref, uy_ref, uz_ref, lane_ref, row_ref,
    out_hbm,
    spec_ref, iterate_ref, out_ref, load_sem, store_sem,
):
    load = pltpu.make_async_copy(iterate_hbm, iterate_ref, load_sem)
    load.start()
    lane = lax.broadcasted_iota(jnp.int32, (8, 128), 1)
    sub = lax.broadcasted_iota(jnp.int32, (8, 128), 0)
    block = lane // 32

    @pl.loop(0, 4)
    def _(t):
        first_row = (sub + t) == 0
        found = chunk_factors(t, lane_ref, row_ref, velocity_ref, MU)
        bases = [pl.multiple_of(base + 8 * t, 8) for base in (0, 32)]

        def take(value):
            values = [
                got_ref[pl.ds((32 * h + 8 * t) * ROWS + value, 8, stride=ROWS), :] for h in range(4)
            ]
            return unpacked_from(values, block)

        last = [[None, None] for x in range(WIDE)]
        for x in range(8):
            packed = take(x)
            partners = plane_partner(packed[0], packed[1], lane, first_row)
            for half in range(2):
                both, apart = plus(packed[half], partners[half]), minus(packed[half], partners[half])
                last[x][half] = (0.5 * both[0], 0.5 * both[1])
                last[x + 8][half] = (0.5 * apart[1], -0.5 * apart[0])
        for m in range(2):
            start, end = take(8 + m * 2), take(9 + m * 2)
            for half in range(2):
                base = bases[half]
                p, q, kappa, inv = found[half][m]

                def old(x):
                    return (
                        u_ref[m * 16 + x, pl.ds(base, 8), :],
                        u_ref[m * 16 + x, pl.ds(base + 64, 8), :],
                    )

                u = start[half]
                totals = [plus(u, old(0))]
                for x in range(1, WIDE - 1):
                    u = plus(scaled(EPS[m], last[x][half]), times(p, u))
                    totals.append(plus(u, old(x)))
                y = plus(times(inv, old(WIDE - 1)), end[half])
                for x in range(WIDE - 1, -1, -1):
                    if x < WIDE - 1:
                        y = plus(times(inv, totals[x]), times(q, y))
                    spec_ref[m * 16 + x, pl.ds(base, 8), :] = y[0]
                    spec_ref[m * 16 + x, pl.ds(base + 64, 8), :] = y[1]

    load.wait()

    def finished(block):
        planes = [2 * block, 2 * block + 1, 16 + 2 * block, 17 + 2 * block]
        stacked = jnp.concatenate([spec_ref[at] for at in planes], axis=1)
        mid = left_dot(uz_ref[...], stacked)
        rows = jnp.concatenate(
            [
                jnp.concatenate([mid[:64, 128 * k : 128 * k + 128], mid[64:, 128 * k : 128 * k + 128]], axis=1)
                for k in range(4)
            ],
            axis=0,
        )
        high, low = halves(rows)
        return right_dot(high, low, uy_ref[0], uy_ref[1])

    def store(block):
        planes = pl.ds(2 * block, 2)
        return pltpu.make_async_copy(out_ref.at[:, planes], out_hbm.at[:, planes], store_sem.at[block])

    def added(block, out):
        for k in range(2):
            x = 2 * block + k
            parts = []
            for m in range(2):
                piece = out[(2 * m + k) * 64 : (2 * m + k) * 64 + 64]
                parts.append((piece[:, :128], piece[:, 128:]))
            for n in range(4):
                total = iterate_ref[n, x]
                for m in range(2):
                    c = COLUMN[m][n]
                    total = total + (2.0 * c.real) * parts[m][0] - (2.0 * c.imag) * parts[m][1]
                out_ref[n, x] = total

    @pl.loop(0, 4)
    def _(i):
        blocks = (2 * i, 2 * i + 1)
        outs = [finished(block) for block in blocks]
        for block, out in zip(blocks, outs):
            added(block, out)

        @pl.when(i > 0)
        def _():
            store(2 * i - 2).start()
            store(2 * i - 1).start()

    store(6).start()
    store(7).start()

    @pl.loop(0, 8)
    def _(block):
        store(block).wait()


def other_places(tm, space, work):
    pair = lax.div(tm, 2)
    x, side = lax.div(space, 2), lax.rem(space, 2)
    places = [
        lax.rem(x + k // 2, SLABS // 2) * 2 + lax.rem(side + k, 2) for k in range(SLABS)
    ]
    for k in range(1, SLABS):
        work(pair, places[k])

    @pl.loop(1, STEPS // 2)
    def _(i):
        other = lax.rem(pair + STEPS // 2 - i, STEPS // 2)
        for k in range(SLABS):
            work(other, places[k])


def whole_kernel(
    remote, velocity_ref, iterate_hbm, right_hbm, kappa_hbm,
    ty_ref, tz_ref, lane_ref, row_ref, own_ref, wave_ref, tg_ref, td_ref, tw_ref, tb_ref,
    u_hbm, returned_ref,
    iterate_ref, right_ref, kappa_ref, u_ref,
    high_a, low_a, high_b, low_b, spec_ref, mixed_ref, below_ref, above_ref, sent_ref,
    got_ref, back_ref, damp_ref, ratio_ref, last_ref, mate_ref, drive_ref, kept_ref, turn_ref,
    load_sem, u_sem, edge_out_sem, below_sem, above_sem,
    gather_sem, arrive_sem, swap_out_sem, swap_in_sem, mate_out_sem, mate_in_sem,
    scatter_sem, return_sem, own_sem,
):
    tm, space = remote.place()
    core = lax.rem(tm, 2)
    owner = lax.div(tm, 2) * SLABS + space

    def rows_of(index, number=1):
        return pl.ds(pl.multiple_of(index * ROWS, 4), number * ROWS)

    def loads(piece):
        planes = pl.ds(2 * piece, 2)
        return [
            remote.local(iterate_hbm.at[:, planes], iterate_ref.at[:, planes], load_sem.at[0, piece]),
            remote.local(right_hbm.at[:, planes], right_ref.at[:, planes], load_sem.at[1, piece]),
            remote.local(kappa_hbm.at[planes], kappa_ref.at[planes], load_sem.at[2, piece]),
        ]

    for piece in range(8):
        for copy in loads(piece):
            copy.start()

    def ready(piece):
        for copy in loads(piece):
            copy.wait()

    remote.greet((tm + 1 - 2 * core, space))
    other_places(tm, space, lambda pair, place: remote.greet((2 * pair + core, place)))

    def middle():
        remote.all_here(OWNERS)
        remote.start(
            kappa_ref.at[WIDE - 1], below_ref, edge_out_sem, below_sem, (tm, lax.rem(space + 1, SLABS))
        )
        remote.start(
            kappa_ref.at[0], above_ref, edge_out_sem, above_sem, (tm, lax.rem(space + SLABS - 1, SLABS))
        )

    keep = jnp.where(tm < STEPS - 1, 1.0, 0.0).astype(f32)
    source_stage(
        keep, ready, middle, velocity_ref, iterate_ref, right_ref, kappa_ref, ty_ref, tz_ref,
        spec_ref, mixed_ref, ((high_a, low_a), (high_b, low_b)),
    )
    remote.wait_got(below_ref, below_sem)
    remote.wait_got(above_ref, above_sem)
    slab_stage(
        velocity_ref, spec_ref, mixed_ref, below_ref, above_ref, ty_ref, tz_ref, lane_ref, row_ref,
        u_ref, sent_ref,
    )

    here = rows_of(owner)

    def send(pair, place):
        remote.start(
            sent_ref.at[rows_of(pair * SLABS + place), :], got_ref.at[here, :],
            gather_sem, arrive_sem.at[lax.div(tm, 2)], (2 * pair + core, place),
        )

    other_places(tm, space, send)
    keep_u = remote.local(u_ref, u_hbm, u_sem)
    keep_u.start()
    got_ref[here, :] = sent_ref[here, :]
    solve_modes(
        remote, 2, owner, tm, space, rows_of,
        velocity_ref, own_ref, wave_ref, tg_ref, td_ref, tw_ref, tb_ref, returned_ref,
        got_ref, back_ref, damp_ref, ratio_ref, last_ref, mate_ref, drive_ref, kept_ref, turn_ref,
        arrive_sem, swap_out_sem, swap_in_sem, mate_out_sem, mate_in_sem, scatter_sem, return_sem, own_sem,
    )
    keep_u.wait()
    remote.wait_sent(kappa_ref.at[pl.ds(0, 2)], edge_out_sem)
    remote.wait_sent(sent_ref.at[rows_of(0, OWNERS - 1), :], gather_sem)
    remote.wait_sent(back_ref.at[rows_of(0, OWNERS - 1), :], scatter_sem)
    remote.local(back_ref.at[here, :], returned_ref.at[here, :], own_sem).wait()
    remote.wait_got(returned_ref.at[rows_of(0, OWNERS - 1), :], return_sem)


GROUP = 2


def solve_modes(
    remote, share, owner, tm, space, rows_of,
    velocity_ref, own_ref, wave_ref, tg_ref, td_ref, tw_ref, tb_ref, returned_ref,
    got_ref, back_ref, damp_ref, ratio_ref, last_ref, mate_ref, drive_ref, kept_ref, turn_ref,
    arrive_sem, swap_out_sem, swap_in_sem, mate_out_sem, mate_in_sem, scatter_sem, return_sem, own_sem,
):
    rounds = STEPS // share // GROUP
    core = lax.rem(tm, share)
    v0, v1, v2 = velocity_ref[0], velocity_ref[1], velocity_ref[2]
    own = own_ref[owner]
    line = [own[k : k + 1, :] for k in range(8)]
    wide = [jnp.broadcast_to(v, (8, 128)) for v in line]
    sign = wide[6]
    cross = cross_symbol(wide[0], wide[1], wide[2], wide[3], v1, v2)
    mu = [MU[0], MU[1], MU[0].conjugate(), MU[1].conjugate()]
    eps = [EPS[0], EPS[1], EPS[0].conjugate(), EPS[1].conjugate()]
    found = [factors(number, cross, v0) for number in mu]

    def crossed(a):
        return (a[0], -(sign * a[1]))

    def times_lanes(v, table):
        return v * table[0] + pltpu.roll(v, 64, 1) * table[1]

    def repeated(v, count):
        return jnp.concatenate([v] * count, axis=0)

    row = lax.broadcasted_iota(jnp.int32, (128, 128), 0).astype(f32)
    turn_ref[:, 0:128] = jnp.where(row == line[4], line[6], 0.0).astype(bf16)
    turn_ref[:, 128:256] = jnp.where(row == line[5], -1.0, 0.0).astype(bf16)

    @pl.loop(0, 16)
    def _(at):
        rows = pl.ds(pl.multiple_of(at * 8, 8), 8)
        symbol = (
            diffusion_number * (2.0 * wave_ref[0, rows, :] - 2.0) + cross[0],
            cross[1] - v0 * wave_ref[1, rows, :],
        )
        total = None
        for m in range(4):
            moved = scaled(mu[m], symbol)
            damp = inverse_of((1.0 - moved[0], -moved[1]))
            for k, value in enumerate(crossed(damp)):
                damp_ref[m, k, rows, :] = value
            term = scaled(eps[m], damp)
            if m < 2:
                for k, value in enumerate(crossed(term)):
                    damp_ref[4 + m, k, rows, :] = value
            total = term if total is None else plus(total, term)
        for k, value in enumerate(crossed(total)):
            ratio_ref[k, rows, :] = value
        power = times(total, total)
        for k, value in enumerate(crossed(power if share == 2 else total)):
            ratio_ref[4 + k, rows, :] = value
        for k in range(4):
            power = times(power, power)
        closing = inverse_of((1.0 - circulant_alpha * power[0], -circulant_alpha * power[1]))
        for k, value in enumerate(crossed(closing)):
            ratio_ref[2 + k, rows, :] = value

    first_step = tm - lax.rem(tm, 2)
    roots = [crossed(found[m][0]) for m in range(4)]
    flip = repeated(sign, 12)

    def step_of(i):
        return lax.rem(first_step + share * i + core, STEPS)

    def wrapped(s, v):
        return jnp.where(s == 0, circulant_alpha, 1.0).astype(f32) * v

    def swap(i):
        remote.start(
            drive_ref.at[step_of(i)], drive_ref.at[step_of(i)],
            swap_out_sem, swap_in_sem, (tm + 1 - 2 * core, space),
        )

    last_ref[...] = jnp.zeros((128, 128), f32)

    @pl.loop(0, rounds)
    def _(round_at):
        values, crossings = [], []
        for k in range(GROUP):
            s = step_of(round_at * GROUP + k)
            slot = lax.div(s, share)
            top = slot * (SLABS * ROWS)
            if k > 0:
                remote.wait_got(got_ref.at[rows_of(0, SLABS), :], arrive_sem.at[slot])
            else:

                @pl.when(round_at == 0)
                def _():
                    remote.wait_got(got_ref.at[rows_of(0, SLABS - 1), :], arrive_sem.at[slot])

                @pl.when(round_at > 0)
                def _():
                    remote.wait_got(got_ref.at[rows_of(0, SLABS), :], arrive_sem.at[slot])

            pieces = [got_ref[pl.ds(top + x * ROWS, 8), :] for x in range(SLABS)]
            pieces += [got_ref[pl.ds(top + 8 + f, SLABS, stride=ROWS), :] for f in range(4)]
            v = jnp.concatenate(pieces, axis=0)
            values.append(halves(v))
            crossings.append(halves(flip * pltpu.roll(v, 64, 1)))
        stacked = jnp.concatenate([half for pair in values for half in pair], axis=0)
        turned = jnp.dot(stacked, turn_ref[...], preferred_element_type=f32).astype(bf16)
        columns, own_points, other_points = [], [], []
        for k in range(GROUP):
            parts = []
            for half in range(2):
                rows = slice(96 * (2 * k + half), 96 * (2 * k + half) + 96)
                parts.append((values[k][half], crossings[k][half], turned[rows, :128], turned[rows, 128:]))
            order = (parts[0], parts[1], parts[0])
            columns.append(jnp.concatenate([piece[:64] for part in order for piece in part], axis=0))
            own_points.append(jnp.concatenate([piece[64:] for part in order for piece in part[:2]], axis=0))
            other_points.append(jnp.concatenate([piece[64:] for part in order for piece in part[2:]], axis=0))
        drive = jnp.dot(tg_ref[...], jnp.concatenate(columns, axis=1), preferred_element_type=f32)
        points = jnp.dot(
            td_ref[...], jnp.concatenate(own_points + other_points, axis=1), preferred_element_type=f32
        )
        for k in range(GROUP):
            s = step_of(round_at * GROUP + k)
            total = drive[:, 128 * k : 128 * k + 128]
            for m in range(4):
                at = 128 * (k + GROUP * (m // 2))
                j = m % 2
                point = times_lanes(points[256 + 8 * j : 264 + 8 * j, at : at + 128], roots[m])
                d = points[128 * j : 128 * j + 128, at : at + 128] - repeated(point, 16)
                y = times_lanes(d, (damp_ref[m, 0], damp_ref[m, 1]))
                if m < 2:
                    kept_ref[lax.div(s, share), m] = y
                total = total + y
            drive_ref[s] = total
            summed = wrapped(s - core, last_ref[...])
            last_ref[...] = total + times_lanes(summed, (ratio_ref[4], ratio_ref[5]))
        if share > 1:
            @pl.when(round_at > 0)
            def _():
                for k in range(GROUP):
                    swap((round_at - 1) * GROUP + k)

    if share > 1:
        mate = (tm + 1 - 2 * core, space)
        for k in range(GROUP):
            swap((rounds - 1) * GROUP + k)
        remote.start(last_ref, mate_ref, mate_out_sem, mate_in_sem, mate)
        remote.wait_got(mate_ref, mate_in_sem)
        remote.wait_sent(last_ref, mate_out_sem)
        mine, theirs = last_ref[...], mate_ref[...]
        last_ref[...] = jnp.where(core == 0, theirs, mine) + times_lanes(
            jnp.where(core == 0, mine, theirs), (ratio_ref[0], ratio_ref[1])
        )
        remote.wait_got(drive_ref.at[pl.ds(0, STEPS // 2)], swap_in_sem)

    def following(s, v):
        return drive_ref[s] + times_lanes(v, (ratio_ref[0], ratio_ref[1]))

    last_ref[...] = times_lanes(last_ref[...], (ratio_ref[2], ratio_ref[3]))
    kappas = [crossed(found[m][2]) for m in range(2)]
    ups = [crossed(found[m][1]) for m in range(2)]
    flip_all = repeated(sign, 16)

    def both_parts(v):
        return jnp.concatenate([v, flip_all * pltpu.roll(v, 64, 1)], axis=0)

    x_at, side = lax.div(space, 2), lax.rem(space, 2)
    places = [lax.rem(x_at + k // 2, SLABS // 2) * 2 + lax.rem(side + k, 2) for k in range(SLABS)]
    here = rows_of(owner)

    def send(i):
        s = step_of(i)
        top = lax.div(s, share) * SLABS

        def put(place):
            remote.start(
                back_ref.at[rows_of(top + place), :], returned_ref.at[here, :],
                scatter_sem, return_sem, (s, place),
            )

        @pl.when(i == 0)
        def _():
            remote.local(back_ref.at[here, :], returned_ref.at[here, :], own_sem).start()

        @pl.when(i > 0)
        def _():
            put(places[0])

        for place in places[1:]:
            put(place)

    @pl.loop(0, rounds)
    def _(round_at):
        inputs = []
        last = last_ref[...]
        for k in range(GROUP):
            mine = None
            for c in range(share):
                s = lax.rem(first_step + share * (round_at * GROUP + k) + c, STEPS)
                last = wrapped(s, last)
                mine = last if mine is None else jnp.where(core == c, last, mine)
                last = following(s, last)
            inputs.append(mine)
        last_ref[...] = last
        packed = left_dot(tw_ref[...], jnp.concatenate([both_parts(v) for v in inputs], axis=1))
        lines = []
        for k in range(GROUP):
            slot = lax.div(step_of(round_at * GROUP + k), share)
            for m in range(2):
                y = times_lanes(inputs[k], (damp_ref[4 + m, 0], damp_ref[4 + m, 1])) + kept_ref[slot, m]
                lines.append(both_parts(y))
        ends = left_dot(tb_ref[...], jnp.concatenate(lines, axis=1))
        for k in range(GROUP):
            top = lax.div(step_of(round_at * GROUP + k), share) * (SLABS * ROWS)
            for x in range(SLABS):
                back_ref[pl.ds(top + x * ROWS, 8), :] = packed[8 * x : 8 * x + 8, 128 * k : 128 * k + 128]
            for m in range(2):
                at = 128 * (2 * k + m)
                part = [ends[8 * j : 8 * j + 8, at : at + 128] for j in range(3)]
                u = times_lanes(part[0] - times_lanes(part[1], ups[m]), kappas[m])
                back_ref[pl.ds(top + 8 + m * 2, SLABS, stride=ROWS), :] = u
                back_ref[pl.ds(top + 9 + m * 2, SLABS, stride=ROWS), :] = part[2]

        @pl.when(round_at > 0)
        def _():
            @pl.loop(0, GROUP)
            def _(k):
                send((round_at - 1) * GROUP + k)

    @pl.loop(0, GROUP)
    def _(k):
        send((rounds - 1) * GROUP + k)

    if share > 1:
        remote.wait_sent(drive_ref.at[pl.ds(0, STEPS // 2)], swap_out_sem)


class Remote:
    def place(self):
        return lax.axis_index("tm"), lax.axis_index("space")

    def greet(self, device):
        pl.semaphore_signal(
            pltpu.get_barrier_semaphore(), inc=1, device_id=device, device_id_type=MESH
        )

    def all_here(self, count):
        pl.semaphore_wait(pltpu.get_barrier_semaphore(), count)

    def start(self, source, target, send_sem, recv_sem, device):
        pltpu.make_async_remote_copy(
            src_ref=source, dst_ref=target, send_sem=send_sem, recv_sem=recv_sem,
            device_id=device, device_id_type=MESH,
        ).start()

    def local(self, source, target, sem):
        return pltpu.make_async_copy(source, target, sem)

    def bytes_of(self, ref, sem):
        return pltpu.make_async_remote_copy(
            src_ref=ref, dst_ref=ref, send_sem=sem, recv_sem=sem,
            device_id=self.place(), device_id_type=MESH,
        )

    def wait_sent(self, ref, sem):
        self.bytes_of(ref, sem).wait_send()

    def wait_got(self, ref, sem):
        self.bytes_of(ref, sem).wait_recv()


VMEM, SMEM, ANY = pltpu.VMEM, pltpu.SMEM, pl.ANY


def spec(space):
    return pl.BlockSpec(memory_space=space)


def shape(*dims):
    return jax.ShapeDtypeStruct(dims, f32)


PARAMS = pltpu.CompilerParams(vmem_limit_bytes=60 * 1024 * 1024)


def whole(velocity, iterate, right_side, kappa, remote=Remote(), interpret=False):
    dma = pltpu.SemaphoreType.DMA
    return pl.pallas_call(
        functools.partial(whole_kernel, remote),
        out_shape=(shape(32, 128, 128), shape(OWNERS * ROWS, 128)),
        in_specs=[spec(SMEM)] + [spec(ANY)] * 3 + [spec(VMEM)] * 10,
        out_specs=(spec(ANY), spec(ANY)),
        scratch_shapes=[
            VMEM((4, WIDE, NZ, NY), f32), VMEM((4, WIDE, NZ, NY), f32), VMEM((WIDE, NZ, NY), f32),
            VMEM((32, 128, 128), f32),
        ]
        + [VMEM((256, 256), bf16)] * 4
        + [
            VMEM((44, 128, 128), f32), VMEM((8, NZ, NY), f32), VMEM((NZ, NY), f32), VMEM((NZ, NY), f32),
            VMEM((OWNERS * ROWS, 128), f32),
            VMEM((OWNERS * ROWS, 128), f32), VMEM((OWNERS * ROWS, 128), f32),
            VMEM((6, 2, 128, 128), f32), VMEM((6, 128, 128), f32), VMEM((128, 128), f32), VMEM((128, 128), f32),
            VMEM((STEPS, 128, 128), f32), VMEM((STEPS // 2, 2, 128, 128), f32), VMEM((128, 256), bf16),
            dma((3, 8)), dma, dma, dma, dma, dma, dma((STEPS // 2,)), dma, dma, dma, dma, dma, dma, dma,
        ],
        compiler_params=pltpu.CompilerParams(
            vmem_limit_bytes=60 * 1024 * 1024, has_side_effects=True, collective_id=0
        ),
        interpret=interpret,
        name="whole",
    )(
        velocity, iterate, right_side, kappa,
        TABLES["ty"], TABLES["tz"], TABLES["lane"], TABLES["row"], TABLES["own"], TABLES["wave_x"],
        TABLES["tg"], TABLES["td"], TABLES["tw"], TABLES["tb"],
    )


def backward(velocity, iterate, u, got, interpret=False):
    return pl.pallas_call(
        backward_kernel,
        out_shape=shape(4, WIDE, NZ, NY),
        in_specs=[spec(SMEM), spec(ANY)] + [spec(VMEM)] * 6,
        out_specs=spec(ANY),
        scratch_shapes=[
            VMEM((32, 128, 128), f32), VMEM((4, WIDE, NZ, NY), f32), VMEM((4, WIDE, NZ, NY), f32),
            pltpu.SemaphoreType.DMA, pltpu.SemaphoreType.DMA((8,)),
        ],
        compiler_params=PARAMS,
        interpret=interpret,
        name="backward",
    )(velocity, iterate, u, got, TABLES["uy"], TABLES["uz"], TABLES["lane"], TABLES["row"])


def shards(iterate, right_side, diffusivity, velocity):
    iterate, right_side = iterate[0], right_side[0]
    u, returned = whole(velocity, iterate, right_side, diffusivity)
    return backward(velocity, iterate, u, returned)[None]


def solution(mesh):
    placed = (
        P("tm", None, "space", None, None),
        P("tm", None, "space", None, None),
        P("space", None, None),
        P(),
    )
    return jax.shard_map(
        shards,
        mesh=mesh,
        in_specs=placed,
        out_specs=P("tm", None, "space", None, None),
        check_vma=False,
    )
```

```python
import functools
import math

import jax
import jax.numpy as jnp
import numpy as np
from jax import lax
from jax.experimental import pallas as pl
from jax.experimental.pallas import tpu as pltpu
from jax.sharding import PartitionSpec as P

NX, NY, NZ, STEPS = 128, 128, 64, 32
SLABS, WIDE = 8, 16
OWNERS = 128
ROWS = 12
LINES = 16
MESH = pl.DeviceIdType.MESH
f32, bf16 = jnp.float32, jnp.bfloat16

diffusion_number = 16.0
circulant_alpha = 0.1


def collocation_matrix():
    radau_nodes = [0.08858795951270394, 0.4094668644407347, 0.7876594617608471, 1.0]
    matrix = [[0.0] * 4 for row_index in range(4)]
    for column_index in range(4):
        coefficients = [1.0]
        for other_index in range(4):
            if other_index != column_index:
                scale_value = 1.0 / (radau_nodes[column_index] - radau_nodes[other_index])
                shifted = [0.0] + [value * scale_value for value in coefficients]
                lowered = [
                    -radau_nodes[other_index] * scale_value * value for value in coefficients
                ] + [0.0]
                coefficients = [
                    left_value + right_value for left_value, right_value in zip(shifted, lowered)
                ]
        for row_index in range(4):
            total = 0.0
            for power_index in range(len(coefficients)):
                total = total + coefficients[power_index] * radau_nodes[row_index] ** (
                    power_index + 1
                ) / (power_index + 1)
            matrix[row_index][column_index] = total
    return matrix


def solve_system(matrix, target):
    count = len(target)
    rows_list = [list(matrix[row_index]) + [target[row_index]] for row_index in range(count)]
    for column in range(count):
        best_row = column
        for candidate in range(column + 1, count):
            if abs(rows_list[candidate][column]) > abs(rows_list[best_row][column]):
                best_row = candidate
        saved_row = rows_list[column]
        rows_list[column] = rows_list[best_row]
        rows_list[best_row] = saved_row
        leader = rows_list[column][column]
        for other_row in range(count):
            if other_row != column:
                factor = rows_list[other_row][column] / leader
                rows_list[other_row] = [
                    left_value - factor * right_value
                    for left_value, right_value in zip(rows_list[other_row], rows_list[column])
                ]
    return [
        rows_list[row_index][count] / rows_list[row_index][row_index] for row_index in range(count)
    ]


def node_basis():
    matrix = collocation_matrix()
    helper = [[0.0] * 4 for row_index in range(4)]
    coefficients = [0.0, 0.0, 0.0, 0.0, 1.0]
    for order in range(1, 5):
        product = [
            [
                sum((matrix[row_index][inner] * helper[inner][column] for inner in range(4)))
                for column in range(4)
            ]
            for row_index in range(4)
        ]
        for row_index in range(4):
            product[row_index][row_index] = product[row_index][row_index] + coefficients[5 - order]
        helper = product
        trace_value = sum(
            (
                sum((matrix[row_index][inner] * helper[inner][row_index] for inner in range(4)))
                for row_index in range(4)
            )
        )
        coefficients[4 - order] = -trace_value / order
    roots_list = [(0.4 + 0.9j) ** power_index for power_index in range(4)]
    for sweep in range(400):
        for root_index in range(4):
            current = roots_list[root_index]
            numer = 0.0
            for power_index in range(4, -1, -1):
                numer = numer * current + coefficients[power_index]
            denom = 1.0
            for other_index in range(4):
                if other_index != root_index:
                    denom = denom * (current - roots_list[other_index])
            roots_list[root_index] = current - numer / denom
    vectors = [[0.0] * 4 for row_index in range(4)]
    for root_index in range(4):
        shifted = [
            [
                matrix[row_index][column] - (roots_list[root_index] if row_index == column else 0.0)
                for column in range(3)
            ]
            for row_index in range(3)
        ]
        target = [-matrix[row_index][3] for row_index in range(3)]
        parts = solve_system(shifted, target) + [1.0 + 0j]
        for row_index in range(4):
            vectors[row_index][root_index] = parts[row_index]
    inverse = [[0.0] * 4 for row_index in range(4)]
    for column in range(4):
        unit = [1.0 if row_index == column else 0.0 for row_index in range(4)]
        parts = solve_system(vectors, unit)
        for row_index in range(4):
            inverse[row_index][column] = parts[row_index]
    weights = [sum((inverse[row_index][column] for column in range(4))) for row_index in range(4)]
    return (roots_list, vectors, inverse, weights)


VALUES, VECTORS, INVERSE, WEIGHTS = node_basis()
PAIRS = [m for m in range(4) if complex(VALUES[m]).imag > 0]
MU = [complex(VALUES[m]) for m in PAIRS]
COLUMN = [[complex(VECTORS[n][m]) for n in range(4)] for m in PAIRS]
ROW = [[complex(INVERSE[m][n]) for n in range(4)] for m in PAIRS]
EPS = [complex(WEIGHTS[m]) for m in PAIRS]


def wave_order_z():
    index = np.arange(NZ)
    return np.where(index <= NZ // 2, index, NZ + NZ // 2 - index)


def wave_order_y():
    lane = np.arange(NY)
    index = 16 * (lane // 32) + lane % 16
    return np.where(lane % 32 < 16, index, np.where(index == 0, NY // 2, NY - index))


def split(values):
    values = np.asarray(values, np.float64)
    high = values.astype(np.float32).astype(bf16)
    low = (values - high.astype(np.float64)).astype(np.float32).astype(bf16)
    return high, low


def side_table(values):
    high, low = split(values)
    return np.concatenate([high, high, low], axis=1)


def halves(x):
    high = x.astype(bf16)
    return high, (x - high.astype(f32)).astype(bf16)


def left_dot(table, x):
    high, low = halves(x)
    return jnp.dot(table, jnp.concatenate([high, low, high], axis=0), preferred_element_type=f32)


def right_dot(high, low, table_high, table_low):
    return (
        jnp.dot(high, table_high, preferred_element_type=f32)
        + jnp.dot(low, table_high, preferred_element_type=f32)
        + jnp.dot(high, table_low, preferred_element_type=f32)
    )


def complex_block(matrix):
    return np.block([[matrix.real, -matrix.imag], [matrix.imag, matrix.real]])


def make_tables():
    ky, kz = wave_order_y(), wave_order_z()
    kx, x = np.arange(NX), np.arange(NX)
    to_y = np.exp(-2j * np.pi * np.outer(ky, np.arange(NY)) / NY)
    to_z = np.exp(-2j * np.pi * np.outer(kz, np.arange(NZ)) / NZ)
    tables = {}
    tables["ty"] = np.stack(split(complex_block(to_y).T))
    tables["tz"] = side_table(complex_block(to_z))
    tables["uy"] = np.stack(split(complex_block(np.conj(to_y.T) / NY).T))
    tables["uz"] = side_table(complex_block(np.conj(to_z.T) / NZ))
    cells = (np.arange(SLABS)[:, None] * WIDE + np.arange(8)[None, :]).reshape(-1)
    theta = 2 * np.pi * kx / NX
    at = np.exp(-1j * np.outer(theta, cells))
    shifted = np.exp(-8j * theta)[:, None]
    from_own = at * (1 - 1j * shifted) / 2
    from_partner = at * (1 + 1j * shifted) / 2
    firsts = np.arange(SLABS) * WIDE

    def lane_block(matrix):
        return np.concatenate([matrix.real, -matrix.imag], axis=1)

    tables["tg"] = side_table(np.concatenate([lane_block(from_own), lane_block(from_partner)], axis=1))

    def point_rows(waves, shifts):
        out = []
        for m in range(2):
            table = np.zeros((len(waves), 4, SLABS), complex)
            for field, shift in shifts:
                table[:, 2 * m + field] = np.exp(-1j * np.outer(waves, firsts + shift))
            out.append(table.reshape(len(waves), 4 * SLABS))
        return out

    tables["td"] = side_table(
        lane_block(
            np.concatenate(
                point_rows(theta, ((0, WIDE), (1, -1))) + point_rows(theta[:8], ((1, 0),)), axis=0
            )
        )
    )
    back = np.exp(1j * np.outer(cells, theta)) * (1 + 1j * np.exp(8j * theta))[None, :] / NX
    tables["tw"] = side_table(lane_block(back))
    ends = [np.exp(1j * np.outer(firsts + k, theta)) / NX for k in (0, 1, 15)]
    tables["tb"] = side_table(lane_block(np.concatenate(ends, axis=0)))
    trig_y = 2 * np.pi * ky / NY
    trig_z = 2 * np.pi * kz / NZ
    tables["lane"] = np.stack([np.cos(trig_y), np.sin(trig_y)]).astype(np.float32)
    tables["row"] = np.stack(
        [np.broadcast_to(v[:, None], (NZ, NY)) for v in (np.cos(trig_z), np.sin(trig_z))]
    ).astype(np.float32)
    tables["wave_x"] = np.stack(
        [np.broadcast_to(v[:, None], (NX, 128)) for v in (np.cos(theta), np.sin(theta))]
    ).astype(np.float32)
    lane = np.arange(128)
    own = np.zeros((OWNERS, 8, 128))
    for owner in range(OWNERS):
        part, pair = owner // 32, owner % 32
        piece = (lane // 32 - part) % 4
        at_y, row = (lane - 32 * piece) % 128, piece % 2
        other_y = np.where((at_y == 0) | (at_y == 16), at_y, at_y ^ 16)
        other_row = row if pair == 0 else 1 - row
        other = (other_y + 32 * (2 * (piece // 2) + other_row)) % 128
        y, z = trig_y[at_y], trig_z[pair + 32 * row]
        own[owner] = np.stack(
            [
                np.cos(y), np.sin(y), np.cos(z), np.sin(z),
                other, np.roll(other, -64), np.where(piece < 2, 1.0, -1.0), (lane + 64) % 128,
            ]
        )
    tables["own"] = own.astype(np.float32)
    return tables


TABLES = make_tables()


def times(a, b):
    return (a[0] * b[0] - a[1] * b[1], a[0] * b[1] + a[1] * b[0])


def plus(a, b):
    return (a[0] + b[0], a[1] + b[1])


def minus(a, b):
    return (a[0] - b[0], a[1] - b[1])


def scaled(number, a):
    return (number.real * a[0] - number.imag * a[1], number.real * a[1] + number.imag * a[0])


def inverse_of(a):
    size = 1.0 / (a[0] * a[0] + a[1] * a[1])
    return (a[0] * size, -a[1] * size)


def root_of(a):
    size = jnp.sqrt(a[0] * a[0] + a[1] * a[1])
    main = jnp.sqrt(0.5 * (size + jnp.abs(a[0])))
    other = a[1] / (2.0 * main)
    positive = a[0] >= 0.0
    return (
        jnp.where(positive, main, jnp.abs(other)),
        jnp.where(positive, other, jnp.where(a[1] >= 0.0, main, -main)),
    )


def cross_symbol(cos_y, sin_y, cos_z, sin_z, v1, v2):
    return (
        diffusion_number * ((2.0 * cos_y - 2.0) + (2.0 * cos_z - 2.0)),
        -(v1 * sin_y + v2 * sin_z),
    )


def factors(mu, cross, v0):
    c_up = -mu.real * (diffusion_number - 0.5 * v0), -mu.imag * (diffusion_number - 0.5 * v0)
    c_down = -mu.real * (diffusion_number + 0.5 * v0), -mu.imag * (diffusion_number + 0.5 * v0)
    moved = scaled(mu, cross)
    c_mid = (1.0 + 2.0 * diffusion_number * mu.real - moved[0], 2.0 * diffusion_number * mu.imag - moved[1])
    product = times(c_up, c_down)
    square = times(c_mid, c_mid)
    root = root_of((square[0] - 4.0 * product[0], square[1] - 4.0 * product[1]))
    same = c_mid[0] * root[0] + c_mid[1] * root[1] >= 0.0
    kappa = (
        0.5 * (c_mid[0] + jnp.where(same, root[0], -root[0])),
        0.5 * (c_mid[1] + jnp.where(same, root[1], -root[1])),
    )
    inv = inverse_of(kappa)
    p = times(inv, c_down)
    q = times(inv, c_up)
    return (-p[0], -p[1]), (-q[0], -q[1]), kappa, inv


def plane_partner(low, high, lane, first_row):
    ends = (lane == 0) | (lane == 16)
    first = (lane % 32) < 16

    def turned(v):
        return jnp.where(ends, v, jnp.where(first, pltpu.roll(v, 112, 1), pltpu.roll(v, 16, 1)))

    low_turned, high_turned = [turned(v) for v in low], [turned(v) for v in high]
    to_low = [jnp.where(first_row, a, b) for a, b in zip(low_turned, high_turned)]
    to_high = [jnp.where(first_row, b, a) for a, b in zip(low_turned, high_turned)]
    return (to_low[0], -to_low[1]), (to_high[0], -to_high[1])


def packed_for(low, high, block):
    pieces = [low[0], high[0], low[1], high[1]]
    pieces = [pieces[0]] + [pltpu.roll(pieces[c], 32 * c, 1) for c in (1, 2, 3)]
    out = []
    for h in range(4):
        value = pieces[3]
        for c in (2, 1, 0):
            value = jnp.where(block == (h + c) % 4, pieces[c], value)
        out.append(value)
    return out


def unpacked_from(values, block):
    out = []
    for c in range(4):
        piece = values[(3 - c) % 4]
        for d in (2, 1, 0):
            piece = jnp.where(block == d, values[(d - c) % 4], piece)
        out.append(piece if c == 0 else pltpu.roll(piece, 128 - 32 * c, 1))
    return (out[0], out[2]), (out[1], out[3])


def chunk_factors(t, lane_ref, row_ref, velocity_ref, mu):
    cos_y, sin_y = lane_ref[0:1, :], lane_ref[1:2, :]
    found = []
    for base in (0, 32):
        rows = pl.ds(pl.multiple_of(base + 8 * t, 8), 8)
        cross = cross_symbol(
            cos_y, sin_y, row_ref[0, rows, :], row_ref[1, rows, :], velocity_ref[1], velocity_ref[2]
        )
        found.append([factors(number, cross, velocity_ref[0]) for number in mu])
    return found


def dft_block(high, low, ty_ref, tz_ref):
    mid = right_dot(high, low, ty_ref[0], ty_ref[1])
    stacked = jnp.concatenate(
        [
            jnp.concatenate([mid[64 * k : 64 * k + 64, :128], mid[64 * k : 64 * k + 64, 128:]], axis=0)
            for k in range(4)
        ],
        axis=1,
    )
    return left_dot(tz_ref[...], stacked)


def put_rows(slot, at, real, imag):
    for k, part in enumerate((real, imag)):
        for ref, value in zip(slot, halves(part)):
            ref[64 * at : 64 * at + 64, k * 128 : (k + 1) * 128] = value


def mixture(m, groups):
    real = imag = None
    for scale, values in groups:
        for n in range(4):
            factor = scale * ROW[m][n]
            a, b = factor.real * values[n], factor.imag * values[n]
            real = a if real is None else real + a
            imag = b if imag is None else imag + b
    return real, imag


def source_stage(
    keep, ready, middle, velocity_ref, iterate_ref, right_ref, kappa_ref, ty_ref, tz_ref, spec_ref, mixed_ref, slots,
):
    v0, v1, v2 = velocity_ref[0], velocity_ref[1], velocity_ref[2]

    def stencil(x, slot, at, below, above):
        plain, applied = [], []
        kappa = diffusion_number * kappa_ref[x]
        for n in range(4):
            f = iterate_ref[n, x]
            up_z, down_z = pltpu.roll(f, NZ - 1, 0), pltpu.roll(f, 1, 0)
            up_y, down_y = pltpu.roll(f, NY - 1, 1), pltpu.roll(f, 1, 1)
            total = (up_z + down_z) + (up_y + down_y) - 6.0 * f
            moved = v1 * (up_y - down_y) + v2 * (up_z - down_z)
            if above:
                up_x = iterate_ref[n, x + 1]
                total, moved = total + up_x, moved + v0 * up_x
            if below:
                down_x = iterate_ref[n, x - 1]
                total, moved = total + down_x, moved - v0 * down_x
            applied.append(kappa * total - 0.5 * moved)
            plain.append(right_ref[n, x] - f)
        for m in range(2):
            put_rows(slot, 2 * m + at, *mixture(m, [(1.0, plain), (MU[m], applied)]))

    def produce(block, slot, first=False, final=False):
        stencil(2 * block, slot, 0, not first, True)
        stencil(2 * block + 1, slot, 1, True, not final)

    def last_node(block, slot):
        for k in range(4):
            x = 4 * block + k
            put_rows(slot, k, keep * iterate_ref[3, x], keep * iterate_ref[3, x + 8])

    def transformed(block, slot):
        out = dft_block(slot[0][...], slot[1][...], ty_ref, tz_ref)
        for k in range(4):
            spec_ref[block * 4 + k] = out[:, 128 * k : 128 * k + 128]

    first, second = slots
    ready(0)
    ready(1)
    produce(0, first, first=True)

    @pl.loop(0, 3)
    def _(i):
        ready(2 * i + 2)
        transformed(2 * i, first)
        produce(2 * i + 1, second)
        ready(2 * i + 3)
        transformed(2 * i + 1, second)
        produce(2 * i + 2, first)

    middle()
    for side, x in enumerate((0, WIDE - 1)):
        for m in range(2):
            real, imag = mixture(m, [(MU[m], [iterate_ref[n, x] for n in range(4)])])
            mixed_ref[side * 4 + m * 2] = real
            mixed_ref[side * 4 + m * 2 + 1] = imag
    transformed(6, first)
    produce(7, second, final=True)
    transformed(7, second)
    last_node(0, first)
    transformed(8, first)
    last_node(1, second)
    transformed(9, second)


def put_chunk(ref, t, x, low, high):
    for k, value in enumerate((low[0], high[0], low[1], high[1])):
        ref[pl.ds(pl.multiple_of(256 * t + 32 * x + 8 * k, 8), 8), :] = value


def get_chunk(ref, t, x):
    parts = [ref[pl.ds(pl.multiple_of(256 * t + 32 * x + 8 * k, 8), 8), :] for k in range(4)]
    return (parts[0], parts[2]), (parts[1], parts[3])


def packed_planes(sums, x, lane, first_row):
    own, other = [], []
    for half in range(2):
        first, second = sums[x][half], sums[x + 8][half]
        own.append((first[0] - second[1], first[1] + second[0]))
        other.append((first[0] + second[1], first[1] - second[0]))
    partners = plane_partner(other[0], other[1], lane, first_row)
    return [plus(own[half], partners[half]) for half in range(2)]


def unpacked_planes(fetch, lane, first_row):
    last = [[None, None] for x in range(WIDE)]
    for x in range(8):
        packed = fetch(x)
        partners = plane_partner(packed[0], packed[1], lane, first_row)
        for half in range(2):
            both, apart = plus(packed[half], partners[half]), minus(packed[half], partners[half])
            last[x][half] = (0.5 * both[0], 0.5 * both[1])
            last[x + 8][half] = (0.5 * apart[1], -0.5 * apart[0])
    return last


def edge_stage(velocity_ref, spec_ref, mixed_ref, below_ref, above_ref, ty_ref, tz_ref):
    v0 = velocity_ref[0]
    outer = [diffusion_number * below_ref[...] - 0.5 * v0, diffusion_number * above_ref[...] + 0.5 * v0]
    edges = [
        jnp.concatenate([outer[side] * mixed_ref[side * 4 + m * 2 + part] for part in range(2)], axis=1)
        for m in range(2)
        for side in range(2)
    ]
    high, low = halves(jnp.concatenate(edges, axis=0))
    out = dft_block(high, low, ty_ref, tz_ref)
    for k in range(4):
        spec_ref[40 + k] = out[:, 128 * k : 128 * k + 128]


def slab_stage(odd, begin, velocity_ref, spec_ref, lane_ref, row_ref, y_ref, send_ref, chunk_ref):
    lane = lax.broadcasted_iota(jnp.int32, (8, 128), 1)
    sub = lax.broadcasted_iota(jnp.int32, (8, 128), 0)
    block = lane // 32

    @pl.loop(0, 4)
    def _(t):
        begin(t)
        first_row = (sub + t) == 0
        found = chunk_factors(t, lane_ref, row_ref, velocity_ref, MU)
        bases = [pl.multiple_of(base + 8 * t, 8) for base in (0, 32)]
        if odd:
            last = unpacked_planes(lambda x: get_chunk(chunk_ref, t, x), lane, first_row)

        def plane(at, base):
            return spec_ref[at, pl.ds(base, 8), :], spec_ref[at, pl.ds(base + 64, 8), :]

        def field(m, x, half):
            value = plane(4 * (x // 2) + 2 * m + x % 2, bases[half])
            return plus(value, scaled(EPS[m], last[x][half])) if odd else value

        def send(value, low, high):
            for h, packed in enumerate(packed_for(low, high, block)):
                send_ref[pl.ds((32 * h + 8 * t) * ROWS + value, 8, stride=ROWS), :] = packed

        sums = [[None, None] for x in range(WIDE)]
        for m in range(2):
            carries = []
            for half in range(2):
                base = bases[half]
                p, q, kappa, inv = found[half][m]
                under, over = plane(40 + 2 * m, base), plane(41 + 2 * m, base)
                u = plus(field(m, 0, half), times(p, under))
                us = [u]
                for x in range(1, WIDE):
                    u = plus(field(m, x, half), times(p, u))
                    us.append(u)
                outflow = plus(times(p, us[-1]), over)
                y = us[-1]
                for x in range(WIDE - 1, -1, -1):
                    if x < WIDE - 1:
                        y = plus(us[x], times(q, y))
                    z = times(inv, y)
                    y_ref[m * 16 + x, pl.ds(base, 8), :] = z[0]
                    y_ref[m * 16 + x, pl.ds(base + 64, 8), :] = z[1]
                    sums[x][half] = z if m == 0 else plus(sums[x][half], z)
                carries.append((outflow, plus(times(q, y), under)))
            for k in range(2):
                send(8 + m * 2 + k, carries[0][k], carries[1][k])
        for x in range(8):
            packed = packed_planes(sums, x, lane, first_row)
            packed = [plus(packed[half], plane(32 + x, bases[half])) for half in range(2)]
            if odd:
                send(x, packed[0], packed[1])
            else:
                put_chunk(chunk_ref, t, x, packed[0], packed[1])


def finish_stage(odd, begin, velocity_ref, lane_ref, row_ref, y_ref, got_ref, chunk_ref):
    lane = lax.broadcasted_iota(jnp.int32, (8, 128), 1)
    sub = lax.broadcasted_iota(jnp.int32, (8, 128), 0)
    block = lane // 32

    @pl.loop(0, 4)
    def _(t):
        begin(t)
        first_row = (sub + t) == 0
        found = chunk_factors(t, lane_ref, row_ref, velocity_ref, MU)
        bases = [pl.multiple_of(base + 8 * t, 8) for base in (0, 32)]

        def take(value):
            values = [
                got_ref[pl.ds((32 * h + 8 * t) * ROWS + value, 8, stride=ROWS), :] for h in range(4)
            ]
            return unpacked_from(values, block)

        last = unpacked_planes(
            (lambda x: get_chunk(chunk_ref, t, x)) if odd else take, lane, first_row
        )
        sums = [[None, None] for x in range(WIDE)]
        for m in range(2):
            start, end = take(8 + m * 2), take(9 + m * 2)
            for half in range(2):
                base = bases[half]
                p, q, kappa, inv = found[half][m]
                u = start[half]
                us = [u]
                for x in range(1, WIDE - 1):
                    u = plus(scaled(EPS[m], last[x][half]), times(p, u))
                    us.append(u)
                y = end[half]
                for x in range(WIDE - 1, -1, -1):
                    if x < WIDE - 1:
                        y = plus(times(inv, us[x]), times(q, y))
                    for k in range(2):
                        rows = pl.ds(base + 64 * k, 8)
                        y_ref[m * 16 + x, rows, :] = y_ref[m * 16 + x, rows, :] + y[k]
                    if not odd:
                        sums[x][half] = y if m == 0 else plus(sums[x][half], y)
        if not odd:
            for x in range(8):
                packed = packed_planes(sums, x, lane, first_row)
                put_chunk(chunk_ref, t, x, packed[0], packed[1])


def backward_kernel(
    iterate_hbm, spec_ref, uy_ref, uz_ref, out_hbm, iterate_ref, out_ref, load_sem, store_sem
):
    load = pltpu.make_async_copy(iterate_hbm, iterate_ref, load_sem)
    load.start()
    load.wait()

    def finished(block):
        planes = [2 * block, 2 * block + 1, 16 + 2 * block, 17 + 2 * block]
        stacked = jnp.concatenate([spec_ref[at] for at in planes], axis=1)
        mid = left_dot(uz_ref[...], stacked)
        rows = jnp.concatenate(
            [
                jnp.concatenate([mid[:64, 128 * k : 128 * k + 128], mid[64:, 128 * k : 128 * k + 128]], axis=1)
                for k in range(4)
            ],
            axis=0,
        )
        high, low = halves(rows)
        return right_dot(high, low, uy_ref[0], uy_ref[1])

    def store(block):
        planes = pl.ds(2 * block, 2)
        return pltpu.make_async_copy(out_ref.at[:, planes], out_hbm.at[:, planes], store_sem.at[block])

    def added(block, out):
        for k in range(2):
            x = 2 * block + k
            parts = []
            for m in range(2):
                piece = out[(2 * m + k) * 64 : (2 * m + k) * 64 + 64]
                parts.append((piece[:, :128], piece[:, 128:]))
            for n in range(4):
                total = iterate_ref[n, x]
                for m in range(2):
                    c = COLUMN[m][n]
                    total = total + (2.0 * c.real) * parts[m][0] - (2.0 * c.imag) * parts[m][1]
                out_ref[n, x] = total

    @pl.loop(0, 4)
    def _(i):
        blocks = (2 * i, 2 * i + 1)
        outs = [finished(block) for block in blocks]
        for block, out in zip(blocks, outs):
            added(block, out)

        @pl.when(i > 0)
        def _():
            store(2 * i - 2).start()
            store(2 * i - 1).start()

    store(6).start()
    store(7).start()

    @pl.loop(0, 8)
    def _(block):
        store(block).wait()


def other_places(tm, space, work):
    pair = lax.div(tm, 2)
    x, side = lax.div(space, 2), lax.rem(space, 2)
    places = [
        lax.rem(x + k // 2, SLABS // 2) * 2 + lax.rem(side + k, 2) for k in range(SLABS)
    ]
    for k in range(1, SLABS):
        work(pair, places[k])

    @pl.loop(1, STEPS // 2)
    def _(i):
        other = lax.rem(pair + STEPS // 2 - i, STEPS // 2)
        for k in range(SLABS):
            work(other, places[k])


def whole_kernel(
    remote, velocity_ref, iterate_hbm, right_hbm, kappa_hbm,
    ty_ref, tz_ref, lane_ref, row_ref, own_ref, wave_ref, tg_ref, td_ref, tw_ref, tb_ref,
    y_hbm,
    iterate_ref, right_ref, kappa_ref, y_ref,
    high_a, low_a, high_b, low_b, spec_ref, mixed_ref, below_ref, above_ref, sent_ref,
    chunk_out, chunk_in, chunk_back_out, chunk_back_in, returned_ref,
    got_ref, back_ref, damp_ref, ratio_ref, last_ref, mate_ref, drive_ref, kept_ref, turn_ref,
    load_sem, y_sem, chunk_out_sem, chunk_in_sem, edge_out_sem, below_sem, above_sem,
    gather_sem, arrive_sem, swap_out_sem, swap_in_sem, mate_out_sem, mate_in_sem,
    scatter_sem, return_sem, own_sem,
):
    tm, space = remote.place()
    core = lax.rem(tm, 2)
    owner = lax.div(tm, 2) * SLABS + space

    def rows_of(index, number=1):
        return pl.ds(pl.multiple_of(index * ROWS, 4), number * ROWS)

    def loads(piece):
        planes = pl.ds(2 * piece, 2)
        return [
            remote.local(iterate_hbm.at[:, planes], iterate_ref.at[:, planes], load_sem.at[0, piece]),
            remote.local(right_hbm.at[:, planes], right_ref.at[:, planes], load_sem.at[1, piece]),
            remote.local(kappa_hbm.at[planes], kappa_ref.at[planes], load_sem.at[2, piece]),
        ]

    for piece in range(8):
        for copy in loads(piece):
            copy.start()

    def ready(piece):
        for copy in loads(piece):
            copy.wait()

    mate = (tm + 1 - 2 * core, space)

    def greet(pair, place):
        remote.greet((2 * pair, place))
        remote.greet((2 * pair + 1, place))

    remote.greet(mate)
    other_places(tm, space, greet)

    def middle():
        remote.all_here(2 * OWNERS - 1)
        remote.start(
            kappa_ref.at[WIDE - 1], below_ref, edge_out_sem, below_sem, (tm, lax.rem(space + 1, SLABS))
        )
        remote.start(
            kappa_ref.at[0], above_ref, edge_out_sem, above_sem, (tm, lax.rem(space + SLABS - 1, SLABS))
        )

    keep = jnp.where(tm < STEPS - 1, 1.0, 0.0).astype(f32)
    source_stage(
        keep, ready, middle, velocity_ref, iterate_ref, right_ref, kappa_ref, ty_ref, tz_ref,
        spec_ref, mixed_ref, ((high_a, low_a), (high_b, low_b)),
    )
    remote.wait_got(below_ref, below_sem)
    remote.wait_got(above_ref, above_sem)
    edge_stage(velocity_ref, spec_ref, mixed_ref, below_ref, above_ref, ty_ref, tz_ref)
    is_odd = core == 1

    def chunk_at(ref, t):
        return ref.at[pl.ds(pl.multiple_of(256 * t, 256), 256), :]

    def hand_over(source, target, t, base):
        remote.start(
            chunk_at(source, t), chunk_at(target, t), chunk_out_sem.at[base // 4],
            chunk_in_sem.at[base + t], mate,
        )

    def stage(work, source, target, base):
        @pl.when(jnp.logical_not(is_odd))
        def _():
            def begin(t):
                @pl.when(t > 0)
                def _():
                    hand_over(source, target, t - 1, base)

            work(False, begin, source)
            hand_over(source, target, 3, base)

        @pl.when(is_odd)
        def _():
            work(True, lambda t: remote.wait_got(chunk_at(target, t), chunk_in_sem.at[base + t]), target)

    stage(
        lambda odd, begin, ref: slab_stage(
            odd, begin, velocity_ref, spec_ref, lane_ref, row_ref, y_ref, sent_ref, ref
        ),
        chunk_out, chunk_in, 0,
    )

    pair = lax.div(tm, 2)
    side = lax.rem(pair, 2)
    at_home = side == core
    slot = lax.div(pair, 2) * SLABS + space

    def even_rows(index):
        return pl.ds(pl.multiple_of(index * ROWS + 8, 4), 4)

    def send_even(other, place):
        remote.start(
            sent_ref.at[even_rows(other * SLABS + place), :],
            got_ref.at[pl.ds(pl.multiple_of(slot * LINES + ROWS, 4), 4), :],
            gather_sem, arrive_sem.at[lax.div(pair, 2)], (2 * other + side, place),
        )

    def send_odd(other, place):
        remote.start(
            sent_ref.at[rows_of(other * SLABS + place), :],
            got_ref.at[pl.ds(pl.multiple_of(slot * LINES, 4), ROWS), :],
            gather_sem, arrive_sem.at[lax.div(pair, 2)], (2 * other + side, place),
        )

    @pl.when(is_odd)
    def _():
        other_places(tm, space, send_odd)

        @pl.when(at_home)
        def _():
            got_ref[pl.ds(pl.multiple_of(slot * LINES, 4), ROWS), :] = sent_ref[rows_of(owner), :]

        @pl.when(jnp.logical_not(at_home))
        def _():
            send_odd(pair, space)

    @pl.when(jnp.logical_not(is_odd))
    def _():
        other_places(tm, space, send_even)

        @pl.when(at_home)
        def _():
            got_ref[pl.ds(pl.multiple_of(slot * LINES + ROWS, 4), 4), :] = sent_ref[even_rows(owner), :]

        @pl.when(jnp.logical_not(at_home))
        def _():
            send_even(pair, space)

    solve_modes(
        remote, 2, owner, tm, space, rows_of,
        velocity_ref, own_ref, wave_ref, tg_ref, td_ref, tw_ref, tb_ref, returned_ref,
        got_ref, back_ref, damp_ref, ratio_ref, last_ref, mate_ref, drive_ref, kept_ref, turn_ref,
        arrive_sem, swap_out_sem, swap_in_sem, mate_out_sem, mate_in_sem, scatter_sem, return_sem, own_sem,
    )

    def settle(rows):
        @pl.when(at_home)
        def _():
            remote.wait_got(returned_ref.at[pl.ds(0, (OWNERS - 1) * rows), :], return_sem)
            remote.wait_sent(sent_ref.at[pl.ds(0, (OWNERS - 1) * (LINES - rows)), :], gather_sem)
            remote.wait_sent(back_ref.at[pl.ds(0, (OWNERS // 2) * LINES - rows), :], scatter_sem)

        @pl.when(jnp.logical_not(at_home))
        def _():
            remote.wait_got(returned_ref.at[pl.ds(0, OWNERS * rows), :], return_sem)
            remote.wait_sent(sent_ref.at[pl.ds(0, OWNERS * (LINES - rows)), :], gather_sem)
            remote.wait_sent(back_ref.at[pl.ds(0, (OWNERS // 2) * LINES), :], scatter_sem)

    @pl.when(jnp.logical_not(is_odd))
    def _():
        settle(ROWS)

    @pl.when(is_odd)
    def _():
        settle(4)

    stage(
        lambda odd, begin, ref: finish_stage(
            odd, begin, velocity_ref, lane_ref, row_ref, y_ref, returned_ref, ref
        ),
        chunk_back_out, chunk_back_in, 4,
    )
    keep_y = remote.local(y_ref, y_hbm, y_sem)
    keep_y.start()

    @pl.when(jnp.logical_not(is_odd))
    def _():
        remote.wait_sent(chunk_out, chunk_out_sem.at[0])
        remote.wait_sent(chunk_back_out, chunk_out_sem.at[1])

    remote.wait_sent(kappa_ref.at[pl.ds(0, 2)], edge_out_sem)
    keep_y.wait()


GROUP = 2


def solve_modes(
    remote, share, owner, tm, space, rows_of,
    velocity_ref, own_ref, wave_ref, tg_ref, td_ref, tw_ref, tb_ref, returned_ref,
    got_ref, back_ref, damp_ref, ratio_ref, last_ref, mate_ref, drive_ref, kept_ref, turn_ref,
    arrive_sem, swap_out_sem, swap_in_sem, mate_out_sem, mate_in_sem, scatter_sem, return_sem, own_sem,
):
    pairs = STEPS // 2
    rounds = pairs // share // GROUP
    core = lax.rem(tm, share)
    pair = lax.div(tm, 2)
    at_home = lax.rem(pair, share) == core
    v0, v1, v2 = velocity_ref[0], velocity_ref[1], velocity_ref[2]
    own = own_ref[owner]
    line = [own[k : k + 1, :] for k in range(8)]
    wide = [jnp.broadcast_to(v, (8, 128)) for v in line]
    sign = wide[6]
    cross = cross_symbol(wide[0], wide[1], wide[2], wide[3], v1, v2)
    mu = [MU[0], MU[1], MU[0].conjugate(), MU[1].conjugate()]
    eps = [EPS[0], EPS[1], EPS[0].conjugate(), EPS[1].conjugate()]
    found = [factors(number, cross, v0) for number in mu]

    def crossed(a):
        return (a[0], -(sign * a[1]))

    def times_lanes(v, table):
        return v * table[0] + pltpu.roll(v, 64, 1) * table[1]

    def repeated(v, count):
        return jnp.concatenate([v] * count, axis=0)

    row = lax.broadcasted_iota(jnp.int32, (128, 128), 0).astype(f32)
    turn_ref[:, 0:128] = jnp.where(row == line[4], line[6], 0.0).astype(bf16)
    turn_ref[:, 128:256] = jnp.where(row == line[5], -1.0, 0.0).astype(bf16)

    @pl.loop(0, 16)
    def _(at):
        rows = pl.ds(pl.multiple_of(at * 8, 8), 8)
        symbol = (
            diffusion_number * (2.0 * wave_ref[0, rows, :] - 2.0) + cross[0],
            cross[1] - v0 * wave_ref[1, rows, :],
        )
        total = None
        for m in range(4):
            moved = scaled(mu[m], symbol)
            damp = inverse_of((1.0 - moved[0], -moved[1]))
            for k, value in enumerate(crossed(damp)):
                damp_ref[m, k, rows, :] = value
            term = scaled(eps[m], damp)
            if m < 2:
                for k, value in enumerate(crossed(term)):
                    damp_ref[4 + m, k, rows, :] = value
            total = term if total is None else plus(total, term)
        for k, value in enumerate(crossed(total)):
            ratio_ref[k, rows, :] = value
        power = times(total, total)
        for k, value in enumerate(crossed(power)):
            ratio_ref[4 + k, rows, :] = value
        fourth = times(power, power)
        for k, value in enumerate(crossed(fourth if share == 2 else power)):
            ratio_ref[6 + k, rows, :] = value
        power = fourth
        for k in range(3):
            power = times(power, power)
        closing = inverse_of((1.0 - circulant_alpha * power[0], -circulant_alpha * power[1]))
        for k, value in enumerate(crossed(closing)):
            ratio_ref[2 + k, rows, :] = value

    first_pair = pair - lax.rem(pair, 2)
    roots = [crossed(found[m][0]) for m in range(4)]
    flip = repeated(sign, 16)
    ratio = (ratio_ref.at[0], ratio_ref.at[1])
    square = (ratio_ref.at[4], ratio_ref.at[5])

    def times_refs(v, table):
        return times_lanes(v, (table[0][...], table[1][...]))

    def pair_of(i):
        return lax.rem(first_pair + share * i + core, pairs)

    def wrapped(at, v):
        return jnp.where(at == 0, circulant_alpha, 1.0).astype(f32) * v

    def swap(i):
        remote.start(
            drive_ref.at[pair_of(i)], drive_ref.at[pair_of(i)],
            swap_out_sem, swap_in_sem, (tm + 1 - 2 * core, space),
        )

    last_ref[...] = jnp.zeros((128, 128), f32)

    @pl.loop(0, rounds)
    def _(round_at):
        values, crossings = [], []
        for k in range(GROUP):
            at = pair_of(round_at * GROUP + k)
            slot = lax.div(at, share)
            top = slot * (SLABS * LINES)

            def arrived(rows):
                remote.wait_got(got_ref.at[pl.ds(0, rows), :], arrive_sem.at[slot])

            if k > 0:
                arrived(SLABS * LINES)
            else:
                home = (round_at == 0) & at_home

                @pl.when(home & (core == 0))
                def _():
                    arrived(SLABS * LINES - 4)

                @pl.when(home & (core == 1))
                def _():
                    arrived(SLABS * LINES - ROWS)

                @pl.when(jnp.logical_not(home))
                def _():
                    arrived(SLABS * LINES)

            pieces = [got_ref[pl.ds(top + x * LINES, 8), :] for x in range(SLABS)]
            pieces += [got_ref[pl.ds(top + 8 + f, SLABS, stride=LINES), :] for f in range(8)]
            v = jnp.concatenate(pieces, axis=0)
            values.append(halves(v))
            crossings.append(halves(flip * pltpu.roll(v, 64, 1)))
        stacked = jnp.concatenate([half for pieces in values for half in pieces], axis=0)
        turned = jnp.dot(stacked, turn_ref[...], preferred_element_type=f32).astype(bf16)
        columns, own_points, other_points = [], [], []
        for k in range(GROUP):
            parts = []
            for half in range(2):
                rows = slice(128 * (2 * k + half), 128 * (2 * k + half) + 128)
                parts.append((values[k][half], crossings[k][half], turned[rows, :128], turned[rows, 128:]))
            order = (parts[0], parts[1], parts[0])
            columns.append(jnp.concatenate([piece[:64] for part in order for piece in part], axis=0))
            for step in range(2):
                lines = slice(64 + 32 * step, 96 + 32 * step)
                own_points.append(
                    jnp.concatenate([piece[lines] for part in order for piece in part[:2]], axis=0)
                )
                other_points.append(
                    jnp.concatenate([piece[lines] for part in order for piece in part[2:]], axis=0)
                )
        drive = jnp.dot(tg_ref[...], jnp.concatenate(columns, axis=1), preferred_element_type=f32)
        points = jnp.dot(
            td_ref[...], jnp.concatenate(own_points + other_points, axis=1), preferred_element_type=f32
        )
        for k in range(GROUP):
            at = pair_of(round_at * GROUP + k)
            slot = lax.div(at, share)
            total = drive[:, 128 * k : 128 * k + 128]
            for step, store in ((1, 0), (0, 1)):
                summed = None
                for m in range(4):
                    where = 128 * (2 * k + step + 2 * GROUP * (m // 2))
                    j = m % 2
                    point = times_lanes(points[256 + 8 * j : 264 + 8 * j, where : where + 128], roots[m])
                    d = points[128 * j : 128 * j + 128, where : where + 128] - repeated(point, 16)
                    y = times_lanes(d, (damp_ref[m, 0], damp_ref[m, 1]))
                    summed = y if summed is None else summed + y
                    if m < 2:
                        if store == 1:
                            y = y + times_lanes(early, (damp_ref[4 + m, 0], damp_ref[4 + m, 1]))
                        kept_ref[slot, 2 * store + m] = y
                if store == 0:
                    early = summed
                    total = total + times_refs(summed, ratio)
                else:
                    total = total + summed
            drive_ref[at] = total
            before = wrapped(at - core, last_ref[...])
            last_ref[...] = total + times_lanes(before, (ratio_ref[6], ratio_ref[7]))
        if share > 1:
            @pl.when(round_at > 0)
            def _():
                for k in range(GROUP):
                    swap((round_at - 1) * GROUP + k)

    if share > 1:
        mate = (tm + 1 - 2 * core, space)
        for k in range(GROUP):
            swap((rounds - 1) * GROUP + k)
        remote.start(last_ref, mate_ref, mate_out_sem, mate_in_sem, mate)
        remote.wait_got(mate_ref, mate_in_sem)
        remote.wait_sent(last_ref, mate_out_sem)
        mine, theirs = last_ref[...], mate_ref[...]
        last_ref[...] = jnp.where(core == 0, theirs, mine) + times_refs(
            jnp.where(core == 0, mine, theirs), square
        )
        remote.wait_got(drive_ref.at[pl.ds(0, pairs // 2)], swap_in_sem)

    def following(at, v):
        return drive_ref[at] + times_refs(v, square)

    last_ref[...] = times_lanes(last_ref[...], (ratio_ref[2], ratio_ref[3]))
    kappas = [crossed(found[m][2]) for m in range(2)]
    ups = [crossed(found[m][1]) for m in range(2)]
    flip_all = flip

    def both_parts(v):
        return jnp.concatenate([v, flip_all * pltpu.roll(v, 64, 1)], axis=0)

    x_at, side = lax.div(space, 2), lax.rem(space, 2)
    places = [lax.rem(x_at + k // 2, SLABS // 2) * 2 + lax.rem(side + k, 2) for k in range(SLABS)]
    here = rows_of(owner)

    def send(i):
        at = pair_of(i)
        top = lax.div(at, share) * SLABS

        def put(place, even, odd):
            lines = (top + place) * LINES
            if even is not None:
                even(
                    back_ref.at[pl.ds(pl.multiple_of(lines, 4), ROWS), :], returned_ref.at[here, :],
                    scatter_sem, return_sem, (2 * at, place),
                )
            if odd is not None:
                odd(
                    back_ref.at[pl.ds(pl.multiple_of(lines + ROWS, 4), 4), :],
                    returned_ref.at[pl.ds(pl.multiple_of(owner * ROWS + 8, 4), 4), :],
                    scatter_sem, return_sem, (2 * at + 1, place),
                )

        def stay(source, target, *others):
            target[...] = source[...]

        home = (i == 0) & at_home

        @pl.when(jnp.logical_not(home))
        def _():
            put(places[0], remote.start, remote.start)

        @pl.when(home & (core == 0))
        def _():
            put(places[0], stay, remote.start)

        @pl.when(home & (core == 1))
        def _():
            put(places[0], remote.start, stay)

        for place in places[1:]:
            put(place, remote.start, remote.start)

    @pl.loop(0, rounds)
    def _(round_at):
        inputs = []
        last = last_ref[...]
        for k in range(GROUP):
            mine = None
            for c in range(share):
                at = lax.rem(first_pair + share * (round_at * GROUP + k) + c, pairs)
                last = wrapped(at, last)
                mine = last if mine is None else jnp.where(core == c, last, mine)
                last = following(at, last)
            inputs.append(mine)
        last_ref[...] = last
        packed = left_dot(tw_ref[...], jnp.concatenate([both_parts(v) for v in inputs], axis=1))
        lines = []
        for k in range(GROUP):
            slot = lax.div(pair_of(round_at * GROUP + k), share)
            for step, v in enumerate((inputs[k], times_refs(inputs[k], ratio))):
                for m in range(2):
                    y = times_lanes(v, (damp_ref[4 + m, 0], damp_ref[4 + m, 1]))
                    lines.append(both_parts(y + kept_ref[slot, 2 * step + m]))
        ends = left_dot(tb_ref[...], jnp.concatenate(lines, axis=1))
        for k in range(GROUP):
            top = lax.div(pair_of(round_at * GROUP + k), share) * (SLABS * LINES)
            for x in range(SLABS):
                back_ref[pl.ds(top + x * LINES, 8), :] = packed[8 * x : 8 * x + 8, 128 * k : 128 * k + 128]
            for step in range(2):
                for m in range(2):
                    where = 128 * (4 * k + 2 * step + m)
                    part = [ends[8 * j : 8 * j + 8, where : where + 128] for j in range(3)]
                    u = times_lanes(part[0] - times_lanes(part[1], ups[m]), kappas[m])
                    line = top + 8 + 4 * step + 2 * m
                    back_ref[pl.ds(line, SLABS, stride=LINES), :] = u
                    back_ref[pl.ds(line + 1, SLABS, stride=LINES), :] = part[2]

        @pl.when(round_at > 0)
        def _():
            @pl.loop(0, GROUP)
            def _(k):
                send((round_at - 1) * GROUP + k)

    @pl.loop(0, GROUP)
    def _(k):
        send((rounds - 1) * GROUP + k)

    if share > 1:
        remote.wait_sent(drive_ref.at[pl.ds(0, pairs // 2)], swap_out_sem)


class Remote:
    def place(self):
        return lax.axis_index("tm"), lax.axis_index("space")

    def greet(self, device):
        pl.semaphore_signal(
            pltpu.get_barrier_semaphore(), inc=1, device_id=device, device_id_type=MESH
        )

    def all_here(self, count):
        pl.semaphore_wait(pltpu.get_barrier_semaphore(), count)

    def start(self, source, target, send_sem, recv_sem, device):
        pltpu.make_async_remote_copy(
            src_ref=source, dst_ref=target, send_sem=send_sem, recv_sem=recv_sem,
            device_id=device, device_id_type=MESH,
        ).start()

    def local(self, source, target, sem):
        return pltpu.make_async_copy(source, target, sem)

    def bytes_of(self, ref, sem):
        return pltpu.make_async_remote_copy(
            src_ref=ref, dst_ref=ref, send_sem=sem, recv_sem=sem,
            device_id=self.place(), device_id_type=MESH,
        )

    def wait_sent(self, ref, sem):
        self.bytes_of(ref, sem).wait_send()

    def wait_got(self, ref, sem):
        self.bytes_of(ref, sem).wait_recv()


VMEM, SMEM, ANY = pltpu.VMEM, pltpu.SMEM, pl.ANY


def spec(space):
    return pl.BlockSpec(memory_space=space)


def shape(*dims):
    return jax.ShapeDtypeStruct(dims, f32)


PARAMS = pltpu.CompilerParams(vmem_limit_bytes=60 * 1024 * 1024)


def whole(velocity, iterate, right_side, kappa, remote=Remote(), interpret=False):
    dma = pltpu.SemaphoreType.DMA
    return pl.pallas_call(
        functools.partial(whole_kernel, remote),
        out_shape=shape(32, 128, 128),
        in_specs=[spec(SMEM)] + [spec(ANY)] * 3 + [spec(VMEM)] * 10,
        out_specs=spec(ANY),
        scratch_shapes=[
            VMEM((4, WIDE, NZ, NY), f32), VMEM((4, WIDE, NZ, NY), f32), VMEM((WIDE, NZ, NY), f32),
            VMEM((32, 128, 128), f32),
        ]
        + [VMEM((256, 256), bf16)] * 4
        + [
            VMEM((44, 128, 128), f32), VMEM((8, NZ, NY), f32), VMEM((NZ, NY), f32), VMEM((NZ, NY), f32),
            VMEM((OWNERS * ROWS, 128), f32),
            VMEM((1024, 128), f32), VMEM((1024, 128), f32), VMEM((1024, 128), f32), VMEM((1024, 128), f32),
            VMEM((OWNERS * ROWS, 128), f32),
            VMEM((OWNERS // 2 * LINES, 128), f32), VMEM((OWNERS // 2 * LINES, 128), f32),
            VMEM((6, 2, 128, 128), f32), VMEM((8, 128, 128), f32), VMEM((128, 128), f32), VMEM((128, 128), f32),
            VMEM((STEPS // 2, 128, 128), f32), VMEM((STEPS // 4, 4, 128, 128), f32), VMEM((128, 256), bf16),
            dma((3, 8)), dma, dma((2,)), dma((8,)), dma, dma, dma,
            dma, dma((STEPS // 4,)), dma, dma, dma, dma, dma, dma, dma,
        ],
        compiler_params=pltpu.CompilerParams(
            vmem_limit_bytes=60 * 1024 * 1024, has_side_effects=True, collective_id=0
        ),
        interpret=interpret,
        name="whole",
    )(
        velocity, iterate, right_side, kappa,
        TABLES["ty"], TABLES["tz"], TABLES["lane"], TABLES["row"], TABLES["own"], TABLES["wave_x"],
        TABLES["tg"], TABLES["td"], TABLES["tw"], TABLES["tb"],
    )


def backward(iterate, y, interpret=False):
    return pl.pallas_call(
        backward_kernel,
        out_shape=shape(4, WIDE, NZ, NY),
        in_specs=[spec(ANY)] + [spec(VMEM)] * 3,
        out_specs=spec(ANY),
        scratch_shapes=[
            VMEM((4, WIDE, NZ, NY), f32), VMEM((4, WIDE, NZ, NY), f32),
            pltpu.SemaphoreType.DMA, pltpu.SemaphoreType.DMA((8,)),
        ],
        compiler_params=PARAMS,
        interpret=interpret,
        name="backward",
    )(iterate, y, TABLES["uy"], TABLES["uz"])


def shards(iterate, right_side, diffusivity, velocity):
    iterate, right_side = iterate[0], right_side[0]
    y = whole(velocity, iterate, right_side, diffusivity)
    return backward(iterate, y)[None]


def solution(mesh):
    placed = (
        P("tm", None, "space", None, None),
        P("tm", None, "space", None, None),
        P("space", None, None),
        P(),
    )
    return jax.shard_map(
        shards,
        mesh=mesh,
        in_specs=placed,
        out_specs=P("tm", None, "space", None, None),
        check_vma=False,
    )
```

```python
import functools
import math

import jax
import jax.numpy as jnp
import numpy as np
from jax import lax
from jax.experimental import pallas as pl
from jax.experimental.pallas import tpu as pltpu
from jax.sharding import PartitionSpec as P

NX, NY, NZ, STEPS = 128, 128, 64, 32
SLABS, WIDE = 8, 16
OWNERS = 128
ROWS = 12
LINES = 16
MESH = pl.DeviceIdType.MESH
f32, bf16 = jnp.float32, jnp.bfloat16

diffusion_number = 16.0
circulant_alpha = 0.1


def collocation_matrix():
    radau_nodes = [0.08858795951270394, 0.4094668644407347, 0.7876594617608471, 1.0]
    matrix = [[0.0] * 4 for row_index in range(4)]
    for column_index in range(4):
        coefficients = [1.0]
        for other_index in range(4):
            if other_index != column_index:
                scale_value = 1.0 / (radau_nodes[column_index] - radau_nodes[other_index])
                shifted = [0.0] + [value * scale_value for value in coefficients]
                lowered = [
                    -radau_nodes[other_index] * scale_value * value for value in coefficients
                ] + [0.0]
                coefficients = [
                    left_value + right_value for left_value, right_value in zip(shifted, lowered)
                ]
        for row_index in range(4):
            total = 0.0
            for power_index in range(len(coefficients)):
                total = total + coefficients[power_index] * radau_nodes[row_index] ** (
                    power_index + 1
                ) / (power_index + 1)
            matrix[row_index][column_index] = total
    return matrix


def solve_system(matrix, target):
    count = len(target)
    rows_list = [list(matrix[row_index]) + [target[row_index]] for row_index in range(count)]
    for column in range(count):
        best_row = column
        for candidate in range(column + 1, count):
            if abs(rows_list[candidate][column]) > abs(rows_list[best_row][column]):
                best_row = candidate
        saved_row = rows_list[column]
        rows_list[column] = rows_list[best_row]
        rows_list[best_row] = saved_row
        leader = rows_list[column][column]
        for other_row in range(count):
            if other_row != column:
                factor = rows_list[other_row][column] / leader
                rows_list[other_row] = [
                    left_value - factor * right_value
                    for left_value, right_value in zip(rows_list[other_row], rows_list[column])
                ]
    return [
        rows_list[row_index][count] / rows_list[row_index][row_index] for row_index in range(count)
    ]


def node_basis():
    matrix = collocation_matrix()
    helper = [[0.0] * 4 for row_index in range(4)]
    coefficients = [0.0, 0.0, 0.0, 0.0, 1.0]
    for order in range(1, 5):
        product = [
            [
                sum((matrix[row_index][inner] * helper[inner][column] for inner in range(4)))
                for column in range(4)
            ]
            for row_index in range(4)
        ]
        for row_index in range(4):
            product[row_index][row_index] = product[row_index][row_index] + coefficients[5 - order]
        helper = product
        trace_value = sum(
            (
                sum((matrix[row_index][inner] * helper[inner][row_index] for inner in range(4)))
                for row_index in range(4)
            )
        )
        coefficients[4 - order] = -trace_value / order
    roots_list = [(0.4 + 0.9j) ** power_index for power_index in range(4)]
    for sweep in range(400):
        for root_index in range(4):
            current = roots_list[root_index]
            numer = 0.0
            for power_index in range(4, -1, -1):
                numer = numer * current + coefficients[power_index]
            denom = 1.0
            for other_index in range(4):
                if other_index != root_index:
                    denom = denom * (current - roots_list[other_index])
            roots_list[root_index] = current - numer / denom
    vectors = [[0.0] * 4 for row_index in range(4)]
    for root_index in range(4):
        shifted = [
            [
                matrix[row_index][column] - (roots_list[root_index] if row_index == column else 0.0)
                for column in range(3)
            ]
            for row_index in range(3)
        ]
        target = [-matrix[row_index][3] for row_index in range(3)]
        parts = solve_system(shifted, target) + [1.0 + 0j]
        for row_index in range(4):
            vectors[row_index][root_index] = parts[row_index]
    inverse = [[0.0] * 4 for row_index in range(4)]
    for column in range(4):
        unit = [1.0 if row_index == column else 0.0 for row_index in range(4)]
        parts = solve_system(vectors, unit)
        for row_index in range(4):
            inverse[row_index][column] = parts[row_index]
    weights = [sum((inverse[row_index][column] for column in range(4))) for row_index in range(4)]
    return (roots_list, vectors, inverse, weights)


VALUES, VECTORS, INVERSE, WEIGHTS = node_basis()
PAIRS = [m for m in range(4) if complex(VALUES[m]).imag > 0]
MU = [complex(VALUES[m]) for m in PAIRS]
COLUMN = [[complex(VECTORS[n][m]) for n in range(4)] for m in PAIRS]
ROW = [[complex(INVERSE[m][n]) for n in range(4)] for m in PAIRS]
EPS = [complex(WEIGHTS[m]) for m in PAIRS]


def wave_order_z():
    index = np.arange(NZ)
    return np.where(index <= NZ // 2, index, NZ + NZ // 2 - index)


def wave_order_y():
    lane = np.arange(NY)
    index = 16 * (lane // 32) + lane % 16
    return np.where(lane % 32 < 16, index, np.where(index == 0, NY // 2, NY - index))


def split(values):
    values = np.asarray(values, np.float64)
    high = values.astype(np.float32).astype(bf16)
    low = (values - high.astype(np.float64)).astype(np.float32).astype(bf16)
    return high, low


def side_table(values):
    high, low = split(values)
    return np.concatenate([high, high, low], axis=1)


def halves(x):
    high = x.astype(bf16)
    return high, (x - high.astype(f32)).astype(bf16)


def left_dot(table, x):
    high, low = halves(x)
    return jnp.dot(table, jnp.concatenate([high, low, high], axis=0), preferred_element_type=f32)


def right_dot(high, low, table_high, table_low):
    return (
        jnp.dot(high, table_high, preferred_element_type=f32)
        + jnp.dot(low, table_high, preferred_element_type=f32)
        + jnp.dot(high, table_low, preferred_element_type=f32)
    )


def complex_block(matrix):
    return np.block([[matrix.real, -matrix.imag], [matrix.imag, matrix.real]])


def make_tables():
    ky, kz = wave_order_y(), wave_order_z()
    kx, x = np.arange(NX), np.arange(NX)
    to_y = np.exp(-2j * np.pi * np.outer(ky, np.arange(NY)) / NY)
    to_z = np.exp(-2j * np.pi * np.outer(kz, np.arange(NZ)) / NZ)
    tables = {}
    tables["ty"] = np.stack(split(complex_block(to_y).T))
    tables["tz"] = side_table(complex_block(to_z))
    tables["uy"] = np.stack(split(complex_block(np.conj(to_y.T) / NY).T))
    tables["uz"] = side_table(complex_block(np.conj(to_z.T) / NZ))
    cells = (np.arange(SLABS)[:, None] * WIDE + np.arange(8)[None, :]).reshape(-1)
    theta = 2 * np.pi * kx / NX
    at = np.exp(-1j * np.outer(theta, cells))
    shifted = np.exp(-8j * theta)[:, None]
    from_own = at * (1 - 1j * shifted) / 2
    from_partner = at * (1 + 1j * shifted) / 2
    firsts = np.arange(SLABS) * WIDE

    def lane_block(matrix):
        return np.concatenate([matrix.real, -matrix.imag], axis=1)

    tables["tg"] = side_table(np.concatenate([lane_block(from_own), lane_block(from_partner)], axis=1))

    def point_rows(waves, shifts):
        out = []
        for m in range(2):
            table = np.zeros((len(waves), 4, SLABS), complex)
            for field, shift in shifts:
                table[:, 2 * m + field] = np.exp(-1j * np.outer(waves, firsts + shift))
            out.append(table.reshape(len(waves), 4 * SLABS))
        return out

    tables["td"] = side_table(
        lane_block(
            np.concatenate(
                point_rows(theta, ((0, WIDE), (1, -1))) + point_rows(theta[:8], ((1, 0),)), axis=0
            )
        )
    )
    back = np.exp(1j * np.outer(cells, theta)) * (1 + 1j * np.exp(8j * theta))[None, :] / NX
    tables["tw"] = side_table(lane_block(back))
    ends = [np.exp(1j * np.outer(firsts + k, theta)) / NX for k in (0, 1, 15)]
    tables["tb"] = side_table(lane_block(np.concatenate(ends, axis=0)))
    trig_y = 2 * np.pi * ky / NY
    trig_z = 2 * np.pi * kz / NZ
    tables["lane"] = np.stack([np.cos(trig_y), np.sin(trig_y)]).astype(np.float32)
    tables["row"] = np.stack(
        [np.broadcast_to(v[:, None], (NZ, NY)) for v in (np.cos(trig_z), np.sin(trig_z))]
    ).astype(np.float32)
    tables["wave_x"] = np.stack(
        [np.broadcast_to(v[:, None], (NX, 128)) for v in (np.cos(theta), np.sin(theta))]
    ).astype(np.float32)
    lane = np.arange(128)
    own = np.zeros((OWNERS, 8, 128))
    for owner in range(OWNERS):
        part, pair = owner // 32, owner % 32
        piece = (lane // 32 - part) % 4
        at_y, row = (lane - 32 * piece) % 128, piece % 2
        other_y = np.where((at_y == 0) | (at_y == 16), at_y, at_y ^ 16)
        other_row = row if pair == 0 else 1 - row
        other = (other_y + 32 * (2 * (piece // 2) + other_row)) % 128
        y, z = trig_y[at_y], trig_z[pair + 32 * row]
        own[owner] = np.stack(
            [
                np.cos(y), np.sin(y), np.cos(z), np.sin(z),
                other, np.roll(other, -64), np.where(piece < 2, 1.0, -1.0), (lane + 64) % 128,
            ]
        )
    tables["own"] = own.astype(np.float32)
    return tables


TABLES = make_tables()


def times(a, b):
    return (a[0] * b[0] - a[1] * b[1], a[0] * b[1] + a[1] * b[0])


def plus(a, b):
    return (a[0] + b[0], a[1] + b[1])


def minus(a, b):
    return (a[0] - b[0], a[1] - b[1])


def scaled(number, a):
    return (number.real * a[0] - number.imag * a[1], number.real * a[1] + number.imag * a[0])


def inverse_of(a):
    size = 1.0 / (a[0] * a[0] + a[1] * a[1])
    return (a[0] * size, -a[1] * size)


def root_of(a):
    size = jnp.sqrt(a[0] * a[0] + a[1] * a[1])
    main = jnp.sqrt(0.5 * (size + jnp.abs(a[0])))
    other = a[1] / (2.0 * main)
    positive = a[0] >= 0.0
    return (
        jnp.where(positive, main, jnp.abs(other)),
        jnp.where(positive, other, jnp.where(a[1] >= 0.0, main, -main)),
    )


def cross_symbol(cos_y, sin_y, cos_z, sin_z, v1, v2):
    return (
        diffusion_number * ((2.0 * cos_y - 2.0) + (2.0 * cos_z - 2.0)),
        -(v1 * sin_y + v2 * sin_z),
    )


def factors(mu, cross, v0):
    c_up = -mu.real * (diffusion_number - 0.5 * v0), -mu.imag * (diffusion_number - 0.5 * v0)
    c_down = -mu.real * (diffusion_number + 0.5 * v0), -mu.imag * (diffusion_number + 0.5 * v0)
    moved = scaled(mu, cross)
    c_mid = (1.0 + 2.0 * diffusion_number * mu.real - moved[0], 2.0 * diffusion_number * mu.imag - moved[1])
    product = times(c_up, c_down)
    square = times(c_mid, c_mid)
    root = root_of((square[0] - 4.0 * product[0], square[1] - 4.0 * product[1]))
    same = c_mid[0] * root[0] + c_mid[1] * root[1] >= 0.0
    kappa = (
        0.5 * (c_mid[0] + jnp.where(same, root[0], -root[0])),
        0.5 * (c_mid[1] + jnp.where(same, root[1], -root[1])),
    )
    inv = inverse_of(kappa)
    p = times(inv, c_down)
    q = times(inv, c_up)
    return (-p[0], -p[1]), (-q[0], -q[1]), kappa, inv


def plane_partner(low, high, lane, first_row):
    ends = (lane == 0) | (lane == 16)
    first = (lane % 32) < 16

    def turned(v):
        return jnp.where(ends, v, jnp.where(first, pltpu.roll(v, 112, 1), pltpu.roll(v, 16, 1)))

    low_turned, high_turned = [turned(v) for v in low], [turned(v) for v in high]
    to_low = [jnp.where(first_row, a, b) for a, b in zip(low_turned, high_turned)]
    to_high = [jnp.where(first_row, b, a) for a, b in zip(low_turned, high_turned)]
    return (to_low[0], -to_low[1]), (to_high[0], -to_high[1])


def packed_for(low, high, block):
    pieces = [low[0], high[0], low[1], high[1]]
    pieces = [pieces[0]] + [pltpu.roll(pieces[c], 32 * c, 1) for c in (1, 2, 3)]
    out = []
    for h in range(4):
        value = pieces[3]
        for c in (2, 1, 0):
            value = jnp.where(block == (h + c) % 4, pieces[c], value)
        out.append(value)
    return out


def unpacked_from(values, block):
    out = []
    for c in range(4):
        piece = values[(3 - c) % 4]
        for d in (2, 1, 0):
            piece = jnp.where(block == d, values[(d - c) % 4], piece)
        out.append(piece if c == 0 else pltpu.roll(piece, 128 - 32 * c, 1))
    return (out[0], out[2]), (out[1], out[3])


def chunk_factors(t, lane_ref, row_ref, velocity_ref, mu):
    cos_y, sin_y = lane_ref[0:1, :], lane_ref[1:2, :]
    found = []
    for base in (0, 32):
        rows = pl.ds(pl.multiple_of(base + 8 * t, 8), 8)
        cross = cross_symbol(
            cos_y, sin_y, row_ref[0, rows, :], row_ref[1, rows, :], velocity_ref[1], velocity_ref[2]
        )
        found.append([factors(number, cross, velocity_ref[0]) for number in mu])
    return found


def dft_block(high, low, ty_ref, tz_ref):
    mid = right_dot(high, low, ty_ref[0], ty_ref[1])
    stacked = jnp.concatenate(
        [
            jnp.concatenate([mid[64 * k : 64 * k + 64, :128], mid[64 * k : 64 * k + 64, 128:]], axis=0)
            for k in range(4)
        ],
        axis=1,
    )
    return left_dot(tz_ref[...], stacked)


def put_rows(slot, at, real, imag):
    for k, part in enumerate((real, imag)):
        for ref, value in zip(slot, halves(part)):
            ref[64 * at : 64 * at + 64, k * 128 : (k + 1) * 128] = value


def mixture(m, groups):
    real = imag = None
    for scale, values in groups:
        for n in range(4):
            factor = scale * ROW[m][n]
            a, b = factor.real * values[n], factor.imag * values[n]
            real = a if real is None else real + a
            imag = b if imag is None else imag + b
    return real, imag


def source_stage(
    keep, ready, middle, velocity_ref, iterate_ref, right_ref, kappa_ref, ty_ref, tz_ref, spec_ref, mixed_ref, slots,
):
    v0, v1, v2 = velocity_ref[0], velocity_ref[1], velocity_ref[2]

    def stencil(x, slot, at, below, above):
        plain, applied = [], []
        kappa = diffusion_number * kappa_ref[x]
        for n in range(4):
            f = iterate_ref[n, x]
            up_z, down_z = pltpu.roll(f, NZ - 1, 0), pltpu.roll(f, 1, 0)
            up_y, down_y = pltpu.roll(f, NY - 1, 1), pltpu.roll(f, 1, 1)
            total = (up_z + down_z) + (up_y + down_y) - 6.0 * f
            moved = v1 * (up_y - down_y) + v2 * (up_z - down_z)
            if above:
                up_x = iterate_ref[n, x + 1]
                total, moved = total + up_x, moved + v0 * up_x
            if below:
                down_x = iterate_ref[n, x - 1]
                total, moved = total + down_x, moved - v0 * down_x
            applied.append(kappa * total - 0.5 * moved)
            plain.append(right_ref[n, x] - f)
        for m in range(2):
            put_rows(slot, 2 * m + at, *mixture(m, [(1.0, plain), (MU[m], applied)]))

    def produce(block, slot, first=False, final=False):
        stencil(2 * block, slot, 0, not first, True)
        stencil(2 * block + 1, slot, 1, True, not final)

    def last_node(block, slot):
        for k in range(4):
            x = 4 * block + k
            put_rows(slot, k, keep * iterate_ref[3, x], keep * iterate_ref[3, x + 8])

    def transformed(block, slot):
        out = dft_block(slot[0][...], slot[1][...], ty_ref, tz_ref)
        for k in range(4):
            spec_ref[block * 4 + k] = out[:, 128 * k : 128 * k + 128]

    first, second = slots
    ready(0)
    ready(1)
    produce(0, first, first=True)

    @pl.loop(0, 3)
    def _(i):
        ready(2 * i + 2)
        transformed(2 * i, first)
        produce(2 * i + 1, second)
        ready(2 * i + 3)
        transformed(2 * i + 1, second)
        produce(2 * i + 2, first)

    middle()
    for side, x in enumerate((0, WIDE - 1)):
        for m in range(2):
            real, imag = mixture(m, [(MU[m], [iterate_ref[n, x] for n in range(4)])])
            mixed_ref[side * 4 + m * 2] = real
            mixed_ref[side * 4 + m * 2 + 1] = imag
    transformed(6, first)
    produce(7, second, final=True)
    transformed(7, second)
    last_node(0, first)
    transformed(8, first)
    last_node(1, second)
    transformed(9, second)


def put_chunk(ref, t, x, low, high):
    for k, value in enumerate((low[0], high[0], low[1], high[1])):
        ref[pl.ds(pl.multiple_of(256 * t + 32 * x + 8 * k, 8), 8), :] = value


def get_chunk(ref, t, x):
    parts = [ref[pl.ds(pl.multiple_of(256 * t + 32 * x + 8 * k, 8), 8), :] for k in range(4)]
    return (parts[0], parts[2]), (parts[1], parts[3])


def packed_planes(sums, x, lane, first_row):
    own, other = [], []
    for half in range(2):
        first, second = sums[x][half], sums[x + 8][half]
        own.append((first[0] - second[1], first[1] + second[0]))
        other.append((first[0] + second[1], first[1] - second[0]))
    partners = plane_partner(other[0], other[1], lane, first_row)
    return [plus(own[half], partners[half]) for half in range(2)]


def unpacked_planes(fetch, lane, first_row):
    last = [[None, None] for x in range(WIDE)]
    for x in range(8):
        packed = fetch(x)
        partners = plane_partner(packed[0], packed[1], lane, first_row)
        for half in range(2):
            both, apart = plus(packed[half], partners[half]), minus(packed[half], partners[half])
            last[x][half] = (0.5 * both[0], 0.5 * both[1])
            last[x + 8][half] = (0.5 * apart[1], -0.5 * apart[0])
    return last


def edge_stage(velocity_ref, spec_ref, mixed_ref, below_ref, above_ref, ty_ref, tz_ref):
    v0 = velocity_ref[0]
    outer = [diffusion_number * below_ref[...] - 0.5 * v0, diffusion_number * above_ref[...] + 0.5 * v0]
    edges = [
        jnp.concatenate([outer[side] * mixed_ref[side * 4 + m * 2 + part] for part in range(2)], axis=1)
        for m in range(2)
        for side in range(2)
    ]
    high, low = halves(jnp.concatenate(edges, axis=0))
    out = dft_block(high, low, ty_ref, tz_ref)
    for k in range(4):
        spec_ref[40 + k] = out[:, 128 * k : 128 * k + 128]


def slab_stage(odd, begin, velocity_ref, spec_ref, lane_ref, row_ref, y_ref, send_ref, chunk_ref):
    lane = lax.broadcasted_iota(jnp.int32, (8, 128), 1)
    sub = lax.broadcasted_iota(jnp.int32, (8, 128), 0)
    block = lane // 32

    @pl.loop(0, 4)
    def _(t):
        begin(t)
        first_row = (sub + t) == 0
        found = chunk_factors(t, lane_ref, row_ref, velocity_ref, MU)
        bases = [pl.multiple_of(base + 8 * t, 8) for base in (0, 32)]
        if odd:
            last = unpacked_planes(lambda x: get_chunk(chunk_ref, t, x), lane, first_row)

        def plane(at, base):
            return spec_ref[at, pl.ds(base, 8), :], spec_ref[at, pl.ds(base + 64, 8), :]

        def field(m, x, half):
            value = plane(4 * (x // 2) + 2 * m + x % 2, bases[half])
            return plus(value, scaled(EPS[m], last[x][half])) if odd else value

        def send(value, low, high):
            for h, packed in enumerate(packed_for(low, high, block)):
                send_ref[pl.ds((32 * h + 8 * t) * ROWS + value, 8, stride=ROWS), :] = packed

        sums = [[None, None] for x in range(WIDE)]
        for m in range(2):
            carries = []
            for half in range(2):
                base = bases[half]
                p, q, kappa, inv = found[half][m]
                under, over = plane(40 + 2 * m, base), plane(41 + 2 * m, base)
                u = plus(field(m, 0, half), times(p, under))
                us = [u]
                for x in range(1, WIDE):
                    u = plus(field(m, x, half), times(p, u))
                    us.append(u)
                outflow = plus(times(p, us[-1]), over)
                y = us[-1]
                for x in range(WIDE - 1, -1, -1):
                    if x < WIDE - 1:
                        y = plus(us[x], times(q, y))
                    z = times(inv, y)
                    y_ref[m * 16 + x, pl.ds(base, 8), :] = z[0]
                    y_ref[m * 16 + x, pl.ds(base + 64, 8), :] = z[1]
                    sums[x][half] = z if m == 0 else plus(sums[x][half], z)
                carries.append((outflow, plus(times(q, y), under)))
            for k in range(2):
                send(8 + m * 2 + k, carries[0][k], carries[1][k])
        for x in range(8):
            packed = packed_planes(sums, x, lane, first_row)
            packed = [plus(packed[half], plane(32 + x, bases[half])) for half in range(2)]
            if odd:
                send(x, packed[0], packed[1])
            else:
                put_chunk(chunk_ref, t, x, packed[0], packed[1])


def finish_stage(odd, begin, velocity_ref, lane_ref, row_ref, y_ref, got_ref, chunk_ref):
    lane = lax.broadcasted_iota(jnp.int32, (8, 128), 1)
    sub = lax.broadcasted_iota(jnp.int32, (8, 128), 0)
    block = lane // 32

    @pl.loop(0, 4)
    def _(t):
        begin(t)
        first_row = (sub + t) == 0
        found = chunk_factors(t, lane_ref, row_ref, velocity_ref, MU)
        bases = [pl.multiple_of(base + 8 * t, 8) for base in (0, 32)]

        def take(value):
            values = [
                got_ref[pl.ds((32 * h + 8 * t) * ROWS + value, 8, stride=ROWS), :] for h in range(4)
            ]
            return unpacked_from(values, block)

        last = unpacked_planes(
            (lambda x: get_chunk(chunk_ref, t, x)) if odd else take, lane, first_row
        )
        sums = [[None, None] for x in range(WIDE)]
        for m in range(2):
            start, end = take(8 + m * 2), take(9 + m * 2)
            for half in range(2):
                base = bases[half]
                p, q, kappa, inv = found[half][m]
                u = start[half]
                us = [u]
                for x in range(1, WIDE - 1):
                    u = plus(scaled(EPS[m], last[x][half]), times(p, u))
                    us.append(u)
                y = end[half]
                for x in range(WIDE - 1, -1, -1):
                    if x < WIDE - 1:
                        y = plus(times(inv, us[x]), times(q, y))
                    for k in range(2):
                        rows = pl.ds(base + 64 * k, 8)
                        y_ref[m * 16 + x, rows, :] = y_ref[m * 16 + x, rows, :] + y[k]
                    if not odd:
                        sums[x][half] = y if m == 0 else plus(sums[x][half], y)
        if not odd:
            for x in range(8):
                packed = packed_planes(sums, x, lane, first_row)
                put_chunk(chunk_ref, t, x, packed[0], packed[1])


def backward_kernel(
    iterate_hbm, spec_hbm, uy_ref, uz_ref, out_hbm, spec_ref, iterate_ref, out_ref, load_sem, store_sem
):
    def loads(group):
        planes = pl.ds(4 * group, 4)
        upper = pl.ds(16 + 4 * group, 4)
        return [
            pltpu.make_async_copy(spec_hbm.at[planes], spec_ref.at[planes], load_sem.at[0, group]),
            pltpu.make_async_copy(spec_hbm.at[upper], spec_ref.at[upper], load_sem.at[1, group]),
            pltpu.make_async_copy(
                iterate_hbm.at[:, planes], iterate_ref.at[:, planes], load_sem.at[2, group]
            ),
        ]

    for group in range(4):
        for copy in loads(group):
            copy.start()

    def finished(block):
        planes = [2 * block, 2 * block + 1, 16 + 2 * block, 17 + 2 * block]
        stacked = jnp.concatenate([spec_ref[at] for at in planes], axis=1)
        mid = left_dot(uz_ref[...], stacked)
        rows = jnp.concatenate(
            [
                jnp.concatenate([mid[:64, 128 * k : 128 * k + 128], mid[64:, 128 * k : 128 * k + 128]], axis=1)
                for k in range(4)
            ],
            axis=0,
        )
        high, low = halves(rows)
        return right_dot(high, low, uy_ref[0], uy_ref[1])

    def store(block):
        planes = pl.ds(2 * block, 2)
        return pltpu.make_async_copy(out_ref.at[:, planes], out_hbm.at[:, planes], store_sem.at[block])

    def added(block, out):
        for k in range(2):
            x = 2 * block + k
            parts = []
            for m in range(2):
                piece = out[(2 * m + k) * 64 : (2 * m + k) * 64 + 64]
                parts.append((piece[:, :128], piece[:, 128:]))
            for n in range(4):
                total = iterate_ref[n, x]
                for m in range(2):
                    c = COLUMN[m][n]
                    total = total + (2.0 * c.real) * parts[m][0] - (2.0 * c.imag) * parts[m][1]
                out_ref[n, x] = total

    pending = None
    for group in range(4):
        for copy in loads(group):
            copy.wait()
        blocks = (2 * group, 2 * group + 1)
        outs = [finished(block) for block in blocks]
        if pending is not None:
            for block, out in pending:
                added(block, out)
        pending = list(zip(blocks, outs))
        if group > 1:
            store(2 * group - 4).start()
            store(2 * group - 3).start()
    for block, out in pending:
        added(block, out)
    for block in range(4, 8):
        store(block).start()
    for block in range(8):
        store(block).wait()


def other_places(tm, space, work):
    pair = lax.div(tm, 2)
    x, side = lax.div(space, 2), lax.rem(space, 2)
    places = [
        lax.rem(x + k // 2, SLABS // 2) * 2 + lax.rem(side + k, 2) for k in range(SLABS)
    ]
    for k in range(1, SLABS):
        work(pair, places[k])

    @pl.loop(1, STEPS // 2)
    def _(i):
        other = lax.rem(pair + STEPS // 2 - i, STEPS // 2)
        for k in range(SLABS):
            work(other, places[k])


def whole_kernel(
    remote, velocity_ref, iterate_hbm, right_hbm, kappa_hbm,
    ty_ref, tz_ref, lane_ref, row_ref, own_ref, wave_ref, tg_ref, td_ref, tw_ref, tb_ref,
    y_hbm,
    iterate_ref, right_ref, kappa_ref, y_ref,
    high_a, low_a, high_b, low_b, spec_ref, mixed_ref, below_ref, above_ref, sent_ref,
    chunk_out, chunk_in, chunk_back_out, chunk_back_in, returned_ref,
    got_ref, back_ref, damp_ref, ratio_ref, last_ref, mate_ref, drive_ref, kept_ref, turn_ref,
    vouch_sem, load_sem, y_sem, chunk_out_sem, chunk_in_sem, edge_out_sem, below_sem, above_sem,
    gather_sem, arrive_sem, swap_out_sem, swap_in_sem, mate_out_sem, mate_in_sem,
    scatter_sem, return_sem, own_sem,
):
    tm, space = remote.place()
    core = lax.rem(tm, 2)
    owner = lax.div(tm, 2) * SLABS + space

    def rows_of(index, number=1):
        return pl.ds(pl.multiple_of(index * ROWS, 4), number * ROWS)

    def loads(piece):
        planes = pl.ds(2 * piece, 2)
        return [
            remote.local(iterate_hbm.at[:, planes], iterate_ref.at[:, planes], load_sem.at[0, piece]),
            remote.local(right_hbm.at[:, planes], right_ref.at[:, planes], load_sem.at[1, piece]),
            remote.local(kappa_hbm.at[planes], kappa_ref.at[planes], load_sem.at[2, piece]),
        ]

    for piece in range(8):
        for copy in loads(piece):
            copy.start()

    def ready(piece):
        for copy in loads(piece):
            copy.wait()

    mate = (tm + 1 - 2 * core, space)

    for k in range(1, SLABS):
        remote.greet((tm, lax.rem(space + k, SLABS)))

    @pl.loop(1, STEPS)
    def _(k):
        remote.greet((lax.rem(tm + k, STEPS), space))

    def middle():
        remote.all_here(SLABS + STEPS - 2)
        for k in range(1, SLABS):
            remote.vouch(vouch_sem, (tm, lax.rem(space + k, SLABS)))
        remote.start(
            kappa_ref.at[WIDE - 1], below_ref, edge_out_sem, below_sem, (tm, lax.rem(space + 1, SLABS))
        )
        remote.start(
            kappa_ref.at[0], above_ref, edge_out_sem, above_sem, (tm, lax.rem(space + SLABS - 1, SLABS))
        )

    keep = jnp.where(tm < STEPS - 1, 1.0, 0.0).astype(f32)
    source_stage(
        keep, ready, middle, velocity_ref, iterate_ref, right_ref, kappa_ref, ty_ref, tz_ref,
        spec_ref, mixed_ref, ((high_a, low_a), (high_b, low_b)),
    )
    remote.wait_got(below_ref, below_sem)
    remote.wait_got(above_ref, above_sem)
    edge_stage(velocity_ref, spec_ref, mixed_ref, below_ref, above_ref, ty_ref, tz_ref)
    is_odd = core == 1

    def chunk_at(ref, t):
        return ref.at[pl.ds(pl.multiple_of(256 * t, 256), 256), :]

    def hand_over(source, target, t, base):
        remote.start(
            chunk_at(source, t), chunk_at(target, t), chunk_out_sem.at[base // 4],
            chunk_in_sem.at[base + t], mate,
        )

    def stage(work, source, target, base, done):
        @pl.when(jnp.logical_not(is_odd))
        def _():
            def begin(t):
                done(t)

                @pl.when(t > 0)
                def _():
                    hand_over(source, target, t - 1, base)

            work(False, begin, source)
            hand_over(source, target, 3, base)

        @pl.when(is_odd)
        def _():
            def begin(t):
                done(t)
                remote.wait_got(chunk_at(target, t), chunk_in_sem.at[base + t])

            work(True, begin, target)

    stage(
        lambda odd, begin, ref: slab_stage(
            odd, begin, velocity_ref, spec_ref, lane_ref, row_ref, y_ref, sent_ref, ref
        ),
        chunk_out, chunk_in, 0, lambda t: None,
    )

    remote.vouched(vouch_sem, SLABS - 1)

    pair = lax.div(tm, 2)
    side = lax.rem(pair, 2)
    at_home = side == core
    slot = lax.div(pair, 2) * SLABS + space

    def even_rows(index):
        return pl.ds(pl.multiple_of(index * ROWS + 8, 4), 4)

    def send_even(other, place):
        remote.start(
            sent_ref.at[even_rows(other * SLABS + place), :],
            got_ref.at[pl.ds(pl.multiple_of(slot * LINES + ROWS, 4), 4), :],
            gather_sem, arrive_sem.at[lax.div(pair, 2)], (2 * other + side, place),
        )

    def send_odd(other, place):
        remote.start(
            sent_ref.at[rows_of(other * SLABS + place), :],
            got_ref.at[pl.ds(pl.multiple_of(slot * LINES, 4), ROWS), :],
            gather_sem, arrive_sem.at[lax.div(pair, 2)], (2 * other + side, place),
        )

    @pl.when(is_odd)
    def _():
        other_places(tm, space, send_odd)

        @pl.when(at_home)
        def _():
            got_ref[pl.ds(pl.multiple_of(slot * LINES, 4), ROWS), :] = sent_ref[rows_of(owner), :]

        @pl.when(jnp.logical_not(at_home))
        def _():
            send_odd(pair, space)

    @pl.when(jnp.logical_not(is_odd))
    def _():
        other_places(tm, space, send_even)

        @pl.when(at_home)
        def _():
            got_ref[pl.ds(pl.multiple_of(slot * LINES + ROWS, 4), 4), :] = sent_ref[even_rows(owner), :]

        @pl.when(jnp.logical_not(at_home))
        def _():
            send_even(pair, space)

    solve_modes(
        remote, 2, owner, tm, space, rows_of,
        velocity_ref, own_ref, wave_ref, tg_ref, td_ref, tw_ref, tb_ref, returned_ref,
        got_ref, back_ref, damp_ref, ratio_ref, last_ref, mate_ref, drive_ref, kept_ref, turn_ref,
        arrive_sem, swap_out_sem, swap_in_sem, mate_out_sem, mate_in_sem, scatter_sem, return_sem, own_sem,
    )

    def settle(rows):
        @pl.when(at_home)
        def _():
            remote.wait_got(returned_ref.at[pl.ds(0, (OWNERS - 1) * rows), :], return_sem)
            remote.wait_sent(sent_ref.at[pl.ds(0, (OWNERS - 1) * (LINES - rows)), :], gather_sem)
            remote.wait_sent(back_ref.at[pl.ds(0, (OWNERS // 2) * LINES - rows), :], scatter_sem)

        @pl.when(jnp.logical_not(at_home))
        def _():
            remote.wait_got(returned_ref.at[pl.ds(0, OWNERS * rows), :], return_sem)
            remote.wait_sent(sent_ref.at[pl.ds(0, OWNERS * (LINES - rows)), :], gather_sem)
            remote.wait_sent(back_ref.at[pl.ds(0, (OWNERS // 2) * LINES), :], scatter_sem)

    @pl.when(jnp.logical_not(is_odd))
    def _():
        settle(ROWS)

    @pl.when(is_odd)
    def _():
        settle(4)

    def store_chunk(t):
        for base in (0, 32, 64, 96):
            rows = pl.ds(pl.multiple_of(base + 8 * t, 8), 8)
            remote.local(y_ref.at[:, rows, :], y_hbm.at[:, rows, :], y_sem).start()

    def store_before(t):
        @pl.when(t > 0)
        def _():
            store_chunk(t - 1)

    stage(
        lambda odd, begin, ref: finish_stage(
            odd, begin, velocity_ref, lane_ref, row_ref, y_ref, returned_ref, ref
        ),
        chunk_back_out, chunk_back_in, 4, store_before,
    )
    store_chunk(3)

    @pl.when(jnp.logical_not(is_odd))
    def _():
        remote.wait_sent(chunk_out, chunk_out_sem.at[0])
        remote.wait_sent(chunk_back_out, chunk_out_sem.at[1])

    remote.wait_sent(kappa_ref.at[pl.ds(0, 2)], edge_out_sem)
    remote.local(y_ref, y_hbm, y_sem).wait()


GROUP = 2


def solve_modes(
    remote, share, owner, tm, space, rows_of,
    velocity_ref, own_ref, wave_ref, tg_ref, td_ref, tw_ref, tb_ref, returned_ref,
    got_ref, back_ref, damp_ref, ratio_ref, last_ref, mate_ref, drive_ref, kept_ref, turn_ref,
    arrive_sem, swap_out_sem, swap_in_sem, mate_out_sem, mate_in_sem, scatter_sem, return_sem, own_sem,
):
    pairs = STEPS // 2
    rounds = pairs // share // GROUP
    core = lax.rem(tm, share)
    pair = lax.div(tm, 2)
    at_home = lax.rem(pair, share) == core
    v0, v1, v2 = velocity_ref[0], velocity_ref[1], velocity_ref[2]
    own = own_ref[owner]
    line = [own[k : k + 1, :] for k in range(8)]
    wide = [jnp.broadcast_to(v, (8, 128)) for v in line]
    sign = wide[6]
    cross = cross_symbol(wide[0], wide[1], wide[2], wide[3], v1, v2)
    mu = [MU[0], MU[1], MU[0].conjugate(), MU[1].conjugate()]
    eps = [EPS[0], EPS[1], EPS[0].conjugate(), EPS[1].conjugate()]
    found = [factors(number, cross, v0) for number in mu]

    def crossed(a):
        return (a[0], -(sign * a[1]))

    def times_lanes(v, table):
        return v * table[0] + pltpu.roll(v, 64, 1) * table[1]

    def repeated(v, count):
        return jnp.concatenate([v] * count, axis=0)

    row = lax.broadcasted_iota(jnp.int32, (128, 128), 0).astype(f32)
    turn_ref[:, 0:128] = jnp.where(row == line[4], line[6], 0.0).astype(bf16)
    turn_ref[:, 128:256] = jnp.where(row == line[5], -1.0, 0.0).astype(bf16)

    @pl.loop(0, 16)
    def _(at):
        rows = pl.ds(pl.multiple_of(at * 8, 8), 8)
        symbol = (
            diffusion_number * (2.0 * wave_ref[0, rows, :] - 2.0) + cross[0],
            cross[1] - v0 * wave_ref[1, rows, :],
        )
        total = None
        for m in range(4):
            moved = scaled(mu[m], symbol)
            damp = inverse_of((1.0 - moved[0], -moved[1]))
            for k, value in enumerate(crossed(damp)):
                damp_ref[m, k, rows, :] = value
            term = scaled(eps[m], damp)
            if m < 2:
                for k, value in enumerate(crossed(term)):
                    damp_ref[4 + m, k, rows, :] = value
            total = term if total is None else plus(total, term)
        for k, value in enumerate(crossed(total)):
            ratio_ref[k, rows, :] = value
        power = times(total, total)
        for k, value in enumerate(crossed(power)):
            ratio_ref[4 + k, rows, :] = value
        fourth = times(power, power)
        for k, value in enumerate(crossed(fourth if share == 2 else power)):
            ratio_ref[6 + k, rows, :] = value
        power = fourth
        for k in range(3):
            power = times(power, power)
        closing = inverse_of((1.0 - circulant_alpha * power[0], -circulant_alpha * power[1]))
        for k, value in enumerate(crossed(closing)):
            ratio_ref[2 + k, rows, :] = value

    first_pair = pair - lax.rem(pair, 2)
    roots = [crossed(found[m][0]) for m in range(4)]
    flip = repeated(sign, 16)
    ratio = (ratio_ref.at[0], ratio_ref.at[1])
    square = (ratio_ref.at[4], ratio_ref.at[5])

    def times_refs(v, table):
        return times_lanes(v, (table[0][...], table[1][...]))

    def pair_of(i):
        return lax.rem(first_pair + share * i + core, pairs)

    def wrapped(at, v):
        return jnp.where(at == 0, circulant_alpha, 1.0).astype(f32) * v

    def swap(i):
        remote.start(
            drive_ref.at[pair_of(i)], drive_ref.at[pair_of(i)],
            swap_out_sem, swap_in_sem, (tm + 1 - 2 * core, space),
        )

    last_ref[...] = jnp.zeros((128, 128), f32)

    @pl.loop(0, rounds)
    def _(round_at):
        values, crossings = [], []
        for k in range(GROUP):
            at = pair_of(round_at * GROUP + k)
            slot = lax.div(at, share)
            top = slot * (SLABS * LINES)

            def arrived(rows):
                remote.wait_got(got_ref.at[pl.ds(0, rows), :], arrive_sem.at[slot])

            if k > 0:
                arrived(SLABS * LINES)
            else:
                home = (round_at == 0) & at_home

                @pl.when(home & (core == 0))
                def _():
                    arrived(SLABS * LINES - 4)

                @pl.when(home & (core == 1))
                def _():
                    arrived(SLABS * LINES - ROWS)

                @pl.when(jnp.logical_not(home))
                def _():
                    arrived(SLABS * LINES)

            pieces = [got_ref[pl.ds(top + x * LINES, 8), :] for x in range(SLABS)]
            pieces += [got_ref[pl.ds(top + 8 + f, SLABS, stride=LINES), :] for f in range(8)]
            v = jnp.concatenate(pieces, axis=0)
            values.append(halves(v))
            crossings.append(halves(flip * pltpu.roll(v, 64, 1)))
        stacked = jnp.concatenate([half for pieces in values for half in pieces], axis=0)
        turned = jnp.dot(stacked, turn_ref[...], preferred_element_type=f32).astype(bf16)
        columns, own_points, other_points = [], [], []
        for k in range(GROUP):
            parts = []
            for half in range(2):
                rows = slice(128 * (2 * k + half), 128 * (2 * k + half) + 128)
                parts.append((values[k][half], crossings[k][half], turned[rows, :128], turned[rows, 128:]))
            order = (parts[0], parts[1], parts[0])
            columns.append(jnp.concatenate([piece[:64] for part in order for piece in part], axis=0))
            for step in range(2):
                lines = slice(64 + 32 * step, 96 + 32 * step)
                own_points.append(
                    jnp.concatenate([piece[lines] for part in order for piece in part[:2]], axis=0)
                )
                other_points.append(
                    jnp.concatenate([piece[lines] for part in order for piece in part[2:]], axis=0)
                )
        drive = jnp.dot(tg_ref[...], jnp.concatenate(columns, axis=1), preferred_element_type=f32)
        points = jnp.dot(
            td_ref[...], jnp.concatenate(own_points + other_points, axis=1), preferred_element_type=f32
        )
        for k in range(GROUP):
            at = pair_of(round_at * GROUP + k)
            slot = lax.div(at, share)
            total = drive[:, 128 * k : 128 * k + 128]
            for step, store in ((1, 0), (0, 1)):
                summed = None
                for m in range(4):
                    where = 128 * (2 * k + step + 2 * GROUP * (m // 2))
                    j = m % 2
                    point = times_lanes(points[256 + 8 * j : 264 + 8 * j, where : where + 128], roots[m])
                    d = points[128 * j : 128 * j + 128, where : where + 128] - repeated(point, 16)
                    y = times_lanes(d, (damp_ref[m, 0], damp_ref[m, 1]))
                    summed = y if summed is None else summed + y
                    if m < 2:
                        if store == 1:
                            y = y + times_lanes(early, (damp_ref[4 + m, 0], damp_ref[4 + m, 1]))
                        kept_ref[slot, 2 * store + m] = y
                if store == 0:
                    early = summed
                    total = total + times_refs(summed, ratio)
                else:
                    total = total + summed
            drive_ref[at] = total
            before = wrapped(at - core, last_ref[...])
            last_ref[...] = total + times_lanes(before, (ratio_ref[6], ratio_ref[7]))
        if share > 1:
            @pl.when(round_at > 0)
            def _():
                for k in range(GROUP):
                    swap((round_at - 1) * GROUP + k)

    if share > 1:
        mate = (tm + 1 - 2 * core, space)
        for k in range(GROUP):
            swap((rounds - 1) * GROUP + k)
        remote.start(last_ref, mate_ref, mate_out_sem, mate_in_sem, mate)
        remote.wait_got(mate_ref, mate_in_sem)
        remote.wait_sent(last_ref, mate_out_sem)
        mine, theirs = last_ref[...], mate_ref[...]
        last_ref[...] = jnp.where(core == 0, theirs, mine) + times_refs(
            jnp.where(core == 0, mine, theirs), square
        )
        remote.wait_got(drive_ref.at[pl.ds(0, pairs // 2)], swap_in_sem)

    def following(at, v):
        return drive_ref[at] + times_refs(v, square)

    last_ref[...] = times_lanes(last_ref[...], (ratio_ref[2], ratio_ref[3]))
    kappas = [crossed(found[m][2]) for m in range(2)]
    ups = [crossed(found[m][1]) for m in range(2)]
    flip_all = flip

    def both_parts(v):
        return jnp.concatenate([v, flip_all * pltpu.roll(v, 64, 1)], axis=0)

    x_at, side = lax.div(space, 2), lax.rem(space, 2)
    places = [lax.rem(x_at + k // 2, SLABS // 2) * 2 + lax.rem(side + k, 2) for k in range(SLABS)]
    here = rows_of(owner)

    def send(i):
        at = pair_of(i)
        top = lax.div(at, share) * SLABS

        def put(place, even, odd):
            lines = (top + place) * LINES
            if even is not None:
                even(
                    back_ref.at[pl.ds(pl.multiple_of(lines, 4), ROWS), :], returned_ref.at[here, :],
                    scatter_sem, return_sem, (2 * at, place),
                )
            if odd is not None:
                odd(
                    back_ref.at[pl.ds(pl.multiple_of(lines + ROWS, 4), 4), :],
                    returned_ref.at[pl.ds(pl.multiple_of(owner * ROWS + 8, 4), 4), :],
                    scatter_sem, return_sem, (2 * at + 1, place),
                )

        def stay(source, target, *others):
            target[...] = source[...]

        home = (i == 0) & at_home

        @pl.when(jnp.logical_not(home))
        def _():
            put(places[0], remote.start, remote.start)

        @pl.when(home & (core == 0))
        def _():
            put(places[0], stay, remote.start)

        @pl.when(home & (core == 1))
        def _():
            put(places[0], remote.start, stay)

        for place in places[1:]:
            put(place, remote.start, remote.start)

    @pl.loop(0, rounds)
    def _(round_at):
        inputs = []
        last = last_ref[...]
        for k in range(GROUP):
            mine = None
            for c in range(share):
                at = lax.rem(first_pair + share * (round_at * GROUP + k) + c, pairs)
                last = wrapped(at, last)
                mine = last if mine is None else jnp.where(core == c, last, mine)
                last = following(at, last)
            inputs.append(mine)
        last_ref[...] = last
        packed = left_dot(tw_ref[...], jnp.concatenate([both_parts(v) for v in inputs], axis=1))
        lines = []
        for k in range(GROUP):
            slot = lax.div(pair_of(round_at * GROUP + k), share)
            for step, v in enumerate((inputs[k], times_refs(inputs[k], ratio))):
                for m in range(2):
                    y = times_lanes(v, (damp_ref[4 + m, 0], damp_ref[4 + m, 1]))
                    lines.append(both_parts(y + kept_ref[slot, 2 * step + m]))
        ends = left_dot(tb_ref[...], jnp.concatenate(lines, axis=1))
        for k in range(GROUP):
            top = lax.div(pair_of(round_at * GROUP + k), share) * (SLABS * LINES)
            for x in range(SLABS):
                back_ref[pl.ds(top + x * LINES, 8), :] = packed[8 * x : 8 * x + 8, 128 * k : 128 * k + 128]
            for step in range(2):
                for m in range(2):
                    where = 128 * (4 * k + 2 * step + m)
                    part = [ends[8 * j : 8 * j + 8, where : where + 128] for j in range(3)]
                    u = times_lanes(part[0] - times_lanes(part[1], ups[m]), kappas[m])
                    line = top + 8 + 4 * step + 2 * m
                    back_ref[pl.ds(line, SLABS, stride=LINES), :] = u
                    back_ref[pl.ds(line + 1, SLABS, stride=LINES), :] = part[2]

        @pl.when(round_at > 0)
        def _():
            @pl.loop(0, GROUP)
            def _(k):
                send((round_at - 1) * GROUP + k)

    @pl.loop(0, GROUP)
    def _(k):
        send((rounds - 1) * GROUP + k)

    if share > 1:
        remote.wait_sent(drive_ref.at[pl.ds(0, pairs // 2)], swap_out_sem)


class Remote:
    def place(self):
        return lax.axis_index("tm"), lax.axis_index("space")

    def greet(self, device):
        pl.semaphore_signal(
            pltpu.get_barrier_semaphore(), inc=1, device_id=device, device_id_type=MESH
        )

    def all_here(self, count):
        pl.semaphore_wait(pltpu.get_barrier_semaphore(), count)

    def vouch(self, sem, device):
        pl.semaphore_signal(sem, inc=1, device_id=device, device_id_type=MESH)

    def vouched(self, sem, count):
        pl.semaphore_wait(sem, count)

    def start(self, source, target, send_sem, recv_sem, device):
        pltpu.make_async_remote_copy(
            src_ref=source, dst_ref=target, send_sem=send_sem, recv_sem=recv_sem,
            device_id=device, device_id_type=MESH,
        ).start()

    def local(self, source, target, sem):
        return pltpu.make_async_copy(source, target, sem)

    def bytes_of(self, ref, sem):
        return pltpu.make_async_remote_copy(
            src_ref=ref, dst_ref=ref, send_sem=sem, recv_sem=sem,
            device_id=self.place(), device_id_type=MESH,
        )

    def wait_sent(self, ref, sem):
        self.bytes_of(ref, sem).wait_send()

    def wait_got(self, ref, sem):
        self.bytes_of(ref, sem).wait_recv()


VMEM, SMEM, ANY = pltpu.VMEM, pltpu.SMEM, pl.ANY


def spec(space):
    return pl.BlockSpec(memory_space=space)


def shape(*dims):
    return jax.ShapeDtypeStruct(dims, f32)


PARAMS = pltpu.CompilerParams(vmem_limit_bytes=60 * 1024 * 1024)


def whole(velocity, iterate, right_side, kappa, remote=Remote(), interpret=False):
    dma = pltpu.SemaphoreType.DMA
    return pl.pallas_call(
        functools.partial(whole_kernel, remote),
        out_shape=shape(32, 128, 128),
        in_specs=[spec(SMEM)] + [spec(ANY)] * 3 + [spec(VMEM)] * 10,
        out_specs=spec(ANY),
        scratch_shapes=[
            VMEM((4, WIDE, NZ, NY), f32), VMEM((4, WIDE, NZ, NY), f32), VMEM((WIDE, NZ, NY), f32),
            VMEM((32, 128, 128), f32),
        ]
        + [VMEM((256, 256), bf16)] * 4
        + [
            VMEM((44, 128, 128), f32), VMEM((8, NZ, NY), f32), VMEM((NZ, NY), f32), VMEM((NZ, NY), f32),
            VMEM((OWNERS * ROWS, 128), f32),
            VMEM((1024, 128), f32), VMEM((1024, 128), f32), VMEM((1024, 128), f32), VMEM((1024, 128), f32),
            VMEM((OWNERS * ROWS, 128), f32),
            VMEM((OWNERS // 2 * LINES, 128), f32), VMEM((OWNERS // 2 * LINES, 128), f32),
            VMEM((6, 2, 128, 128), f32), VMEM((8, 128, 128), f32), VMEM((128, 128), f32), VMEM((128, 128), f32),
            VMEM((STEPS // 2, 128, 128), f32), VMEM((STEPS // 4, 4, 128, 128), f32), VMEM((128, 256), bf16),
            pltpu.SemaphoreType.REGULAR, dma((3, 8)), dma, dma((2,)), dma((8,)), dma, dma, dma,
            dma, dma((STEPS // 4,)), dma, dma, dma, dma, dma, dma, dma,
        ],
        compiler_params=pltpu.CompilerParams(
            vmem_limit_bytes=60 * 1024 * 1024, has_side_effects=True, collective_id=0
        ),
        interpret=interpret,
        name="whole",
    )(
        velocity, iterate, right_side, kappa,
        TABLES["ty"], TABLES["tz"], TABLES["lane"], TABLES["row"], TABLES["own"], TABLES["wave_x"],
        TABLES["tg"], TABLES["td"], TABLES["tw"], TABLES["tb"],
    )


def backward(iterate, y, interpret=False):
    return pl.pallas_call(
        backward_kernel,
        out_shape=shape(4, WIDE, NZ, NY),
        in_specs=[spec(ANY)] * 2 + [spec(VMEM)] * 2,
        out_specs=spec(ANY),
        scratch_shapes=[
            VMEM((32, 128, 128), f32), VMEM((4, WIDE, NZ, NY), f32), VMEM((4, WIDE, NZ, NY), f32),
            pltpu.SemaphoreType.DMA((3, 4)), pltpu.SemaphoreType.DMA((8,)),
        ],
        compiler_params=PARAMS,
        interpret=interpret,
        name="backward",
    )(iterate, y, TABLES["uy"], TABLES["uz"])


def shards(iterate, right_side, diffusivity, velocity):
    iterate, right_side = iterate[0], right_side[0]
    y = whole(velocity, iterate, right_side, diffusivity)
    return backward(iterate, y)[None]


def solution(mesh):
    placed = (
        P("tm", None, "space", None, None),
        P("tm", None, "space", None, None),
        P("space", None, None),
        P(),
    )
    return jax.shard_map(
        shards,
        mesh=mesh,
        in_specs=placed,
        out_specs=P("tm", None, "space", None, None),
        check_vma=False,
    )
```

```python
import functools
import math

import jax
import jax.numpy as jnp
import numpy as np
from jax import lax
from jax.experimental import pallas as pl
from jax.experimental.pallas import tpu as pltpu
from jax.sharding import PartitionSpec as P

NX, NY, NZ, STEPS = 128, 128, 64, 32
SLABS, WIDE = 8, 16
OWNERS = 128
ROWS = 12
LINES = 16
MESH = pl.DeviceIdType.MESH
f32, bf16 = jnp.float32, jnp.bfloat16

diffusion_number = 16.0
circulant_alpha = 0.1


def collocation_matrix():
    radau_nodes = [0.08858795951270394, 0.4094668644407347, 0.7876594617608471, 1.0]
    matrix = [[0.0] * 4 for row_index in range(4)]
    for column_index in range(4):
        coefficients = [1.0]
        for other_index in range(4):
            if other_index != column_index:
                scale_value = 1.0 / (radau_nodes[column_index] - radau_nodes[other_index])
                shifted = [0.0] + [value * scale_value for value in coefficients]
                lowered = [
                    -radau_nodes[other_index] * scale_value * value for value in coefficients
                ] + [0.0]
                coefficients = [
                    left_value + right_value for left_value, right_value in zip(shifted, lowered)
                ]
        for row_index in range(4):
            total = 0.0
            for power_index in range(len(coefficients)):
                total = total + coefficients[power_index] * radau_nodes[row_index] ** (
                    power_index + 1
                ) / (power_index + 1)
            matrix[row_index][column_index] = total
    return matrix


def solve_system(matrix, target):
    count = len(target)
    rows_list = [list(matrix[row_index]) + [target[row_index]] for row_index in range(count)]
    for column in range(count):
        best_row = column
        for candidate in range(column + 1, count):
            if abs(rows_list[candidate][column]) > abs(rows_list[best_row][column]):
                best_row = candidate
        saved_row = rows_list[column]
        rows_list[column] = rows_list[best_row]
        rows_list[best_row] = saved_row
        leader = rows_list[column][column]
        for other_row in range(count):
            if other_row != column:
                factor = rows_list[other_row][column] / leader
                rows_list[other_row] = [
                    left_value - factor * right_value
                    for left_value, right_value in zip(rows_list[other_row], rows_list[column])
                ]
    return [
        rows_list[row_index][count] / rows_list[row_index][row_index] for row_index in range(count)
    ]


def node_basis():
    matrix = collocation_matrix()
    helper = [[0.0] * 4 for row_index in range(4)]
    coefficients = [0.0, 0.0, 0.0, 0.0, 1.0]
    for order in range(1, 5):
        product = [
            [
                sum((matrix[row_index][inner] * helper[inner][column] for inner in range(4)))
                for column in range(4)
            ]
            for row_index in range(4)
        ]
        for row_index in range(4):
            product[row_index][row_index] = product[row_index][row_index] + coefficients[5 - order]
        helper = product
        trace_value = sum(
            (
                sum((matrix[row_index][inner] * helper[inner][row_index] for inner in range(4)))
                for row_index in range(4)
            )
        )
        coefficients[4 - order] = -trace_value / order
    roots_list = [(0.4 + 0.9j) ** power_index for power_index in range(4)]
    for sweep in range(400):
        for root_index in range(4):
            current = roots_list[root_index]
            numer = 0.0
            for power_index in range(4, -1, -1):
                numer = numer * current + coefficients[power_index]
            denom = 1.0
            for other_index in range(4):
                if other_index != root_index:
                    denom = denom * (current - roots_list[other_index])
            roots_list[root_index] = current - numer / denom
    vectors = [[0.0] * 4 for row_index in range(4)]
    for root_index in range(4):
        shifted = [
            [
                matrix[row_index][column] - (roots_list[root_index] if row_index == column else 0.0)
                for column in range(3)
            ]
            for row_index in range(3)
        ]
        target = [-matrix[row_index][3] for row_index in range(3)]
        parts = solve_system(shifted, target) + [1.0 + 0j]
        for row_index in range(4):
            vectors[row_index][root_index] = parts[row_index]
    inverse = [[0.0] * 4 for row_index in range(4)]
    for column in range(4):
        unit = [1.0 if row_index == column else 0.0 for row_index in range(4)]
        parts = solve_system(vectors, unit)
        for row_index in range(4):
            inverse[row_index][column] = parts[row_index]
    weights = [sum((inverse[row_index][column] for column in range(4))) for row_index in range(4)]
    return (roots_list, vectors, inverse, weights)


VALUES, VECTORS, INVERSE, WEIGHTS = node_basis()
PAIRS = [m for m in range(4) if complex(VALUES[m]).imag > 0]
MU = [complex(VALUES[m]) for m in PAIRS]
COLUMN = [[complex(VECTORS[n][m]) for n in range(4)] for m in PAIRS]
ROW = [[complex(INVERSE[m][n]) for n in range(4)] for m in PAIRS]
EPS = [complex(WEIGHTS[m]) for m in PAIRS]


def wave_order_z():
    index = np.arange(NZ)
    return np.where(index <= NZ // 2, index, NZ + NZ // 2 - index)


def wave_order_y():
    lane = np.arange(NY)
    index = 16 * (lane // 32) + lane % 16
    return np.where(lane % 32 < 16, index, np.where(index == 0, NY // 2, NY - index))


def split(values):
    values = np.asarray(values, np.float64)
    high = values.astype(np.float32).astype(bf16)
    low = (values - high.astype(np.float64)).astype(np.float32).astype(bf16)
    return high, low


def side_table(values):
    high, low = split(values)
    return np.concatenate([high, high, low], axis=1)


def halves(x):
    high = x.astype(bf16)
    return high, (x - high.astype(f32)).astype(bf16)


def left_dot(table, x):
    high, low = halves(x)
    return jnp.dot(table, jnp.concatenate([high, low, high], axis=0), preferred_element_type=f32)


def right_dot(high, low, table_high, table_low):
    return (
        jnp.dot(high, table_high, preferred_element_type=f32)
        + jnp.dot(low, table_high, preferred_element_type=f32)
        + jnp.dot(high, table_low, preferred_element_type=f32)
    )


def complex_block(matrix):
    return np.block([[matrix.real, -matrix.imag], [matrix.imag, matrix.real]])


def make_tables():
    ky, kz = wave_order_y(), wave_order_z()
    kx, x = np.arange(NX), np.arange(NX)
    to_y = np.exp(-2j * np.pi * np.outer(ky, np.arange(NY)) / NY)
    to_z = np.exp(-2j * np.pi * np.outer(kz, np.arange(NZ)) / NZ)
    tables = {}
    tables["ty"] = np.stack(split(complex_block(to_y).T))
    tables["tz"] = side_table(complex_block(to_z))
    tables["uy"] = np.stack(split(complex_block(np.conj(to_y.T) / NY).T))
    tables["uz"] = side_table(complex_block(np.conj(to_z.T) / NZ))
    cells = (np.arange(SLABS)[:, None] * WIDE + np.arange(8)[None, :]).reshape(-1)
    theta = 2 * np.pi * kx / NX
    at = np.exp(-1j * np.outer(theta, cells))
    shifted = np.exp(-8j * theta)[:, None]
    from_own = at * (1 - 1j * shifted) / 2
    from_partner = at * (1 + 1j * shifted) / 2
    firsts = np.arange(SLABS) * WIDE

    def lane_block(matrix):
        return np.concatenate([matrix.real, -matrix.imag], axis=1)

    tables["tg"] = side_table(np.concatenate([lane_block(from_own), lane_block(from_partner)], axis=1))

    def point_rows(waves, shifts):
        out = []
        for m in range(2):
            table = np.zeros((len(waves), 4, SLABS), complex)
            for field, shift in shifts:
                table[:, 2 * m + field] = np.exp(-1j * np.outer(waves, firsts + shift))
            out.append(table.reshape(len(waves), 4 * SLABS))
        return out

    tables["td"] = side_table(
        lane_block(
            np.concatenate(
                point_rows(theta, ((0, WIDE), (1, -1))) + point_rows(theta[:8], ((1, 0),)), axis=0
            )
        )
    )
    back = np.exp(1j * np.outer(cells, theta)) * (1 + 1j * np.exp(8j * theta))[None, :] / NX
    tables["tw"] = side_table(lane_block(back))
    ends = [np.exp(1j * np.outer(firsts + k, theta)) / NX for k in (0, 1, 15)]
    tables["tb"] = side_table(lane_block(np.concatenate(ends, axis=0)))
    trig_y = 2 * np.pi * ky / NY
    trig_z = 2 * np.pi * kz / NZ
    tables["lane"] = np.stack([np.cos(trig_y), np.sin(trig_y)]).astype(np.float32)
    tables["row"] = np.stack(
        [np.broadcast_to(v[:, None], (NZ, NY)) for v in (np.cos(trig_z), np.sin(trig_z))]
    ).astype(np.float32)
    tables["wave_x"] = np.stack(
        [np.broadcast_to(v[:, None], (NX, 128)) for v in (np.cos(theta), np.sin(theta))]
    ).astype(np.float32)
    lane = np.arange(128)
    own = np.zeros((OWNERS, 8, 128))
    for owner in range(OWNERS):
        part, pair = owner // 32, owner % 32
        piece = (lane // 32 - part) % 4
        at_y, row = (lane - 32 * piece) % 128, piece % 2
        other_y = np.where((at_y == 0) | (at_y == 16), at_y, at_y ^ 16)
        other_row = row if pair == 0 else 1 - row
        other = (other_y + 32 * (2 * (piece // 2) + other_row)) % 128
        y, z = trig_y[at_y], trig_z[pair + 32 * row]
        own[owner] = np.stack(
            [
                np.cos(y), np.sin(y), np.cos(z), np.sin(z),
                other, np.roll(other, -64), np.where(piece < 2, 1.0, -1.0), (lane + 64) % 128,
            ]
        )
    tables["own"] = own.astype(np.float32)
    return tables


TABLES = make_tables()


def times(a, b):
    return (a[0] * b[0] - a[1] * b[1], a[0] * b[1] + a[1] * b[0])


def plus(a, b):
    return (a[0] + b[0], a[1] + b[1])


def minus(a, b):
    return (a[0] - b[0], a[1] - b[1])


def scaled(number, a):
    return (number.real * a[0] - number.imag * a[1], number.real * a[1] + number.imag * a[0])


def inverse_of(a):
    size = 1.0 / (a[0] * a[0] + a[1] * a[1])
    return (a[0] * size, -a[1] * size)


def root_of(a):
    size = jnp.sqrt(a[0] * a[0] + a[1] * a[1])
    main = jnp.sqrt(0.5 * (size + jnp.abs(a[0])))
    other = a[1] / (2.0 * main)
    positive = a[0] >= 0.0
    return (
        jnp.where(positive, main, jnp.abs(other)),
        jnp.where(positive, other, jnp.where(a[1] >= 0.0, main, -main)),
    )


def cross_symbol(cos_y, sin_y, cos_z, sin_z, v1, v2):
    return (
        diffusion_number * ((2.0 * cos_y - 2.0) + (2.0 * cos_z - 2.0)),
        -(v1 * sin_y + v2 * sin_z),
    )


def factors(mu, cross, v0):
    c_up = -mu.real * (diffusion_number - 0.5 * v0), -mu.imag * (diffusion_number - 0.5 * v0)
    c_down = -mu.real * (diffusion_number + 0.5 * v0), -mu.imag * (diffusion_number + 0.5 * v0)
    moved = scaled(mu, cross)
    c_mid = (1.0 + 2.0 * diffusion_number * mu.real - moved[0], 2.0 * diffusion_number * mu.imag - moved[1])
    product = times(c_up, c_down)
    square = times(c_mid, c_mid)
    root = root_of((square[0] - 4.0 * product[0], square[1] - 4.0 * product[1]))
    same = c_mid[0] * root[0] + c_mid[1] * root[1] >= 0.0
    kappa = (
        0.5 * (c_mid[0] + jnp.where(same, root[0], -root[0])),
        0.5 * (c_mid[1] + jnp.where(same, root[1], -root[1])),
    )
    inv = inverse_of(kappa)
    p = times(inv, c_down)
    q = times(inv, c_up)
    return (-p[0], -p[1]), (-q[0], -q[1]), kappa, inv


def plane_partner(low, high, lane, first_row):
    ends = (lane == 0) | (lane == 16)
    first = (lane % 32) < 16

    def turned(v):
        return jnp.where(ends, v, jnp.where(first, pltpu.roll(v, 112, 1), pltpu.roll(v, 16, 1)))

    low_turned, high_turned = [turned(v) for v in low], [turned(v) for v in high]
    to_low = [jnp.where(first_row, a, b) for a, b in zip(low_turned, high_turned)]
    to_high = [jnp.where(first_row, b, a) for a, b in zip(low_turned, high_turned)]
    return (to_low[0], -to_low[1]), (to_high[0], -to_high[1])


def packed_for(low, high, block):
    pieces = [low[0], high[0], low[1], high[1]]
    pieces = [pieces[0]] + [pltpu.roll(pieces[c], 32 * c, 1) for c in (1, 2, 3)]
    out = []
    for h in range(4):
        value = pieces[3]
        for c in (2, 1, 0):
            value = jnp.where(block == (h + c) % 4, pieces[c], value)
        out.append(value)
    return out


def unpacked_from(values, block):
    out = []
    for c in range(4):
        piece = values[(3 - c) % 4]
        for d in (2, 1, 0):
            piece = jnp.where(block == d, values[(d - c) % 4], piece)
        out.append(piece if c == 0 else pltpu.roll(piece, 128 - 32 * c, 1))
    return (out[0], out[2]), (out[1], out[3])


def chunk_factors(t, lane_ref, row_ref, velocity_ref, mu):
    cos_y, sin_y = lane_ref[0:1, :], lane_ref[1:2, :]
    found = []
    for base in (0, 32):
        rows = pl.ds(pl.multiple_of(base + 8 * t, 8), 8)
        cross = cross_symbol(
            cos_y, sin_y, row_ref[0, rows, :], row_ref[1, rows, :], velocity_ref[1], velocity_ref[2]
        )
        found.append([factors(number, cross, velocity_ref[0]) for number in mu])
    return found


def dft_block(high, low, ty_ref, tz_ref):
    mid = right_dot(high, low, ty_ref[0], ty_ref[1])
    stacked = jnp.concatenate(
        [
            jnp.concatenate([mid[64 * k : 64 * k + 64, :128], mid[64 * k : 64 * k + 64, 128:]], axis=0)
            for k in range(4)
        ],
        axis=1,
    )
    return left_dot(tz_ref[...], stacked)


def put_rows(slot, at, real, imag):
    for k, part in enumerate((real, imag)):
        for ref, value in zip(slot, halves(part)):
            ref[64 * at : 64 * at + 64, k * 128 : (k + 1) * 128] = value


def mixture(m, groups):
    real = imag = None
    for scale, values in groups:
        for n in range(4):
            factor = scale * ROW[m][n]
            a, b = factor.real * values[n], factor.imag * values[n]
            real = a if real is None else real + a
            imag = b if imag is None else imag + b
    return real, imag


def source_stage(
    keep, ready, middle, velocity_ref, iterate_ref, right_ref, kappa_ref, ty_ref, tz_ref, spec_ref, mixed_ref, slots,
):
    v0, v1, v2 = velocity_ref[0], velocity_ref[1], velocity_ref[2]

    def stencil(x, slot, at, below, above):
        plain, applied = [], []
        kappa = diffusion_number * kappa_ref[x]
        for n in range(4):
            f = iterate_ref[n, x]
            up_z, down_z = pltpu.roll(f, NZ - 1, 0), pltpu.roll(f, 1, 0)
            up_y, down_y = pltpu.roll(f, NY - 1, 1), pltpu.roll(f, 1, 1)
            total = (up_z + down_z) + (up_y + down_y) - 6.0 * f
            moved = v1 * (up_y - down_y) + v2 * (up_z - down_z)
            if above:
                up_x = iterate_ref[n, x + 1]
                total, moved = total + up_x, moved + v0 * up_x
            if below:
                down_x = iterate_ref[n, x - 1]
                total, moved = total + down_x, moved - v0 * down_x
            applied.append(kappa * total - 0.5 * moved)
            plain.append(right_ref[n, x] - f)
        for m in range(2):
            put_rows(slot, 2 * m + at, *mixture(m, [(1.0, plain), (MU[m], applied)]))

    def produce(block, slot, first=False, final=False):
        stencil(2 * block, slot, 0, not first, True)
        stencil(2 * block + 1, slot, 1, True, not final)

    def last_node(block, slot):
        for k in range(4):
            x = 4 * block + k
            put_rows(slot, k, keep * iterate_ref[3, x], keep * iterate_ref[3, x + 8])

    def transformed(block, slot):
        out = dft_block(slot[0][...], slot[1][...], ty_ref, tz_ref)
        for k in range(4):
            spec_ref[block * 4 + k] = out[:, 128 * k : 128 * k + 128]

    first, second = slots
    ready(0)
    ready(1)
    produce(0, first, first=True)

    @pl.loop(0, 3)
    def _(i):
        ready(2 * i + 2)
        transformed(2 * i, first)
        produce(2 * i + 1, second)
        ready(2 * i + 3)
        transformed(2 * i + 1, second)
        produce(2 * i + 2, first)

    middle()
    for side, x in enumerate((0, WIDE - 1)):
        for m in range(2):
            real, imag = mixture(m, [(MU[m], [iterate_ref[n, x] for n in range(4)])])
            mixed_ref[side * 4 + m * 2] = real
            mixed_ref[side * 4 + m * 2 + 1] = imag
    transformed(6, first)
    produce(7, second, final=True)
    transformed(7, second)
    last_node(0, first)
    transformed(8, first)
    last_node(1, second)
    transformed(9, second)


def put_chunk(ref, t, x, low, high):
    for k, value in enumerate((low[0], high[0], low[1], high[1])):
        ref[pl.ds(pl.multiple_of(256 * t + 32 * x + 8 * k, 8), 8), :] = value


def get_chunk(ref, t, x):
    parts = [ref[pl.ds(pl.multiple_of(256 * t + 32 * x + 8 * k, 8), 8), :] for k in range(4)]
    return (parts[0], parts[2]), (parts[1], parts[3])


def packed_planes(sums, x, lane, first_row):
    own, other = [], []
    for half in range(2):
        first, second = sums[x][half], sums[x + 8][half]
        own.append((first[0] - second[1], first[1] + second[0]))
        other.append((first[0] + second[1], first[1] - second[0]))
    partners = plane_partner(other[0], other[1], lane, first_row)
    return [plus(own[half], partners[half]) for half in range(2)]


def unpacked_planes(fetch, lane, first_row):
    last = [[None, None] for x in range(WIDE)]
    for x in range(8):
        packed = fetch(x)
        partners = plane_partner(packed[0], packed[1], lane, first_row)
        for half in range(2):
            both, apart = plus(packed[half], partners[half]), minus(packed[half], partners[half])
            last[x][half] = (0.5 * both[0], 0.5 * both[1])
            last[x + 8][half] = (0.5 * apart[1], -0.5 * apart[0])
    return last


def edge_stage(velocity_ref, spec_ref, mixed_ref, below_ref, above_ref, ty_ref, tz_ref):
    v0 = velocity_ref[0]
    outer = [diffusion_number * below_ref[...] - 0.5 * v0, diffusion_number * above_ref[...] + 0.5 * v0]
    edges = [
        jnp.concatenate([outer[side] * mixed_ref[side * 4 + m * 2 + part] for part in range(2)], axis=1)
        for m in range(2)
        for side in range(2)
    ]
    high, low = halves(jnp.concatenate(edges, axis=0))
    out = dft_block(high, low, ty_ref, tz_ref)
    for k in range(4):
        spec_ref[40 + k] = out[:, 128 * k : 128 * k + 128]


def slab_stage(odd, begin, velocity_ref, spec_ref, lane_ref, row_ref, y_ref, send_ref, chunk_ref):
    lane = lax.broadcasted_iota(jnp.int32, (8, 128), 1)
    sub = lax.broadcasted_iota(jnp.int32, (8, 128), 0)
    block = lane // 32

    @pl.loop(0, 4)
    def _(t):
        begin(t)
        first_row = (sub + t) == 0
        found = chunk_factors(t, lane_ref, row_ref, velocity_ref, MU)
        bases = [pl.multiple_of(base + 8 * t, 8) for base in (0, 32)]
        if odd:
            last = unpacked_planes(lambda x: get_chunk(chunk_ref, t, x), lane, first_row)

        def plane(at, base):
            return spec_ref[at, pl.ds(base, 8), :], spec_ref[at, pl.ds(base + 64, 8), :]

        def field(m, x, half):
            value = plane(4 * (x // 2) + 2 * m + x % 2, bases[half])
            return plus(value, scaled(EPS[m], last[x][half])) if odd else value

        def send(value, low, high):
            for h, packed in enumerate(packed_for(low, high, block)):
                send_ref[pl.ds((32 * h + 8 * t) * ROWS + value, 8, stride=ROWS), :] = packed

        sums = [[None, None] for x in range(WIDE)]
        for m in range(2):
            carries = []
            for half in range(2):
                base = bases[half]
                p, q, kappa, inv = found[half][m]
                under, over = plane(40 + 2 * m, base), plane(41 + 2 * m, base)
                u = plus(field(m, 0, half), times(p, under))
                us = [u]
                for x in range(1, WIDE):
                    u = plus(field(m, x, half), times(p, u))
                    us.append(u)
                outflow = plus(times(p, us[-1]), over)
                y = us[-1]
                for x in range(WIDE - 1, -1, -1):
                    if x < WIDE - 1:
                        y = plus(us[x], times(q, y))
                    z = times(inv, y)
                    y_ref[m * 16 + x, pl.ds(base, 8), :] = z[0]
                    y_ref[m * 16 + x, pl.ds(base + 64, 8), :] = z[1]
                    sums[x][half] = z if m == 0 else plus(sums[x][half], z)
                carries.append((outflow, plus(times(q, y), under)))
            for k in range(2):
                send(8 + m * 2 + k, carries[0][k], carries[1][k])
        for x in range(8):
            packed = packed_planes(sums, x, lane, first_row)
            packed = [plus(packed[half], plane(32 + x, bases[half])) for half in range(2)]
            if odd:
                send(x, packed[0], packed[1])
            else:
                put_chunk(chunk_ref, t, x, packed[0], packed[1])


def finish_stage(odd, begin, velocity_ref, lane_ref, row_ref, y_ref, got_ref, chunk_ref):
    lane = lax.broadcasted_iota(jnp.int32, (8, 128), 1)
    sub = lax.broadcasted_iota(jnp.int32, (8, 128), 0)
    block = lane // 32

    @pl.loop(0, 4)
    def _(t):
        begin(t)
        first_row = (sub + t) == 0
        found = chunk_factors(t, lane_ref, row_ref, velocity_ref, MU)
        bases = [pl.multiple_of(base + 8 * t, 8) for base in (0, 32)]

        def take(value):
            values = [
                got_ref[pl.ds((32 * h + 8 * t) * ROWS + value, 8, stride=ROWS), :] for h in range(4)
            ]
            return unpacked_from(values, block)

        last = unpacked_planes(
            (lambda x: get_chunk(chunk_ref, t, x)) if odd else take, lane, first_row
        )
        sums = [[None, None] for x in range(WIDE)]
        for m in range(2):
            start, end = take(8 + m * 2), take(9 + m * 2)
            for half in range(2):
                base = bases[half]
                p, q, kappa, inv = found[half][m]
                u = start[half]
                us = [u]
                for x in range(1, WIDE - 1):
                    u = plus(scaled(EPS[m], last[x][half]), times(p, u))
                    us.append(u)
                y = end[half]
                for x in range(WIDE - 1, -1, -1):
                    if x < WIDE - 1:
                        y = plus(times(inv, us[x]), times(q, y))
                    for k in range(2):
                        rows = pl.ds(base + 64 * k, 8)
                        y_ref[m * 16 + x, rows, :] = y_ref[m * 16 + x, rows, :] + y[k]
                    if not odd:
                        sums[x][half] = y if m == 0 else plus(sums[x][half], y)
        if not odd:
            for x in range(8):
                packed = packed_planes(sums, x, lane, first_row)
                put_chunk(chunk_ref, t, x, packed[0], packed[1])


def backward_kernel(
    iterate_hbm, spec_hbm, uy_ref, uz_ref, out_hbm, spec_ref, iterate_ref, out_ref, load_sem, store_sem
):
    def loads(group):
        planes = pl.ds(4 * group, 4)
        upper = pl.ds(16 + 4 * group, 4)
        return [
            pltpu.make_async_copy(spec_hbm.at[planes], spec_ref.at[planes], load_sem.at[0, group]),
            pltpu.make_async_copy(spec_hbm.at[upper], spec_ref.at[upper], load_sem.at[1, group]),
            pltpu.make_async_copy(
                iterate_hbm.at[:, planes], iterate_ref.at[:, planes], load_sem.at[2, group]
            ),
        ]

    for group in range(4):
        for copy in loads(group):
            copy.start()

    def finished(block):
        planes = [2 * block, 2 * block + 1, 16 + 2 * block, 17 + 2 * block]
        stacked = jnp.concatenate([spec_ref[at] for at in planes], axis=1)
        mid = left_dot(uz_ref[...], stacked)
        rows = jnp.concatenate(
            [
                jnp.concatenate([mid[:64, 128 * k : 128 * k + 128], mid[64:, 128 * k : 128 * k + 128]], axis=1)
                for k in range(4)
            ],
            axis=0,
        )
        high, low = halves(rows)
        return right_dot(high, low, uy_ref[0], uy_ref[1])

    def store(block):
        planes = pl.ds(2 * block, 2)
        return pltpu.make_async_copy(out_ref.at[:, planes], out_hbm.at[:, planes], store_sem.at[block])

    def added(block, out):
        for k in range(2):
            x = 2 * block + k
            parts = []
            for m in range(2):
                piece = out[(2 * m + k) * 64 : (2 * m + k) * 64 + 64]
                parts.append((piece[:, :128], piece[:, 128:]))
            for n in range(4):
                total = iterate_ref[n, x]
                for m in range(2):
                    c = COLUMN[m][n]
                    total = total + (2.0 * c.real) * parts[m][0] - (2.0 * c.imag) * parts[m][1]
                out_ref[n, x] = total

    pending = None
    for group in range(4):
        for copy in loads(group):
            copy.wait()
        blocks = (2 * group, 2 * group + 1)
        outs = [finished(block) for block in blocks]
        if pending is not None:
            for block, out in pending:
                added(block, out)
        pending = list(zip(blocks, outs))
        if group > 1:
            store(2 * group - 4).start()
            store(2 * group - 3).start()
    for block, out in pending:
        added(block, out)
    for block in range(4, 8):
        store(block).start()
    for block in range(8):
        store(block).wait()


def other_places(tm, space, work):
    pair = lax.div(tm, 2)
    x, side = lax.div(space, 2), lax.rem(space, 2)
    places = [
        lax.rem(x + k // 2, SLABS // 2) * 2 + lax.rem(side + k, 2) for k in range(SLABS)
    ]
    for k in range(1, SLABS):
        work(pair, places[k])

    @pl.loop(1, STEPS // 2)
    def _(i):
        other = lax.rem(pair + STEPS // 2 - i, STEPS // 2)
        for k in range(SLABS):
            work(other, places[k])


def whole_kernel(
    remote, velocity_ref, iterate_hbm, right_hbm, kappa_hbm,
    own_hbm, ty_ref, tz_ref, lane_ref, row_ref, wave_ref, tg_ref, td_ref, tw_ref, tb_ref,
    y_hbm,
    iterate_ref, right_ref, kappa_ref, y_ref,
    high_a, low_a, high_b, low_b, spec_ref, mixed_ref, below_ref, above_ref, sent_ref,
    chunk_out, chunk_in, chunk_back_out, chunk_back_in, returned_ref,
    got_ref, back_ref, damp_ref, ratio_ref, last_ref, mate_ref, drive_ref, kept_ref, turn_ref,
    line_ref, line_sem, vouch_sem, load_sem, y_sem, chunk_out_sem, chunk_in_sem, edge_out_sem, below_sem, above_sem,
    gather_sem, arrive_sem, swap_out_sem, swap_in_sem, mate_out_sem, mate_in_sem,
    scatter_sem, return_sem, own_sem,
):
    tm, space = remote.place()
    core = lax.rem(tm, 2)
    owner = lax.div(tm, 2) * SLABS + space

    def rows_of(index, number=1):
        return pl.ds(pl.multiple_of(index * ROWS, 4), number * ROWS)

    def loads(piece):
        planes = pl.ds(2 * piece, 2)
        return [
            remote.local(iterate_hbm.at[:, planes], iterate_ref.at[:, planes], load_sem.at[0, piece]),
            remote.local(right_hbm.at[:, planes], right_ref.at[:, planes], load_sem.at[1, piece]),
            remote.local(kappa_hbm.at[planes], kappa_ref.at[planes], load_sem.at[2, piece]),
        ]

    for piece in range(8):
        for copy in loads(piece):
            copy.start()

    line_load = remote.local(own_hbm.at[owner], line_ref, line_sem)
    line_load.start()

    def ready(piece):
        for copy in loads(piece):
            copy.wait()

    mate = (tm + 1 - 2 * core, space)

    for k in range(1, SLABS):
        remote.greet((tm, lax.rem(space + k, SLABS)))

    @pl.loop(1, STEPS)
    def _(k):
        remote.greet((lax.rem(tm + k, STEPS), space))

    def middle():
        remote.all_here(SLABS + STEPS - 2)
        for k in range(1, SLABS):
            remote.vouch(vouch_sem, (tm, lax.rem(space + k, SLABS)))
        remote.start(
            kappa_ref.at[WIDE - 1], below_ref, edge_out_sem, below_sem, (tm, lax.rem(space + 1, SLABS))
        )
        remote.start(
            kappa_ref.at[0], above_ref, edge_out_sem, above_sem, (tm, lax.rem(space + SLABS - 1, SLABS))
        )

    keep = jnp.where(tm < STEPS - 1, 1.0, 0.0).astype(f32)
    source_stage(
        keep, ready, middle, velocity_ref, iterate_ref, right_ref, kappa_ref, ty_ref, tz_ref,
        spec_ref, mixed_ref, ((high_a, low_a), (high_b, low_b)),
    )
    remote.wait_got(below_ref, below_sem)
    remote.wait_got(above_ref, above_sem)
    edge_stage(velocity_ref, spec_ref, mixed_ref, below_ref, above_ref, ty_ref, tz_ref)
    is_odd = core == 1

    def chunk_at(ref, t):
        return ref.at[pl.ds(pl.multiple_of(256 * t, 256), 256), :]

    def hand_over(source, target, t, base):
        remote.start(
            chunk_at(source, t), chunk_at(target, t), chunk_out_sem.at[base // 4],
            chunk_in_sem.at[base + t], mate,
        )

    def stage(work, source, target, base, done):
        @pl.when(jnp.logical_not(is_odd))
        def _():
            def begin(t):
                done(t)

                @pl.when(t > 0)
                def _():
                    hand_over(source, target, t - 1, base)

            work(False, begin, source)
            hand_over(source, target, 3, base)

        @pl.when(is_odd)
        def _():
            def begin(t):
                done(t)
                remote.wait_got(chunk_at(target, t), chunk_in_sem.at[base + t])

            work(True, begin, target)

    stage(
        lambda odd, begin, ref: slab_stage(
            odd, begin, velocity_ref, spec_ref, lane_ref, row_ref, y_ref, sent_ref, ref
        ),
        chunk_out, chunk_in, 0, lambda t: None,
    )

    remote.vouched(vouch_sem, SLABS - 1)

    pair = lax.div(tm, 2)
    side = lax.rem(pair, 2)
    at_home = side == core
    slot = lax.div(pair, 2) * SLABS + space

    def even_rows(index):
        return pl.ds(pl.multiple_of(index * ROWS + 8, 4), 4)

    def send_even(other, place):
        remote.start(
            sent_ref.at[even_rows(other * SLABS + place), :],
            got_ref.at[pl.ds(pl.multiple_of(slot * LINES + ROWS, 4), 4), :],
            gather_sem, arrive_sem.at[lax.div(pair, 2)], (2 * other + side, place),
        )

    def send_odd(other, place):
        remote.start(
            sent_ref.at[rows_of(other * SLABS + place), :],
            got_ref.at[pl.ds(pl.multiple_of(slot * LINES, 4), ROWS), :],
            gather_sem, arrive_sem.at[lax.div(pair, 2)], (2 * other + side, place),
        )

    @pl.when(is_odd)
    def _():
        other_places(tm, space, send_odd)

        @pl.when(at_home)
        def _():
            got_ref[pl.ds(pl.multiple_of(slot * LINES, 4), ROWS), :] = sent_ref[rows_of(owner), :]

        @pl.when(jnp.logical_not(at_home))
        def _():
            send_odd(pair, space)

    @pl.when(jnp.logical_not(is_odd))
    def _():
        other_places(tm, space, send_even)

        @pl.when(at_home)
        def _():
            got_ref[pl.ds(pl.multiple_of(slot * LINES + ROWS, 4), 4), :] = sent_ref[even_rows(owner), :]

        @pl.when(jnp.logical_not(at_home))
        def _():
            send_even(pair, space)

    line_load.wait()
    solve_modes(
        remote, 2, owner, tm, space, rows_of,
        velocity_ref, line_ref, wave_ref, tg_ref, td_ref, tw_ref, tb_ref, returned_ref,
        got_ref, back_ref, damp_ref, ratio_ref, last_ref, mate_ref, drive_ref, kept_ref, turn_ref,
        arrive_sem, swap_out_sem, swap_in_sem, mate_out_sem, mate_in_sem, scatter_sem, return_sem, own_sem,
    )

    def settle(rows):
        @pl.when(at_home)
        def _():
            remote.wait_got(returned_ref.at[pl.ds(0, (OWNERS - 1) * rows), :], return_sem)
            remote.wait_sent(sent_ref.at[pl.ds(0, (OWNERS - 1) * (LINES - rows)), :], gather_sem)
            remote.wait_sent(back_ref.at[pl.ds(0, (OWNERS // 2) * LINES - rows), :], scatter_sem)

        @pl.when(jnp.logical_not(at_home))
        def _():
            remote.wait_got(returned_ref.at[pl.ds(0, OWNERS * rows), :], return_sem)
            remote.wait_sent(sent_ref.at[pl.ds(0, OWNERS * (LINES - rows)), :], gather_sem)
            remote.wait_sent(back_ref.at[pl.ds(0, (OWNERS // 2) * LINES), :], scatter_sem)

    @pl.when(jnp.logical_not(is_odd))
    def _():
        settle(ROWS)

    @pl.when(is_odd)
    def _():
        settle(4)

    def store_chunk(t):
        for base in (0, 32, 64, 96):
            rows = pl.ds(pl.multiple_of(base + 8 * t, 8), 8)
            remote.local(y_ref.at[:, rows, :], y_hbm.at[:, rows, :], y_sem).start()

    def store_before(t):
        @pl.when(t > 0)
        def _():
            store_chunk(t - 1)

    stage(
        lambda odd, begin, ref: finish_stage(
            odd, begin, velocity_ref, lane_ref, row_ref, y_ref, returned_ref, ref
        ),
        chunk_back_out, chunk_back_in, 4, store_before,
    )
    store_chunk(3)

    @pl.when(jnp.logical_not(is_odd))
    def _():
        remote.wait_sent(chunk_out, chunk_out_sem.at[0])
        remote.wait_sent(chunk_back_out, chunk_out_sem.at[1])

    remote.wait_sent(kappa_ref.at[pl.ds(0, 2)], edge_out_sem)
    remote.local(y_ref, y_hbm, y_sem).wait()


GROUP = 4
TAIL = 2


def solve_modes(
    remote, share, owner, tm, space, rows_of,
    velocity_ref, own_ref, wave_ref, tg_ref, td_ref, tw_ref, tb_ref, returned_ref,
    got_ref, back_ref, damp_ref, ratio_ref, last_ref, mate_ref, drive_ref, kept_ref, turn_ref,
    arrive_sem, swap_out_sem, swap_in_sem, mate_out_sem, mate_in_sem, scatter_sem, return_sem, own_sem,
):
    pairs = STEPS // 2
    rounds = pairs // share // GROUP
    core = lax.rem(tm, share)
    pair = lax.div(tm, 2)
    at_home = lax.rem(pair, share) == core
    v0, v1, v2 = velocity_ref[0], velocity_ref[1], velocity_ref[2]
    own = own_ref[...]
    line = [own[k : k + 1, :] for k in range(8)]
    wide = [jnp.broadcast_to(v, (8, 128)) for v in line]
    sign = wide[6]
    cross = cross_symbol(wide[0], wide[1], wide[2], wide[3], v1, v2)
    mu = [MU[0], MU[1], MU[0].conjugate(), MU[1].conjugate()]
    eps = [EPS[0], EPS[1], EPS[0].conjugate(), EPS[1].conjugate()]
    found = [factors(number, cross, v0) for number in mu]

    def crossed(a):
        return (a[0], -(sign * a[1]))

    def times_lanes(v, table):
        return v * table[0] + pltpu.roll(v, 64, 1) * table[1]

    def repeated(v, count):
        return jnp.concatenate([v] * count, axis=0)

    row = lax.broadcasted_iota(jnp.int32, (128, 128), 0).astype(f32)
    turn_ref[:, 0:128] = jnp.where(row == line[4], line[6], 0.0).astype(bf16)
    turn_ref[:, 128:256] = jnp.where(row == line[5], -1.0, 0.0).astype(bf16)

    @pl.loop(0, 16)
    def _(at):
        rows = pl.ds(pl.multiple_of(at * 8, 8), 8)
        symbol = (
            diffusion_number * (2.0 * wave_ref[0, rows, :] - 2.0) + cross[0],
            cross[1] - v0 * wave_ref[1, rows, :],
        )
        total = None
        for m in range(4):
            moved = scaled(mu[m], symbol)
            damp = inverse_of((1.0 - moved[0], -moved[1]))
            for k, value in enumerate(crossed(damp)):
                damp_ref[m, k, rows, :] = value
            term = scaled(eps[m], damp)
            if m < 2:
                for k, value in enumerate(crossed(term)):
                    damp_ref[4 + m, k, rows, :] = value
            total = term if total is None else plus(total, term)
        for k, value in enumerate(crossed(total)):
            ratio_ref[k, rows, :] = value
        power = times(total, total)
        for k, value in enumerate(crossed(power)):
            ratio_ref[4 + k, rows, :] = value
        fourth = times(power, power)
        for k, value in enumerate(crossed(fourth if share == 2 else power)):
            ratio_ref[6 + k, rows, :] = value
        power = fourth
        for k in range(3):
            power = times(power, power)
        closing = inverse_of((1.0 - circulant_alpha * power[0], -circulant_alpha * power[1]))
        for k, value in enumerate(crossed(closing)):
            ratio_ref[2 + k, rows, :] = value

    first_pair = pair - lax.rem(pair, 2)
    roots = [crossed(found[m][0]) for m in range(4)]
    flip = repeated(sign, 16)
    ratio = (ratio_ref.at[0], ratio_ref.at[1])
    square = (ratio_ref.at[4], ratio_ref.at[5])

    def times_refs(v, table):
        return times_lanes(v, (table[0][...], table[1][...]))

    def pair_of(i):
        return lax.rem(first_pair + share * i + core, pairs)

    def wrapped(at, v):
        return jnp.where(at == 0, circulant_alpha, 1.0).astype(f32) * v

    def swap(i):
        remote.start(
            drive_ref.at[pair_of(i)], drive_ref.at[pair_of(i)],
            swap_out_sem, swap_in_sem, (tm + 1 - 2 * core, space),
        )

    last_ref[...] = jnp.zeros((128, 128), f32)

    @pl.loop(0, rounds)
    def _(round_at):
        if share > 1:

            @pl.when(round_at > 0)
            def _():
                for k in range(GROUP):
                    swap((round_at - 1) * GROUP + k)

        values, crossings = [], []
        for k in range(GROUP):
            at = pair_of(round_at * GROUP + k)
            slot = lax.div(at, share)
            top = slot * (SLABS * LINES)

            def arrived(rows):
                remote.wait_got(got_ref.at[pl.ds(0, rows), :], arrive_sem.at[slot])

            if k > 0:
                arrived(SLABS * LINES)
            else:
                home = (round_at == 0) & at_home

                @pl.when(home & (core == 0))
                def _():
                    arrived(SLABS * LINES - 4)

                @pl.when(home & (core == 1))
                def _():
                    arrived(SLABS * LINES - ROWS)

                @pl.when(jnp.logical_not(home))
                def _():
                    arrived(SLABS * LINES)

            pieces = [got_ref[pl.ds(top + x * LINES, 8), :] for x in range(SLABS)]
            pieces += [got_ref[pl.ds(top + 8 + f, SLABS, stride=LINES), :] for f in range(8)]
            v = jnp.concatenate(pieces, axis=0)
            values.append(halves(v))
            crossings.append(halves(flip * pltpu.roll(v, 64, 1)))
        stacked = jnp.concatenate([half for pieces in values for half in pieces], axis=0)
        turned = jnp.dot(stacked, turn_ref[...], preferred_element_type=f32).astype(bf16)
        columns, own_points, other_points = [], [], []
        for k in range(GROUP):
            parts = []
            for half in range(2):
                rows = slice(128 * (2 * k + half), 128 * (2 * k + half) + 128)
                parts.append((values[k][half], crossings[k][half], turned[rows, :128], turned[rows, 128:]))
            order = (parts[0], parts[1], parts[0])
            columns.append(jnp.concatenate([piece[:64] for part in order for piece in part], axis=0))
            for step in range(2):
                lines = slice(64 + 32 * step, 96 + 32 * step)
                own_points.append(
                    jnp.concatenate([piece[lines] for part in order for piece in part[:2]], axis=0)
                )
                other_points.append(
                    jnp.concatenate([piece[lines] for part in order for piece in part[2:]], axis=0)
                )
        drive = jnp.dot(tg_ref[...], jnp.concatenate(columns, axis=1), preferred_element_type=f32)
        points = jnp.dot(
            td_ref[...], jnp.concatenate(own_points + other_points, axis=1), preferred_element_type=f32
        )
        for k in range(GROUP):
            at = pair_of(round_at * GROUP + k)
            slot = lax.div(at, share)
            total = drive[:, 128 * k : 128 * k + 128]
            for step, store in ((1, 0), (0, 1)):
                summed = None
                for m in range(4):
                    where = 128 * (2 * k + step + 2 * GROUP * (m // 2))
                    j = m % 2
                    point = times_lanes(points[256 + 8 * j : 264 + 8 * j, where : where + 128], roots[m])
                    d = points[128 * j : 128 * j + 128, where : where + 128] - repeated(point, 16)
                    y = times_lanes(d, (damp_ref[m, 0], damp_ref[m, 1]))
                    summed = y if summed is None else summed + y
                    if m < 2:
                        if store == 1:
                            y = y + times_lanes(early, (damp_ref[4 + m, 0], damp_ref[4 + m, 1]))
                        kept_ref[slot, 2 * store + m] = y
                if store == 0:
                    early = summed
                    total = total + times_refs(summed, ratio)
                else:
                    total = total + summed
            drive_ref[at] = total
            before = wrapped(at - core, last_ref[...])
            last_ref[...] = total + times_lanes(before, (ratio_ref[6], ratio_ref[7]))

    if share > 1:
        mate = (tm + 1 - 2 * core, space)
        for k in range(GROUP):
            swap((rounds - 1) * GROUP + k)
        remote.start(last_ref, mate_ref, mate_out_sem, mate_in_sem, mate)
        remote.wait_got(mate_ref, mate_in_sem)
        remote.wait_sent(last_ref, mate_out_sem)
        mine, theirs = last_ref[...], mate_ref[...]
        last_ref[...] = jnp.where(core == 0, theirs, mine) + times_refs(
            jnp.where(core == 0, mine, theirs), square
        )
        remote.wait_got(drive_ref.at[pl.ds(0, pairs // 2)], swap_in_sem)

    def following(at, v):
        return drive_ref[at] + times_refs(v, square)

    last_ref[...] = times_lanes(last_ref[...], (ratio_ref[2], ratio_ref[3]))
    kappas = [crossed(found[m][2]) for m in range(2)]
    ups = [crossed(found[m][1]) for m in range(2)]
    flip_all = flip

    def both_parts(v):
        return jnp.concatenate([v, flip_all * pltpu.roll(v, 64, 1)], axis=0)

    x_at, side = lax.div(space, 2), lax.rem(space, 2)
    places = [lax.rem(x_at + k // 2, SLABS // 2) * 2 + lax.rem(side + k, 2) for k in range(SLABS)]
    here = rows_of(owner)

    def send(i):
        at = pair_of(i)
        top = lax.div(at, share) * SLABS

        def put(place, even, odd):
            lines = (top + place) * LINES
            if even is not None:
                even(
                    back_ref.at[pl.ds(pl.multiple_of(lines, 4), ROWS), :], returned_ref.at[here, :],
                    scatter_sem, return_sem, (2 * at, place),
                )
            if odd is not None:
                odd(
                    back_ref.at[pl.ds(pl.multiple_of(lines + ROWS, 4), 4), :],
                    returned_ref.at[pl.ds(pl.multiple_of(owner * ROWS + 8, 4), 4), :],
                    scatter_sem, return_sem, (2 * at + 1, place),
                )

        def stay(source, target, *others):
            target[...] = source[...]

        home = (i == 0) & at_home

        @pl.when(jnp.logical_not(home))
        def _():
            put(places[0], remote.start, remote.start)

        @pl.when(home & (core == 0))
        def _():
            put(places[0], stay, remote.start)

        @pl.when(home & (core == 1))
        def _():
            put(places[0], remote.start, stay)

        for place in places[1:]:
            put(place, remote.start, remote.start)

    tail_rounds = pairs // share // TAIL

    @pl.loop(0, tail_rounds)
    def _(round_at):
        @pl.when(round_at > 0)
        def _():
            @pl.loop(0, TAIL)
            def _(k):
                send((round_at - 1) * TAIL + k)

        inputs = []
        last = last_ref[...]
        for k in range(TAIL):
            mine = None
            for c in range(share):
                at = lax.rem(first_pair + share * (round_at * TAIL + k) + c, pairs)
                last = wrapped(at, last)
                mine = last if mine is None else jnp.where(core == c, last, mine)
                last = following(at, last)
            inputs.append(mine)
        last_ref[...] = last
        packed = left_dot(tw_ref[...], jnp.concatenate([both_parts(v) for v in inputs], axis=1))
        lines = []
        for k in range(TAIL):
            slot = lax.div(pair_of(round_at * TAIL + k), share)
            for step, v in enumerate((inputs[k], times_refs(inputs[k], ratio))):
                for m in range(2):
                    y = times_lanes(v, (damp_ref[4 + m, 0], damp_ref[4 + m, 1]))
                    lines.append(both_parts(y + kept_ref[slot, 2 * step + m]))
        ends = left_dot(tb_ref[...], jnp.concatenate(lines, axis=1))
        for k in range(TAIL):
            top = lax.div(pair_of(round_at * TAIL + k), share) * (SLABS * LINES)
            for x in range(SLABS):
                back_ref[pl.ds(top + x * LINES, 8), :] = packed[8 * x : 8 * x + 8, 128 * k : 128 * k + 128]
            for step in range(2):
                for m in range(2):
                    where = 128 * (4 * k + 2 * step + m)
                    part = [ends[8 * j : 8 * j + 8, where : where + 128] for j in range(3)]
                    u = times_lanes(part[0] - times_lanes(part[1], ups[m]), kappas[m])
                    line = top + 8 + 4 * step + 2 * m
                    back_ref[pl.ds(line, SLABS, stride=LINES), :] = u
                    back_ref[pl.ds(line + 1, SLABS, stride=LINES), :] = part[2]

    @pl.loop(0, TAIL)
    def _(k):
        send((tail_rounds - 1) * TAIL + k)

    if share > 1:
        remote.wait_sent(drive_ref.at[pl.ds(0, pairs // 2)], swap_out_sem)


class Remote:
    def place(self):
        return lax.axis_index("tm"), lax.axis_index("space")

    def greet(self, device):
        pl.semaphore_signal(
            pltpu.get_barrier_semaphore(), inc=1, device_id=device, device_id_type=MESH
        )

    def all_here(self, count):
        pl.semaphore_wait(pltpu.get_barrier_semaphore(), count)

    def vouch(self, sem, device):
        pl.semaphore_signal(sem, inc=1, device_id=device, device_id_type=MESH)

    def vouched(self, sem, count):
        pl.semaphore_wait(sem, count)

    def start(self, source, target, send_sem, recv_sem, device):
        pltpu.make_async_remote_copy(
            src_ref=source, dst_ref=target, send_sem=send_sem, recv_sem=recv_sem,
            device_id=device, device_id_type=MESH,
        ).start()

    def local(self, source, target, sem):
        return pltpu.make_async_copy(source, target, sem)

    def bytes_of(self, ref, sem):
        return pltpu.make_async_remote_copy(
            src_ref=ref, dst_ref=ref, send_sem=sem, recv_sem=sem,
            device_id=self.place(), device_id_type=MESH,
        )

    def wait_sent(self, ref, sem):
        self.bytes_of(ref, sem).wait_send()

    def wait_got(self, ref, sem):
        self.bytes_of(ref, sem).wait_recv()


VMEM, SMEM, ANY = pltpu.VMEM, pltpu.SMEM, pl.ANY


def spec(space):
    return pl.BlockSpec(memory_space=space)


def shape(*dims):
    return jax.ShapeDtypeStruct(dims, f32)


PARAMS = pltpu.CompilerParams(vmem_limit_bytes=60 * 1024 * 1024)


def whole(velocity, iterate, right_side, kappa, remote=Remote(), interpret=False):
    dma = pltpu.SemaphoreType.DMA
    return pl.pallas_call(
        functools.partial(whole_kernel, remote),
        out_shape=shape(32, 128, 128),
        in_specs=[spec(SMEM)] + [spec(ANY)] * 4 + [spec(VMEM)] * 9,
        out_specs=spec(ANY),
        scratch_shapes=[
            VMEM((4, WIDE, NZ, NY), f32), VMEM((4, WIDE, NZ, NY), f32), VMEM((WIDE, NZ, NY), f32),
            VMEM((32, 128, 128), f32),
        ]
        + [VMEM((256, 256), bf16)] * 4
        + [
            VMEM((44, 128, 128), f32), VMEM((8, NZ, NY), f32), VMEM((NZ, NY), f32), VMEM((NZ, NY), f32),
            VMEM((OWNERS * ROWS, 128), f32),
            VMEM((1024, 128), f32), VMEM((1024, 128), f32), VMEM((1024, 128), f32), VMEM((1024, 128), f32),
            VMEM((OWNERS * ROWS, 128), f32),
            VMEM((OWNERS // 2 * LINES, 128), f32), VMEM((OWNERS // 2 * LINES, 128), f32),
            VMEM((6, 2, 128, 128), f32), VMEM((8, 128, 128), f32), VMEM((128, 128), f32), VMEM((128, 128), f32),
            VMEM((STEPS // 2, 128, 128), f32), VMEM((STEPS // 4, 4, 128, 128), f32), VMEM((128, 256), bf16),
            VMEM((8, 128), f32), dma, pltpu.SemaphoreType.REGULAR, dma((3, 8)), dma, dma((2,)), dma((8,)), dma, dma, dma,
            dma, dma((STEPS // 4,)), dma, dma, dma, dma, dma, dma, dma,
        ],
        compiler_params=pltpu.CompilerParams(
            vmem_limit_bytes=60 * 1024 * 1024, has_side_effects=True, collective_id=0
        ),
        interpret=interpret,
        name="whole",
    )(
        velocity, iterate, right_side, kappa,
        TABLES["own"], TABLES["ty"], TABLES["tz"], TABLES["lane"], TABLES["row"], TABLES["wave_x"],
        TABLES["tg"], TABLES["td"], TABLES["tw"], TABLES["tb"],
    )


def backward(iterate, y, interpret=False):
    return pl.pallas_call(
        backward_kernel,
        out_shape=shape(4, WIDE, NZ, NY),
        in_specs=[spec(ANY)] * 2 + [spec(VMEM)] * 2,
        out_specs=spec(ANY),
        scratch_shapes=[
            VMEM((32, 128, 128), f32), VMEM((4, WIDE, NZ, NY), f32), VMEM((4, WIDE, NZ, NY), f32),
            pltpu.SemaphoreType.DMA((3, 4)), pltpu.SemaphoreType.DMA((8,)),
        ],
        compiler_params=PARAMS,
        interpret=interpret,
        name="backward",
    )(iterate, y, TABLES["uy"], TABLES["uz"])


def shards(iterate, right_side, diffusivity, velocity):
    iterate, right_side = iterate[0], right_side[0]
    y = whole(velocity, iterate, right_side, diffusivity)
    return backward(iterate, y)[None]


def solution(mesh):
    placed = (
        P("tm", None, "space", None, None),
        P("tm", None, "space", None, None),
        P("space", None, None),
        P(),
    )
    return jax.shard_map(
        shards,
        mesh=mesh,
        in_specs=placed,
        out_specs=P("tm", None, "space", None, None),
        check_vma=False,
    )
```

```python
import functools
import math

import jax
import jax.numpy as jnp
import numpy as np
from jax import lax
from jax.experimental import pallas as pl
from jax.experimental.pallas import tpu as pltpu
from jax.sharding import PartitionSpec as P

NX, NY, NZ, STEPS = 128, 128, 64, 32
SLABS, WIDE = 8, 16
OWNERS = 128
ROWS = 12
LINES = 16
MESH = pl.DeviceIdType.MESH
f32, bf16 = jnp.float32, jnp.bfloat16

diffusion_number = 16.0
circulant_alpha = 0.1


def collocation_matrix():
    radau_nodes = [0.08858795951270394, 0.4094668644407347, 0.7876594617608471, 1.0]
    matrix = [[0.0] * 4 for row_index in range(4)]
    for column_index in range(4):
        coefficients = [1.0]
        for other_index in range(4):
            if other_index != column_index:
                scale_value = 1.0 / (radau_nodes[column_index] - radau_nodes[other_index])
                shifted = [0.0] + [value * scale_value for value in coefficients]
                lowered = [
                    -radau_nodes[other_index] * scale_value * value for value in coefficients
                ] + [0.0]
                coefficients = [
                    left_value + right_value for left_value, right_value in zip(shifted, lowered)
                ]
        for row_index in range(4):
            total = 0.0
            for power_index in range(len(coefficients)):
                total = total + coefficients[power_index] * radau_nodes[row_index] ** (
                    power_index + 1
                ) / (power_index + 1)
            matrix[row_index][column_index] = total
    return matrix


def solve_system(matrix, target):
    count = len(target)
    rows_list = [list(matrix[row_index]) + [target[row_index]] for row_index in range(count)]
    for column in range(count):
        best_row = column
        for candidate in range(column + 1, count):
            if abs(rows_list[candidate][column]) > abs(rows_list[best_row][column]):
                best_row = candidate
        saved_row = rows_list[column]
        rows_list[column] = rows_list[best_row]
        rows_list[best_row] = saved_row
        leader = rows_list[column][column]
        for other_row in range(count):
            if other_row != column:
                factor = rows_list[other_row][column] / leader
                rows_list[other_row] = [
                    left_value - factor * right_value
                    for left_value, right_value in zip(rows_list[other_row], rows_list[column])
                ]
    return [
        rows_list[row_index][count] / rows_list[row_index][row_index] for row_index in range(count)
    ]


def node_basis():
    matrix = collocation_matrix()
    helper = [[0.0] * 4 for row_index in range(4)]
    coefficients = [0.0, 0.0, 0.0, 0.0, 1.0]
    for order in range(1, 5):
        product = [
            [
                sum((matrix[row_index][inner] * helper[inner][column] for inner in range(4)))
                for column in range(4)
            ]
            for row_index in range(4)
        ]
        for row_index in range(4):
            product[row_index][row_index] = product[row_index][row_index] + coefficients[5 - order]
        helper = product
        trace_value = sum(
            (
                sum((matrix[row_index][inner] * helper[inner][row_index] for inner in range(4)))
                for row_index in range(4)
            )
        )
        coefficients[4 - order] = -trace_value / order
    roots_list = [(0.4 + 0.9j) ** power_index for power_index in range(4)]
    for sweep in range(400):
        for root_index in range(4):
            current = roots_list[root_index]
            numer = 0.0
            for power_index in range(4, -1, -1):
                numer = numer * current + coefficients[power_index]
            denom = 1.0
            for other_index in range(4):
                if other_index != root_index:
                    denom = denom * (current - roots_list[other_index])
            roots_list[root_index] = current - numer / denom
    vectors = [[0.0] * 4 for row_index in range(4)]
    for root_index in range(4):
        shifted = [
            [
                matrix[row_index][column] - (roots_list[root_index] if row_index == column else 0.0)
                for column in range(3)
            ]
            for row_index in range(3)
        ]
        target = [-matrix[row_index][3] for row_index in range(3)]
        parts = solve_system(shifted, target) + [1.0 + 0j]
        for row_index in range(4):
            vectors[row_index][root_index] = parts[row_index]
    inverse = [[0.0] * 4 for row_index in range(4)]
    for column in range(4):
        unit = [1.0 if row_index == column else 0.0 for row_index in range(4)]
        parts = solve_system(vectors, unit)
        for row_index in range(4):
            inverse[row_index][column] = parts[row_index]
    weights = [sum((inverse[row_index][column] for column in range(4))) for row_index in range(4)]
    return (roots_list, vectors, inverse, weights)


VALUES, VECTORS, INVERSE, WEIGHTS = node_basis()
PAIRS = [m for m in range(4) if complex(VALUES[m]).imag > 0]
MU = [complex(VALUES[m]) for m in PAIRS]
COLUMN = [[complex(VECTORS[n][m]) for n in range(4)] for m in PAIRS]
ROW = [[complex(INVERSE[m][n]) for n in range(4)] for m in PAIRS]
EPS = [complex(WEIGHTS[m]) for m in PAIRS]


def wave_order_z():
    index = np.arange(NZ)
    return np.where(index <= NZ // 2, index, NZ + NZ // 2 - index)


def wave_order_y():
    lane = np.arange(NY)
    index = 16 * (lane // 32) + lane % 16
    return np.where(lane % 32 < 16, index, np.where(index == 0, NY // 2, NY - index))


def split(values):
    values = np.asarray(values, np.float64)
    high = values.astype(np.float32).astype(bf16)
    low = (values - high.astype(np.float64)).astype(np.float32).astype(bf16)
    return high, low


def side_table(values):
    high, low = split(values)
    return np.concatenate([high, high, low], axis=1)


def halves(x):
    high = x.astype(bf16)
    return high, (x - high.astype(f32)).astype(bf16)


def left_dot(table, x):
    high, low = halves(x)
    return jnp.dot(table, jnp.concatenate([high, low, high], axis=0), preferred_element_type=f32)


def right_dot(high, low, table_high, table_low):
    return (
        jnp.dot(high, table_high, preferred_element_type=f32)
        + jnp.dot(low, table_high, preferred_element_type=f32)
        + jnp.dot(high, table_low, preferred_element_type=f32)
    )


def complex_block(matrix):
    return np.block([[matrix.real, -matrix.imag], [matrix.imag, matrix.real]])


def make_tables():
    ky, kz = wave_order_y(), wave_order_z()
    kx, x = np.arange(NX), np.arange(NX)
    to_y = np.exp(-2j * np.pi * np.outer(ky, np.arange(NY)) / NY)
    to_z = np.exp(-2j * np.pi * np.outer(kz, np.arange(NZ)) / NZ)
    tables = {}
    tables["ty"] = np.stack(split(complex_block(to_y).T))
    tables["tz"] = side_table(complex_block(to_z))
    tables["uy"] = np.stack(split(complex_block(np.conj(to_y.T) / NY).T))
    tables["uz"] = side_table(complex_block(np.conj(to_z.T) / NZ))
    cells = (np.arange(SLABS)[:, None] * WIDE + np.arange(8)[None, :]).reshape(-1)
    theta = 2 * np.pi * kx / NX
    at = np.exp(-1j * np.outer(theta, cells))
    shifted = np.exp(-8j * theta)[:, None]
    from_own = at * (1 - 1j * shifted) / 2
    from_partner = at * (1 + 1j * shifted) / 2
    firsts = np.arange(SLABS) * WIDE

    def lane_block(matrix):
        return np.concatenate([matrix.real, -matrix.imag], axis=1)

    tables["tg"] = side_table(np.concatenate([lane_block(from_own), lane_block(from_partner)], axis=1))

    def point_rows(waves, shifts):
        out = []
        for m in range(2):
            table = np.zeros((len(waves), 4, SLABS), complex)
            for field, shift in shifts:
                table[:, 2 * m + field] = np.exp(-1j * np.outer(waves, firsts + shift))
            out.append(table.reshape(len(waves), 4 * SLABS))
        return out

    tables["td"] = side_table(
        lane_block(
            np.concatenate(
                point_rows(theta, ((0, WIDE), (1, -1))) + point_rows(theta[:8], ((1, 0),)), axis=0
            )
        )
    )
    back = np.exp(1j * np.outer(cells, theta)) * (1 + 1j * np.exp(8j * theta))[None, :] / NX
    tables["tw"] = side_table(lane_block(back))
    ends = [np.exp(1j * np.outer(firsts + k, theta)) / NX for k in (0, 1, 15)]
    tables["tb"] = side_table(lane_block(np.concatenate(ends, axis=0)))
    trig_y = 2 * np.pi * ky / NY
    trig_z = 2 * np.pi * kz / NZ
    tables["lane"] = np.stack([np.cos(trig_y), np.sin(trig_y)]).astype(np.float32)
    tables["row"] = np.stack(
        [np.broadcast_to(v[:, None], (NZ, NY)) for v in (np.cos(trig_z), np.sin(trig_z))]
    ).astype(np.float32)
    tables["wave_x"] = np.stack(
        [np.broadcast_to(v[:, None], (NX, 128)) for v in (np.cos(theta), np.sin(theta))]
    ).astype(np.float32)
    lane = np.arange(128)
    own = np.zeros((OWNERS, 8, 128))
    for owner in range(OWNERS):
        part, pair = owner // 32, owner % 32
        piece = (lane // 32 - part) % 4
        at_y, row = (lane - 32 * piece) % 128, piece % 2
        other_y = np.where((at_y == 0) | (at_y == 16), at_y, at_y ^ 16)
        other_row = row if pair == 0 else 1 - row
        other = (other_y + 32 * (2 * (piece // 2) + other_row)) % 128
        y, z = trig_y[at_y], trig_z[pair + 32 * row]
        own[owner] = np.stack(
            [
                np.cos(y), np.sin(y), np.cos(z), np.sin(z),
                other, np.roll(other, -64), np.where(piece < 2, 1.0, -1.0), (lane + 64) % 128,
            ]
        )
    tables["own"] = own.astype(np.float32)
    return tables


TABLES = make_tables()


def times(a, b):
    return (a[0] * b[0] - a[1] * b[1], a[0] * b[1] + a[1] * b[0])


def plus(a, b):
    return (a[0] + b[0], a[1] + b[1])


def minus(a, b):
    return (a[0] - b[0], a[1] - b[1])


def scaled(number, a):
    return (number.real * a[0] - number.imag * a[1], number.real * a[1] + number.imag * a[0])


def inverse_of(a):
    size = 1.0 / (a[0] * a[0] + a[1] * a[1])
    return (a[0] * size, -a[1] * size)


def root_of(a):
    size = jnp.sqrt(a[0] * a[0] + a[1] * a[1])
    main = jnp.sqrt(0.5 * (size + jnp.abs(a[0])))
    other = a[1] / (2.0 * main)
    positive = a[0] >= 0.0
    return (
        jnp.where(positive, main, jnp.abs(other)),
        jnp.where(positive, other, jnp.where(a[1] >= 0.0, main, -main)),
    )


def cross_symbol(cos_y, sin_y, cos_z, sin_z, v1, v2):
    return (
        diffusion_number * ((2.0 * cos_y - 2.0) + (2.0 * cos_z - 2.0)),
        -(v1 * sin_y + v2 * sin_z),
    )


def factors(mu, cross, v0):
    c_up = -mu.real * (diffusion_number - 0.5 * v0), -mu.imag * (diffusion_number - 0.5 * v0)
    c_down = -mu.real * (diffusion_number + 0.5 * v0), -mu.imag * (diffusion_number + 0.5 * v0)
    moved = scaled(mu, cross)
    c_mid = (1.0 + 2.0 * diffusion_number * mu.real - moved[0], 2.0 * diffusion_number * mu.imag - moved[1])
    product = times(c_up, c_down)
    square = times(c_mid, c_mid)
    root = root_of((square[0] - 4.0 * product[0], square[1] - 4.0 * product[1]))
    same = c_mid[0] * root[0] + c_mid[1] * root[1] >= 0.0
    kappa = (
        0.5 * (c_mid[0] + jnp.where(same, root[0], -root[0])),
        0.5 * (c_mid[1] + jnp.where(same, root[1], -root[1])),
    )
    inv = inverse_of(kappa)
    p = times(inv, c_down)
    q = times(inv, c_up)
    return (-p[0], -p[1]), (-q[0], -q[1]), kappa, inv


def plane_partner(low, high, lane, first_row):
    ends = (lane == 0) | (lane == 16)
    first = (lane % 32) < 16

    def turned(v):
        return jnp.where(ends, v, jnp.where(first, pltpu.roll(v, 112, 1), pltpu.roll(v, 16, 1)))

    low_turned, high_turned = [turned(v) for v in low], [turned(v) for v in high]
    to_low = [jnp.where(first_row, a, b) for a, b in zip(low_turned, high_turned)]
    to_high = [jnp.where(first_row, b, a) for a, b in zip(low_turned, high_turned)]
    return (to_low[0], -to_low[1]), (to_high[0], -to_high[1])


def packed_for(low, high, block):
    pieces = [low[0], high[0], low[1], high[1]]
    pieces = [pieces[0]] + [pltpu.roll(pieces[c], 32 * c, 1) for c in (1, 2, 3)]
    out = []
    for h in range(4):
        value = pieces[3]
        for c in (2, 1, 0):
            value = jnp.where(block == (h + c) % 4, pieces[c], value)
        out.append(value)
    return out


def unpacked_from(values, block):
    out = []
    for c in range(4):
        piece = values[(3 - c) % 4]
        for d in (2, 1, 0):
            piece = jnp.where(block == d, values[(d - c) % 4], piece)
        out.append(piece if c == 0 else pltpu.roll(piece, 128 - 32 * c, 1))
    return (out[0], out[2]), (out[1], out[3])


def chunk_factors(t, lane_ref, row_ref, velocity_ref, mu):
    cos_y, sin_y = lane_ref[0:1, :], lane_ref[1:2, :]
    found = []
    for base in (0, 32):
        rows = pl.ds(pl.multiple_of(base + 8 * t, 8), 8)
        cross = cross_symbol(
            cos_y, sin_y, row_ref[0, rows, :], row_ref[1, rows, :], velocity_ref[1], velocity_ref[2]
        )
        found.append([factors(number, cross, velocity_ref[0]) for number in mu])
    return found


def dft_block(high, low, ty_ref, tz_ref):
    mid = right_dot(high, low, ty_ref[0], ty_ref[1])
    stacked = jnp.concatenate(
        [
            jnp.concatenate([mid[64 * k : 64 * k + 64, :128], mid[64 * k : 64 * k + 64, 128:]], axis=0)
            for k in range(4)
        ],
        axis=1,
    )
    return left_dot(tz_ref[...], stacked)


def put_rows(slot, at, real, imag):
    for k, part in enumerate((real, imag)):
        for ref, value in zip(slot, halves(part)):
            ref[64 * at : 64 * at + 64, k * 128 : (k + 1) * 128] = value


def mixture(m, groups):
    real = imag = None
    for scale, values in groups:
        for n in range(4):
            factor = scale * ROW[m][n]
            a, b = factor.real * values[n], factor.imag * values[n]
            real = a if real is None else real + a
            imag = b if imag is None else imag + b
    return real, imag


def source_stage(
    keep, ready, middle, velocity_ref, iterate_ref, right_ref, kappa_ref, ty_ref, tz_ref, spec_ref, mixed_ref, slots,
):
    v0, v1, v2 = velocity_ref[0], velocity_ref[1], velocity_ref[2]

    def stencil(x, slot, at, below, above):
        plain, applied = [], []
        kappa = diffusion_number * kappa_ref[x]
        for n in range(4):
            f = iterate_ref[n, x]
            up_z, down_z = pltpu.roll(f, NZ - 1, 0), pltpu.roll(f, 1, 0)
            up_y, down_y = pltpu.roll(f, NY - 1, 1), pltpu.roll(f, 1, 1)
            total = (up_z + down_z) + (up_y + down_y) - 6.0 * f
            moved = v1 * (up_y - down_y) + v2 * (up_z - down_z)
            if above:
                up_x = iterate_ref[n, x + 1]
                total, moved = total + up_x, moved + v0 * up_x
            if below:
                down_x = iterate_ref[n, x - 1]
                total, moved = total + down_x, moved - v0 * down_x
            applied.append(kappa * total - 0.5 * moved)
            plain.append(right_ref[n, x] - f)
        for m in range(2):
            put_rows(slot, 2 * m + at, *mixture(m, [(1.0, plain), (MU[m], applied)]))

    def produce(block, slot, first=False, final=False):
        stencil(2 * block, slot, 0, not first, True)
        stencil(2 * block + 1, slot, 1, True, not final)

    def last_node(block, slot):
        for k in range(4):
            x = 4 * block + k
            put_rows(slot, k, keep * iterate_ref[3, x], keep * iterate_ref[3, x + 8])

    def transformed(block, slot):
        out = dft_block(slot[0][...], slot[1][...], ty_ref, tz_ref)
        for k in range(4):
            spec_ref[block * 4 + k] = out[:, 128 * k : 128 * k + 128]

    first, second = slots
    ready(0)
    ready(1)
    produce(0, first, first=True)

    @pl.loop(0, 3)
    def _(i):
        ready(2 * i + 2)
        transformed(2 * i, first)
        produce(2 * i + 1, second)
        ready(2 * i + 3)
        transformed(2 * i + 1, second)
        produce(2 * i + 2, first)

    middle()
    for side, x in enumerate((0, WIDE - 1)):
        for m in range(2):
            real, imag = mixture(m, [(MU[m], [iterate_ref[n, x] for n in range(4)])])
            mixed_ref[side * 4 + m * 2] = real
            mixed_ref[side * 4 + m * 2 + 1] = imag
    transformed(6, first)
    produce(7, second, final=True)
    transformed(7, second)
    last_node(0, first)
    transformed(8, first)
    last_node(1, second)
    transformed(9, second)


def put_chunk(ref, t, x, low, high):
    for k, value in enumerate((low[0], high[0], low[1], high[1])):
        ref[pl.ds(pl.multiple_of(256 * t + 32 * x + 8 * k, 8), 8), :] = value


def get_chunk(ref, t, x):
    parts = [ref[pl.ds(pl.multiple_of(256 * t + 32 * x + 8 * k, 8), 8), :] for k in range(4)]
    return (parts[0], parts[2]), (parts[1], parts[3])


def packed_planes(sums, x, lane, first_row):
    own, other = [], []
    for half in range(2):
        first, second = sums[x][half], sums[x + 8][half]
        own.append((first[0] - second[1], first[1] + second[0]))
        other.append((first[0] + second[1], first[1] - second[0]))
    partners = plane_partner(other[0], other[1], lane, first_row)
    return [plus(own[half], partners[half]) for half in range(2)]


def unpacked_planes(fetch, lane, first_row):
    last = [[None, None] for x in range(WIDE)]
    for x in range(8):
        packed = fetch(x)
        partners = plane_partner(packed[0], packed[1], lane, first_row)
        for half in range(2):
            both, apart = plus(packed[half], partners[half]), minus(packed[half], partners[half])
            last[x][half] = (0.5 * both[0], 0.5 * both[1])
            last[x + 8][half] = (0.5 * apart[1], -0.5 * apart[0])
    return last


def edge_stage(velocity_ref, spec_ref, mixed_ref, below_ref, above_ref, ty_ref, tz_ref):
    v0 = velocity_ref[0]
    outer = [diffusion_number * below_ref[...] - 0.5 * v0, diffusion_number * above_ref[...] + 0.5 * v0]
    edges = [
        jnp.concatenate([outer[side] * mixed_ref[side * 4 + m * 2 + part] for part in range(2)], axis=1)
        for m in range(2)
        for side in range(2)
    ]
    high, low = halves(jnp.concatenate(edges, axis=0))
    out = dft_block(high, low, ty_ref, tz_ref)
    for k in range(4):
        spec_ref[40 + k] = out[:, 128 * k : 128 * k + 128]


def slab_stage(odd, begin, velocity_ref, spec_ref, lane_ref, row_ref, y_ref, send_ref, chunk_ref, factor_ref):
    lane = lax.broadcasted_iota(jnp.int32, (8, 128), 1)
    sub = lax.broadcasted_iota(jnp.int32, (8, 128), 0)
    block = lane // 32

    @pl.loop(0, 4)
    def _(t):
        begin(t)
        first_row = (sub + t) == 0
        found = chunk_factors(t, lane_ref, row_ref, velocity_ref, MU)
        bases = [pl.multiple_of(base + 8 * t, 8) for base in (0, 32)]
        for half in range(2):
            for m in range(2):
                for k, j in enumerate((0, 1, 3)):
                    for part in range(2):
                        factor_ref[m * 6 + 2 * k + part, pl.ds(bases[half], 8), :] = found[half][m][j][part]
        if odd:
            last = unpacked_planes(lambda x: get_chunk(chunk_ref, t, x), lane, first_row)

        def plane(at, base):
            return spec_ref[at, pl.ds(base, 8), :], spec_ref[at, pl.ds(base + 64, 8), :]

        def field(m, x, half):
            value = plane(4 * (x // 2) + 2 * m + x % 2, bases[half])
            return plus(value, scaled(EPS[m], last[x][half])) if odd else value

        def send(value, low, high):
            for h, packed in enumerate(packed_for(low, high, block)):
                send_ref[pl.ds((32 * h + 8 * t) * ROWS + value, 8, stride=ROWS), :] = packed

        sums = [[None, None] for x in range(WIDE)]
        for m in range(2):
            carries = []
            for half in range(2):
                base = bases[half]
                p, q, kappa, inv = found[half][m]
                under, over = plane(40 + 2 * m, base), plane(41 + 2 * m, base)
                u = plus(field(m, 0, half), times(p, under))
                us = [u]
                for x in range(1, WIDE):
                    u = plus(field(m, x, half), times(p, u))
                    us.append(u)
                outflow = plus(times(p, us[-1]), over)
                y = us[-1]
                for x in range(WIDE - 1, -1, -1):
                    if x < WIDE - 1:
                        y = plus(us[x], times(q, y))
                    z = times(inv, y)
                    y_ref[m * 16 + x, pl.ds(base, 8), :] = z[0]
                    y_ref[m * 16 + x, pl.ds(base + 64, 8), :] = z[1]
                    sums[x][half] = z if m == 0 else plus(sums[x][half], z)
                carries.append((outflow, plus(times(q, y), under)))
            for k in range(2):
                send(8 + m * 2 + k, carries[0][k], carries[1][k])
        for x in range(8):
            packed = packed_planes(sums, x, lane, first_row)
            packed = [plus(packed[half], plane(32 + x, bases[half])) for half in range(2)]
            if odd:
                send(x, packed[0], packed[1])
            else:
                put_chunk(chunk_ref, t, x, packed[0], packed[1])


def finish_stage(odd, begin, y_ref, got_ref, chunk_ref, factor_ref):
    lane = lax.broadcasted_iota(jnp.int32, (8, 128), 1)
    sub = lax.broadcasted_iota(jnp.int32, (8, 128), 0)
    block = lane // 32

    @pl.loop(0, 4)
    def _(t):
        begin(t)
        first_row = (sub + t) == 0
        bases = [pl.multiple_of(base + 8 * t, 8) for base in (0, 32)]

        def take(value):
            values = [
                got_ref[pl.ds((32 * h + 8 * t) * ROWS + value, 8, stride=ROWS), :] for h in range(4)
            ]
            return unpacked_from(values, block)

        last = unpacked_planes(
            (lambda x: get_chunk(chunk_ref, t, x)) if odd else take, lane, first_row
        )
        sums = [[None, None] for x in range(WIDE)]
        for m in range(2):
            start, end = take(8 + m * 2), take(9 + m * 2)
            for half in range(2):
                base = bases[half]
                p, q, inv = [
                    tuple(factor_ref[m * 6 + 2 * k + part, pl.ds(base, 8), :] for part in range(2))
                    for k in range(3)
                ]
                u = start[half]
                us = [u]
                for x in range(1, WIDE - 1):
                    u = plus(scaled(EPS[m], last[x][half]), times(p, u))
                    us.append(u)
                y = end[half]
                for x in range(WIDE - 1, -1, -1):
                    if x < WIDE - 1:
                        y = plus(times(inv, us[x]), times(q, y))
                    for k in range(2):
                        rows = pl.ds(base + 64 * k, 8)
                        y_ref[m * 16 + x, rows, :] = y_ref[m * 16 + x, rows, :] + y[k]
                    if not odd:
                        sums[x][half] = y if m == 0 else plus(sums[x][half], y)
        if not odd:
            for x in range(8):
                packed = packed_planes(sums, x, lane, first_row)
                put_chunk(chunk_ref, t, x, packed[0], packed[1])


def backward_kernel(
    iterate_hbm, spec_hbm, uy_ref, uz_ref, out_hbm, spec_ref, iterate_ref, out_ref, load_sem, store_sem
):
    def loads(group):
        planes = pl.ds(4 * group, 4)
        upper = pl.ds(16 + 4 * group, 4)
        return [
            pltpu.make_async_copy(spec_hbm.at[planes], spec_ref.at[planes], load_sem.at[0, group]),
            pltpu.make_async_copy(spec_hbm.at[upper], spec_ref.at[upper], load_sem.at[1, group]),
            pltpu.make_async_copy(
                iterate_hbm.at[:, planes], iterate_ref.at[:, planes], load_sem.at[2, group]
            ),
        ]

    for group in range(4):
        for copy in loads(group):
            copy.start()

    def finished(block):
        planes = [2 * block, 2 * block + 1, 16 + 2 * block, 17 + 2 * block]
        stacked = jnp.concatenate([spec_ref[at] for at in planes], axis=1)
        mid = left_dot(uz_ref[...], stacked)
        rows = jnp.concatenate(
            [
                jnp.concatenate([mid[:64, 128 * k : 128 * k + 128], mid[64:, 128 * k : 128 * k + 128]], axis=1)
                for k in range(4)
            ],
            axis=0,
        )
        high, low = halves(rows)
        return right_dot(high, low, uy_ref[0], uy_ref[1])

    def store(block):
        planes = pl.ds(2 * block, 2)
        return pltpu.make_async_copy(out_ref.at[:, planes], out_hbm.at[:, planes], store_sem.at[block])

    def added(block, out):
        for k in range(2):
            x = 2 * block + k
            parts = []
            for m in range(2):
                piece = out[(2 * m + k) * 64 : (2 * m + k) * 64 + 64]
                parts.append((piece[:, :128], piece[:, 128:]))
            for n in range(4):
                total = iterate_ref[n, x]
                for m in range(2):
                    c = COLUMN[m][n]
                    total = total + (2.0 * c.real) * parts[m][0] - (2.0 * c.imag) * parts[m][1]
                out_ref[n, x] = total

    pending = None
    for group in range(4):
        if group % 2 == 0:
            for copy in loads(group) + loads(group + 1):
                copy.wait()
        blocks = (2 * group, 2 * group + 1)
        outs = [finished(block) for block in blocks]
        if pending is not None:
            for block, out in pending:
                added(block, out)
        pending = list(zip(blocks, outs))
        if group > 1:
            store(2 * group - 4).start()
            store(2 * group - 3).start()
    for block, out in pending:
        added(block, out)
    for block in range(4, 8):
        store(block).start()
    for block in range(8):
        store(block).wait()


def other_places(tm, space, work):
    pair = lax.div(tm, 2)
    x, side = lax.div(space, 2), lax.rem(space, 2)
    places = [
        lax.rem(x + k // 2, SLABS // 2) * 2 + lax.rem(side + k, 2) for k in range(SLABS)
    ]
    for k in range(1, SLABS):
        work(pair, places[k])

    @pl.loop(1, STEPS // 2)
    def _(i):
        other = lax.rem(pair + STEPS // 2 - i, STEPS // 2)
        for k in range(SLABS):
            work(other, places[k])


def whole_kernel(
    remote, velocity_ref, iterate_hbm, right_hbm, kappa_hbm,
    own_hbm, ty_ref, tz_ref, lane_ref, row_ref, wave_ref, tg_ref, td_ref, tw_ref, tb_ref,
    y_hbm,
    iterate_ref, right_ref, kappa_ref, y_ref,
    high_a, low_a, high_b, low_b, spec_ref, mixed_ref, below_ref, above_ref, sent_ref,
    chunk_out, chunk_in, chunk_back_out, chunk_back_in, returned_ref,
    got_ref, back_ref, damp_ref, ratio_ref, last_ref, mate_ref, drive_ref, kept_ref, turn_ref,
    line_ref, factor_ref, line_sem, vouch_sem, load_sem, y_sem, chunk_out_sem, chunk_in_sem, edge_out_sem, below_sem, above_sem,
    gather_sem, arrive_sem, swap_out_sem, swap_in_sem, mate_out_sem, mate_in_sem,
    scatter_sem, return_sem, own_sem,
):
    tm, space = remote.place()
    core = lax.rem(tm, 2)
    owner = lax.div(tm, 2) * SLABS + space

    def rows_of(index, number=1):
        return pl.ds(pl.multiple_of(index * ROWS, 4), number * ROWS)

    def loads(piece):
        planes = pl.ds(2 * piece, 2)
        return [
            remote.local(iterate_hbm.at[:, planes], iterate_ref.at[:, planes], load_sem.at[0, piece]),
            remote.local(right_hbm.at[:, planes], right_ref.at[:, planes], load_sem.at[1, piece]),
            remote.local(kappa_hbm.at[planes], kappa_ref.at[planes], load_sem.at[2, piece]),
        ]

    for piece in range(8):
        for copy in loads(piece):
            copy.start()

    line_load = remote.local(own_hbm.at[owner], line_ref, line_sem)
    line_load.start()

    def ready(piece):
        for copy in loads(piece):
            copy.wait()

    mate = (tm + 1 - 2 * core, space)

    for k in range(1, SLABS):
        remote.greet((tm, lax.rem(space + k, SLABS)))

    @pl.loop(1, STEPS)
    def _(k):
        remote.greet((lax.rem(tm + k, STEPS), space))

    def middle():
        remote.all_here(SLABS + STEPS - 2)
        for k in range(1, SLABS):
            remote.vouch(vouch_sem, (tm, lax.rem(space + k, SLABS)))
        remote.start(
            kappa_ref.at[WIDE - 1], below_ref, edge_out_sem, below_sem, (tm, lax.rem(space + 1, SLABS))
        )
        remote.start(
            kappa_ref.at[0], above_ref, edge_out_sem, above_sem, (tm, lax.rem(space + SLABS - 1, SLABS))
        )

    keep = jnp.where(tm < STEPS - 1, 1.0, 0.0).astype(f32)
    source_stage(
        keep, ready, middle, velocity_ref, iterate_ref, right_ref, kappa_ref, ty_ref, tz_ref,
        spec_ref, mixed_ref, ((high_a, low_a), (high_b, low_b)),
    )
    remote.wait_got(below_ref, below_sem)
    remote.wait_got(above_ref, above_sem)
    edge_stage(velocity_ref, spec_ref, mixed_ref, below_ref, above_ref, ty_ref, tz_ref)
    is_odd = core == 1

    def chunk_at(ref, t):
        return ref.at[pl.ds(pl.multiple_of(256 * t, 256), 256), :]

    def hand_over(source, target, t, base):
        remote.start(
            chunk_at(source, t), chunk_at(target, t), chunk_out_sem.at[base // 4],
            chunk_in_sem.at[base + t], mate,
        )

    def stage(work, source, target, base, done):
        @pl.when(jnp.logical_not(is_odd))
        def _():
            def begin(t):
                done(t)

                @pl.when(t > 0)
                def _():
                    hand_over(source, target, t - 1, base)

            work(False, begin, source)
            hand_over(source, target, 3, base)

        @pl.when(is_odd)
        def _():
            def begin(t):
                done(t)
                remote.wait_got(chunk_at(target, t), chunk_in_sem.at[base + t])

            work(True, begin, target)

    stage(
        lambda odd, begin, ref: slab_stage(
            odd, begin, velocity_ref, spec_ref, lane_ref, row_ref, y_ref, sent_ref, ref, factor_ref
        ),
        chunk_out, chunk_in, 0, lambda t: None,
    )

    remote.vouched(vouch_sem, SLABS - 1)

    pair = lax.div(tm, 2)
    side = lax.rem(pair, 2)
    at_home = side == core
    slot = lax.div(pair, 2) * SLABS + space

    def even_rows(index):
        return pl.ds(pl.multiple_of(index * ROWS + 8, 4), 4)

    def send_even(other, place):
        remote.start(
            sent_ref.at[even_rows(other * SLABS + place), :],
            got_ref.at[pl.ds(pl.multiple_of(slot * LINES + ROWS, 4), 4), :],
            gather_sem, arrive_sem.at[lax.div(pair, 2)], (2 * other + side, place),
        )

    def send_odd(other, place):
        remote.start(
            sent_ref.at[rows_of(other * SLABS + place), :],
            got_ref.at[pl.ds(pl.multiple_of(slot * LINES, 4), ROWS), :],
            gather_sem, arrive_sem.at[lax.div(pair, 2)], (2 * other + side, place),
        )

    @pl.when(is_odd)
    def _():
        other_places(tm, space, send_odd)

        @pl.when(at_home)
        def _():
            got_ref[pl.ds(pl.multiple_of(slot * LINES, 4), ROWS), :] = sent_ref[rows_of(owner), :]

        @pl.when(jnp.logical_not(at_home))
        def _():
            send_odd(pair, space)

    @pl.when(jnp.logical_not(is_odd))
    def _():
        other_places(tm, space, send_even)

        @pl.when(at_home)
        def _():
            got_ref[pl.ds(pl.multiple_of(slot * LINES + ROWS, 4), 4), :] = sent_ref[even_rows(owner), :]

        @pl.when(jnp.logical_not(at_home))
        def _():
            send_even(pair, space)

    line_load.wait()
    solve_modes(
        remote, 2, owner, tm, space, rows_of,
        velocity_ref, line_ref, wave_ref, tg_ref, td_ref, tw_ref, tb_ref, returned_ref,
        got_ref, back_ref, damp_ref, ratio_ref, last_ref, mate_ref, drive_ref, kept_ref, turn_ref,
        arrive_sem, swap_out_sem, swap_in_sem, mate_out_sem, mate_in_sem, scatter_sem, return_sem, own_sem,
    )

    def settle(rows):
        @pl.when(at_home)
        def _():
            remote.wait_got(returned_ref.at[pl.ds(0, (OWNERS - 1) * rows), :], return_sem)
            remote.wait_sent(sent_ref.at[pl.ds(0, (OWNERS - 1) * (LINES - rows)), :], gather_sem)
            remote.wait_sent(back_ref.at[pl.ds(0, (OWNERS // 2) * LINES - rows), :], scatter_sem)

        @pl.when(jnp.logical_not(at_home))
        def _():
            remote.wait_got(returned_ref.at[pl.ds(0, OWNERS * rows), :], return_sem)
            remote.wait_sent(sent_ref.at[pl.ds(0, OWNERS * (LINES - rows)), :], gather_sem)
            remote.wait_sent(back_ref.at[pl.ds(0, (OWNERS // 2) * LINES), :], scatter_sem)

    @pl.when(jnp.logical_not(is_odd))
    def _():
        settle(ROWS)

    @pl.when(is_odd)
    def _():
        settle(4)

    def store_chunk(t):
        for base in (0, 32, 64, 96):
            rows = pl.ds(pl.multiple_of(base + 8 * t, 8), 8)
            remote.local(y_ref.at[:, rows, :], y_hbm.at[:, rows, :], y_sem).start()

    def store_before(t):
        @pl.when(t > 0)
        def _():
            store_chunk(t - 1)

    stage(
        lambda odd, begin, ref: finish_stage(
            odd, begin, y_ref, returned_ref, ref, factor_ref
        ),
        chunk_back_out, chunk_back_in, 4, store_before,
    )
    store_chunk(3)

    @pl.when(jnp.logical_not(is_odd))
    def _():
        remote.wait_sent(chunk_out, chunk_out_sem.at[0])
        remote.wait_sent(chunk_back_out, chunk_out_sem.at[1])

    remote.wait_sent(kappa_ref.at[pl.ds(0, 2)], edge_out_sem)
    remote.local(y_ref, y_hbm, y_sem).wait()


GROUP = 4
TAIL = 2


def solve_modes(
    remote, share, owner, tm, space, rows_of,
    velocity_ref, own_ref, wave_ref, tg_ref, td_ref, tw_ref, tb_ref, returned_ref,
    got_ref, back_ref, damp_ref, ratio_ref, last_ref, mate_ref, drive_ref, kept_ref, turn_ref,
    arrive_sem, swap_out_sem, swap_in_sem, mate_out_sem, mate_in_sem, scatter_sem, return_sem, own_sem,
):
    pairs = STEPS // 2
    rounds = pairs // share // GROUP
    core = lax.rem(tm, share)
    pair = lax.div(tm, 2)
    at_home = lax.rem(pair, share) == core
    v0, v1, v2 = velocity_ref[0], velocity_ref[1], velocity_ref[2]
    own = own_ref[...]
    line = [own[k : k + 1, :] for k in range(8)]
    wide = [jnp.broadcast_to(v, (8, 128)) for v in line]
    sign = wide[6]
    cross = cross_symbol(wide[0], wide[1], wide[2], wide[3], v1, v2)
    mu = [MU[0], MU[1], MU[0].conjugate(), MU[1].conjugate()]
    eps = [EPS[0], EPS[1], EPS[0].conjugate(), EPS[1].conjugate()]
    found = [factors(number, cross, v0) for number in mu]

    def crossed(a):
        return (a[0], -(sign * a[1]))

    def times_lanes(v, table):
        return v * table[0] + pltpu.roll(v, 64, 1) * table[1]

    def repeated(v, count):
        return jnp.concatenate([v] * count, axis=0)

    row = lax.broadcasted_iota(jnp.int32, (128, 128), 0).astype(f32)
    turn_ref[:, 0:128] = jnp.where(row == line[4], line[6], 0.0).astype(bf16)
    turn_ref[:, 128:256] = jnp.where(row == line[5], -1.0, 0.0).astype(bf16)

    @pl.loop(0, 16)
    def _(at):
        rows = pl.ds(pl.multiple_of(at * 8, 8), 8)
        symbol = (
            diffusion_number * (2.0 * wave_ref[0, rows, :] - 2.0) + cross[0],
            cross[1] - v0 * wave_ref[1, rows, :],
        )
        total = None
        for m in range(4):
            moved = scaled(mu[m], symbol)
            damp = inverse_of((1.0 - moved[0], -moved[1]))
            for k, value in enumerate(crossed(damp)):
                damp_ref[m, k, rows, :] = value
            term = scaled(eps[m], damp)
            if m < 2:
                for k, value in enumerate(crossed(term)):
                    damp_ref[4 + m, k, rows, :] = value
            total = term if total is None else plus(total, term)
        for k, value in enumerate(crossed(total)):
            ratio_ref[k, rows, :] = value
        power = times(total, total)
        for k, value in enumerate(crossed(power)):
            ratio_ref[4 + k, rows, :] = value
        fourth = times(power, power)
        for k, value in enumerate(crossed(fourth if share == 2 else power)):
            ratio_ref[6 + k, rows, :] = value
        power = fourth
        for k in range(3):
            power = times(power, power)
        closing = inverse_of((1.0 - circulant_alpha * power[0], -circulant_alpha * power[1]))
        for k, value in enumerate(crossed(closing)):
            ratio_ref[2 + k, rows, :] = value

    first_pair = pair - lax.rem(pair, 2)
    roots = [crossed(found[m][0]) for m in range(4)]
    flip = repeated(sign, 16)
    ratio = (ratio_ref.at[0], ratio_ref.at[1])
    square = (ratio_ref.at[4], ratio_ref.at[5])

    def times_refs(v, table):
        return times_lanes(v, (table[0][...], table[1][...]))

    def pair_of(i):
        return lax.rem(first_pair + share * i + core, pairs)

    def wrapped(at, v):
        return jnp.where(at == 0, circulant_alpha, 1.0).astype(f32) * v

    def swap(i):
        remote.start(
            drive_ref.at[pair_of(i)], drive_ref.at[pair_of(i)],
            swap_out_sem, swap_in_sem, (tm + 1 - 2 * core, space),
        )

    last_ref[...] = jnp.zeros((128, 128), f32)

    @pl.loop(0, rounds)
    def _(round_at):
        if share > 1:

            @pl.when(round_at > 0)
            def _():
                for k in range(GROUP):
                    swap((round_at - 1) * GROUP + k)

        values, crossings = [], []
        for k in range(GROUP):
            at = pair_of(round_at * GROUP + k)
            slot = lax.div(at, share)
            top = slot * (SLABS * LINES)

            def arrived(rows):
                remote.wait_got(got_ref.at[pl.ds(0, rows), :], arrive_sem.at[slot])

            if k > 0:
                arrived(SLABS * LINES)
            else:
                home = (round_at == 0) & at_home

                @pl.when(home & (core == 0))
                def _():
                    arrived(SLABS * LINES - 4)

                @pl.when(home & (core == 1))
                def _():
                    arrived(SLABS * LINES - ROWS)

                @pl.when(jnp.logical_not(home))
                def _():
                    arrived(SLABS * LINES)

            pieces = [got_ref[pl.ds(top + x * LINES, 8), :] for x in range(SLABS)]
            pieces += [got_ref[pl.ds(top + 8 + f, SLABS, stride=LINES), :] for f in range(8)]
            v = jnp.concatenate(pieces, axis=0)
            values.append(halves(v))
            crossings.append(halves(flip * pltpu.roll(v, 64, 1)))
        stacked = jnp.concatenate([half for pieces in values for half in pieces], axis=0)
        turned = jnp.dot(stacked, turn_ref[...], preferred_element_type=f32).astype(bf16)
        columns, own_points, other_points = [], [], []
        for k in range(GROUP):
            parts = []
            for half in range(2):
                rows = slice(128 * (2 * k + half), 128 * (2 * k + half) + 128)
                parts.append((values[k][half], crossings[k][half], turned[rows, :128], turned[rows, 128:]))
            order = (parts[0], parts[1], parts[0])
            columns.append(jnp.concatenate([piece[:64] for part in order for piece in part], axis=0))
            for step in range(2):
                lines = slice(64 + 32 * step, 96 + 32 * step)
                own_points.append(
                    jnp.concatenate([piece[lines] for part in order for piece in part[:2]], axis=0)
                )
                other_points.append(
                    jnp.concatenate([piece[lines] for part in order for piece in part[2:]], axis=0)
                )
        drive = jnp.dot(tg_ref[...], jnp.concatenate(columns, axis=1), preferred_element_type=f32)
        points = jnp.dot(
            td_ref[...], jnp.concatenate(own_points + other_points, axis=1), preferred_element_type=f32
        )
        for k in range(GROUP):
            at = pair_of(round_at * GROUP + k)
            slot = lax.div(at, share)
            total = drive[:, 128 * k : 128 * k + 128]
            for step, store in ((1, 0), (0, 1)):
                summed = None
                for m in range(4):
                    where = 128 * (2 * k + step + 2 * GROUP * (m // 2))
                    j = m % 2
                    point = times_lanes(points[256 + 8 * j : 264 + 8 * j, where : where + 128], roots[m])
                    d = points[128 * j : 128 * j + 128, where : where + 128] - repeated(point, 16)
                    y = times_lanes(d, (damp_ref[m, 0], damp_ref[m, 1]))
                    summed = y if summed is None else summed + y
                    if m < 2:
                        if store == 1:
                            y = y + times_lanes(early, (damp_ref[4 + m, 0], damp_ref[4 + m, 1]))
                        kept_ref[slot, 2 * store + m] = y
                if store == 0:
                    early = summed
                    total = total + times_refs(summed, ratio)
                else:
                    total = total + summed
            drive_ref[at] = total
            before = wrapped(at - core, last_ref[...])
            last_ref[...] = total + times_lanes(before, (ratio_ref[6], ratio_ref[7]))

    if share > 1:
        mate = (tm + 1 - 2 * core, space)
        for k in range(GROUP):
            swap((rounds - 1) * GROUP + k)
        remote.start(last_ref, mate_ref, mate_out_sem, mate_in_sem, mate)
        remote.wait_got(mate_ref, mate_in_sem)
        remote.wait_sent(last_ref, mate_out_sem)
        mine, theirs = last_ref[...], mate_ref[...]
        last_ref[...] = jnp.where(core == 0, theirs, mine) + times_refs(
            jnp.where(core == 0, mine, theirs), square
        )
        remote.wait_got(drive_ref.at[pl.ds(0, pairs // 2)], swap_in_sem)

    def following(at, v):
        return drive_ref[at] + times_refs(v, square)

    last_ref[...] = times_lanes(last_ref[...], (ratio_ref[2], ratio_ref[3]))
    kappas = [crossed(found[m][2]) for m in range(2)]
    ups = [crossed(found[m][1]) for m in range(2)]
    flip_all = flip

    def both_parts(v):
        return jnp.concatenate([v, flip_all * pltpu.roll(v, 64, 1)], axis=0)

    x_at, side = lax.div(space, 2), lax.rem(space, 2)
    places = [lax.rem(x_at + k // 2, SLABS // 2) * 2 + lax.rem(side + k, 2) for k in range(SLABS)]
    here = rows_of(owner)

    def send(i):
        at = pair_of(i)
        top = lax.div(at, share) * SLABS

        def put(place, even, odd):
            lines = (top + place) * LINES
            if even is not None:
                even(
                    back_ref.at[pl.ds(pl.multiple_of(lines, 4), ROWS), :], returned_ref.at[here, :],
                    scatter_sem, return_sem, (2 * at, place),
                )
            if odd is not None:
                odd(
                    back_ref.at[pl.ds(pl.multiple_of(lines + ROWS, 4), 4), :],
                    returned_ref.at[pl.ds(pl.multiple_of(owner * ROWS + 8, 4), 4), :],
                    scatter_sem, return_sem, (2 * at + 1, place),
                )

        def stay(source, target, *others):
            target[...] = source[...]

        home = (i == 0) & at_home

        @pl.when(jnp.logical_not(home))
        def _():
            put(places[0], remote.start, remote.start)

        @pl.when(home & (core == 0))
        def _():
            put(places[0], stay, remote.start)

        @pl.when(home & (core == 1))
        def _():
            put(places[0], remote.start, stay)

        for place in places[1:]:
            put(place, remote.start, remote.start)

    tail_rounds = pairs // share // TAIL

    @pl.loop(0, tail_rounds)
    def _(round_at):
        @pl.when(round_at > 0)
        def _():
            @pl.loop(0, TAIL)
            def _(k):
                send((round_at - 1) * TAIL + k)

        inputs = []
        last = last_ref[...]
        for k in range(TAIL):
            mine = None
            for c in range(share):
                at = lax.rem(first_pair + share * (round_at * TAIL + k) + c, pairs)
                last = wrapped(at, last)
                mine = last if mine is None else jnp.where(core == c, last, mine)
                last = following(at, last)
            inputs.append(mine)
        last_ref[...] = last
        packed = left_dot(tw_ref[...], jnp.concatenate([both_parts(v) for v in inputs], axis=1))
        lines = []
        for k in range(TAIL):
            slot = lax.div(pair_of(round_at * TAIL + k), share)
            for step, v in enumerate((inputs[k], times_refs(inputs[k], ratio))):
                for m in range(2):
                    y = times_lanes(v, (damp_ref[4 + m, 0], damp_ref[4 + m, 1]))
                    lines.append(both_parts(y + kept_ref[slot, 2 * step + m]))
        ends = left_dot(tb_ref[...], jnp.concatenate(lines, axis=1))
        for k in range(TAIL):
            top = lax.div(pair_of(round_at * TAIL + k), share) * (SLABS * LINES)
            for x in range(SLABS):
                back_ref[pl.ds(top + x * LINES, 8), :] = packed[8 * x : 8 * x + 8, 128 * k : 128 * k + 128]
            for step in range(2):
                for m in range(2):
                    where = 128 * (4 * k + 2 * step + m)
                    part = [ends[8 * j : 8 * j + 8, where : where + 128] for j in range(3)]
                    u = times_lanes(part[0] - times_lanes(part[1], ups[m]), kappas[m])
                    line = top + 8 + 4 * step + 2 * m
                    back_ref[pl.ds(line, SLABS, stride=LINES), :] = u
                    back_ref[pl.ds(line + 1, SLABS, stride=LINES), :] = part[2]

    @pl.loop(0, TAIL)
    def _(k):
        send((tail_rounds - 1) * TAIL + k)

    if share > 1:
        remote.wait_sent(drive_ref.at[pl.ds(0, pairs // 2)], swap_out_sem)


class Remote:
    def place(self):
        return lax.axis_index("tm"), lax.axis_index("space")

    def greet(self, device):
        pl.semaphore_signal(
            pltpu.get_barrier_semaphore(), inc=1, device_id=device, device_id_type=MESH
        )

    def all_here(self, count):
        pl.semaphore_wait(pltpu.get_barrier_semaphore(), count)

    def vouch(self, sem, device):
        pl.semaphore_signal(sem, inc=1, device_id=device, device_id_type=MESH)

    def vouched(self, sem, count):
        pl.semaphore_wait(sem, count)

    def start(self, source, target, send_sem, recv_sem, device):
        pltpu.make_async_remote_copy(
            src_ref=source, dst_ref=target, send_sem=send_sem, recv_sem=recv_sem,
            device_id=device, device_id_type=MESH,
        ).start()

    def local(self, source, target, sem):
        return pltpu.make_async_copy(source, target, sem)

    def bytes_of(self, ref, sem):
        return pltpu.make_async_remote_copy(
            src_ref=ref, dst_ref=ref, send_sem=sem, recv_sem=sem,
            device_id=self.place(), device_id_type=MESH,
        )

    def wait_sent(self, ref, sem):
        self.bytes_of(ref, sem).wait_send()

    def wait_got(self, ref, sem):
        self.bytes_of(ref, sem).wait_recv()


VMEM, SMEM, ANY = pltpu.VMEM, pltpu.SMEM, pl.ANY


def spec(space):
    return pl.BlockSpec(memory_space=space)


def shape(*dims):
    return jax.ShapeDtypeStruct(dims, f32)


PARAMS = pltpu.CompilerParams(vmem_limit_bytes=60 * 1024 * 1024)


def whole(velocity, iterate, right_side, kappa, remote=Remote(), interpret=False):
    dma = pltpu.SemaphoreType.DMA
    return pl.pallas_call(
        functools.partial(whole_kernel, remote),
        out_shape=shape(32, 128, 128),
        in_specs=[spec(SMEM)] + [spec(ANY)] * 4 + [spec(VMEM)] * 9,
        out_specs=spec(ANY),
        scratch_shapes=[
            VMEM((4, WIDE, NZ, NY), f32), VMEM((4, WIDE, NZ, NY), f32), VMEM((WIDE, NZ, NY), f32),
            VMEM((32, 128, 128), f32),
        ]
        + [VMEM((256, 256), bf16)] * 4
        + [
            VMEM((44, 128, 128), f32), VMEM((8, NZ, NY), f32), VMEM((NZ, NY), f32), VMEM((NZ, NY), f32),
            VMEM((OWNERS * ROWS, 128), f32),
            VMEM((1024, 128), f32), VMEM((1024, 128), f32), VMEM((1024, 128), f32), VMEM((1024, 128), f32),
            VMEM((OWNERS * ROWS, 128), f32),
            VMEM((OWNERS // 2 * LINES, 128), f32), VMEM((OWNERS // 2 * LINES, 128), f32),
            VMEM((6, 2, 128, 128), f32), VMEM((8, 128, 128), f32), VMEM((128, 128), f32), VMEM((128, 128), f32),
            VMEM((STEPS // 2, 128, 128), f32), VMEM((STEPS // 4, 4, 128, 128), f32), VMEM((128, 256), bf16),
            VMEM((8, 128), f32), VMEM((12, NZ, NY), f32), dma, pltpu.SemaphoreType.REGULAR, dma((3, 8)), dma, dma((2,)), dma((8,)), dma, dma, dma,
            dma, dma((STEPS // 4,)), dma, dma, dma, dma, dma, dma, dma,
        ],
        compiler_params=pltpu.CompilerParams(
            vmem_limit_bytes=60 * 1024 * 1024, has_side_effects=True, collective_id=0
        ),
        interpret=interpret,
        name="whole",
    )(
        velocity, iterate, right_side, kappa,
        TABLES["own"], TABLES["ty"], TABLES["tz"], TABLES["lane"], TABLES["row"], TABLES["wave_x"],
        TABLES["tg"], TABLES["td"], TABLES["tw"], TABLES["tb"],
    )


def backward(iterate, y, interpret=False):
    return pl.pallas_call(
        backward_kernel,
        out_shape=shape(4, WIDE, NZ, NY),
        in_specs=[spec(ANY)] * 2 + [spec(VMEM)] * 2,
        out_specs=spec(ANY),
        scratch_shapes=[
            VMEM((32, 128, 128), f32), VMEM((4, WIDE, NZ, NY), f32), VMEM((4, WIDE, NZ, NY), f32),
            pltpu.SemaphoreType.DMA((3, 4)), pltpu.SemaphoreType.DMA((8,)),
        ],
        compiler_params=PARAMS,
        interpret=interpret,
        name="backward",
    )(iterate, y, TABLES["uy"], TABLES["uz"])


def shards(iterate, right_side, diffusivity, velocity):
    iterate, right_side = iterate[0], right_side[0]
    y = whole(velocity, iterate, right_side, diffusivity)
    return backward(iterate, y)[None]


def solution(mesh):
    placed = (
        P("tm", None, "space", None, None),
        P("tm", None, "space", None, None),
        P("space", None, None),
        P(),
    )
    return jax.shard_map(
        shards,
        mesh=mesh,
        in_specs=placed,
        out_specs=P("tm", None, "space", None, None),
        check_vma=False,
    )
```
